32 devices in a mesh: dp: 4 (over z), expert: 2 (over core), tensor: 4 (over y, x).
Axes of the slice: x: 2, y: 2, z: 4, core: 2. Of those that a mesh axis runs over, the one named last changes fastest.
Arguments:
- tokens: bfloat16 [2048, 1536], P(('dp', 'expert')), may hold values from -6 to 6
- gain_attn: float32 [1536], replicated, may hold values from 0.5 to 1.5
- w_query: bfloat16 [1536, 1536], P(None, 'tensor'), may hold values from -0.15625 to 0.15625
- key_projection: bfloat16 [1536, 512], P(None, 'tensor'), may hold values from -0.15625 to 0.15625
- value_projection: bfloat16 [1536, 512], P(None, 'tensor'), may hold values from -0.15625 to 0.15625
- w_out: bfloat16 [1536, 1536], P('tensor'), may hold values from -0.625 to 0.625
- gain_moe: float32 [1536], replicated, may hold values from 0.5 to 1.5
- w_router: bfloat16 [1536, 40], replicated, may hold values from -0.15625 to 0.15625
- w_gate: bfloat16 [40, 1536, 512], P('expert', None, 'tensor'), may hold values from -0.15625 to 0.15625
- w_up: bfloat16 [40, 1536, 512], P('expert', None, 'tensor'), may hold values from -0.15625 to 0.15625
- w_down: bfloat16 [40, 512, 1536], P('expert', 'tensor'), may hold values from -0.5 to 0.5
- routes: int32 [2048, 8], P(('dp', 'expert')), may hold values from 0 to 39, all different within a row; in each aligned block of 256 rows (0 to 255, 256 to 511, ...) at most 64 rows name the same one
- cotangent: bfloat16 [2048, 1536], P(('dp', 'expert')), may hold values from -6 to 6
Outputs:
- output: bfloat16 [2048, 1536], P(('dp', 'expert'))
- input_grad: bfloat16 [2048, 1536], P(('dp', 'expert'))
- gain_attn_grad: float32 [1536], P(('dp', 'expert'))
- query_grad: float32 [1536, 1536], P(('dp', 'expert'), 'tensor')
- key_grad: float32 [1536, 512], P(('dp', 'expert'), 'tensor')
- value_grad: float32 [1536, 512], P(('dp', 'expert'), 'tensor')
- out_grad: float32 [1536, 1536], P('tensor', ('dp', 'expert'))
- gain_moe_grad: float32 [1536], P(('dp', 'expert'))
- router_grad: float32 [1536, 40], P(('dp', 'expert'))
- gate_grad: float32 [40, 1536, 512], P('expert', 'dp', 'tensor')
- up_grad: float32 [40, 1536, 512], P('expert', 'dp', 'tensor')
- down_grad: float32 [40, 512, 1536], P('expert', 'tensor', 'dp')
The draws below stay inside these ranges and needn't reach their ends.
Inputs may be any that keep to these rules, and one draw needn't show every extreme that they name: `routes`: each row names 8 different experts. Within the rows of one sequence (aligned blocks of 256 rows) no expert is named by more than 64 rows, and in every draw some expert is named by exactly 64 rows of some block.
All inputs are finite; a program needn't handle non-finite values.
Results may differ from the reference program's by a relative error of at most 0.023.
Values may be sent and summed in bfloat16 or wider, within the bound.
A program may use at most 256 MiB of HBM per device.

```python
import math
import jax
import jax.numpy as jnp
import numpy as np
from jax import lax

MODEL_DIMENSION = 1536
QUERY_HEAD_COUNT = 24
KEY_VALUE_HEADS = 8
HEAD_SIZE = 64
EXPERTS = 40
TOPK = 8
HE = 512
SEQUENCE_LENGTH = 256
CAP = 64
TOKENS = 2048
N_TENSOR = 4


def steps_of(key, extent, cuts, least, top_value):
    loudness = 1.0
    for position, blocks in cuts:
        draws = jax.random.uniform(jax.random.fold_in(jax.random.fold_in(key, 6), position), (blocks,), jnp.float32, least / len(cuts), top_value / len(cuts))
        loudness = loudness * jnp.repeat(jnp.exp(draws), extent[position] // blocks).reshape((-1,) + (1,) * (len(extent) - 1 - position))
    return loudness


def deal_out(own_key, own, number, rows, number_of, top, bound, slope):
    ranking = jax.random.permutation(own_key, number_of)
    heavy_load, usual = load_shares(number_of, rows * top, bound, slope, True), load_shares(number_of, rows * top, bound, slope, False)
    places = jnp.arange(number_of)

    def named(lengths, offset_by):
        used = int((lengths > 0).sum())
        fixed = max(1, used // 4)
        passed = fixed + (places - fixed + offset_by * (used - fixed)) % max(1, number_of - fixed)
        return jnp.zeros((number_of,), jnp.int32).at[ranking[jnp.where(places < fixed, places, passed)]].set(jnp.asarray(lengths, jnp.int32))

    lengths = jnp.where(number % 4 == 0, named(heavy_load, number // 4), named(usual, number - number // 4 - 1))
    mixed = jax.random.permutation(jax.random.fold_in(own, 3), number_of)
    donor, receiver = mixed[0:number_of // 2 * 2:2], mixed[1:number_of // 2 * 2:2]
    margin = jnp.minimum(lengths[donor] - 1, bound - lengths[receiver]) // 2
    margin = jnp.where((donor == ranking[0]) | (receiver == ranking[0]) | (lengths[receiver] == 0), 0, jnp.maximum(margin, 0))
    passed = jax.random.randint(jax.random.fold_in(own, 4), (number_of // 2,), 0, 1 << 20) % (margin + 1)
    lengths = lengths.at[donor].add(-passed).at[receiver].add(passed)
    members = jnp.searchsorted(jnp.cumsum(lengths), jnp.arange(rows * top), side="right").astype(jnp.int32)
    table = members.reshape(top, rows).T
    table = table[jax.random.permutation(jax.random.fold_in(own, 1), rows)]
    offset_by = jax.random.randint(jax.random.fold_in(own, 2), (rows, 1), 0, top)
    return jnp.take_along_axis(table, (jnp.arange(top)[None, :] + offset_by) % top, axis=1)


def load_shares(amount, total, bound, slope, full):
    weights = [(1 << 20) // math.isqrt(rank ** slope) + 1 for rank in range(1, amount + 1)]
    largest = bound if full else min(bound, max(-(-total // amount), total * weights[0] // sum(weights)))
    least = 1 if total - largest >= amount - 1 else 0
    given, surplus = [largest] + [least] * (amount - 1), total - largest - least * (amount - 1)
    while surplus > 0:
        candidates = [i for i in range(1, amount) if given[i] < largest] or [i for i in range(1, amount) if given[i] < bound]
        whole, remaining = sum([weights[i] for i in candidates]), surplus
        for i in candidates:
            extra = min(bound - given[i], max(1, remaining * weights[i] // whole), surplus)
            given[i] = given[i] + extra
            surplus = surplus - extra
    return np.array(given)


def gaussian(stream_key, extent, scale, limit, shards=(), kind=jnp.bfloat16):
    drawn = scale * jax.random.normal(stream_key, extent, jnp.float32)
    if shards:
        drawn = drawn * steps_of(stream_key, extent, shards, -0.22, 0.18)
    return jnp.clip(drawn, -limit, limit).astype(kind)


def setup_inputs(seed: int = 0) -> dict:
    keys = jax.random.split(jax.random.key(seed), 14)
    tokens = gaussian(keys[0], (TOKENS, MODEL_DIMENSION), 1.0, 6.0, ((0, 8),))
    gain_attn = jnp.clip(1.0 + 0.1 * jax.random.normal(keys[1], (MODEL_DIMENSION,), jnp.float32), 0.5, 1.5)
    w_query = gaussian(keys[2], (MODEL_DIMENSION, QUERY_HEAD_COUNT * HEAD_SIZE), MODEL_DIMENSION ** -0.5, 0.15625, ((1, 4),))
    key_projection = gaussian(keys[3], (MODEL_DIMENSION, KEY_VALUE_HEADS * HEAD_SIZE), MODEL_DIMENSION ** -0.5, 0.15625, ((1, 4),))
    value_projection = gaussian(keys[4], (MODEL_DIMENSION, KEY_VALUE_HEADS * HEAD_SIZE), MODEL_DIMENSION ** -0.5, 0.15625, ((1, 4),))
    w_out = gaussian(keys[5], (QUERY_HEAD_COUNT * HEAD_SIZE, MODEL_DIMENSION), (QUERY_HEAD_COUNT * HEAD_SIZE // 16) ** -0.5, 0.625, ((0, 4),))
    gain_moe = jnp.clip(1.0 + 0.1 * jax.random.normal(keys[6], (MODEL_DIMENSION,), jnp.float32), 0.5, 1.5)
    w_router = gaussian(keys[7], (MODEL_DIMENSION, EXPERTS), MODEL_DIMENSION ** -0.5, 0.15625)
    w_gate = gaussian(keys[8], (EXPERTS, MODEL_DIMENSION, HE), MODEL_DIMENSION ** -0.5, 0.15625, ((0, 2), (2, 4)))
    w_up = gaussian(keys[9], (EXPERTS, MODEL_DIMENSION, HE), MODEL_DIMENSION ** -0.5, 0.15625, ((0, 2), (2, 4)))
    w_down = gaussian(keys[10], (EXPERTS, HE, MODEL_DIMENSION), (HE // 4) ** -0.5, 0.5, ((0, 2), (1, 4)))
    routes_keys = jax.random.split(jax.random.fold_in(keys[11], 1), TOKENS // SEQUENCE_LENGTH)
    routes_turns = jax.random.permutation(jax.random.fold_in(keys[11], 3), TOKENS // SEQUENCE_LENGTH)
    routes = jax.vmap(lambda own, number: deal_out(jax.random.fold_in(keys[11], 2), own, number, SEQUENCE_LENGTH, EXPERTS, TOPK, CAP, 1))(routes_keys, routes_turns).reshape((TOKENS, TOPK))
    cotangent = gaussian(keys[12], (TOKENS, MODEL_DIMENSION), 1.0, 6.0, ((0, 8),))
    return dict(tokens=tokens, gain_attn=gain_attn, w_query=w_query, key_projection=key_projection, value_projection=value_projection, w_out=w_out, gain_moe=gain_moe, w_router=w_router, w_gate=w_gate, w_up=w_up, w_down=w_down, routes=routes, cotangent=cotangent)


EPSILON = 1e-06
ROPE_BASE = 10000.0

def rms_scale(hidden):
    return lax.rsqrt(lax.optimization_barrier(jnp.mean(hidden * hidden, axis=-1, keepdims=True)) + EPSILON)

def norm_back(hidden, scaling, gain_vec, grad_out):
    weighted = grad_out * gain_vec
    gain_grad = lax.optimization_barrier(jnp.sum(grad_out * hidden * scaling, axis=0))
    inner_mean = lax.optimization_barrier(jnp.mean(weighted * hidden, axis=-1, keepdims=True))
    return (scaling * weighted - hidden * (scaling * scaling * scaling) * inner_mean, gain_grad)

def rope_tables(positions, head_dim):
    half_dim = head_dim // 2
    frequency = jnp.exp(jnp.arange(half_dim, dtype=jnp.float32) * (-2.0 * math.log(ROPE_BASE) / head_dim))
    angles = positions[:, None] * frequency[None, :]
    return (jnp.cos(angles), jnp.sin(angles))

def apply_rotary(vectors, cosine_table, sine_component):
    half_dim = vectors.shape[-1] // 2
    first_half = vectors[..., :half_dim]
    second_half = vectors[..., half_dim:]
    cos_rows = cosine_table[:, None, :]
    sin_rows = sine_component[:, None, :]
    return jnp.concatenate([first_half * cos_rows - second_half * sin_rows, first_half * sin_rows + second_half * cos_rows], axis=-1)

def slot_table(route_ids, expert_count, capacity):
    number_of_rows, top_count = route_ids.shape
    flat_ids = route_ids.reshape(-1)
    one_hot = (flat_ids[:, None] == jnp.arange(expert_count, dtype=jnp.int32)[None, :]).astype(jnp.int32)
    earlier = jnp.cumsum(one_hot, axis=0) - one_hot
    slot_ids = lax.optimization_barrier(jnp.sum(earlier * one_hot, axis=1))
    slot_where = (flat_ids * capacity + slot_ids).astype(jnp.int32)
    pick_ids = jnp.arange(number_of_rows * top_count, dtype=jnp.int32)
    token_of = jnp.full((expert_count * capacity,), number_of_rows, jnp.int32).at[slot_where].set(pick_ids // top_count)
    pick_of = jnp.full((expert_count * capacity,), number_of_rows * top_count, jnp.int32).at[slot_where].set(pick_ids)
    return (slot_where, token_of, pick_of)

def seq_scores(query_rows, key_rows, query_group_width):
    length, kv_heads, head_dim = key_rows.shape
    grouped = query_rows.astype(jnp.float32).reshape(length, kv_heads, query_group_width, head_dim)
    scores = jnp.einsum('qhgd,khd->hgqk', grouped, key_rows.astype(jnp.float32)) * head_dim ** (-0.5)
    row_pos = jnp.arange(length, dtype=jnp.int32)[:, None]
    col_pos = jnp.arange(length, dtype=jnp.int32)[None, :]
    return (jnp.where(col_pos <= row_pos, scores, -1e+30), grouped)

def seq_forward(query_rows, key_rows, value_rows, query_group_width):
    length, kv_heads, head_dim = key_rows.shape
    scores, grouped = seq_scores(query_rows, key_rows, query_group_width)
    largest = lax.optimization_barrier(jnp.max(scores, axis=-1, keepdims=True))
    log_total = largest + jnp.log(lax.optimization_barrier(jnp.sum(jnp.exp(scores - largest), axis=-1, keepdims=True)))
    weights = jnp.exp(scores - log_total).astype(jnp.bfloat16)
    attended = jnp.einsum('hgqk,khd->qhgd', weights.astype(jnp.float32), value_rows.astype(jnp.float32))
    return (attended.reshape(length, -1, head_dim).astype(jnp.bfloat16), log_total)

def seq_backward(query_rows, key_rows, value_rows, attended, log_total, d_attended, query_group_width):
    length, kv_heads, head_dim = key_rows.shape
    scale_factor = head_dim ** (-0.5)
    scores, grouped = seq_scores(query_rows, key_rows, query_group_width)
    weights = jnp.exp(scores - log_total)
    d_grouped = d_attended.astype(jnp.float32).reshape(length, kv_heads, query_group_width, head_dim)
    o_grouped = attended.astype(jnp.float32).reshape(length, kv_heads, query_group_width, head_dim)
    delta = jnp.transpose(lax.optimization_barrier(jnp.sum(d_grouped * o_grouped, axis=-1)), (1, 2, 0))[..., None]
    d_weights = jnp.einsum('qhgd,khd->hgqk', d_grouped, value_rows.astype(jnp.float32))
    d_scores = (weights * (d_weights - delta)).astype(jnp.bfloat16).astype(jnp.float32)
    d_query = jnp.einsum('hgqk,khd->qhgd', d_scores, key_rows.astype(jnp.float32)) * scale_factor
    key_gradient = jnp.einsum('hgqk,qhgd->khd', d_scores, grouped) * scale_factor
    weights_low = weights.astype(jnp.bfloat16).astype(jnp.float32)
    value_gradient = jnp.einsum('hgqk,qhgd->khd', weights_low, d_grouped)
    return (d_query.reshape(length, -1, head_dim), key_gradient, value_gradient)

def reference(tokens, gain_attn, w_query, key_projection, value_projection, w_out, gain_moe, w_router, w_gate, w_up, w_down, routes, cotangent):
    number_of_rows = tokens.shape[0]
    query_group_width = QUERY_HEAD_COUNT // KEY_VALUE_HEADS
    sequence_number = number_of_rows // SEQUENCE_LENGTH
    quarter = HE // N_TENSOR
    resid = tokens.astype(jnp.float32)
    scale_one = rms_scale(resid)
    first_normalized = (resid * scale_one * gain_attn).astype(jnp.bfloat16)
    positions = (jnp.arange(number_of_rows, dtype=jnp.int32) % SEQUENCE_LENGTH).astype(jnp.float32)
    cosine_table, sine_component = rope_tables(positions, HEAD_SIZE)
    q_lin = jnp.dot(first_normalized, w_query, preferred_element_type=jnp.float32).reshape(number_of_rows, QUERY_HEAD_COUNT, HEAD_SIZE)
    linear_key = jnp.dot(first_normalized, key_projection, preferred_element_type=jnp.float32).reshape(number_of_rows, KEY_VALUE_HEADS, HEAD_SIZE)
    linear_value = jnp.dot(first_normalized, value_projection, preferred_element_type=jnp.float32).reshape(number_of_rows, KEY_VALUE_HEADS, HEAD_SIZE)
    q_rot = apply_rotary(q_lin, cosine_table, sine_component).astype(jnp.bfloat16)
    rotated_key = apply_rotary(linear_key, cosine_table, sine_component).astype(jnp.bfloat16)
    value_reduced = linear_value.astype(jnp.bfloat16)
    q_seq = q_rot.reshape(sequence_number, SEQUENCE_LENGTH, QUERY_HEAD_COUNT, HEAD_SIZE)
    sequence_key = rotated_key.reshape(sequence_number, SEQUENCE_LENGTH, KEY_VALUE_HEADS, HEAD_SIZE)
    sequence_value = value_reduced.reshape(sequence_number, SEQUENCE_LENGTH, KEY_VALUE_HEADS, HEAD_SIZE)

    def forward_step(running, inputs):
        return (running, seq_forward(inputs[0], inputs[1], inputs[2], query_group_width))
    _, (attended, log_total) = lax.scan(forward_step, 0, (q_seq, sequence_key, sequence_value))
    flat_att = attended.reshape(number_of_rows, QUERY_HEAD_COUNT * HEAD_SIZE)
    hidden1 = resid + jnp.dot(flat_att, w_out, preferred_element_type=jnp.float32)
    scale_two = rms_scale(hidden1)
    normed2 = (hidden1 * scale_two * gain_moe).astype(jnp.bfloat16)
    logits = jnp.dot(normed2, w_router, preferred_element_type=jnp.float32)
    chosen = jnp.take_along_axis(logits, routes, axis=1)
    gate_probs = jax.nn.softmax(chosen, axis=-1)
    block_count = number_of_rows // SEQUENCE_LENGTH
    _, token_of, pick_of = jax.vmap(lambda route_block: slot_table(route_block, EXPERTS, CAP))(routes.reshape(block_count, SEQUENCE_LENGTH, TOPK))
    block_base = jnp.arange(block_count, dtype=jnp.int32)[:, None]
    token_glob = jnp.where(token_of < SEQUENCE_LENGTH, token_of + block_base * SEQUENCE_LENGTH, number_of_rows).astype(jnp.int32)
    pick_glob = jnp.where(pick_of < SEQUENCE_LENGTH * TOPK, pick_of + block_base * (SEQUENCE_LENGTH * TOPK), number_of_rows * TOPK).astype(jnp.int32)
    token_exp = jnp.transpose(token_glob.reshape(block_count, EXPERTS, CAP), (1, 0, 2)).reshape(EXPERTS, block_count * CAP)
    pick_exp = jnp.transpose(pick_glob.reshape(block_count, EXPERTS, CAP), (1, 0, 2)).reshape(EXPERTS, block_count * CAP)
    normed_pad = jnp.concatenate([normed2, jnp.zeros((1, MODEL_DIMENSION), jnp.bfloat16)], axis=0)
    grad_pad = jnp.concatenate([cotangent, jnp.zeros((1, MODEL_DIMENSION), jnp.bfloat16)], axis=0)
    gate_pad = jnp.concatenate([gate_probs.reshape(-1), jnp.zeros((1,), jnp.float32)], axis=0)

    def expert_step(running, inputs):
        moe_acc, dgate_acc, back_acc = running
        token_ids, pick_ids, gate_w, up_w, down_w = inputs
        rows_in = normed_pad[token_ids]
        gate_pre = jnp.dot(rows_in, gate_w, preferred_element_type=jnp.float32)
        up_pre = jnp.dot(rows_in, up_w, preferred_element_type=jnp.float32)
        sig_gate = jax.nn.sigmoid(gate_pre)
        activated = gate_pre * sig_gate
        hid_low = (activated * up_pre).astype(jnp.bfloat16)
        pieces = jnp.einsum('rjh,jhd->rjd', hid_low.reshape(-1, N_TENSOR, quarter).astype(jnp.float32), down_w.reshape(N_TENSOR, quarter, MODEL_DIMENSION).astype(jnp.float32)).astype(jnp.bfloat16)
        pieces = lax.optimization_barrier(pieces)
        piece_sum = lax.optimization_barrier(jnp.sum(pieces.astype(jnp.float32), axis=1))
        gate_slot = gate_pad[pick_ids]
        moe_acc = moe_acc.at[token_ids].add(piece_sum * gate_slot[:, None])
        grad_rows = grad_pad[token_ids].astype(jnp.float32)
        dgate_acc = dgate_acc.at[pick_ids].add(lax.optimization_barrier(jnp.sum(piece_sum * grad_rows, axis=1)))
        sent = (grad_rows * gate_slot[:, None]).astype(jnp.bfloat16)
        d_hid = jnp.dot(sent, down_w.T, preferred_element_type=jnp.float32)
        down_g = jnp.dot(hid_low.T, sent, preferred_element_type=jnp.float32)
        d_gate = (d_hid * up_pre * sig_gate * (1.0 + gate_pre * (1.0 - sig_gate))).astype(jnp.bfloat16)
        d_up = (d_hid * activated).astype(jnp.bfloat16)
        gate_g = jnp.dot(rows_in.T, d_gate, preferred_element_type=jnp.float32)
        up_g = jnp.dot(rows_in.T, d_up, preferred_element_type=jnp.float32)
        back_pieces = jnp.einsum('rjh,djh->rjd', d_gate.reshape(-1, N_TENSOR, quarter).astype(jnp.float32), gate_w.reshape(MODEL_DIMENSION, N_TENSOR, quarter).astype(jnp.float32))
        back_pieces = back_pieces + jnp.einsum('rjh,djh->rjd', d_up.reshape(-1, N_TENSOR, quarter).astype(jnp.float32), up_w.reshape(MODEL_DIMENSION, N_TENSOR, quarter).astype(jnp.float32))
        back_pieces = lax.optimization_barrier(back_pieces.astype(jnp.bfloat16))
        back_acc = back_acc.at[token_ids].add(lax.optimization_barrier(jnp.sum(back_pieces.astype(jnp.float32), axis=1)))
        return ((moe_acc, dgate_acc, back_acc), (gate_g, up_g, down_g))
    start_state = (jnp.zeros((number_of_rows + 1, MODEL_DIMENSION), jnp.float32), jnp.zeros((number_of_rows * TOPK + 1,), jnp.float32), jnp.zeros((number_of_rows + 1, MODEL_DIMENSION), jnp.float32))
    (moe_acc, dgate_acc, back_acc), (gate_grad, up_grad, down_grad) = lax.scan(expert_step, start_state, (token_exp, pick_exp, w_gate, w_up, w_down))
    moe_out = moe_acc[:number_of_rows]
    output = (hidden1 + moe_out).astype(jnp.bfloat16)
    grad = cotangent.astype(jnp.float32)
    dgate = dgate_acc[:number_of_rows * TOPK].reshape(number_of_rows, TOPK)
    inner_sum = lax.optimization_barrier(jnp.sum(gate_probs * dgate, axis=1, keepdims=True))
    d_chosen = gate_probs * (dgate - inner_sum)
    matches = routes[:, :, None] == jnp.arange(EXPERTS, dtype=jnp.int32)[None, None, :]
    d_logits = lax.optimization_barrier(jnp.sum(jnp.where(matches, d_chosen[:, :, None], 0.0), axis=1)).astype(jnp.bfloat16)
    router_grad = jnp.dot(normed2.T, d_logits, preferred_element_type=jnp.float32)
    d_normed2 = back_acc[:number_of_rows] + jnp.dot(d_logits, w_router.T, preferred_element_type=jnp.float32)
    d_hidden_part, gain_moe_grad = norm_back(hidden1, scale_two, gain_moe, d_normed2)
    d_hidden1 = grad + d_hidden_part
    d_mixed = d_hidden1.astype(jnp.bfloat16)
    out_grad = jnp.dot(flat_att.T, d_mixed, preferred_element_type=jnp.float32)
    d_att = jnp.dot(d_mixed, w_out.T, preferred_element_type=jnp.float32).astype(jnp.bfloat16).reshape(sequence_number, SEQUENCE_LENGTH, QUERY_HEAD_COUNT, HEAD_SIZE)

    def backward_step(running, inputs):
        return (running, seq_backward(inputs[0], inputs[1], inputs[2], inputs[3], inputs[4], inputs[5], query_group_width))
    _, (dq_rot, rotated_key_gradient, value_gradient_total) = lax.scan(backward_step, 0, (q_seq, sequence_key, sequence_value, attended, log_total, d_att))
    d_query = apply_rotary(dq_rot.reshape(number_of_rows, QUERY_HEAD_COUNT, HEAD_SIZE), cosine_table, -sine_component).astype(jnp.bfloat16).reshape(number_of_rows, QUERY_HEAD_COUNT * HEAD_SIZE)
    key_gradient = apply_rotary(rotated_key_gradient.reshape(number_of_rows, KEY_VALUE_HEADS, HEAD_SIZE), cosine_table, -sine_component).astype(jnp.bfloat16).reshape(number_of_rows, KEY_VALUE_HEADS * HEAD_SIZE)
    value_gradient = value_gradient_total.astype(jnp.bfloat16).reshape(number_of_rows, KEY_VALUE_HEADS * HEAD_SIZE)
    query_grad = jnp.dot(first_normalized.T, d_query, preferred_element_type=jnp.float32)
    key_grad = jnp.dot(first_normalized.T, key_gradient, preferred_element_type=jnp.float32)
    value_grad = jnp.dot(first_normalized.T, value_gradient, preferred_element_type=jnp.float32)
    d_normed1 = jnp.dot(d_query, w_query.T, preferred_element_type=jnp.float32)
    d_normed1 = d_normed1 + jnp.dot(key_gradient, key_projection.T, preferred_element_type=jnp.float32)
    d_normed1 = d_normed1 + jnp.dot(value_gradient, value_projection.T, preferred_element_type=jnp.float32)
    d_resid_part, gain_attn_grad = norm_back(resid, scale_one, gain_attn, d_normed1)
    input_grad = (d_hidden1 + d_resid_part).astype(jnp.bfloat16)
    return (output, input_grad, gain_attn_grad, query_grad, key_grad, value_grad, out_grad, gain_moe_grad, router_grad, gate_grad, up_grad, down_grad)
```

```python
import math

import jax
import jax.numpy as jnp
from jax import lax
from jax.experimental import pallas as pl
from jax.experimental.pallas import tpu as pltpu
from jax.sharding import PartitionSpec as P

HEAD_SIZE = 64
SEQUENCE_LENGTH = 256
CAP = 64


EPSILON = 1e-06
ROPE_BASE = 10000.0
BLOCK_ROWS = 512


def split_up(x, dim, count):
    dims = x.shape
    tiles = x.reshape(*dims[:dim], count, dims[dim] // count, *dims[dim + 1 :])
    return jnp.moveaxis(tiles, dim, 0)


def sum_at_owner(x, axis, dim):
    tiles = split_up(x, dim, lax.axis_size(axis))
    arrived = lax.all_to_all(tiles, axis, split_axis=0, concat_axis=0, tiled=True)
    return arrived.astype(jnp.float32).sum(axis=0)


def side_by_side(arrays, axis, dim, along):
    both = jnp.concatenate(arrays, axis=along)
    filled, at, outs = (sum_at_owner(both, axis, dim), 0, [])
    for a in arrays:
        outs.append(lax.slice_in_dim(filled, at, at + a.shape[along], axis=along))
        at += a.shape[along]
    return tuple(outs)


def sent_together(arrays, axis, dim, along):
    widths = [math.prod(a.shape[along:]) for a in arrays]
    both = jnp.concatenate(
        [a.reshape(*a.shape[:along], w) for a, w in zip(arrays, widths)], axis=along
    )
    filled = sum_at_owner(both, axis, dim)
    tiles = jnp.split(filled, [sum(widths[:k]) for k in range(1, len(widths))], axis=along)
    return tuple(
        (b.reshape(*filled.shape[:along], *a.shape[along:]) for a, b in zip(arrays, tiles))
    )


def rms_scale(hidden):
    return lax.rsqrt(jnp.mean(hidden * hidden, axis=-1, keepdims=True) + EPSILON)


def norm_back(hidden, scaling, gain_vec, grad_out):
    weighted = grad_out * gain_vec
    gain_grad = jnp.sum(grad_out * hidden * scaling, axis=0)
    inner_mean = jnp.mean(weighted * hidden, axis=-1, keepdims=True)
    return (scaling * weighted - hidden * (scaling * scaling * scaling) * inner_mean, gain_grad)


def rope_tables(positions, head_dim):
    half_dim = head_dim // 2
    frequency = jnp.exp(
        jnp.arange(half_dim, dtype=jnp.float32) * (-2.0 * math.log(ROPE_BASE) / head_dim)
    )
    angles = positions[:, None] * frequency[None, :]
    return (jnp.cos(angles), jnp.sin(angles))


def apply_rotary(vectors, cosine_table, sine_component):
    half_dim = vectors.shape[-1] // 2
    first_half = vectors[..., :half_dim]
    second_half = vectors[..., half_dim:]
    cos_rows = cosine_table[:, None, :]
    sin_rows = sine_component[:, None, :]
    return jnp.concatenate(
        [
            first_half * cos_rows - second_half * sin_rows,
            first_half * sin_rows + second_half * cos_rows,
        ],
        axis=-1,
    )


def slot_table(route_ids, expert_count, capacity):
    number_of_rows, top_count = route_ids.shape
    flat_ids = route_ids.reshape(-1)
    one_hot = (flat_ids[:, None] == jnp.arange(expert_count, dtype=jnp.int32)[None, :]).astype(
        jnp.int32
    )
    earlier = jnp.cumsum(one_hot, axis=0) - one_hot
    slot_ids = jnp.sum(earlier * one_hot, axis=1)
    slot_where = flat_ids * capacity + slot_ids
    pick_ids = jnp.arange(number_of_rows * top_count, dtype=jnp.int32)
    token_of = (
        jnp.full((expert_count * capacity,), number_of_rows, jnp.int32)
        .at[slot_where]
        .set(pick_ids // top_count)
    )
    pick_of = (
        jnp.full((expert_count * capacity,), number_of_rows * top_count, jnp.int32)
        .at[slot_where]
        .set(pick_ids)
    )
    return (slot_where, token_of, pick_of)


def block_scores(query_rows, key_rows, query_group_width):
    block_len = query_rows.shape[0]
    key_count, kv_heads, head_dim = key_rows.shape
    grouped = query_rows.reshape(block_len, kv_heads, query_group_width, head_dim)
    scores = jnp.einsum(
        "qhgd,khd->hgqk", grouped, key_rows, preferred_element_type=jnp.float32
    ) * head_dim ** (-0.5)
    row_pos = jnp.arange(block_len, dtype=jnp.int32)[:, None]
    col_pos = jnp.arange(key_count, dtype=jnp.int32)[None, :]
    return (jnp.where(col_pos <= row_pos, scores, -1e30), grouped)


def sequence_forward(query_rows, key_rows, value_rows, query_group_width):
    length, kv_heads, head_dim = key_rows.shape
    block_len = min(BLOCK_ROWS, length)
    scores, grouped = block_scores(query_rows, key_rows, query_group_width)
    largest = jnp.max(scores, axis=-1, keepdims=True)
    log_total = largest + jnp.log(jnp.sum(jnp.exp(scores - largest), axis=-1, keepdims=True))
    weights = jnp.exp(scores - log_total).astype(jnp.bfloat16)
    attended = jnp.einsum("hgqk,khd->qhgd", weights, value_rows, preferred_element_type=jnp.float32)
    outputs = attended.reshape(block_len, -1, head_dim).astype(jnp.bfloat16)
    return (outputs, log_total)


def sequence_backward(
    query_rows, key_rows, value_rows, attended, log_total, d_attended, query_group_width
):
    length, kv_heads, head_dim = key_rows.shape
    block_len = min(BLOCK_ROWS, length)
    scale_factor = head_dim ** (-0.5)
    key_gradient = jnp.zeros((length, kv_heads, head_dim), jnp.float32)
    value_gradient = jnp.zeros((length, kv_heads, head_dim), jnp.float32)
    scores, grouped = block_scores(query_rows, key_rows, query_group_width)
    weights = jnp.exp(scores - log_total)
    d_grouped = d_attended.reshape(block_len, kv_heads, query_group_width, head_dim)
    o_grouped = attended.reshape(block_len, kv_heads, query_group_width, head_dim)
    delta = jnp.sum(d_grouped.astype(jnp.float32) * o_grouped.astype(jnp.float32), axis=-1)
    delta = jnp.transpose(delta, (1, 2, 0))[..., None]
    d_weights = jnp.einsum(
        "qhgd,khd->hgqk", d_grouped, value_rows, preferred_element_type=jnp.float32
    )
    d_scores = (weights * (d_weights - delta)).astype(jnp.bfloat16)
    block_query = (
        jnp.einsum("hgqk,khd->qhgd", d_scores, key_rows, preferred_element_type=jnp.float32)
        * scale_factor
    )
    query_parts = block_query.reshape(block_len, -1, head_dim)
    key_gradient = key_gradient.at[:block_len].add(
        jnp.einsum("hgqk,qhgd->khd", d_scores, grouped, preferred_element_type=jnp.float32)
        * scale_factor
    )
    value_gradient = value_gradient.at[:block_len].add(
        jnp.einsum(
            "hgqk,qhgd->khd",
            weights.astype(jnp.bfloat16),
            d_grouped,
            preferred_element_type=jnp.float32,
        )
    )
    return (query_parts, key_gradient, value_gradient)


def reduce_plan(
    tokens,
    gain_attn,
    w_query,
    key_projection,
    value_projection,
    w_out,
    gain_moe,
    w_router,
    w_gate,
    w_up,
    w_down,
    routes,
    cotangent,
):
    number_of_rows, model_width = tokens.shape
    head_dim = HEAD_SIZE
    query_heads = w_query.shape[1] // head_dim
    kv_heads = key_projection.shape[1] // head_dim
    query_group_width = query_heads // kv_heads
    expert_count = w_router.shape[1]
    local_experts = w_gate.shape[0]
    source_count = expert_count // local_experts
    capacity = CAP
    top_count = routes.shape[1]
    resid = tokens.astype(jnp.float32)
    scale_one = rms_scale(resid)
    first_normalized = (resid * scale_one * gain_attn).astype(jnp.bfloat16)
    positions = (jnp.arange(number_of_rows, dtype=jnp.int32) % SEQUENCE_LENGTH).astype(jnp.float32)
    cosine_table, sine_component = rope_tables(positions, head_dim)
    q_lin = jnp.dot(first_normalized, w_query, preferred_element_type=jnp.float32).reshape(
        number_of_rows, query_heads, head_dim
    )
    linear_key = jnp.dot(
        first_normalized, key_projection, preferred_element_type=jnp.float32
    ).reshape(number_of_rows, kv_heads, head_dim)
    value_reduced = (
        jnp.dot(first_normalized, value_projection, preferred_element_type=jnp.float32)
        .astype(jnp.bfloat16)
        .reshape(number_of_rows, kv_heads, head_dim)
    )
    q_rot = apply_rotary(q_lin, cosine_table, sine_component).astype(jnp.bfloat16)
    rotated_key = apply_rotary(linear_key, cosine_table, sine_component).astype(jnp.bfloat16)
    attended, log_total = sequence_forward(q_rot, rotated_key, value_reduced, query_group_width)
    flat_att = attended.reshape(number_of_rows, query_heads * head_dim)
    attn_part = jnp.dot(flat_att, w_out, preferred_element_type=jnp.float32)
    hidden1 = resid + lax.psum(attn_part.astype(jnp.bfloat16), "tensor").astype(jnp.float32)
    scale_two = rms_scale(hidden1)
    normed2 = (hidden1 * scale_two * gain_moe).astype(jnp.bfloat16)
    logits = jnp.dot(normed2, w_router, preferred_element_type=jnp.float32)
    chosen = jnp.take_along_axis(logits, routes, axis=1)
    gate_probs = jax.nn.softmax(chosen, axis=-1)
    slot_where, token_of, pick_of = slot_table(routes, expert_count, capacity)
    normed_pad = jnp.concatenate([normed2, jnp.zeros((1, model_width), jnp.bfloat16)], axis=0)
    outgoing = normed_pad[token_of].reshape(expert_count, capacity, model_width)
    received = lax.all_to_all(outgoing, "expert", split_axis=0, concat_axis=0, tiled=True)
    arrived = received.reshape(source_count, local_experts, capacity, model_width)
    gate_pre = jnp.einsum("secd,edh->sech", arrived, w_gate, preferred_element_type=jnp.float32)
    up_pre = jnp.einsum("secd,edh->sech", arrived, w_up, preferred_element_type=jnp.float32)
    sig_gate = jax.nn.sigmoid(gate_pre)
    activated = gate_pre * sig_gate
    hid_low = (activated * up_pre).astype(jnp.bfloat16)
    expert_out = jnp.einsum(
        "sech,ehd->secd", hid_low, w_down, preferred_element_type=jnp.float32
    ).astype(jnp.bfloat16)
    returned = lax.all_to_all(
        expert_out.reshape(expert_count, capacity, model_width),
        "expert",
        split_axis=0,
        concat_axis=0,
        tiled=True,
    )
    picked = returned.reshape(expert_count * capacity, model_width)[slot_where].reshape(
        number_of_rows, top_count, model_width
    )
    moe_part = jnp.zeros((number_of_rows, model_width), jnp.float32)
    for choice_index in range(top_count):
        moe_part = (
            moe_part
            + picked[:, choice_index].astype(jnp.float32)
            * gate_probs[:, choice_index : choice_index + 1]
        )
    moe_out = lax.psum(moe_part.astype(jnp.bfloat16), "tensor").astype(jnp.float32)
    output = (hidden1 + moe_out).astype(jnp.bfloat16)
    grad = cotangent.astype(jnp.float32)
    gate_dot = jnp.einsum("rjd,rd->rj", picked, cotangent, preferred_element_type=jnp.float32)
    grad_pad = jnp.concatenate([cotangent, jnp.zeros((1, model_width), jnp.bfloat16)], axis=0)
    gate_pad = jnp.concatenate([gate_probs.reshape(-1), jnp.zeros((1,), jnp.float32)], axis=0)
    sent_grad = (grad_pad[token_of].astype(jnp.float32) * gate_pad[pick_of][:, None]).astype(
        jnp.bfloat16
    )
    sent_grad = sent_grad.reshape(expert_count, capacity, model_width)
    grad_received = lax.all_to_all(sent_grad, "expert", split_axis=0, concat_axis=0, tiled=True)
    arrived_grad = grad_received.reshape(source_count, local_experts, capacity, model_width)
    d_hid = jnp.einsum("secd,ehd->sech", arrived_grad, w_down, preferred_element_type=jnp.float32)
    down_local = jnp.einsum(
        "sech,secd->ehd", hid_low, arrived_grad, preferred_element_type=jnp.float32
    )
    d_gate = (d_hid * up_pre * sig_gate * (1.0 + gate_pre * (1.0 - sig_gate))).astype(jnp.bfloat16)
    d_up = (d_hid * activated).astype(jnp.bfloat16)
    gate_local = jnp.einsum("secd,sech->edh", arrived, d_gate, preferred_element_type=jnp.float32)
    up_local = jnp.einsum("secd,sech->edh", arrived, d_up, preferred_element_type=jnp.float32)
    back_rows = jnp.einsum("sech,edh->secd", d_gate, w_gate, preferred_element_type=jnp.float32)
    back_rows = (
        back_rows + jnp.einsum("sech,edh->secd", d_up, w_up, preferred_element_type=jnp.float32)
    ).astype(jnp.bfloat16)
    came_back = lax.all_to_all(
        back_rows.reshape(expert_count, capacity, model_width),
        "expert",
        split_axis=0,
        concat_axis=0,
        tiled=True,
    )
    back_picked = came_back.reshape(expert_count * capacity, model_width)[slot_where].reshape(
        number_of_rows, top_count, model_width
    )
    back_part = jnp.zeros((number_of_rows, model_width), jnp.float32)
    for choice_index in range(top_count):
        back_part = back_part + back_picked[:, choice_index].astype(jnp.float32)
    back_total, dgate = (
        lax.psum(back_part.astype(jnp.bfloat16), "tensor").astype(jnp.float32),
        lax.psum(gate_dot.astype(jnp.bfloat16), "tensor").astype(jnp.float32),
    )
    inner_sum = jnp.sum(gate_probs * dgate, axis=1, keepdims=True)
    d_chosen = gate_probs * (dgate - inner_sum)
    matches = routes[:, :, None] == jnp.arange(expert_count, dtype=jnp.int32)[None, None, :]
    d_logits = jnp.sum(jnp.where(matches, d_chosen[:, :, None], 0.0), axis=1).astype(jnp.bfloat16)
    router_local = jnp.dot(normed2.T, d_logits, preferred_element_type=jnp.float32)
    d_normed2 = back_total + jnp.dot(d_logits, w_router.T, preferred_element_type=jnp.float32)
    d_hidden_part, gain_moe_local = norm_back(hidden1, scale_two, gain_moe, d_normed2)
    d_hidden1 = grad + d_hidden_part
    d_mixed = d_hidden1.astype(jnp.bfloat16)
    out_local = jnp.dot(flat_att.T, d_mixed, preferred_element_type=jnp.float32)
    d_att = (
        jnp.dot(d_mixed, w_out.T, preferred_element_type=jnp.float32)
        .astype(jnp.bfloat16)
        .reshape(number_of_rows, query_heads, head_dim)
    )
    dq_rot, rotated_key_gradient, dv_rows = sequence_backward(
        q_rot, rotated_key, value_reduced, attended, log_total, d_att, query_group_width
    )
    d_query = (
        apply_rotary(dq_rot, cosine_table, -sine_component)
        .astype(jnp.bfloat16)
        .reshape(number_of_rows, query_heads * head_dim)
    )
    key_gradient = (
        apply_rotary(rotated_key_gradient, cosine_table, -sine_component)
        .astype(jnp.bfloat16)
        .reshape(number_of_rows, kv_heads * head_dim)
    )
    value_gradient = dv_rows.astype(jnp.bfloat16).reshape(number_of_rows, kv_heads * head_dim)
    query_local = jnp.dot(first_normalized.T, d_query, preferred_element_type=jnp.float32)
    key_local = jnp.dot(first_normalized.T, key_gradient, preferred_element_type=jnp.float32)
    value_local = jnp.dot(first_normalized.T, value_gradient, preferred_element_type=jnp.float32)
    d_normed_part = jnp.dot(d_query, w_query.T, preferred_element_type=jnp.float32)
    d_normed_part = d_normed_part + jnp.dot(
        key_gradient, key_projection.T, preferred_element_type=jnp.float32
    )
    d_normed_part = d_normed_part + jnp.dot(
        value_gradient, value_projection.T, preferred_element_type=jnp.float32
    )
    d_normed1 = lax.psum(d_normed_part.astype(jnp.bfloat16), "tensor").astype(jnp.float32)
    d_resid_part, gain_attn_local = norm_back(resid, scale_one, gain_attn, d_normed1)
    input_grad = (d_hidden1 + d_resid_part).astype(jnp.bfloat16)
    gate_grad, up_grad, down_grad = (
        lax.psum_scatter(
            gate_local.astype(jnp.bfloat16), "dp", scatter_dimension=1, tiled=True
        ).astype(jnp.float32),
        lax.psum_scatter(
            up_local.astype(jnp.bfloat16), "dp", scatter_dimension=1, tiled=True
        ).astype(jnp.float32),
        lax.psum_scatter(
            down_local.astype(jnp.bfloat16), "dp", scatter_dimension=2, tiled=True
        ).astype(jnp.float32),
    )
    query_grad, key_grad, value_grad, out_grad, router_grad, gain_attn_grad, gain_moe_grad = (
        *side_by_side(
            (
                query_local.astype(jnp.bfloat16),
                key_local.astype(jnp.bfloat16),
                value_local.astype(jnp.bfloat16),
            ),
            ("dp", "expert"),
            0,
            1,
        ),
        sum_at_owner(out_local.astype(jnp.bfloat16), ("dp", "expert"), 1),
        *sent_together(
            (
                router_local.astype(jnp.bfloat16),
                gain_attn_local.astype(jnp.bfloat16),
                gain_moe_local.astype(jnp.bfloat16),
            ),
            ("dp", "expert"),
            0,
            1,
        ),
    )
    return (
        output,
        input_grad,
        gain_attn_grad,
        query_grad,
        key_grad,
        value_grad,
        out_grad,
        gain_moe_grad,
        router_grad,
        gate_grad,
        up_grad,
        down_grad,
    )


GATHER_ROWS = 4096
CHUNK = 512
ALL = ("dp", "expert", "tensor")
SEQ = ("dp", "expert")


def dot(a, b):
    return jnp.dot(a, b, preferred_element_type=jnp.float32)


def dot_nt(a, b):
    return lax.dot_general(a, b, (((1,), (1,)), ((), ())), preferred_element_type=jnp.float32)


def expert_kernel(
    plane_ref,
    x_ref,
    g_ref,
    xt_ref,
    gt_ref,
    gates_ref,
    wg_ref,
    wu_ref,
    wd_ref,
    gate_grad_ref,
    up_grad_ref,
    down_grad_ref,
    moe_ref,
    back_ref,
    dgate_ref,
    hid_buf,
    dgate_buf,
    dup_buf,
    down_buf,
    moe_acc,
    back_acc,
    dg_acc,
):
    step = pl.program_id(0)
    rows = x_ref.shape[0]
    width = wg_ref.shape[2]
    plane_rows = moe_ref.shape[0]
    plane = plane_ref[0]

    @pl.when(step == 0)
    def _():
        moe_acc[...] = jnp.zeros_like(moe_acc)
        back_acc[...] = jnp.zeros_like(back_acc)
        dg_acc[...] = jnp.zeros_like(dg_acc)

    k_pos = lax.broadcasted_iota(jnp.int32, (128, 2 * width), 0)
    l_pos = lax.broadcasted_iota(jnp.int32, (128, 2 * width), 1)
    pick = jnp.where(k_pos % 64 == 2 * step + l_pos // width, 1.0, 0.0).astype(jnp.bfloat16)
    wd_pair = wd_ref[...].reshape(2 * width, wd_ref.shape[2])

    def chunk_step(chunk, _):
        at = pl.ds(pl.multiple_of(chunk * CHUNK, CHUNK), CHUNK)
        x = x_ref[at, :]
        gate_pair = dot(gates_ref[at, :], pick)
        dh_pair = dot_nt(g_ref[at, :], wd_pair)
        for k in range(2):
            both = dot(x, jnp.concatenate([wg_ref[k], wu_ref[k]], axis=1))
            gate_pre, up_pre = both[:, :width], both[:, width:]
            lanes = slice(k * width, (k + 1) * width)
            gate = gate_pair[:, lanes]
            dh = dh_pair[:, lanes]
            sig = jax.nn.sigmoid(gate_pre)
            act = gate_pre * sig
            hid = act * up_pre
            ghid = hid * gate
            d_hid = dh * gate
            dgp = d_hid * up_pre * sig * (1.0 + gate_pre * (1.0 - sig))
            dup = d_hid * act
            hid_buf[at, lanes] = ghid.astype(jnp.bfloat16)
            dgate_buf[at, lanes] = dgp.astype(jnp.bfloat16)
            dup_buf[at, lanes] = dup.astype(jnp.bfloat16)

            @pl.when(chunk == plane)
            def _():
                down_buf[:, lanes] = hid * dh

        return 0

    lax.fori_loop(0, rows // CHUNK, chunk_step, 0)
    own = pl.ds(pl.multiple_of(plane * plane_rows, plane_rows), plane_rows)
    moe_acc[...] += dot(hid_buf[own, :], wd_pair)
    for k in range(2):
        lanes = slice(k * width, (k + 1) * width)
        back_acc[...] += dot_nt(dgate_buf[own, lanes], wg_ref[k]) + dot_nt(dup_buf[own, lanes], wu_ref[k])
        row_sum = jnp.sum(down_buf[:, lanes], axis=1, keepdims=True)
        lane_of = lax.broadcasted_iota(jnp.int32, dg_acc.shape, 1)
        dg_acc[...] += jnp.where(lane_of == 2 * step + k, row_sum, 0.0)
    gate_both = dot(xt_ref[...], dgate_buf[...])
    up_both = dot(xt_ref[...], dup_buf[...])
    down_both = dot(gt_ref[...], hid_buf[...]).T
    for k in range(2):
        lanes = slice(k * width, (k + 1) * width)
        gate_grad_ref[k] = gate_both[:, lanes]
        up_grad_ref[k] = up_both[:, lanes]
        down_grad_ref[k] = down_both[lanes, :]

    @pl.when(step == pl.num_programs(0) - 1)
    def _():
        moe_ref[...] = moe_acc[...].astype(jnp.bfloat16)
        back_ref[...] = back_acc[...].astype(jnp.bfloat16)
        dgate_ref[...] = dg_acc[...]


def experts(plane, x_all, g_all, x_cols, g_cols, gates, w_gate, w_up, w_down, plane_rows):
    rows, model = x_all.shape
    count, _, width = w_gate.shape
    block = x_cols.shape[0]
    whole = lambda shape: pl.BlockSpec(shape, lambda i, p: (0,) * len(shape), pipeline_mode=pl.Buffered(1))
    by_pair = lambda shape: pl.BlockSpec((2,) + shape, lambda i, p: (i, 0, 0))
    return pl.pallas_call(
        expert_kernel,
        grid_spec=pltpu.PrefetchScalarGridSpec(
            num_scalar_prefetch=1,
            grid=(count // 2,),
            in_specs=[
                whole((rows, model)),
                whole((rows, model)),
                whole((block, rows)),
                whole((block, rows)),
                whole((rows, 128)),
                by_pair((model, width)),
                by_pair((model, width)),
                by_pair((width, model)),
            ],
            out_specs=[
                by_pair((block, width)),
                by_pair((block, width)),
                by_pair((width, block)),
                whole((plane_rows, model)),
                whole((plane_rows, model)),
                whole((plane_rows, 128)),
            ],
            scratch_shapes=[
                pltpu.VMEM((rows, 2 * width), jnp.bfloat16),
                pltpu.VMEM((rows, 2 * width), jnp.bfloat16),
                pltpu.VMEM((rows, 2 * width), jnp.bfloat16),
                pltpu.VMEM((plane_rows, 2 * width), jnp.float32),
                pltpu.VMEM((plane_rows, model), jnp.float32),
                pltpu.VMEM((plane_rows, model), jnp.float32),
                pltpu.VMEM((plane_rows, 128), jnp.float32),
            ],
        ),
        out_shape=[
            jax.ShapeDtypeStruct((count, block, width), jnp.float32),
            jax.ShapeDtypeStruct((count, block, width), jnp.float32),
            jax.ShapeDtypeStruct((count, width, block), jnp.float32),
            jax.ShapeDtypeStruct((plane_rows, model), jnp.bfloat16),
            jax.ShapeDtypeStruct((plane_rows, model), jnp.bfloat16),
            jax.ShapeDtypeStruct((plane_rows, 128), jnp.float32),
        ],
        compiler_params=pltpu.CompilerParams(vmem_limit_bytes=60 * 2**20),
        name="experts",
    )(plane, x_all, g_all, x_cols, g_cols, gates, w_gate, w_up, w_down)


def dense_gates(logits, routes):
    expert_ids = jnp.arange(logits.shape[1], dtype=jnp.int32)[None, :]
    chosen = routes[:, 0:1] == expert_ids
    for j in range(1, routes.shape[1]):
        chosen = chosen | (routes[:, j : j + 1] == expert_ids)
    top = jnp.max(jnp.where(chosen, logits, -jnp.inf), axis=1, keepdims=True)
    weight = jnp.where(chosen, jnp.exp(jnp.where(chosen, logits - top, 0.0)), 0.0)
    return weight / jnp.sum(weight, axis=1, keepdims=True)


def gather_plan(
    tokens,
    gain_attn,
    w_query,
    key_projection,
    value_projection,
    w_out,
    gain_moe,
    w_router,
    w_gate,
    w_up,
    w_down,
    routes,
    cotangent,
):
    number_of_rows, model_width = tokens.shape
    head_dim = HEAD_SIZE
    query_heads = w_query.shape[1] // head_dim
    kv_heads = key_projection.shape[1] // head_dim
    query_group_width = query_heads // kv_heads
    expert_count = w_router.shape[1]
    local_experts = w_gate.shape[0]
    dp, ex, tp = lax.axis_size("dp"), lax.axis_size("expert"), lax.axis_size("tensor")
    z, core, t = lax.axis_index("dp"), lax.axis_index("expert"), lax.axis_index("tensor")
    own_rows = number_of_rows // tp
    plane_rows = number_of_rows * ex
    mine = lambda a: lax.dynamic_slice_in_dim(a, t * own_rows, own_rows, axis=0)

    g_all = lax.all_gather(cotangent, SEQ, axis=0, tiled=True)
    routes_all = lax.all_gather(routes, SEQ, axis=0, tiled=True)
    resid = tokens.astype(jnp.float32)
    scale_one = rms_scale(resid)
    normed1 = (resid * scale_one * gain_attn).astype(jnp.bfloat16)
    n1_cols = lax.all_to_all(
        split_up(normed1, 1, dp * ex), SEQ, split_axis=0, concat_axis=0, tiled=True
    ).reshape(dp * ex * number_of_rows, -1)
    positions = (jnp.arange(number_of_rows, dtype=jnp.int32) % SEQUENCE_LENGTH).astype(jnp.float32)
    cosine_table, sine_component = rope_tables(positions, head_dim)
    q_lin = dot(normed1, w_query).reshape(number_of_rows, query_heads, head_dim)
    k_lin = dot(normed1, key_projection).reshape(number_of_rows, kv_heads, head_dim)
    v_low = (
        dot(normed1, value_projection)
        .astype(jnp.bfloat16)
        .reshape(number_of_rows, kv_heads, head_dim)
    )
    q_rot = apply_rotary(q_lin, cosine_table, sine_component).astype(jnp.bfloat16)
    k_rot = apply_rotary(k_lin, cosine_table, sine_component).astype(jnp.bfloat16)
    attended, log_total = sequence_forward(q_rot, k_rot, v_low, query_group_width)
    flat_att = attended.reshape(number_of_rows, query_heads * head_dim)
    att_all = lax.all_gather(flat_att, SEQ, axis=0, tiled=True)
    attn_part = dot(flat_att, w_out).astype(jnp.bfloat16)
    resid_own = mine(tokens).astype(jnp.float32)
    hidden1 = resid_own + lax.psum_scatter(
        attn_part, "tensor", scatter_dimension=0, tiled=True
    ).astype(jnp.float32)
    scale_two = rms_scale(hidden1)
    normed2 = (hidden1 * scale_two * gain_moe).astype(jnp.bfloat16)
    x_all = lax.all_gather(normed2, ALL, axis=0, tiled=True)

    gates = dense_gates(dot(x_all, w_router), routes_all)
    gates_own = lax.dynamic_slice_in_dim(gates, core * local_experts, local_experts, axis=1)
    high = gates_own.astype(jnp.bfloat16)
    low = (gates_own - high.astype(jnp.float32)).astype(jnp.bfloat16)
    pad = jnp.zeros((gates.shape[0], 64 - local_experts), jnp.bfloat16)
    gate_pack = jnp.concatenate([high, pad, low, pad], axis=1)
    block = model_width // dp
    x_cols = lax.dynamic_slice_in_dim(x_all, z * block, block, axis=1).T
    g_cols = lax.dynamic_slice_in_dim(g_all, z * block, block, axis=1).T
    plane = z.astype(jnp.int32).reshape(1)
    gate_grad, up_grad, down_grad, moe_part, back_part, dgate_part = experts(
        plane, x_all, g_all, x_cols, g_cols, gate_pack, w_gate, w_up, w_down, plane_rows
    )

    dgate_part = dgate_part[:, :local_experts]
    wide = jnp.zeros((plane_rows, expert_count), jnp.float32)
    wide = lax.dynamic_update_slice_in_dim(wide, dgate_part, core * local_experts, axis=1)
    pair = ("expert", "tensor")
    back = lax.psum_scatter(back_part, pair, scatter_dimension=0, tiled=True).astype(jnp.float32)
    moe = lax.psum_scatter(moe_part, pair, scatter_dimension=0, tiled=True).astype(jnp.float32)
    dgate = lax.psum_scatter(wide, pair, scatter_dimension=0, tiled=True)
    output_own = (hidden1 + moe).astype(jnp.bfloat16)
    output = lax.all_gather(output_own, "tensor", axis=0, tiled=True)

    first = ((z * ex + core) * tp + t) * own_rows
    gates_mine = lax.dynamic_slice_in_dim(gates, first, own_rows, axis=0)
    inner_sum = jnp.sum(gates_mine * dgate, axis=1, keepdims=True)
    d_logits = (gates_mine * (dgate - inner_sum)).astype(jnp.bfloat16)
    d_logits_all = lax.all_gather(d_logits, ALL, axis=0, tiled=True)
    part = model_width // (dp * ex)
    seq = z * ex + core
    x_part = lax.dynamic_slice_in_dim(x_all, seq * part, part, axis=1)
    router_grad = dot(x_part.T, d_logits_all)
    d_normed2 = back + dot(d_logits, w_router.T)
    grad_own = mine(cotangent).astype(jnp.float32)
    d_hidden_part, gain_moe_local = norm_back(hidden1, scale_two, gain_moe, d_normed2)
    d_hidden1 = grad_own + d_hidden_part
    d_mixed_own = d_hidden1.astype(jnp.bfloat16)
    d_mixed = lax.all_gather(d_mixed_own, "tensor", axis=0, tiled=True)
    da_cols = lax.all_to_all(
        split_up(d_mixed, 1, dp * ex), SEQ, split_axis=0, concat_axis=0, tiled=True
    ).reshape(dp * ex * number_of_rows, -1)
    out_grad = dot(att_all.T, da_cols)
    d_att = (
        dot_nt(d_mixed, w_out)
        .astype(jnp.bfloat16)
        .reshape(number_of_rows, query_heads, head_dim)
    )
    dq_rot, dk_rot, dv_rows = sequence_backward(
        q_rot, k_rot, v_low, attended, log_total, d_att, query_group_width
    )
    d_query = (
        apply_rotary(dq_rot, cosine_table, -sine_component)
        .astype(jnp.bfloat16)
        .reshape(number_of_rows, query_heads * head_dim)
    )
    d_key = (
        apply_rotary(dk_rot, cosine_table, -sine_component)
        .astype(jnp.bfloat16)
        .reshape(number_of_rows, kv_heads * head_dim)
    )
    d_value = dv_rows.astype(jnp.bfloat16).reshape(number_of_rows, kv_heads * head_dim)
    d_qkv = jnp.concatenate([d_query, d_key, d_value], axis=1)
    d_qkv_all = lax.all_gather(d_qkv, SEQ, axis=0, tiled=True)
    qkv_grad = dot(n1_cols.T, d_qkv_all)
    q_width, k_width = d_query.shape[1], d_key.shape[1]
    query_grad = qkv_grad[:, :q_width]
    key_grad = qkv_grad[:, q_width : q_width + k_width]
    value_grad = qkv_grad[:, q_width + k_width :]
    w_qkv = jnp.concatenate([w_query, key_projection, value_projection], axis=1)
    d_normed_part = dot_nt(d_qkv, w_qkv).astype(jnp.bfloat16)
    d_normed1 = lax.psum_scatter(
        d_normed_part, "tensor", scatter_dimension=0, tiled=True
    ).astype(jnp.float32)
    d_resid_part, gain_attn_local = norm_back(resid_own, mine(scale_one), gain_attn, d_normed1)
    input_own = (d_hidden1 + d_resid_part).astype(jnp.bfloat16)
    input_grad = lax.all_gather(input_own, "tensor", axis=0, tiled=True)
    gains = jnp.stack([gain_attn_local, gain_moe_local], axis=0)
    gains_all = lax.all_gather(gains, ALL, axis=0, tiled=False)
    gains_sum = gains_all.reshape(-1, 2, model_width).sum(axis=0)
    gains_mine = lax.dynamic_slice_in_dim(gains_sum, seq * part, part, axis=1)
    return (
        output,
        input_grad,
        gains_mine[0],
        query_grad,
        key_grad,
        value_grad,
        out_grad,
        gains_mine[1],
        router_grad,
        gate_grad,
        up_grad,
        down_grad,
    )


def solution(mesh):
    placed = (
        P(("dp", "expert"), None),
        P(),
        P(None, "tensor"),
        P(None, "tensor"),
        P(None, "tensor"),
        P("tensor", None),
        P(),
        P(),
        P("expert", None, "tensor"),
        P("expert", None, "tensor"),
        P("expert", "tensor", None),
        P(("dp", "expert"), None),
        P(("dp", "expert"), None),
    )
    sequences = mesh.shape["dp"] * mesh.shape["expert"]
    few = sequences * SEQUENCE_LENGTH <= GATHER_ROWS and mesh.shape["tensor"] == 4
    return jax.shard_map(
        gather_plan if few else reduce_plan,
        mesh=mesh,
        in_specs=placed,
        out_specs=(
            P(("dp", "expert"), None),
            P(("dp", "expert"), None),
            P(("dp", "expert")),
            P(("dp", "expert"), "tensor"),
            P(("dp", "expert"), "tensor"),
            P(("dp", "expert"), "tensor"),
            P("tensor", ("dp", "expert")),
            P(("dp", "expert")),
            P(("dp", "expert"), None),
            P("expert", "dp", "tensor"),
            P("expert", "dp", "tensor"),
            P("expert", "tensor", "dp"),
        ),
        check_vma=False,
    )
```

```python
import functools
import math

import jax
import jax.numpy as jnp
from jax import lax
from jax.experimental import pallas as pl
from jax.experimental.pallas import tpu as pltpu
from jax.sharding import PartitionSpec as P

HEAD_SIZE = 64
SEQUENCE_LENGTH = 256
CAP = 64


EPSILON = 1e-06
ROPE_BASE = 10000.0
BLOCK_ROWS = 512


def split_up(x, dim, count):
    dims = x.shape
    tiles = x.reshape(*dims[:dim], count, dims[dim] // count, *dims[dim + 1 :])
    return jnp.moveaxis(tiles, dim, 0)


def sum_at_owner(x, axis, dim):
    tiles = split_up(x, dim, lax.axis_size(axis))
    arrived = lax.all_to_all(tiles, axis, split_axis=0, concat_axis=0, tiled=True)
    return arrived.astype(jnp.float32).sum(axis=0)


def side_by_side(arrays, axis, dim, along):
    both = jnp.concatenate(arrays, axis=along)
    filled, at, outs = (sum_at_owner(both, axis, dim), 0, [])
    for a in arrays:
        outs.append(lax.slice_in_dim(filled, at, at + a.shape[along], axis=along))
        at += a.shape[along]
    return tuple(outs)


def sent_together(arrays, axis, dim, along):
    widths = [math.prod(a.shape[along:]) for a in arrays]
    both = jnp.concatenate(
        [a.reshape(*a.shape[:along], w) for a, w in zip(arrays, widths)], axis=along
    )
    filled = sum_at_owner(both, axis, dim)
    tiles = jnp.split(filled, [sum(widths[:k]) for k in range(1, len(widths))], axis=along)
    return tuple(
        (b.reshape(*filled.shape[:along], *a.shape[along:]) for a, b in zip(arrays, tiles))
    )


def rms_scale(hidden):
    return lax.rsqrt(jnp.mean(hidden * hidden, axis=-1, keepdims=True) + EPSILON)


def norm_back(hidden, scaling, gain_vec, grad_out):
    weighted = grad_out * gain_vec
    gain_grad = jnp.sum(grad_out * hidden * scaling, axis=0)
    inner_mean = jnp.mean(weighted * hidden, axis=-1, keepdims=True)
    return (scaling * weighted - hidden * (scaling * scaling * scaling) * inner_mean, gain_grad)


def rope_tables(positions, head_dim):
    half_dim = head_dim // 2
    frequency = jnp.exp(
        jnp.arange(half_dim, dtype=jnp.float32) * (-2.0 * math.log(ROPE_BASE) / head_dim)
    )
    angles = positions[:, None] * frequency[None, :]
    return (jnp.cos(angles), jnp.sin(angles))


def apply_rotary(vectors, cosine_table, sine_component):
    half_dim = vectors.shape[-1] // 2
    first_half = vectors[..., :half_dim]
    second_half = vectors[..., half_dim:]
    cos_rows = cosine_table[:, None, :]
    sin_rows = sine_component[:, None, :]
    return jnp.concatenate(
        [
            first_half * cos_rows - second_half * sin_rows,
            first_half * sin_rows + second_half * cos_rows,
        ],
        axis=-1,
    )


def slot_table(route_ids, expert_count, capacity):
    number_of_rows, top_count = route_ids.shape
    flat_ids = route_ids.reshape(-1)
    one_hot = (flat_ids[:, None] == jnp.arange(expert_count, dtype=jnp.int32)[None, :]).astype(
        jnp.int32
    )
    earlier = jnp.cumsum(one_hot, axis=0) - one_hot
    slot_ids = jnp.sum(earlier * one_hot, axis=1)
    slot_where = flat_ids * capacity + slot_ids
    pick_ids = jnp.arange(number_of_rows * top_count, dtype=jnp.int32)
    token_of = (
        jnp.full((expert_count * capacity,), number_of_rows, jnp.int32)
        .at[slot_where]
        .set(pick_ids // top_count)
    )
    pick_of = (
        jnp.full((expert_count * capacity,), number_of_rows * top_count, jnp.int32)
        .at[slot_where]
        .set(pick_ids)
    )
    return (slot_where, token_of, pick_of)


def block_scores(query_rows, key_rows, query_group_width):
    block_len = query_rows.shape[0]
    key_count, kv_heads, head_dim = key_rows.shape
    grouped = query_rows.reshape(block_len, kv_heads, query_group_width, head_dim)
    scores = jnp.einsum(
        "qhgd,khd->hgqk", grouped, key_rows, preferred_element_type=jnp.float32
    ) * head_dim ** (-0.5)
    row_pos = jnp.arange(block_len, dtype=jnp.int32)[:, None]
    col_pos = jnp.arange(key_count, dtype=jnp.int32)[None, :]
    return (jnp.where(col_pos <= row_pos, scores, -1e30), grouped)


def sequence_forward(query_rows, key_rows, value_rows, query_group_width):
    length, kv_heads, head_dim = key_rows.shape
    block_len = min(BLOCK_ROWS, length)
    scores, grouped = block_scores(query_rows, key_rows, query_group_width)
    largest = jnp.max(scores, axis=-1, keepdims=True)
    log_total = largest + jnp.log(jnp.sum(jnp.exp(scores - largest), axis=-1, keepdims=True))
    weights = jnp.exp(scores - log_total).astype(jnp.bfloat16)
    attended = jnp.einsum("hgqk,khd->qhgd", weights, value_rows, preferred_element_type=jnp.float32)
    outputs = attended.reshape(block_len, -1, head_dim).astype(jnp.bfloat16)
    return (outputs, log_total)


def sequence_backward(
    query_rows, key_rows, value_rows, attended, log_total, d_attended, query_group_width
):
    length, kv_heads, head_dim = key_rows.shape
    block_len = min(BLOCK_ROWS, length)
    scale_factor = head_dim ** (-0.5)
    key_gradient = jnp.zeros((length, kv_heads, head_dim), jnp.float32)
    value_gradient = jnp.zeros((length, kv_heads, head_dim), jnp.float32)
    scores, grouped = block_scores(query_rows, key_rows, query_group_width)
    weights = jnp.exp(scores - log_total)
    d_grouped = d_attended.reshape(block_len, kv_heads, query_group_width, head_dim)
    o_grouped = attended.reshape(block_len, kv_heads, query_group_width, head_dim)
    delta = jnp.sum(d_grouped.astype(jnp.float32) * o_grouped.astype(jnp.float32), axis=-1)
    delta = jnp.transpose(delta, (1, 2, 0))[..., None]
    d_weights = jnp.einsum(
        "qhgd,khd->hgqk", d_grouped, value_rows, preferred_element_type=jnp.float32
    )
    d_scores = (weights * (d_weights - delta)).astype(jnp.bfloat16)
    block_query = (
        jnp.einsum("hgqk,khd->qhgd", d_scores, key_rows, preferred_element_type=jnp.float32)
        * scale_factor
    )
    query_parts = block_query.reshape(block_len, -1, head_dim)
    key_gradient = key_gradient.at[:block_len].add(
        jnp.einsum("hgqk,qhgd->khd", d_scores, grouped, preferred_element_type=jnp.float32)
        * scale_factor
    )
    value_gradient = value_gradient.at[:block_len].add(
        jnp.einsum(
            "hgqk,qhgd->khd",
            weights.astype(jnp.bfloat16),
            d_grouped,
            preferred_element_type=jnp.float32,
        )
    )
    return (query_parts, key_gradient, value_gradient)


def reduce_plan(
    tokens,
    gain_attn,
    w_query,
    key_projection,
    value_projection,
    w_out,
    gain_moe,
    w_router,
    w_gate,
    w_up,
    w_down,
    routes,
    cotangent,
):
    number_of_rows, model_width = tokens.shape
    head_dim = HEAD_SIZE
    query_heads = w_query.shape[1] // head_dim
    kv_heads = key_projection.shape[1] // head_dim
    query_group_width = query_heads // kv_heads
    expert_count = w_router.shape[1]
    local_experts = w_gate.shape[0]
    source_count = expert_count // local_experts
    capacity = CAP
    top_count = routes.shape[1]
    resid = tokens.astype(jnp.float32)
    scale_one = rms_scale(resid)
    first_normalized = (resid * scale_one * gain_attn).astype(jnp.bfloat16)
    positions = (jnp.arange(number_of_rows, dtype=jnp.int32) % SEQUENCE_LENGTH).astype(jnp.float32)
    cosine_table, sine_component = rope_tables(positions, head_dim)
    q_lin = jnp.dot(first_normalized, w_query, preferred_element_type=jnp.float32).reshape(
        number_of_rows, query_heads, head_dim
    )
    linear_key = jnp.dot(
        first_normalized, key_projection, preferred_element_type=jnp.float32
    ).reshape(number_of_rows, kv_heads, head_dim)
    value_reduced = (
        jnp.dot(first_normalized, value_projection, preferred_element_type=jnp.float32)
        .astype(jnp.bfloat16)
        .reshape(number_of_rows, kv_heads, head_dim)
    )
    q_rot = apply_rotary(q_lin, cosine_table, sine_component).astype(jnp.bfloat16)
    rotated_key = apply_rotary(linear_key, cosine_table, sine_component).astype(jnp.bfloat16)
    attended, log_total = sequence_forward(q_rot, rotated_key, value_reduced, query_group_width)
    flat_att = attended.reshape(number_of_rows, query_heads * head_dim)
    attn_part = jnp.dot(flat_att, w_out, preferred_element_type=jnp.float32)
    hidden1 = resid + lax.psum(attn_part.astype(jnp.bfloat16), "tensor").astype(jnp.float32)
    scale_two = rms_scale(hidden1)
    normed2 = (hidden1 * scale_two * gain_moe).astype(jnp.bfloat16)
    logits = jnp.dot(normed2, w_router, preferred_element_type=jnp.float32)
    chosen = jnp.take_along_axis(logits, routes, axis=1)
    gate_probs = jax.nn.softmax(chosen, axis=-1)
    slot_where, token_of, pick_of = slot_table(routes, expert_count, capacity)
    normed_pad = jnp.concatenate([normed2, jnp.zeros((1, model_width), jnp.bfloat16)], axis=0)
    outgoing = normed_pad[token_of].reshape(expert_count, capacity, model_width)
    received = lax.all_to_all(outgoing, "expert", split_axis=0, concat_axis=0, tiled=True)
    arrived = received.reshape(source_count, local_experts, capacity, model_width)
    gate_pre = jnp.einsum("secd,edh->sech", arrived, w_gate, preferred_element_type=jnp.float32)
    up_pre = jnp.einsum("secd,edh->sech", arrived, w_up, preferred_element_type=jnp.float32)
    sig_gate = jax.nn.sigmoid(gate_pre)
    activated = gate_pre * sig_gate
    hid_low = (activated * up_pre).astype(jnp.bfloat16)
    expert_out = jnp.einsum(
        "sech,ehd->secd", hid_low, w_down, preferred_element_type=jnp.float32
    ).astype(jnp.bfloat16)
    returned = lax.all_to_all(
        expert_out.reshape(expert_count, capacity, model_width),
        "expert",
        split_axis=0,
        concat_axis=0,
        tiled=True,
    )
    picked = returned.reshape(expert_count * capacity, model_width)[slot_where].reshape(
        number_of_rows, top_count, model_width
    )
    moe_part = jnp.zeros((number_of_rows, model_width), jnp.float32)
    for choice_index in range(top_count):
        moe_part = (
            moe_part
            + picked[:, choice_index].astype(jnp.float32)
            * gate_probs[:, choice_index : choice_index + 1]
        )
    moe_out = lax.psum(moe_part.astype(jnp.bfloat16), "tensor").astype(jnp.float32)
    output = (hidden1 + moe_out).astype(jnp.bfloat16)
    grad = cotangent.astype(jnp.float32)
    gate_dot = jnp.einsum("rjd,rd->rj", picked, cotangent, preferred_element_type=jnp.float32)
    grad_pad = jnp.concatenate([cotangent, jnp.zeros((1, model_width), jnp.bfloat16)], axis=0)
    gate_pad = jnp.concatenate([gate_probs.reshape(-1), jnp.zeros((1,), jnp.float32)], axis=0)
    sent_grad = (grad_pad[token_of].astype(jnp.float32) * gate_pad[pick_of][:, None]).astype(
        jnp.bfloat16
    )
    sent_grad = sent_grad.reshape(expert_count, capacity, model_width)
    grad_received = lax.all_to_all(sent_grad, "expert", split_axis=0, concat_axis=0, tiled=True)
    arrived_grad = grad_received.reshape(source_count, local_experts, capacity, model_width)
    d_hid = jnp.einsum("secd,ehd->sech", arrived_grad, w_down, preferred_element_type=jnp.float32)
    down_local = jnp.einsum(
        "sech,secd->ehd", hid_low, arrived_grad, preferred_element_type=jnp.float32
    )
    d_gate = (d_hid * up_pre * sig_gate * (1.0 + gate_pre * (1.0 - sig_gate))).astype(jnp.bfloat16)
    d_up = (d_hid * activated).astype(jnp.bfloat16)
    gate_local = jnp.einsum("secd,sech->edh", arrived, d_gate, preferred_element_type=jnp.float32)
    up_local = jnp.einsum("secd,sech->edh", arrived, d_up, preferred_element_type=jnp.float32)
    back_rows = jnp.einsum("sech,edh->secd", d_gate, w_gate, preferred_element_type=jnp.float32)
    back_rows = (
        back_rows + jnp.einsum("sech,edh->secd", d_up, w_up, preferred_element_type=jnp.float32)
    ).astype(jnp.bfloat16)
    came_back = lax.all_to_all(
        back_rows.reshape(expert_count, capacity, model_width),
        "expert",
        split_axis=0,
        concat_axis=0,
        tiled=True,
    )
    back_picked = came_back.reshape(expert_count * capacity, model_width)[slot_where].reshape(
        number_of_rows, top_count, model_width
    )
    back_part = jnp.zeros((number_of_rows, model_width), jnp.float32)
    for choice_index in range(top_count):
        back_part = back_part + back_picked[:, choice_index].astype(jnp.float32)
    back_total, dgate = (
        lax.psum(back_part.astype(jnp.bfloat16), "tensor").astype(jnp.float32),
        lax.psum(gate_dot.astype(jnp.bfloat16), "tensor").astype(jnp.float32),
    )
    inner_sum = jnp.sum(gate_probs * dgate, axis=1, keepdims=True)
    d_chosen = gate_probs * (dgate - inner_sum)
    matches = routes[:, :, None] == jnp.arange(expert_count, dtype=jnp.int32)[None, None, :]
    d_logits = jnp.sum(jnp.where(matches, d_chosen[:, :, None], 0.0), axis=1).astype(jnp.bfloat16)
    router_local = jnp.dot(normed2.T, d_logits, preferred_element_type=jnp.float32)
    d_normed2 = back_total + jnp.dot(d_logits, w_router.T, preferred_element_type=jnp.float32)
    d_hidden_part, gain_moe_local = norm_back(hidden1, scale_two, gain_moe, d_normed2)
    d_hidden1 = grad + d_hidden_part
    d_mixed = d_hidden1.astype(jnp.bfloat16)
    out_local = jnp.dot(flat_att.T, d_mixed, preferred_element_type=jnp.float32)
    d_att = (
        jnp.dot(d_mixed, w_out.T, preferred_element_type=jnp.float32)
        .astype(jnp.bfloat16)
        .reshape(number_of_rows, query_heads, head_dim)
    )
    dq_rot, rotated_key_gradient, dv_rows = sequence_backward(
        q_rot, rotated_key, value_reduced, attended, log_total, d_att, query_group_width
    )
    d_query = (
        apply_rotary(dq_rot, cosine_table, -sine_component)
        .astype(jnp.bfloat16)
        .reshape(number_of_rows, query_heads * head_dim)
    )
    key_gradient = (
        apply_rotary(rotated_key_gradient, cosine_table, -sine_component)
        .astype(jnp.bfloat16)
        .reshape(number_of_rows, kv_heads * head_dim)
    )
    value_gradient = dv_rows.astype(jnp.bfloat16).reshape(number_of_rows, kv_heads * head_dim)
    query_local = jnp.dot(first_normalized.T, d_query, preferred_element_type=jnp.float32)
    key_local = jnp.dot(first_normalized.T, key_gradient, preferred_element_type=jnp.float32)
    value_local = jnp.dot(first_normalized.T, value_gradient, preferred_element_type=jnp.float32)
    d_normed_part = jnp.dot(d_query, w_query.T, preferred_element_type=jnp.float32)
    d_normed_part = d_normed_part + jnp.dot(
        key_gradient, key_projection.T, preferred_element_type=jnp.float32
    )
    d_normed_part = d_normed_part + jnp.dot(
        value_gradient, value_projection.T, preferred_element_type=jnp.float32
    )
    d_normed1 = lax.psum(d_normed_part.astype(jnp.bfloat16), "tensor").astype(jnp.float32)
    d_resid_part, gain_attn_local = norm_back(resid, scale_one, gain_attn, d_normed1)
    input_grad = (d_hidden1 + d_resid_part).astype(jnp.bfloat16)
    gate_grad, up_grad, down_grad = (
        lax.psum_scatter(
            gate_local.astype(jnp.bfloat16), "dp", scatter_dimension=1, tiled=True
        ).astype(jnp.float32),
        lax.psum_scatter(
            up_local.astype(jnp.bfloat16), "dp", scatter_dimension=1, tiled=True
        ).astype(jnp.float32),
        lax.psum_scatter(
            down_local.astype(jnp.bfloat16), "dp", scatter_dimension=2, tiled=True
        ).astype(jnp.float32),
    )
    query_grad, key_grad, value_grad, out_grad, router_grad, gain_attn_grad, gain_moe_grad = (
        *side_by_side(
            (
                query_local.astype(jnp.bfloat16),
                key_local.astype(jnp.bfloat16),
                value_local.astype(jnp.bfloat16),
            ),
            ("dp", "expert"),
            0,
            1,
        ),
        sum_at_owner(out_local.astype(jnp.bfloat16), ("dp", "expert"), 1),
        *sent_together(
            (
                router_local.astype(jnp.bfloat16),
                gain_attn_local.astype(jnp.bfloat16),
                gain_moe_local.astype(jnp.bfloat16),
            ),
            ("dp", "expert"),
            0,
            1,
        ),
    )
    return (
        output,
        input_grad,
        gain_attn_grad,
        query_grad,
        key_grad,
        value_grad,
        out_grad,
        gain_moe_grad,
        router_grad,
        gate_grad,
        up_grad,
        down_grad,
    )


GATHER_ROWS = 4096
MESH = pl.DeviceIdType.MESH
VMEM = pl.BlockSpec(memory_space=pltpu.VMEM)
ANY = pl.BlockSpec(memory_space=pl.ANY)
EXTRA = 128
VMEM_LIMIT = 60 * 2**20
F32, BF16 = jnp.float32, jnp.bfloat16


def dot(a, b):
    return jnp.dot(a, b, preferred_element_type=F32)


def dot_nt(a, b):
    return lax.dot_general(a, b, (((1,), (1,)), ((), ())), preferred_element_type=F32)


def dot_tn(a, b):
    return lax.dot_general(a, b, (((0,), (0,)), ((), ())), preferred_element_type=F32)


def ds(index, size):
    return pl.ds(pl.multiple_of(index * size, size), size)


class Peers:
    def __init__(self, dp, tp, send_sem, recv_sem):
        self.z, self.c, self.t = (lax.axis_index(a) for a in ("dp", "expert", "tensor"))
        self.dp, self.tp = dp, tp
        self.send_sem, self.recv_sem = send_sem, recv_sem
        self.used = 0
        self.open = []

    def tensor(self, k):
        return (self.z, self.c, lax.rem(self.t + k, self.tp))

    def plane(self, k):
        return (lax.rem(self.z + k, self.dp), self.c, self.t)

    def partner(self):
        return (self.z, 1 - self.c, self.t)

    def greet(self):
        barrier = pltpu.get_barrier_semaphore()
        everyone = [self.tensor(k) for k in range(1, self.tp)]
        everyone += [self.plane(k) for k in range(1, self.dp)] + [self.partner()]
        for peer in everyone:
            pl.semaphore_signal(barrier, inc=1, device_id=peer, device_id_type=MESH)
        pl.semaphore_wait(barrier, len(everyone))

    def number(self, count):
        first = self.used
        self.used += count
        return first

    def make(self, src, dst, number, device):
        return pltpu.make_async_remote_copy(
            src_ref=src,
            dst_ref=dst,
            send_sem=self.send_sem.at[number],
            recv_sem=self.recv_sem.at[number],
            device_id=device,
            device_id_type=MESH,
        )

    def to(self, src, dst, device):
        copy = self.make(src, dst, self.number(1), device)
        copy.start()
        self.open.append(copy)
        return copy

    def keep(self, src, dst, sem):
        copy = pltpu.make_async_copy(src, dst, sem)
        copy.start()
        return copy

    def drain(self):
        for copy in self.open:
            copy.wait_send()


def arrived(copies):
    for copy in copies:
        copy.wait_recv()


def rotate(u, rope_ref, sign):
    width = u.shape[1]
    tiles = []
    for at in range(0, width, 128):
        v = u[:, at : at + 128]
        side = pltpu.roll(v, 96, 1) * rope_ref[1] + pltpu.roll(v, 32, 1) * rope_ref[2]
        tiles.append(v * rope_ref[0] + sign * side)
    return tiles[0] if len(tiles) == 1 else jnp.concatenate(tiles, axis=1)


def inverse_rms(u):
    return lax.rsqrt(jnp.mean(u * u, axis=-1, keepdims=True) + EPSILON)


def causal(length):
    row = lax.broadcasted_iota(jnp.int32, (length, length), 0)
    col = lax.broadcasted_iota(jnp.int32, (length, length), 1)
    return col <= row


def forward_kernel(
    dp,
    tp,
    tok_ref,
    cot_ref,
    routes_ref,
    ga_ref,
    gm_ref,
    wq_ref,
    wk_ref,
    wv_ref,
    wo_ref,
    rope_ref,
    x_ref,
    g_ref,
    gz_ref,
    h1_ref,
    n1_ref,
    qkv_ref,
    att_ref,
    lse_ref,
    part_buf,
    rs_buf,
    send_sem,
    recv_sem,
):
    net = Peers(dp, tp, send_sem, recv_sem)
    z, c, t = net.z, net.c, net.t
    length, model = tok_ref.shape
    own = length // tp
    q_width, kv_width = wq_ref.shape[1], wk_ref.shape[1]
    group = q_width // kv_width
    net.greet()
    seq_rows = ds(c, length)
    got_g = [net.to(cot_ref, g_ref.at[seq_rows], net.partner())]
    for k in range(1, dp):
        got_g.append(net.to(cot_ref.at[ds(t, own)], gz_ref.at[dp - 1 - k], net.plane(k)))
    g_ref[seq_rows, :] = cot_ref[...]

    resid = tok_ref[...].astype(F32)
    n1 = (resid * inverse_rms(resid) * ga_ref[...]).astype(BF16)
    n1_ref[...] = n1
    qkv_ref[:, :q_width] = rotate(dot(n1, wq_ref[...]), rope_ref, 1.0).astype(BF16)
    qkv_ref[:, q_width : q_width + kv_width] = rotate(dot(n1, wk_ref[...]), rope_ref, 1.0).astype(BF16)
    qkv_ref[:, q_width + kv_width :] = dot(n1, wv_ref[...]).astype(BF16)

    seen = causal(length)
    lane = lax.broadcasted_iota(jnp.int32, lse_ref.shape, 1)
    lse_all = jnp.zeros(lse_ref.shape, F32)
    scale = HEAD_SIZE ** (-0.5)
    for h in range(q_width // HEAD_SIZE):
        kv = h // group
        at_k = q_width + kv * HEAD_SIZE
        at_v = q_width + kv_width + kv * HEAD_SIZE
        q = qkv_ref[:, h * HEAD_SIZE : (h + 1) * HEAD_SIZE]
        key = qkv_ref[:, at_k : at_k + HEAD_SIZE]
        val = qkv_ref[:, at_v : at_v + HEAD_SIZE]
        s = jnp.where(seen, dot_nt(q, key) * scale, -1e30)
        top = jnp.max(s, axis=-1, keepdims=True)
        lse = top + jnp.log(jnp.sum(jnp.exp(s - top), axis=-1, keepdims=True))
        prob = jnp.exp(s - lse).astype(BF16)
        att_ref[:, h * HEAD_SIZE : (h + 1) * HEAD_SIZE] = dot(prob, val).astype(BF16)
        lse_all = jnp.where(lane == h, lse, lse_all)
    lse_ref[...] = lse_all
    part_buf[...] = dot(att_ref[...], wo_ref[...]).astype(BF16)

    got = []
    for k in range(1, tp):
        block = part_buf.at[ds(lax.rem(t + k, tp), own)]
        got.append(net.to(block, rs_buf.at[k - 1], net.tensor(k)))
    total = tok_ref[ds(t, own), :].astype(F32) + part_buf[ds(t, own), :].astype(F32)
    picked = routes_ref[ds(t, own), :]
    ids = lax.broadcasted_iota(jnp.int32, (own, EXTRA), 1)
    chosen = picked[:, 0:1] == ids
    for j in range(1, picked.shape[1]):
        chosen = chosen | (picked[:, j : j + 1] == ids)
    arrived(got)
    for k in range(1, tp):
        total = total + rs_buf[k - 1].astype(F32)
    h1_ref[...] = total
    n2 = (total * inverse_rms(total) * gm_ref[...]).astype(BF16)
    mine = ds(c * tp + t, own)
    x_ref[mine, :model] = n2
    x_ref[mine, model:] = jnp.where(chosen, 1.0, 0.0).astype(BF16)
    got = [net.to(x_ref.at[mine], x_ref.at[mine], net.tensor(k)) for k in range(1, tp)]
    arrived(got)
    got = [net.to(x_ref.at[seq_rows], x_ref.at[seq_rows], net.partner())]
    arrived(got_g + got)
    net.drain()


def forward(dp, tp, tokens, cotangent, routes, ga, gm, wq, wk, wv, wo, rope):
    length, model = tokens.shape
    own, wide = length // tp, model + EXTRA
    widths = wq.shape[1] + wk.shape[1] + wv.shape[1]
    copies = 2 + (dp - 1) + 2 * (tp - 1)
    shapes = [
        ((2 * length, wide), BF16),
        ((2 * length, model), BF16),
        ((dp - 1, own, model), BF16),
        ((own, model), F32),
        ((length, model), BF16),
        ((length, widths), BF16),
        ((length, wq.shape[1]), BF16),
        ((length, 128), F32),
    ]
    return pl.pallas_call(
        functools.partial(forward_kernel, dp, tp),
        out_shape=[jax.ShapeDtypeStruct(*s) for s in shapes],
        in_specs=[VMEM] * 10,
        out_specs=[VMEM] * len(shapes),
        scratch_shapes=[
            pltpu.VMEM((length, model), BF16),
            pltpu.VMEM((tp - 1, own, model), BF16),
            pltpu.SemaphoreType.DMA((copies,)),
            pltpu.SemaphoreType.DMA((copies,)),
        ],
        compiler_params=pltpu.CompilerParams(
            collective_id=0, has_side_effects=True, vmem_limit_bytes=VMEM_LIMIT
        ),
        name="forward",
    )(tokens, cotangent, routes, ga, gm, wq, wk, wv, wo, rope)


def gates_of(x_ref, wr_ref, model):
    logits = dot(x_ref[:, :model], wr_ref[...])
    chosen = x_ref[:, model:].astype(F32) > 0.5
    top = jnp.max(jnp.where(chosen, logits, -jnp.inf), axis=1, keepdims=True)
    weight = jnp.where(chosen, jnp.exp(jnp.where(chosen, logits - top, 0.0)), 0.0)
    return weight / jnp.sum(weight, axis=1, keepdims=True)


def store_split(gates, split_ref):
    high = gates.astype(BF16)
    split_ref[:, :EXTRA] = high
    split_ref[:, EXTRA:] = (gates - high.astype(F32)).astype(BF16)


def pair_of_gates(split, first, width):
    k_pos = lax.broadcasted_iota(jnp.int32, (2 * EXTRA, 2 * width), 0)
    l_pos = lax.broadcasted_iota(jnp.int32, (2 * EXTRA, 2 * width), 1)
    pick = jnp.where(k_pos % EXTRA == first + l_pos // width, 1.0, 0.0).astype(BF16)
    return dot(split, pick)


def swiglu(both, dh, gate):
    width = dh.shape[1]
    gate_pre, up_pre = both[:, :width], both[:, width:]
    sig = jax.nn.sigmoid(gate_pre)
    act = gate_pre * sig
    hid = act * up_pre
    d_hid = dh * gate
    d_gate = d_hid * up_pre * sig * (1.0 + gate_pre * (1.0 - sig))
    return hid, (hid * gate).astype(BF16), d_gate.astype(BF16), (d_hid * act).astype(BF16)


def plane_kernel(
    dp,
    tp,
    x_ref,
    g_ref,
    gz_ref,
    n1_ref,
    wr_ref,
    wg_ref,
    wu_ref,
    wd_ref,
    xr_ref,
    gr_ref,
    n1c_ref,
    moe_ref,
    back_ref,
    dgate_ref,
    gates_ref,
    ghid_ref,
    dgp_ref,
    dup_ref,
    split,
    moe_acc,
    back_acc,
    send_sem,
    recv_sem,
    keep_sem,
):
    step, last = pl.program_id(0), pl.num_programs(0) - 1
    net = Peers(dp, tp, send_sem, recv_sem)
    z, c, t = net.z, net.c, net.t
    rows, model = g_ref.shape
    length = rows // 2
    own = length // tp
    width = wg_ref.shape[2]
    part = model // dp
    others = range(1, dp)
    sides = range(1, tp)

    def block(plane, core, tensor):
        return ds((plane * 2 + core) * tp + tensor, own)

    def columns(index):
        return pl.ds(pl.multiple_of(index * part, 128), part)

    mine = ds(c * tp + t, own)
    x_z = [
        net.make(x_ref.at[mine], xr_ref.at[block(dp - k, c, t)], net.number(1), net.plane(k))
        for k in others
    ]
    n1_z = [
        net.make(
            n1_ref.at[:, columns(lax.rem(z + k, dp))],
            n1c_ref.at[ds((dp - k) * 2 + c, length)],
            net.number(1),
            net.plane(k),
        )
        for k in others
    ]
    n1_own = net.make(
        n1_ref.at[:, columns(z)], n1c_ref.at[ds(c, length)], net.number(1), net.partner()
    )
    g_t = [
        net.make(gz_ref.at[p - 1], gr_ref.at[block(p, c, t)], net.number(1), net.tensor(k))
        for p in others
        for k in sides
    ]
    x_t = [
        net.make(
            xr_ref.at[block(p, c, t)], xr_ref.at[block(p, c, t)], net.number(1), net.tensor(k)
        )
        for p in others
        for k in sides
    ]

    def over(ref):
        return [
            net.make(
                ref.at[ds(p * 2 + c, length)],
                ref.at[ds(p * 2 + c, length)],
                net.number(1),
                net.partner(),
            )
            for p in others
        ]

    g_c, x_c, n1_c = over(gr_ref), over(xr_ref), over(n1c_ref)
    kept = [
        pltpu.make_async_copy(x_ref, xr_ref.at[pl.ds(0, rows)], keep_sem.at[0]),
        pltpu.make_async_copy(g_ref, gr_ref.at[pl.ds(0, rows)], keep_sem.at[1]),
        pltpu.make_async_copy(
            n1_ref.at[:, columns(z)], n1c_ref.at[ds(c, length)], keep_sem.at[2]
        ),
    ] + [
        pltpu.make_async_copy(gz_ref.at[p - 1], gr_ref.at[block(p, c, t)], keep_sem.at[2 + p])
        for p in others
    ]

    def start(copies):
        for copy in copies:
            copy.start()

    @pl.when(step == 0)
    def _():
        net.greet()
        start(x_z + g_t + n1_z + [n1_own])
        start(kept)
        moe_acc[...] = jnp.zeros_like(moe_acc)
        back_acc[...] = jnp.zeros_like(back_acc)
        dgate_ref[...] = jnp.zeros_like(dgate_ref)
        gates = gates_of(x_ref, wr_ref, model)
        gates_ref[...] = gates
        store_split(gates, split)

    @pl.when(step == 4)
    def _():
        arrived(x_z)
        start(x_t)

    @pl.when(step == 6)
    def _():
        arrived(g_t)
        for copy in kept:
            copy.wait()
        start(g_c)

    @pl.when(step == 8)
    def _():
        arrived(n1_z)
        start(n1_c)

    first = c * (2 * pl.num_programs(0)) + 2 * step
    gate_pair = pair_of_gates(split[...], first, width)
    wd_pair = wd_ref[...].reshape(2 * width, model)
    dh_pair = dot_nt(g_ref[...], wd_pair)
    lane = lax.broadcasted_iota(jnp.int32, dgate_ref.shape, 1)
    for k in range(2):
        lanes = slice(k * width, (k + 1) * width)
        w_both = jnp.concatenate([wg_ref[k], wu_ref[k]], axis=1)
        both = dot(x_ref[:, :model], w_both)
        dh = dh_pair[:, lanes]
        hid, ghid, dgp, dup = swiglu(both, dh, gate_pair[:, lanes])
        ghid_ref[:, lanes] = ghid
        dgp_ref[:, lanes] = dgp
        dup_ref[:, lanes] = dup
        row_sum = jnp.sum(hid * dh, axis=1, keepdims=True)
        dgate_ref[...] += jnp.where(lane == first + k, row_sum, 0.0)
        back_acc[...] += dot_nt(jnp.concatenate([dgp, dup], axis=1), w_both)
    moe_acc[...] += dot(ghid_ref[...], wd_pair)

    @pl.when(step == last)
    def _():
        moe_ref[...] = moe_acc[...].astype(BF16)
        back_ref[...] = back_acc[...].astype(BF16)
        arrived(x_t)
        start(x_c)
        arrived(g_c + n1_c + [n1_own])
        arrived(x_c)
        for copy in x_z + g_t + n1_z + [n1_own] + x_t + g_c + n1_c + x_c:
            copy.wait_send()


def plane_experts(dp, tp, x, g, gz, n1, wr, w_gate, w_up, w_down):
    rows, model = g.shape
    length = rows // 2
    count, _, width = w_gate.shape
    all_rows = rows * dp
    others, sides = dp - 1, tp - 1
    copies = 2 * others + 1 + 2 * others * sides + 3 * others

    def whole(a):
        shape = a.shape
        return pl.BlockSpec(shape, lambda i: (0,) * len(shape), pipeline_mode=pl.Buffered(1))

    by_pair = lambda shape: pl.BlockSpec((2,) + shape, lambda i: (i, 0, 0))
    saved = pl.BlockSpec((rows, 2 * width), lambda i: (0, i))
    shapes = [
        ((all_rows, x.shape[1]), BF16),
        ((all_rows, model), BF16),
        ((all_rows, model // dp), BF16),
        ((rows, model), BF16),
        ((rows, model), BF16),
        ((rows, EXTRA), F32),
        ((rows, EXTRA), F32),
        ((rows, count * width), BF16),
        ((rows, count * width), BF16),
        ((rows, count * width), BF16),
    ]
    shapes = [jax.ShapeDtypeStruct(*s) for s in shapes]
    return pl.pallas_call(
        functools.partial(plane_kernel, dp, tp),
        grid=(count // 2,),
        out_shape=shapes,
        in_specs=[whole(x), whole(g), whole(gz), whole(n1), whole(wr)]
        + [by_pair((model, width)), by_pair((model, width)), by_pair((width, model))],
        out_specs=[ANY, ANY, ANY] + [whole(s) for s in shapes[3:7]] + [saved] * 3,
        scratch_shapes=[
            pltpu.VMEM((rows, 2 * EXTRA), BF16),
            pltpu.VMEM((rows, model), F32),
            pltpu.VMEM((rows, model), F32),
            pltpu.SemaphoreType.DMA((copies,)),
            pltpu.SemaphoreType.DMA((copies,)),
            pltpu.SemaphoreType.DMA((3 + others,)),
        ],
        compiler_params=pltpu.CompilerParams(
            collective_id=1, has_side_effects=True, vmem_limit_bytes=VMEM_LIMIT
        ),
        name="plane_experts",
    )(x, g, gz, n1, wr, w_gate, w_up, w_down)


def backward_kernel(
    dp,
    tp,
    back_ref,
    moe_ref,
    dgate_ref,
    gates_ref,
    h1_ref,
    tok_ref,
    cot_ref,
    ga_ref,
    gm_ref,
    wr_ref,
    wq_ref,
    wk_ref,
    wv_ref,
    wo_ref,
    qkv_ref,
    att_ref,
    lse_ref,
    rope_ref,
    out_ref,
    in_ref,
    att_all,
    da_cols,
    d_all,
    gains_ref,
    pair_b,
    pair_m,
    pair_d,
    sum_b,
    sum_m,
    sum_d,
    rs_b,
    rs_m,
    rs_d,
    da_buf,
    dl_buf,
    d_buf,
    do_buf,
    part_buf,
    rs_3,
    gain_buf,
    gain_t,
    gain_z,
    gain_zs,
    gain_c,
    send_sem,
    recv_sem,
    keep_sem,
):
    net = Peers(dp, tp, send_sem, recv_sem)
    z, c, t = net.z, net.c, net.t
    length, model = tok_ref.shape
    own = length // tp
    part = model // dp
    q_width, kv_width = wq_ref.shape[1], wk_ref.shape[1]
    group = q_width // kv_width
    others, sides = range(1, dp), range(1, tp)
    mine = ds(t, own)
    here, there = ds(c, length), ds(1 - c, length)

    def columns(index):
        return pl.ds(pl.multiple_of(index * part, 128), part)

    def to_sides(ref, into):
        return [
            net.to(ref.at[ds(lax.rem(t + k, tp), own)], into.at[k - 1], net.tensor(k))
            for k in sides
        ]

    def share(ref):
        return [net.to(ref.at[mine], ref.at[mine], net.tensor(k)) for k in sides]

    def on_to_partner(ref):
        rows = [ds(p * 2 + c, length) for p in others]
        return [net.to(ref.at[r], ref.at[r], net.partner()) for r in rows]

    net.greet()
    got_b = [
        net.to(back_ref.at[there], pair_b, net.partner()),
        net.to(dgate_ref.at[there], pair_d, net.partner()),
    ]
    got_m = [net.to(moe_ref.at[there], pair_m, net.partner())]
    att_z = [net.to(att_ref, att_all.at[ds((dp - k) * 2 + c, length)], net.plane(k)) for k in others]
    att_own = net.to(att_ref, att_all.at[here], net.partner())
    kept = [net.keep(att_ref, att_all.at[here], keep_sem.at[0])]
    arrived(got_b)
    sum_b[...] = (back_ref[here, :].astype(F32) + pair_b[...].astype(F32)).astype(BF16)
    sum_d[...] = dgate_ref[here, :] + pair_d[...]
    got_b = to_sides(sum_b, rs_b) + to_sides(sum_d, rs_d)
    arrived(got_m)
    sum_m[...] = (moe_ref[here, :].astype(F32) + pair_m[...].astype(F32)).astype(BF16)
    arrived(got_b)
    d_n2 = sum_b[mine, :].astype(F32)
    dgate = sum_d[mine, :]
    for k in sides:
        d_n2 = d_n2 + rs_b[k - 1].astype(F32)
        dgate = dgate + rs_d[k - 1]
    gates = gates_ref[ds(c * tp + t, own), :]
    d_logits = gates * (dgate - jnp.sum(gates * dgate, axis=1, keepdims=True))
    dl_buf[mine, :] = d_logits.astype(BF16)
    d_n2 = d_n2 + dot_nt(d_logits.astype(BF16), wr_ref[...])
    h1 = h1_ref[...]
    r2 = inverse_rms(h1)
    weighted = d_n2 * gm_ref[...]
    inner = jnp.mean(weighted * h1, axis=-1, keepdims=True)
    gain_buf[...] = jnp.zeros_like(gain_buf)
    gain_buf[1:2, :] = jnp.sum(d_n2 * h1 * r2, axis=0, keepdims=True)
    d_h1 = cot_ref[mine, :].astype(F32) + (r2 * weighted - h1 * (r2 * r2 * r2) * inner)
    da_buf[mine, :] = d_h1.astype(BF16)
    got_da = share(da_buf) + share(dl_buf)
    got_m = to_sides(sum_m, rs_m)
    arrived(att_z)
    att_c = on_to_partner(att_all)
    arrived(got_da)
    d_buf[:, q_width + 2 * kv_width :] = dl_buf[...]
    da_z = [
        net.to(
            da_buf.at[:, columns(lax.rem(z + k, dp))],
            da_cols.at[ds((dp - k) * 2 + c, length)],
            net.plane(k),
        )
        for k in others
    ]
    da_own = net.to(da_buf.at[:, columns(z)], da_cols.at[here], net.partner())
    kept.append(net.keep(da_buf.at[:, columns(z)], da_cols.at[here], keep_sem.at[1]))
    do_buf[...] = dot_nt(da_buf[...], wo_ref[...]).astype(BF16)

    arrived(got_m)
    total = h1 + sum_m[mine, :].astype(F32)
    for k in sides:
        total = total + rs_m[k - 1].astype(F32)
    out_ref[mine, :] = total.astype(BF16)
    got_out = share(out_ref)

    seen = causal(length)
    scale = HEAD_SIZE ** (-0.5)
    d_key, d_val, d_query = [], [], []
    for kv in range(kv_width // HEAD_SIZE):
        at_k = q_width + kv * HEAD_SIZE
        at_v = q_width + kv_width + kv * HEAD_SIZE
        key = qkv_ref[:, at_k : at_k + HEAD_SIZE]
        val = qkv_ref[:, at_v : at_v + HEAD_SIZE]
        dk = jnp.zeros((length, HEAD_SIZE), F32)
        dv = jnp.zeros((length, HEAD_SIZE), F32)
        for h in range(kv * group, (kv + 1) * group):
            at = slice(h * HEAD_SIZE, (h + 1) * HEAD_SIZE)
            q = qkv_ref[:, at]
            d_out = do_buf[:, at]
            s = jnp.where(seen, dot_nt(q, key) * scale, -1e30)
            prob = jnp.exp(s - lse_ref[:, h : h + 1])
            delta = jnp.sum(d_out.astype(F32) * att_ref[:, at].astype(F32), axis=-1, keepdims=True)
            d_s = (prob * (dot_nt(d_out, val) - delta)).astype(BF16)
            d_query.append(dot(d_s, key) * scale)
            dk = dk + dot_tn(d_s, q)
            dv = dv + dot_tn(prob.astype(BF16), d_out)
        d_key.append(dk * scale)
        d_val.append(dv)
    d_buf[:, :q_width] = rotate(jnp.concatenate(d_query, axis=1), rope_ref, -1.0).astype(BF16)
    d_buf[:, q_width : q_width + kv_width] = rotate(
        jnp.concatenate(d_key, axis=1), rope_ref, -1.0
    ).astype(BF16)
    d_buf[:, q_width + kv_width : q_width + 2 * kv_width] = jnp.concatenate(d_val, axis=1).astype(BF16)
    d_z = [net.to(d_buf, d_all.at[ds((dp - k) * 2 + c, length)], net.plane(k)) for k in others]
    d_own = net.to(d_buf, d_all.at[here], net.partner())
    kept.append(net.keep(d_buf, d_all.at[here], keep_sem.at[2]))
    part_n1 = dot_nt(d_buf[:, :q_width], wq_ref[...])
    part_n1 = part_n1 + dot_nt(d_buf[:, q_width : q_width + kv_width], wk_ref[...])
    part_n1 = part_n1 + dot_nt(
        d_buf[:, q_width + kv_width : q_width + 2 * kv_width], wv_ref[...]
    )
    part_buf[...] = part_n1.astype(BF16)
    got_3 = to_sides(part_buf, rs_3)
    arrived(da_z)
    da_c = on_to_partner(da_cols)
    arrived(got_3)
    d_n1 = part_buf[mine, :].astype(F32)
    for k in sides:
        d_n1 = d_n1 + rs_3[k - 1].astype(F32)
    resid = tok_ref[mine, :].astype(F32)
    r1 = inverse_rms(resid)
    weighted = d_n1 * ga_ref[...]
    inner = jnp.mean(weighted * resid, axis=-1, keepdims=True)
    gain_buf[0:1, :] = jnp.sum(d_n1 * resid * r1, axis=0, keepdims=True)
    d_x = d_h1 + (r1 * weighted - resid * (r1 * r1 * r1) * inner)
    in_ref[mine, :] = d_x.astype(BF16)
    got_gain = [net.to(gain_buf, gain_t.at[k - 1], net.tensor(k)) for k in sides]
    got_in = share(in_ref)
    arrived(got_gain)
    gain = gain_buf[...]
    for k in sides:
        gain = gain + gain_t[k - 1]
    gain_zs[...] = gain
    got_gain = [
        net.to(gain_zs.at[:, columns(lax.rem(z + k, dp))], gain_z.at[k - 1], net.plane(k))
        for k in others
    ]
    arrived(got_gain)
    gain = gain_zs[:, columns(z)]
    for k in others:
        gain = gain + gain_z[k - 1]
    gain_c[0] = gain
    got_gain = net.to(gain_c.at[0], gain_c.at[1], net.partner())
    arrived(d_z)
    d_c = on_to_partner(d_all)
    arrived([got_gain])
    gains_ref[...] = gain + gain_c[1]
    arrived(got_out + got_in + [att_own, da_own, d_own] + att_c + da_c + d_c)
    for copy in kept:
        copy.wait()
    net.drain()


def backward(dp, tp, *arrays):
    back, _, _, _, _, tokens, _, _, _, _, wq, wk, wv = arrays[:13]
    rows, model = back.shape
    length = tokens.shape[0]
    own, part = length // tp, model // dp
    q_width = wq.shape[1]
    wide = q_width + wk.shape[1] + wv.shape[1] + EXTRA
    others, sides = dp - 1, tp - 1
    copies = 3 + 3 * (2 * others + 1) + 2 * sides + 2 * sides + 4 * sides + sides + others + 1
    shapes = [
        ((length, model), BF16),
        ((length, model), BF16),
        ((rows * dp, q_width), BF16),
        ((rows * dp, part), BF16),
        ((rows * dp, wide), BF16),
        ((8, part), F32),
    ]
    return pl.pallas_call(
        functools.partial(backward_kernel, dp, tp),
        out_shape=[jax.ShapeDtypeStruct(*s) for s in shapes],
        in_specs=[VMEM] * len(arrays),
        out_specs=[VMEM, VMEM, ANY, ANY, ANY, VMEM],
        scratch_shapes=[
            pltpu.VMEM((length, model), BF16),
            pltpu.VMEM((length, model), BF16),
            pltpu.VMEM((length, EXTRA), F32),
            pltpu.VMEM((length, model), BF16),
            pltpu.VMEM((length, model), BF16),
            pltpu.VMEM((length, EXTRA), F32),
            pltpu.VMEM((sides, own, model), BF16),
            pltpu.VMEM((sides, own, model), BF16),
            pltpu.VMEM((sides, own, EXTRA), F32),
            pltpu.VMEM((length, model), BF16),
            pltpu.VMEM((length, EXTRA), BF16),
            pltpu.VMEM((length, wide), BF16),
            pltpu.VMEM((length, q_width), BF16),
            pltpu.VMEM((length, model), BF16),
            pltpu.VMEM((sides, own, model), BF16),
            pltpu.VMEM((8, model), F32),
            pltpu.VMEM((sides, 8, model), F32),
            pltpu.VMEM((others, 8, part), F32),
            pltpu.VMEM((8, model), F32),
            pltpu.VMEM((2, 8, part), F32),
            pltpu.SemaphoreType.DMA((copies,)),
            pltpu.SemaphoreType.DMA((copies,)),
            pltpu.SemaphoreType.DMA((3,)),
        ],
        compiler_params=pltpu.CompilerParams(
            collective_id=2, has_side_effects=True, vmem_limit_bytes=VMEM_LIMIT
        ),
        name="backward",
    )(*arrays)


def weights_kernel(
    place_ref,
    x_ref,
    g_ref,
    wr_ref,
    att_ref,
    da_ref,
    n1_ref,
    d_ref,
    ghid_ref,
    dgp_ref,
    dup_ref,
    wg_ref,
    wu_ref,
    wd_ref,
    gate_grad_ref,
    up_grad_ref,
    down_grad_ref,
    query_ref,
    key_ref,
    value_ref,
    out_grad_ref,
    router_ref,
    split,
    xt_buf,
    gt_buf,
    hid_buf,
    dgate_buf,
    dup_buf,
    side_buf,
):
    step = pl.program_id(0)
    z, c = place_ref[0], place_ref[1]
    rows, model = g_ref.shape
    width = wg_ref.shape[2]
    part = xt_buf.shape[0]
    plane_rows = ghid_ref.shape[0]
    rest = slice(plane_rows, rows)

    @pl.when(step == 0)
    def _():
        store_split(gates_of(x_ref, wr_ref, model), split)
        cols = pl.ds(pl.multiple_of(z * part, 128), part)
        xt_buf[...] = x_ref[:, cols].T
        gt_buf[...] = g_ref[:, cols].T
        q_width, kv_width = query_ref.shape[1], key_ref.shape[1]
        half = query_ref.shape[0]
        at = pl.ds(pl.multiple_of(c * half, 8), half)
        side_buf[:, : d_ref.shape[1] - EXTRA] = dot_tn(n1_ref[...], d_ref[:, : d_ref.shape[1] - EXTRA])
        side_buf[:, d_ref.shape[1] - EXTRA :] = dot(xt_buf[...], d_ref[:, d_ref.shape[1] - EXTRA :])
        query_ref[...] = side_buf[at, :q_width]
        key_ref[...] = side_buf[at, q_width : q_width + kv_width]
        value_ref[...] = side_buf[at, q_width + kv_width : q_width + 2 * kv_width]
        router_ref[...] = side_buf[at, d_ref.shape[1] - EXTRA :][:, : router_ref.shape[1]]
        out_all = dot_tn(att_ref[...], da_ref[...])
        out_grad_ref[...] = jnp.where(c == 0, out_all[:, :half], out_all[:, half:])

    first = c * (2 * pl.num_programs(0)) + 2 * step
    wd_pair = wd_ref[...].reshape(2 * width, model)
    gate_pair = pair_of_gates(split[rest, :], first, width)
    dh_pair = dot_nt(g_ref[rest, :], wd_pair)
    hid_buf[:plane_rows, :] = ghid_ref[...]
    dgate_buf[:plane_rows, :] = dgp_ref[...]
    dup_buf[:plane_rows, :] = dup_ref[...]
    for k in range(2):
        lanes = slice(k * width, (k + 1) * width)
        both = dot(x_ref[rest, :model], jnp.concatenate([wg_ref[k], wu_ref[k]], axis=1))
        _, ghid, dgp, dup = swiglu(both, dh_pair[:, lanes], gate_pair[:, lanes])
        hid_buf[rest, lanes] = ghid
        dgate_buf[rest, lanes] = dgp
        dup_buf[rest, lanes] = dup
    gate_both = dot(xt_buf[...], dgate_buf[...])
    up_both = dot(xt_buf[...], dup_buf[...])
    down_both = dot(gt_buf[...], hid_buf[...]).T
    for k in range(2):
        lanes = slice(k * width, (k + 1) * width)
        gate_grad_ref[k] = gate_both[:, lanes]
        up_grad_ref[k] = up_both[:, lanes]
        down_grad_ref[k] = down_both[lanes, :]


def weight_grads(place, x, g, wr, att, da, n1, d, ghid, dgp, dup, w_gate, w_up, w_down, kv_width, experts):
    rows, model = g.shape
    count, _, width = w_gate.shape
    part = n1.shape[1]
    q_width, half = att.shape[1], part // 2

    def whole(a):
        shape = a.shape
        return pl.BlockSpec(shape, lambda i, p: (0,) * len(shape), pipeline_mode=pl.Buffered(1))

    by_pair = lambda shape: pl.BlockSpec((2,) + shape, lambda i, p: (i, 0, 0))
    saved = pl.BlockSpec((ghid.shape[0], 2 * width), lambda i, p: (0, i))
    shapes = [
        (count, part, width),
        (count, part, width),
        (count, width, part),
        (half, q_width),
        (half, kv_width),
        (half, kv_width),
        (q_width, half),
        (half, experts),
    ]
    shapes = [jax.ShapeDtypeStruct(s, F32) for s in shapes]
    return pl.pallas_call(
        weights_kernel,
        grid_spec=pltpu.PrefetchScalarGridSpec(
            num_scalar_prefetch=1,
            grid=(count // 2,),
            in_specs=[whole(a) for a in (x, g, wr, att, da, n1, d)]
            + [saved] * 3
            + [by_pair((model, width)), by_pair((model, width)), by_pair((width, model))],
            out_specs=[by_pair((part, width)), by_pair((part, width)), by_pair((width, part))]
            + [whole(s) for s in shapes[3:]],
            scratch_shapes=[
                pltpu.VMEM((rows, 2 * EXTRA), BF16),
                pltpu.VMEM((part, rows), BF16),
                pltpu.VMEM((part, rows), BF16),
                pltpu.VMEM((rows, 2 * width), BF16),
                pltpu.VMEM((rows, 2 * width), BF16),
                pltpu.VMEM((rows, 2 * width), BF16),
                pltpu.VMEM((part, d.shape[1]), F32),
            ],
        ),
        out_shape=shapes,
        compiler_params=pltpu.CompilerParams(vmem_limit_bytes=VMEM_LIMIT),
        name="weight_grads",
    )(place, x, g, wr, att, da, n1, d, ghid, dgp, dup, w_gate, w_up, w_down)


def rope_rows(length):
    positions = jnp.arange(length, dtype=F32)
    cos, sin = rope_tables(positions, HEAD_SIZE)
    none = jnp.zeros_like(sin)
    double = lambda first, second: jnp.concatenate([first, second, first, second], axis=1)
    return jnp.stack([double(cos, cos), double(-sin, none), double(none, sin)])


def gather_plan(
    tokens,
    gain_attn,
    w_query,
    key_projection,
    value_projection,
    w_out,
    gain_moe,
    w_router,
    w_gate,
    w_up,
    w_down,
    routes,
    cotangent,
):
    dp, tp = lax.axis_size("dp"), lax.axis_size("tensor")
    experts = w_router.shape[1]
    half = tokens.shape[1] // dp // 2
    rope = rope_rows(tokens.shape[0])
    ga, gm = gain_attn[None, :], gain_moe[None, :]
    wr = jnp.pad(w_router, ((0, 0), (0, EXTRA - experts)))
    heads = (w_query, key_projection, value_projection, w_out)
    x, g, gz, h1, n1, qkv, att, lse = forward(
        dp, tp, tokens, cotangent, routes, ga, gm, *heads, rope
    )
    x_all, g_all, n1_cols, moe, back, dgate, gates, ghid, dgp, dup = plane_experts(
        dp, tp, x, g, gz, n1, wr, w_gate, w_up, w_down
    )
    output, input_grad, att_all, da_cols, d_all, gains = backward(
        dp, tp, back, moe, dgate, gates, h1, tokens, cotangent, ga, gm, wr, *heads, qkv, att, lse, rope
    )
    z, core = lax.axis_index("dp"), lax.axis_index("expert")
    place = jnp.stack([z, core]).astype(jnp.int32)
    gate_grad, up_grad, down_grad, query_grad, key_grad, value_grad, out_grad, router_grad = weight_grads(
        place,
        x_all,
        g_all,
        wr,
        att_all,
        da_cols,
        n1_cols,
        d_all,
        ghid,
        dgp,
        dup,
        w_gate,
        w_up,
        w_down,
        key_projection.shape[1],
        experts,
    )
    gains = lax.dynamic_slice_in_dim(gains, core * half, half, axis=1)
    return (
        output,
        input_grad,
        gains[0],
        query_grad,
        key_grad,
        value_grad,
        out_grad,
        gains[1],
        router_grad,
        gate_grad,
        up_grad,
        down_grad,
    )


def solution(mesh):
    placed = (
        P(("dp", "expert"), None),
        P(),
        P(None, "tensor"),
        P(None, "tensor"),
        P(None, "tensor"),
        P("tensor", None),
        P(),
        P(),
        P("expert", None, "tensor"),
        P("expert", None, "tensor"),
        P("expert", "tensor", None),
        P(("dp", "expert"), None),
        P(("dp", "expert"), None),
    )
    sequences = mesh.shape["dp"] * mesh.shape["expert"]
    few = sequences * SEQUENCE_LENGTH <= GATHER_ROWS
    few = few and mesh.shape["tensor"] > 1 and mesh.shape["expert"] == 2
    return jax.shard_map(
        gather_plan if few else reduce_plan,
        mesh=mesh,
        in_specs=placed,
        out_specs=(
            P(("dp", "expert"), None),
            P(("dp", "expert"), None),
            P(("dp", "expert")),
            P(("dp", "expert"), "tensor"),
            P(("dp", "expert"), "tensor"),
            P(("dp", "expert"), "tensor"),
            P("tensor", ("dp", "expert")),
            P(("dp", "expert")),
            P(("dp", "expert"), None),
            P("expert", "dp", "tensor"),
            P("expert", "dp", "tensor"),
            P("expert", "tensor", "dp"),
        ),
        check_vma=False,
    )
```

```python
import functools
import math

import jax
import jax.numpy as jnp
from jax import lax
from jax.experimental import pallas as pl
from jax.experimental.pallas import tpu as pltpu
from jax.sharding import PartitionSpec as P

HEAD_SIZE = 64
SEQUENCE_LENGTH = 256
CAP = 64


EPSILON = 1e-06
ROPE_BASE = 10000.0
BLOCK_ROWS = 512


def split_up(x, dim, count):
    dims = x.shape
    tiles = x.reshape(*dims[:dim], count, dims[dim] // count, *dims[dim + 1 :])
    return jnp.moveaxis(tiles, dim, 0)


def sum_at_owner(x, axis, dim):
    tiles = split_up(x, dim, lax.axis_size(axis))
    arrived = lax.all_to_all(tiles, axis, split_axis=0, concat_axis=0, tiled=True)
    return arrived.astype(jnp.float32).sum(axis=0)


def side_by_side(arrays, axis, dim, along):
    both = jnp.concatenate(arrays, axis=along)
    filled, at, outs = (sum_at_owner(both, axis, dim), 0, [])
    for a in arrays:
        outs.append(lax.slice_in_dim(filled, at, at + a.shape[along], axis=along))
        at += a.shape[along]
    return tuple(outs)


def sent_together(arrays, axis, dim, along):
    widths = [math.prod(a.shape[along:]) for a in arrays]
    both = jnp.concatenate(
        [a.reshape(*a.shape[:along], w) for a, w in zip(arrays, widths)], axis=along
    )
    filled = sum_at_owner(both, axis, dim)
    tiles = jnp.split(filled, [sum(widths[:k]) for k in range(1, len(widths))], axis=along)
    return tuple(
        (b.reshape(*filled.shape[:along], *a.shape[along:]) for a, b in zip(arrays, tiles))
    )


def rms_scale(hidden):
    return lax.rsqrt(jnp.mean(hidden * hidden, axis=-1, keepdims=True) + EPSILON)


def norm_back(hidden, scaling, gain_vec, grad_out):
    weighted = grad_out * gain_vec
    gain_grad = jnp.sum(grad_out * hidden * scaling, axis=0)
    inner_mean = jnp.mean(weighted * hidden, axis=-1, keepdims=True)
    return (scaling * weighted - hidden * (scaling * scaling * scaling) * inner_mean, gain_grad)


def rope_tables(positions, head_dim):
    half_dim = head_dim // 2
    frequency = jnp.exp(
        jnp.arange(half_dim, dtype=jnp.float32) * (-2.0 * math.log(ROPE_BASE) / head_dim)
    )
    angles = positions[:, None] * frequency[None, :]
    return (jnp.cos(angles), jnp.sin(angles))


def apply_rotary(vectors, cosine_table, sine_component):
    half_dim = vectors.shape[-1] // 2
    first_half = vectors[..., :half_dim]
    second_half = vectors[..., half_dim:]
    cos_rows = cosine_table[:, None, :]
    sin_rows = sine_component[:, None, :]
    return jnp.concatenate(
        [
            first_half * cos_rows - second_half * sin_rows,
            first_half * sin_rows + second_half * cos_rows,
        ],
        axis=-1,
    )


def slot_table(route_ids, expert_count, capacity):
    number_of_rows, top_count = route_ids.shape
    flat_ids = route_ids.reshape(-1)
    one_hot = (flat_ids[:, None] == jnp.arange(expert_count, dtype=jnp.int32)[None, :]).astype(
        jnp.int32
    )
    earlier = jnp.cumsum(one_hot, axis=0) - one_hot
    slot_ids = jnp.sum(earlier * one_hot, axis=1)
    slot_where = flat_ids * capacity + slot_ids
    pick_ids = jnp.arange(number_of_rows * top_count, dtype=jnp.int32)
    token_of = (
        jnp.full((expert_count * capacity,), number_of_rows, jnp.int32)
        .at[slot_where]
        .set(pick_ids // top_count)
    )
    pick_of = (
        jnp.full((expert_count * capacity,), number_of_rows * top_count, jnp.int32)
        .at[slot_where]
        .set(pick_ids)
    )
    return (slot_where, token_of, pick_of)


def block_scores(query_rows, key_rows, query_group_width):
    block_len = query_rows.shape[0]
    key_count, kv_heads, head_dim = key_rows.shape
    grouped = query_rows.reshape(block_len, kv_heads, query_group_width, head_dim)
    scores = jnp.einsum(
        "qhgd,khd->hgqk", grouped, key_rows, preferred_element_type=jnp.float32
    ) * head_dim ** (-0.5)
    row_pos = jnp.arange(block_len, dtype=jnp.int32)[:, None]
    col_pos = jnp.arange(key_count, dtype=jnp.int32)[None, :]
    return (jnp.where(col_pos <= row_pos, scores, -1e30), grouped)


def sequence_forward(query_rows, key_rows, value_rows, query_group_width):
    length, kv_heads, head_dim = key_rows.shape
    block_len = min(BLOCK_ROWS, length)
    scores, grouped = block_scores(query_rows, key_rows, query_group_width)
    largest = jnp.max(scores, axis=-1, keepdims=True)
    log_total = largest + jnp.log(jnp.sum(jnp.exp(scores - largest), axis=-1, keepdims=True))
    weights = jnp.exp(scores - log_total).astype(jnp.bfloat16)
    attended = jnp.einsum("hgqk,khd->qhgd", weights, value_rows, preferred_element_type=jnp.float32)
    outputs = attended.reshape(block_len, -1, head_dim).astype(jnp.bfloat16)
    return (outputs, log_total)


def sequence_backward(
    query_rows, key_rows, value_rows, attended, log_total, d_attended, query_group_width
):
    length, kv_heads, head_dim = key_rows.shape
    block_len = min(BLOCK_ROWS, length)
    scale_factor = head_dim ** (-0.5)
    key_gradient = jnp.zeros((length, kv_heads, head_dim), jnp.float32)
    value_gradient = jnp.zeros((length, kv_heads, head_dim), jnp.float32)
    scores, grouped = block_scores(query_rows, key_rows, query_group_width)
    weights = jnp.exp(scores - log_total)
    d_grouped = d_attended.reshape(block_len, kv_heads, query_group_width, head_dim)
    o_grouped = attended.reshape(block_len, kv_heads, query_group_width, head_dim)
    delta = jnp.sum(d_grouped.astype(jnp.float32) * o_grouped.astype(jnp.float32), axis=-1)
    delta = jnp.transpose(delta, (1, 2, 0))[..., None]
    d_weights = jnp.einsum(
        "qhgd,khd->hgqk", d_grouped, value_rows, preferred_element_type=jnp.float32
    )
    d_scores = (weights * (d_weights - delta)).astype(jnp.bfloat16)
    block_query = (
        jnp.einsum("hgqk,khd->qhgd", d_scores, key_rows, preferred_element_type=jnp.float32)
        * scale_factor
    )
    query_parts = block_query.reshape(block_len, -1, head_dim)
    key_gradient = key_gradient.at[:block_len].add(
        jnp.einsum("hgqk,qhgd->khd", d_scores, grouped, preferred_element_type=jnp.float32)
        * scale_factor
    )
    value_gradient = value_gradient.at[:block_len].add(
        jnp.einsum(
            "hgqk,qhgd->khd",
            weights.astype(jnp.bfloat16),
            d_grouped,
            preferred_element_type=jnp.float32,
        )
    )
    return (query_parts, key_gradient, value_gradient)


def reduce_plan(
    tokens,
    gain_attn,
    w_query,
    key_projection,
    value_projection,
    w_out,
    gain_moe,
    w_router,
    w_gate,
    w_up,
    w_down,
    routes,
    cotangent,
):
    number_of_rows, model_width = tokens.shape
    head_dim = HEAD_SIZE
    query_heads = w_query.shape[1] // head_dim
    kv_heads = key_projection.shape[1] // head_dim
    query_group_width = query_heads // kv_heads
    expert_count = w_router.shape[1]
    local_experts = w_gate.shape[0]
    source_count = expert_count // local_experts
    capacity = CAP
    top_count = routes.shape[1]
    resid = tokens.astype(jnp.float32)
    scale_one = rms_scale(resid)
    first_normalized = (resid * scale_one * gain_attn).astype(jnp.bfloat16)
    positions = (jnp.arange(number_of_rows, dtype=jnp.int32) % SEQUENCE_LENGTH).astype(jnp.float32)
    cosine_table, sine_component = rope_tables(positions, head_dim)
    q_lin = jnp.dot(first_normalized, w_query, preferred_element_type=jnp.float32).reshape(
        number_of_rows, query_heads, head_dim
    )
    linear_key = jnp.dot(
        first_normalized, key_projection, preferred_element_type=jnp.float32
    ).reshape(number_of_rows, kv_heads, head_dim)
    value_reduced = (
        jnp.dot(first_normalized, value_projection, preferred_element_type=jnp.float32)
        .astype(jnp.bfloat16)
        .reshape(number_of_rows, kv_heads, head_dim)
    )
    q_rot = apply_rotary(q_lin, cosine_table, sine_component).astype(jnp.bfloat16)
    rotated_key = apply_rotary(linear_key, cosine_table, sine_component).astype(jnp.bfloat16)
    attended, log_total = sequence_forward(q_rot, rotated_key, value_reduced, query_group_width)
    flat_att = attended.reshape(number_of_rows, query_heads * head_dim)
    attn_part = jnp.dot(flat_att, w_out, preferred_element_type=jnp.float32)
    hidden1 = resid + lax.psum(attn_part.astype(jnp.bfloat16), "tensor").astype(jnp.float32)
    scale_two = rms_scale(hidden1)
    normed2 = (hidden1 * scale_two * gain_moe).astype(jnp.bfloat16)
    logits = jnp.dot(normed2, w_router, preferred_element_type=jnp.float32)
    chosen = jnp.take_along_axis(logits, routes, axis=1)
    gate_probs = jax.nn.softmax(chosen, axis=-1)
    slot_where, token_of, pick_of = slot_table(routes, expert_count, capacity)
    normed_pad = jnp.concatenate([normed2, jnp.zeros((1, model_width), jnp.bfloat16)], axis=0)
    outgoing = normed_pad[token_of].reshape(expert_count, capacity, model_width)
    received = lax.all_to_all(outgoing, "expert", split_axis=0, concat_axis=0, tiled=True)
    arrived = received.reshape(source_count, local_experts, capacity, model_width)
    gate_pre = jnp.einsum("secd,edh->sech", arrived, w_gate, preferred_element_type=jnp.float32)
    up_pre = jnp.einsum("secd,edh->sech", arrived, w_up, preferred_element_type=jnp.float32)
    sig_gate = jax.nn.sigmoid(gate_pre)
    activated = gate_pre * sig_gate
    hid_low = (activated * up_pre).astype(jnp.bfloat16)
    expert_out = jnp.einsum(
        "sech,ehd->secd", hid_low, w_down, preferred_element_type=jnp.float32
    ).astype(jnp.bfloat16)
    returned = lax.all_to_all(
        expert_out.reshape(expert_count, capacity, model_width),
        "expert",
        split_axis=0,
        concat_axis=0,
        tiled=True,
    )
    picked = returned.reshape(expert_count * capacity, model_width)[slot_where].reshape(
        number_of_rows, top_count, model_width
    )
    moe_part = jnp.zeros((number_of_rows, model_width), jnp.float32)
    for choice_index in range(top_count):
        moe_part = (
            moe_part
            + picked[:, choice_index].astype(jnp.float32)
            * gate_probs[:, choice_index : choice_index + 1]
        )
    moe_out = lax.psum(moe_part.astype(jnp.bfloat16), "tensor").astype(jnp.float32)
    output = (hidden1 + moe_out).astype(jnp.bfloat16)
    grad = cotangent.astype(jnp.float32)
    gate_dot = jnp.einsum("rjd,rd->rj", picked, cotangent, preferred_element_type=jnp.float32)
    grad_pad = jnp.concatenate([cotangent, jnp.zeros((1, model_width), jnp.bfloat16)], axis=0)
    gate_pad = jnp.concatenate([gate_probs.reshape(-1), jnp.zeros((1,), jnp.float32)], axis=0)
    sent_grad = (grad_pad[token_of].astype(jnp.float32) * gate_pad[pick_of][:, None]).astype(
        jnp.bfloat16
    )
    sent_grad = sent_grad.reshape(expert_count, capacity, model_width)
    grad_received = lax.all_to_all(sent_grad, "expert", split_axis=0, concat_axis=0, tiled=True)
    arrived_grad = grad_received.reshape(source_count, local_experts, capacity, model_width)
    d_hid = jnp.einsum("secd,ehd->sech", arrived_grad, w_down, preferred_element_type=jnp.float32)
    down_local = jnp.einsum(
        "sech,secd->ehd", hid_low, arrived_grad, preferred_element_type=jnp.float32
    )
    d_gate = (d_hid * up_pre * sig_gate * (1.0 + gate_pre * (1.0 - sig_gate))).astype(jnp.bfloat16)
    d_up = (d_hid * activated).astype(jnp.bfloat16)
    gate_local = jnp.einsum("secd,sech->edh", arrived, d_gate, preferred_element_type=jnp.float32)
    up_local = jnp.einsum("secd,sech->edh", arrived, d_up, preferred_element_type=jnp.float32)
    back_rows = jnp.einsum("sech,edh->secd", d_gate, w_gate, preferred_element_type=jnp.float32)
    back_rows = (
        back_rows + jnp.einsum("sech,edh->secd", d_up, w_up, preferred_element_type=jnp.float32)
    ).astype(jnp.bfloat16)
    came_back = lax.all_to_all(
        back_rows.reshape(expert_count, capacity, model_width),
        "expert",
        split_axis=0,
        concat_axis=0,
        tiled=True,
    )
    back_picked = came_back.reshape(expert_count * capacity, model_width)[slot_where].reshape(
        number_of_rows, top_count, model_width
    )
    back_part = jnp.zeros((number_of_rows, model_width), jnp.float32)
    for choice_index in range(top_count):
        back_part = back_part + back_picked[:, choice_index].astype(jnp.float32)
    back_total, dgate = (
        lax.psum(back_part.astype(jnp.bfloat16), "tensor").astype(jnp.float32),
        lax.psum(gate_dot.astype(jnp.bfloat16), "tensor").astype(jnp.float32),
    )
    inner_sum = jnp.sum(gate_probs * dgate, axis=1, keepdims=True)
    d_chosen = gate_probs * (dgate - inner_sum)
    matches = routes[:, :, None] == jnp.arange(expert_count, dtype=jnp.int32)[None, None, :]
    d_logits = jnp.sum(jnp.where(matches, d_chosen[:, :, None], 0.0), axis=1).astype(jnp.bfloat16)
    router_local = jnp.dot(normed2.T, d_logits, preferred_element_type=jnp.float32)
    d_normed2 = back_total + jnp.dot(d_logits, w_router.T, preferred_element_type=jnp.float32)
    d_hidden_part, gain_moe_local = norm_back(hidden1, scale_two, gain_moe, d_normed2)
    d_hidden1 = grad + d_hidden_part
    d_mixed = d_hidden1.astype(jnp.bfloat16)
    out_local = jnp.dot(flat_att.T, d_mixed, preferred_element_type=jnp.float32)
    d_att = (
        jnp.dot(d_mixed, w_out.T, preferred_element_type=jnp.float32)
        .astype(jnp.bfloat16)
        .reshape(number_of_rows, query_heads, head_dim)
    )
    dq_rot, rotated_key_gradient, dv_rows = sequence_backward(
        q_rot, rotated_key, value_reduced, attended, log_total, d_att, query_group_width
    )
    d_query = (
        apply_rotary(dq_rot, cosine_table, -sine_component)
        .astype(jnp.bfloat16)
        .reshape(number_of_rows, query_heads * head_dim)
    )
    key_gradient = (
        apply_rotary(rotated_key_gradient, cosine_table, -sine_component)
        .astype(jnp.bfloat16)
        .reshape(number_of_rows, kv_heads * head_dim)
    )
    value_gradient = dv_rows.astype(jnp.bfloat16).reshape(number_of_rows, kv_heads * head_dim)
    query_local = jnp.dot(first_normalized.T, d_query, preferred_element_type=jnp.float32)
    key_local = jnp.dot(first_normalized.T, key_gradient, preferred_element_type=jnp.float32)
    value_local = jnp.dot(first_normalized.T, value_gradient, preferred_element_type=jnp.float32)
    d_normed_part = jnp.dot(d_query, w_query.T, preferred_element_type=jnp.float32)
    d_normed_part = d_normed_part + jnp.dot(
        key_gradient, key_projection.T, preferred_element_type=jnp.float32
    )
    d_normed_part = d_normed_part + jnp.dot(
        value_gradient, value_projection.T, preferred_element_type=jnp.float32
    )
    d_normed1 = lax.psum(d_normed_part.astype(jnp.bfloat16), "tensor").astype(jnp.float32)
    d_resid_part, gain_attn_local = norm_back(resid, scale_one, gain_attn, d_normed1)
    input_grad = (d_hidden1 + d_resid_part).astype(jnp.bfloat16)
    gate_grad, up_grad, down_grad = (
        lax.psum_scatter(
            gate_local.astype(jnp.bfloat16), "dp", scatter_dimension=1, tiled=True
        ).astype(jnp.float32),
        lax.psum_scatter(
            up_local.astype(jnp.bfloat16), "dp", scatter_dimension=1, tiled=True
        ).astype(jnp.float32),
        lax.psum_scatter(
            down_local.astype(jnp.bfloat16), "dp", scatter_dimension=2, tiled=True
        ).astype(jnp.float32),
    )
    query_grad, key_grad, value_grad, out_grad, router_grad, gain_attn_grad, gain_moe_grad = (
        *side_by_side(
            (
                query_local.astype(jnp.bfloat16),
                key_local.astype(jnp.bfloat16),
                value_local.astype(jnp.bfloat16),
            ),
            ("dp", "expert"),
            0,
            1,
        ),
        sum_at_owner(out_local.astype(jnp.bfloat16), ("dp", "expert"), 1),
        *sent_together(
            (
                router_local.astype(jnp.bfloat16),
                gain_attn_local.astype(jnp.bfloat16),
                gain_moe_local.astype(jnp.bfloat16),
            ),
            ("dp", "expert"),
            0,
            1,
        ),
    )
    return (
        output,
        input_grad,
        gain_attn_grad,
        query_grad,
        key_grad,
        value_grad,
        out_grad,
        gain_moe_grad,
        router_grad,
        gate_grad,
        up_grad,
        down_grad,
    )


GATHER_ROWS = 4096
MESH = pl.DeviceIdType.MESH
VMEM = pl.BlockSpec(memory_space=pltpu.VMEM)
ANY = pl.BlockSpec(memory_space=pl.ANY)
EXTRA = 128
VMEM_LIMIT = 60 * 2**20
F32, BF16 = jnp.float32, jnp.bfloat16


def dot(a, b):
    return jnp.dot(a, b, preferred_element_type=F32)


def dot_nt(a, b):
    return lax.dot_general(a, b, (((1,), (1,)), ((), ())), preferred_element_type=F32)


def dot_tn(a, b):
    return lax.dot_general(a, b, (((0,), (0,)), ((), ())), preferred_element_type=F32)


def ds(index, size):
    return pl.ds(pl.multiple_of(index * size, size), size)


class Peers:
    def __init__(self, dp, tp, send_sem, recv_sem):
        self.z, self.c, self.t = (lax.axis_index(a) for a in ("dp", "expert", "tensor"))
        self.dp, self.tp = dp, tp
        self.send_sem, self.recv_sem = send_sem, recv_sem
        self.used = 0
        self.open = []

    def tensor(self, k):
        return (self.z, self.c, lax.rem(self.t + k, self.tp))

    def plane(self, k):
        return (lax.rem(self.z + k, self.dp), self.c, self.t)

    def partner(self):
        return (self.z, 1 - self.c, self.t)

    def greet(self):
        barrier = pltpu.get_barrier_semaphore()
        everyone = [self.tensor(k) for k in range(1, self.tp)]
        everyone += [self.plane(k) for k in range(1, self.dp)] + [self.partner()]
        for peer in everyone:
            pl.semaphore_signal(barrier, inc=1, device_id=peer, device_id_type=MESH)
        pl.semaphore_wait(barrier, len(everyone))

    def number(self, count):
        first = self.used
        self.used += count
        return first

    def make(self, src, dst, number, device):
        return pltpu.make_async_remote_copy(
            src_ref=src,
            dst_ref=dst,
            send_sem=self.send_sem.at[number],
            recv_sem=self.recv_sem.at[number],
            device_id=device,
            device_id_type=MESH,
        )

    def to(self, src, dst, device):
        copy = self.make(src, dst, self.number(1), device)
        copy.start()
        self.open.append(copy)
        return copy

    def keep(self, src, dst, sem):
        copy = pltpu.make_async_copy(src, dst, sem)
        copy.start()
        return copy

    def drain(self):
        for copy in self.open:
            copy.wait_send()


def arrived(copies):
    for copy in copies:
        copy.wait_recv()


def rotate(u, rope_ref, sign):
    width = u.shape[1]
    tiles = []
    for at in range(0, width, 128):
        v = u[:, at : at + 128]
        side = pltpu.roll(v, 96, 1) * rope_ref[1] + pltpu.roll(v, 32, 1) * rope_ref[2]
        tiles.append(v * rope_ref[0] + sign * side)
    return tiles[0] if len(tiles) == 1 else jnp.concatenate(tiles, axis=1)


def inverse_rms(u):
    return lax.rsqrt(jnp.mean(u * u, axis=-1, keepdims=True) + EPSILON)


def causal(length):
    row = lax.broadcasted_iota(jnp.int32, (length, length), 0)
    col = lax.broadcasted_iota(jnp.int32, (length, length), 1)
    return col <= row


def forward_kernel(
    dp,
    tp,
    tok_ref,
    cot_ref,
    routes_ref,
    ga_ref,
    gm_ref,
    wq_ref,
    wk_ref,
    wv_ref,
    wo_ref,
    rope_ref,
    x_ref,
    g_ref,
    gz_ref,
    h1_ref,
    n1_ref,
    qkv_ref,
    att_ref,
    lse_ref,
    part_buf,
    rs_buf,
    send_sem,
    recv_sem,
):
    net = Peers(dp, tp, send_sem, recv_sem)
    z, c, t = net.z, net.c, net.t
    length, model = tok_ref.shape
    own = length // tp
    q_width, kv_width = wq_ref.shape[1], wk_ref.shape[1]
    group = q_width // kv_width
    net.greet()
    seq_rows = ds(c, length)
    got_g = [net.to(cot_ref, g_ref.at[seq_rows], net.partner())]
    for k in range(1, dp):
        got_g.append(net.to(cot_ref.at[ds(t, own)], gz_ref.at[dp - 1 - k], net.plane(k)))
    g_ref[seq_rows, :] = cot_ref[...]

    resid = tok_ref[...].astype(F32)
    n1 = (resid * inverse_rms(resid) * ga_ref[...]).astype(BF16)
    n1_ref[...] = n1
    qkv_ref[:, :q_width] = rotate(dot(n1, wq_ref[...]), rope_ref, 1.0).astype(BF16)
    qkv_ref[:, q_width : q_width + kv_width] = rotate(dot(n1, wk_ref[...]), rope_ref, 1.0).astype(BF16)
    qkv_ref[:, q_width + kv_width :] = dot(n1, wv_ref[...]).astype(BF16)

    seen = causal(length)
    lane = lax.broadcasted_iota(jnp.int32, lse_ref.shape, 1)
    lse_all = jnp.zeros(lse_ref.shape, F32)
    scale = HEAD_SIZE ** (-0.5)
    for h in range(q_width // HEAD_SIZE):
        kv = h // group
        at_k = q_width + kv * HEAD_SIZE
        at_v = q_width + kv_width + kv * HEAD_SIZE
        q = qkv_ref[:, h * HEAD_SIZE : (h + 1) * HEAD_SIZE]
        key = qkv_ref[:, at_k : at_k + HEAD_SIZE]
        val = qkv_ref[:, at_v : at_v + HEAD_SIZE]
        s = jnp.where(seen, dot_nt(q, key) * scale, -1e30)
        top = jnp.max(s, axis=-1, keepdims=True)
        lse = top + jnp.log(jnp.sum(jnp.exp(s - top), axis=-1, keepdims=True))
        prob = jnp.exp(s - lse).astype(BF16)
        att_ref[:, h * HEAD_SIZE : (h + 1) * HEAD_SIZE] = dot(prob, val).astype(BF16)
        lse_all = jnp.where(lane == h, lse, lse_all)
    lse_ref[...] = lse_all
    part_buf[...] = dot(att_ref[...], wo_ref[...]).astype(BF16)

    got = []
    for k in range(1, tp):
        block = part_buf.at[ds(lax.rem(t + k, tp), own)]
        got.append(net.to(block, rs_buf.at[k - 1], net.tensor(k)))
    total = tok_ref[ds(t, own), :].astype(F32) + part_buf[ds(t, own), :].astype(F32)
    picked = routes_ref[ds(t, own), :]
    ids = lax.broadcasted_iota(jnp.int32, (own, EXTRA), 1)
    chosen = picked[:, 0:1] == ids
    for j in range(1, picked.shape[1]):
        chosen = chosen | (picked[:, j : j + 1] == ids)
    arrived(got)
    for k in range(1, tp):
        total = total + rs_buf[k - 1].astype(F32)
    h1_ref[...] = total
    n2 = (total * inverse_rms(total) * gm_ref[...]).astype(BF16)
    mine = ds(c * tp + t, own)
    x_ref[mine, :model] = n2
    x_ref[mine, model:] = jnp.where(chosen, 1.0, 0.0).astype(BF16)
    got = [net.to(x_ref.at[mine], x_ref.at[mine], net.tensor(k)) for k in range(1, tp)]
    arrived(got)
    got = [net.to(x_ref.at[seq_rows], x_ref.at[seq_rows], net.partner())]
    arrived(got_g + got)
    net.drain()


def forward(dp, tp, tokens, cotangent, routes, ga, gm, wq, wk, wv, wo, rope):
    length, model = tokens.shape
    own, wide = length // tp, model + EXTRA
    widths = wq.shape[1] + wk.shape[1] + wv.shape[1]
    copies = 2 + (dp - 1) + 2 * (tp - 1)
    shapes = [
        ((2 * length, wide), BF16),
        ((2 * length, model), BF16),
        ((dp - 1, own, model), BF16),
        ((own, model), F32),
        ((length, model), BF16),
        ((length, widths), BF16),
        ((length, wq.shape[1]), BF16),
        ((length, 128), F32),
    ]
    return pl.pallas_call(
        functools.partial(forward_kernel, dp, tp),
        out_shape=[jax.ShapeDtypeStruct(*s) for s in shapes],
        in_specs=[VMEM] * 10,
        out_specs=[VMEM] * len(shapes),
        scratch_shapes=[
            pltpu.VMEM((length, model), BF16),
            pltpu.VMEM((tp - 1, own, model), BF16),
            pltpu.SemaphoreType.DMA((copies,)),
            pltpu.SemaphoreType.DMA((copies,)),
        ],
        compiler_params=pltpu.CompilerParams(
            collective_id=0, has_side_effects=True, vmem_limit_bytes=VMEM_LIMIT
        ),
        name="forward",
    )(tokens, cotangent, routes, ga, gm, wq, wk, wv, wo, rope)


def gates_of(x_ref, wr_ref, model):
    logits = dot(x_ref[:, :model], wr_ref[...])
    chosen = x_ref[:, model:].astype(F32) > 0.5
    top = jnp.max(jnp.where(chosen, logits, -jnp.inf), axis=1, keepdims=True)
    weight = jnp.where(chosen, jnp.exp(jnp.where(chosen, logits - top, 0.0)), 0.0)
    return weight / jnp.sum(weight, axis=1, keepdims=True)


def store_split(gates, split_ref):
    high = gates.astype(BF16)
    split_ref[:, :EXTRA] = high
    split_ref[:, EXTRA:] = (gates - high.astype(F32)).astype(BF16)


def pair_of_gates(split, first, width):
    k_pos = lax.broadcasted_iota(jnp.int32, (2 * EXTRA, 2 * width), 0)
    l_pos = lax.broadcasted_iota(jnp.int32, (2 * EXTRA, 2 * width), 1)
    pick = jnp.where(k_pos % EXTRA == first + l_pos // width, 1.0, 0.0).astype(BF16)
    return dot(split, pick)


def swiglu(both, dh, gate):
    width = dh.shape[1]
    gate_pre, up_pre = both[:, :width], both[:, width:]
    sig = jax.nn.sigmoid(gate_pre)
    act = gate_pre * sig
    hid = act * up_pre
    d_hid = dh * gate
    d_gate = d_hid * up_pre * sig * (1.0 + gate_pre * (1.0 - sig))
    return hid, (hid * gate).astype(BF16), d_gate.astype(BF16), (d_hid * act).astype(BF16)


def plane_kernel(
    dp,
    tp,
    x_ref,
    g_ref,
    gz_ref,
    n1_ref,
    wr_ref,
    wg_ref,
    wu_ref,
    wd_ref,
    xr_ref,
    gr_ref,
    n1c_ref,
    moe_ref,
    back_ref,
    dgate_ref,
    gates_ref,
    ghid_ref,
    dgp_ref,
    dup_ref,
    split,
    moe_acc,
    back_acc,
    send_sem,
    recv_sem,
    keep_sem,
):
    step, last = pl.program_id(0), pl.num_programs(0) - 1
    net = Peers(dp, tp, send_sem, recv_sem)
    z, c, t = net.z, net.c, net.t
    rows, model = g_ref.shape
    length = rows // 2
    own = length // tp
    width = wg_ref.shape[2]
    part = model // dp
    others = range(1, dp)
    sides = range(1, tp)

    def block(plane, core, tensor):
        return ds((plane * 2 + core) * tp + tensor, own)

    def columns(index):
        return pl.ds(pl.multiple_of(index * part, 128), part)

    mine = ds(c * tp + t, own)
    x_z = [
        net.make(x_ref.at[mine], xr_ref.at[block(dp - k, c, t)], net.number(1), net.plane(k))
        for k in others
    ]
    n1_z = [
        net.make(
            n1_ref.at[:, columns(lax.rem(z + k, dp))],
            n1c_ref.at[ds((dp - k) * 2 + c, length)],
            net.number(1),
            net.plane(k),
        )
        for k in others
    ]
    n1_own = net.make(
        n1_ref.at[:, columns(z)], n1c_ref.at[ds(c, length)], net.number(1), net.partner()
    )
    g_t = [
        net.make(gz_ref.at[p - 1], gr_ref.at[block(p, c, t)], net.number(1), net.tensor(k))
        for p in others
        for k in sides
    ]
    x_t = [
        net.make(
            xr_ref.at[block(p, c, t)], xr_ref.at[block(p, c, t)], net.number(1), net.tensor(k)
        )
        for p in others
        for k in sides
    ]

    def over(ref):
        return [
            net.make(
                ref.at[ds(p * 2 + c, length)],
                ref.at[ds(p * 2 + c, length)],
                net.number(1),
                net.partner(),
            )
            for p in others
        ]

    g_c, x_c, n1_c = over(gr_ref), over(xr_ref), over(n1c_ref)
    kept = [
        pltpu.make_async_copy(x_ref, xr_ref.at[pl.ds(0, rows)], keep_sem.at[0]),
        pltpu.make_async_copy(g_ref, gr_ref.at[pl.ds(0, rows)], keep_sem.at[1]),
        pltpu.make_async_copy(
            n1_ref.at[:, columns(z)], n1c_ref.at[ds(c, length)], keep_sem.at[2]
        ),
    ] + [
        pltpu.make_async_copy(gz_ref.at[p - 1], gr_ref.at[block(p, c, t)], keep_sem.at[2 + p])
        for p in others
    ]

    def start(copies):
        for copy in copies:
            copy.start()

    @pl.when(step == 0)
    def _():
        net.greet()
        start(x_z + g_t + n1_z + [n1_own])
        start(kept)
        moe_acc[...] = jnp.zeros_like(moe_acc)
        back_acc[...] = jnp.zeros_like(back_acc)
        dgate_ref[...] = jnp.zeros_like(dgate_ref)
        gates = gates_of(x_ref, wr_ref, model)
        gates_ref[...] = gates
        store_split(gates, split)

    @pl.when(step == 4)
    def _():
        arrived(x_z)
        start(x_t)

    @pl.when(step == 6)
    def _():
        arrived(g_t)
        for copy in kept:
            copy.wait()
        start(g_c)

    @pl.when(step == 8)
    def _():
        arrived(n1_z)
        start(n1_c)

    first = c * (2 * pl.num_programs(0)) + 2 * step
    gate_pair = pair_of_gates(split[...], first, width)
    wd_pair = wd_ref[...].reshape(2 * width, model)
    dh_pair = dot_nt(g_ref[...], wd_pair)
    lane = lax.broadcasted_iota(jnp.int32, dgate_ref.shape, 1)
    for k in range(2):
        lanes = slice(k * width, (k + 1) * width)
        w_both = jnp.concatenate([wg_ref[k], wu_ref[k]], axis=1)
        both = dot(x_ref[:, :model], w_both)
        dh = dh_pair[:, lanes]
        hid, ghid, dgp, dup = swiglu(both, dh, gate_pair[:, lanes])
        ghid_ref[:, lanes] = ghid
        dgp_ref[:, lanes] = dgp
        dup_ref[:, lanes] = dup
        row_sum = jnp.sum(hid * dh, axis=1, keepdims=True)
        dgate_ref[...] += jnp.where(lane == first + k, row_sum, 0.0)
        back_acc[...] += dot_nt(jnp.concatenate([dgp, dup], axis=1), w_both)
    moe_acc[...] += dot(ghid_ref[...], wd_pair)

    @pl.when(step == last)
    def _():
        moe_ref[...] = moe_acc[...].astype(BF16)
        back_ref[...] = back_acc[...].astype(BF16)
        arrived(x_t)
        start(x_c)
        arrived(g_c + n1_c + [n1_own])
        arrived(x_c)
        for copy in x_z + g_t + n1_z + [n1_own] + x_t + g_c + n1_c + x_c:
            copy.wait_send()


def plane_experts(dp, tp, x, g, gz, n1, wr, w_gate, w_up, w_down):
    rows, model = g.shape
    length = rows // 2
    count, _, width = w_gate.shape
    all_rows = rows * dp
    others, sides = dp - 1, tp - 1
    copies = 2 * others + 1 + 2 * others * sides + 3 * others

    def whole(a):
        shape = a.shape
        return pl.BlockSpec(shape, lambda i: (0,) * len(shape), pipeline_mode=pl.Buffered(1))

    by_pair = lambda shape: pl.BlockSpec((2,) + shape, lambda i: (i, 0, 0))
    saved = pl.BlockSpec((rows, 2 * width), lambda i: (0, i))
    shapes = [
        ((all_rows, x.shape[1]), BF16),
        ((all_rows, model), BF16),
        ((all_rows, model // dp), BF16),
        ((rows, model), BF16),
        ((rows, model), BF16),
        ((rows, EXTRA), F32),
        ((rows, EXTRA), F32),
        ((rows, count * width), BF16),
        ((rows, count * width), BF16),
        ((rows, count * width), BF16),
    ]
    shapes = [jax.ShapeDtypeStruct(*s) for s in shapes]
    return pl.pallas_call(
        functools.partial(plane_kernel, dp, tp),
        grid=(count // 2,),
        out_shape=shapes,
        in_specs=[whole(x), whole(g), whole(gz), whole(n1), whole(wr)]
        + [by_pair((model, width)), by_pair((model, width)), by_pair((width, model))],
        out_specs=[ANY, ANY, ANY] + [whole(s) for s in shapes[3:7]] + [saved] * 3,
        scratch_shapes=[
            pltpu.VMEM((rows, 2 * EXTRA), BF16),
            pltpu.VMEM((rows, model), F32),
            pltpu.VMEM((rows, model), F32),
            pltpu.SemaphoreType.DMA((copies,)),
            pltpu.SemaphoreType.DMA((copies,)),
            pltpu.SemaphoreType.DMA((3 + others,)),
        ],
        compiler_params=pltpu.CompilerParams(
            collective_id=1, has_side_effects=True, vmem_limit_bytes=VMEM_LIMIT
        ),
        name="plane_experts",
    )(x, g, gz, n1, wr, w_gate, w_up, w_down)


def backward_kernel(
    dp,
    tp,
    back_ref,
    moe_ref,
    dgate_ref,
    gates_ref,
    h1_ref,
    tok_ref,
    cot_ref,
    ga_ref,
    gm_ref,
    wr_ref,
    wq_ref,
    wk_ref,
    wv_ref,
    wo_ref,
    qkv_ref,
    att_ref,
    lse_ref,
    rope_ref,
    xr_ref,
    gr_ref,
    wg_ref,
    wu_ref,
    wd_ref,
    out_ref,
    in_ref,
    att_all,
    da_cols,
    d_all,
    gains_ref,
    ghid_ref,
    dgp_ref,
    dup_ref,
    x_rest,
    g_rest,
    split,
    pair_b,
    pair_m,
    pair_d,
    sum_b,
    sum_m,
    sum_d,
    rs_b,
    rs_m,
    rs_d,
    dh1_buf,
    da_buf,
    dl_buf,
    d_buf,
    do_buf,
    part_buf,
    rs_3,
    gain_buf,
    gain_t,
    gain_z,
    gain_zs,
    gain_c,
    out_buf,
    in_buf,
    send_sem,
    recv_sem,
    keep_sem,
):
    step, last = pl.program_id(0), pl.num_programs(0) - 1
    net = Peers(dp, tp, send_sem, recv_sem)
    z, c, t = net.z, net.c, net.t
    length, model = tok_ref.shape
    own = length // tp
    part = model // dp
    width = wg_ref.shape[2]
    q_width, kv_width = wq_ref.shape[1], wk_ref.shape[1]
    group = q_width // kv_width
    others, sides = range(1, dp), range(1, tp)
    mine = ds(t, own)
    here, there = ds(c, length), ds(1 - c, length)

    def columns(index):
        return pl.ds(pl.multiple_of(index * part, 128), part)

    def link(src, dst, device):
        return net.make(src, dst, net.number(1), device)

    def to_sides(ref, into):
        return [
            link(ref.at[ds(lax.rem(t + k, tp), own)], into.at[k - 1], net.tensor(k)) for k in sides
        ]

    def share(ref):
        return [link(ref.at[mine], ref.at[mine], net.tensor(k)) for k in sides]

    def on_to_partner(ref):
        rows = [ds(p * 2 + c, length) for p in others]
        return [link(ref.at[r], ref.at[r], net.partner()) for r in rows]

    def over_planes(ref, into):
        return [link(ref, into.at[ds((dp - k) * 2 + c, length)], net.plane(k)) for k in others]

    def start(copies):
        for copy in copies:
            copy.start()

    pair_bd = [
        link(back_ref.at[there], pair_b, net.partner()),
        link(dgate_ref.at[there], pair_d, net.partner()),
    ]
    pair_mo = [link(moe_ref.at[there], pair_m, net.partner())]
    att_z = over_planes(att_ref, att_all)
    att_c = on_to_partner(att_all)
    att_own = [link(att_ref, att_all.at[here], net.partner())]
    side_bd = to_sides(sum_b, rs_b) + to_sides(sum_d, rs_d)
    side_mo = to_sides(sum_m, rs_m)
    share_da = share(da_buf) + share(dl_buf)
    da_z = [
        link(
            da_buf.at[:, columns(lax.rem(z + k, dp))],
            da_cols.at[ds((dp - k) * 2 + c, length)],
            net.plane(k),
        )
        for k in others
    ]
    da_c = on_to_partner(da_cols)
    da_own = [link(da_buf.at[:, columns(z)], da_cols.at[here], net.partner())]
    share_out = share(out_buf)
    d_z = over_planes(d_buf, d_all)
    d_c = on_to_partner(d_all)
    d_own = [link(d_buf, d_all.at[here], net.partner())]
    side_3 = to_sides(part_buf, rs_3)
    share_in = share(in_buf)
    side_gain = [link(gain_buf, gain_t.at[k - 1], net.tensor(k)) for k in sides]
    plane_gain = [
        link(gain_zs.at[:, columns(lax.rem(z + k, dp))], gain_z.at[k - 1], net.plane(k))
        for k in others
    ]
    pair_gain = [link(gain_c.at[0], gain_c.at[1], net.partner())]
    keep_att = pltpu.make_async_copy(att_ref, att_all.at[here], keep_sem.at[0])
    keep_da = pltpu.make_async_copy(da_buf.at[:, columns(z)], da_cols.at[here], keep_sem.at[1])
    keep_d = pltpu.make_async_copy(d_buf, d_all.at[here], keep_sem.at[2])
    plane_rows = xr_ref.shape[0] // dp
    rest = pl.ds(plane_rows, xr_ref.shape[0] - plane_rows)
    load_x = pltpu.make_async_copy(xr_ref.at[rest], x_rest, keep_sem.at[3])
    load_g = pltpu.make_async_copy(gr_ref.at[rest], g_rest, keep_sem.at[4])

    @pl.when(step == 0)
    def _():
        load_x.start()
        load_g.start()
        net.greet()
        start(pair_bd + pair_mo + att_z + att_own)
        keep_att.start()
        load_x.wait()
        store_split(gates_of(x_rest, wr_ref, model), split)
        load_g.wait()

    @pl.when(step == 1)
    def _():
        arrived(pair_bd)
        sum_b[...] = (back_ref[here, :].astype(F32) + pair_b[...].astype(F32)).astype(BF16)
        sum_d[...] = dgate_ref[here, :] + pair_d[...]
        start(side_bd)

    @pl.when(step == 3)
    def _():
        arrived(side_bd)
        d_n2 = sum_b[mine, :].astype(F32)
        dgate = sum_d[mine, :]
        for k in sides:
            d_n2 = d_n2 + rs_b[k - 1].astype(F32)
            dgate = dgate + rs_d[k - 1]
        gates = gates_ref[ds(c * tp + t, own), :]
        d_logits = gates * (dgate - jnp.sum(gates * dgate, axis=1, keepdims=True))
        dl_buf[mine, :] = d_logits.astype(BF16)
        d_n2 = d_n2 + dot_nt(d_logits.astype(BF16), wr_ref[...])
        h1 = h1_ref[...]
        r2 = inverse_rms(h1)
        weighted = d_n2 * gm_ref[...]
        inner = jnp.mean(weighted * h1, axis=-1, keepdims=True)
        gain_buf[...] = jnp.zeros_like(gain_buf)
        gain_buf[1:2, :] = jnp.sum(d_n2 * h1 * r2, axis=0, keepdims=True)
        d_h1 = cot_ref[mine, :].astype(F32) + (r2 * weighted - h1 * (r2 * r2 * r2) * inner)
        dh1_buf[...] = d_h1
        da_buf[mine, :] = d_h1.astype(BF16)
        start(share_da)
        arrived(pair_mo)
        sum_m[...] = (moe_ref[here, :].astype(F32) + pair_m[...].astype(F32)).astype(BF16)
        start(side_mo)
        arrived(att_z)
        start(att_c)

    @pl.when(step == 5)
    def _():
        arrived(share_da)
        start(da_z + da_own)
        keep_da.start()
        d_buf[:, q_width + 2 * kv_width :] = dl_buf[...]
        do_buf[...] = dot_nt(da_buf[...], wo_ref[...]).astype(BF16)
        arrived(side_mo)
        total = h1_ref[...] + sum_m[mine, :].astype(F32)
        for k in sides:
            total = total + rs_m[k - 1].astype(F32)
        out_buf[mine, :] = total.astype(BF16)
        start(share_out)
        seen = causal(length)
        scale = HEAD_SIZE ** (-0.5)
        d_key, d_val, d_query = [], [], []
        for kv in range(kv_width // HEAD_SIZE):
            at_k = q_width + kv * HEAD_SIZE
            at_v = q_width + kv_width + kv * HEAD_SIZE
            key = qkv_ref[:, at_k : at_k + HEAD_SIZE]
            val = qkv_ref[:, at_v : at_v + HEAD_SIZE]
            dk = jnp.zeros((length, HEAD_SIZE), F32)
            dv = jnp.zeros((length, HEAD_SIZE), F32)
            for h in range(kv * group, (kv + 1) * group):
                at = slice(h * HEAD_SIZE, (h + 1) * HEAD_SIZE)
                q = qkv_ref[:, at]
                d_out = do_buf[:, at]
                s = jnp.where(seen, dot_nt(q, key) * scale, -1e30)
                prob = jnp.exp(s - lse_ref[:, h : h + 1])
                delta = jnp.sum(
                    d_out.astype(F32) * att_ref[:, at].astype(F32), axis=-1, keepdims=True
                )
                d_s = (prob * (dot_nt(d_out, val) - delta)).astype(BF16)
                d_query.append(dot(d_s, key) * scale)
                dk = dk + dot_tn(d_s, q)
                dv = dv + dot_tn(prob.astype(BF16), d_out)
            d_key.append(dk * scale)
            d_val.append(dv)
        d_buf[:, :q_width] = rotate(jnp.concatenate(d_query, axis=1), rope_ref, -1.0).astype(BF16)
        d_buf[:, q_width : q_width + kv_width] = rotate(
            jnp.concatenate(d_key, axis=1), rope_ref, -1.0
        ).astype(BF16)
        d_buf[:, q_width + kv_width : q_width + 2 * kv_width] = jnp.concatenate(
            d_val, axis=1
        ).astype(BF16)
        part_n1 = dot_nt(d_buf[:, :q_width], wq_ref[...])
        part_n1 = part_n1 + dot_nt(d_buf[:, q_width : q_width + kv_width], wk_ref[...])
        part_n1 = part_n1 + dot_nt(
            d_buf[:, q_width + kv_width : q_width + 2 * kv_width], wv_ref[...]
        )
        part_buf[...] = part_n1.astype(BF16)
        start(side_3 + d_z + d_own)
        keep_d.start()

    @pl.when(step == 7)
    def _():
        arrived(side_3)
        d_n1 = part_buf[mine, :].astype(F32)
        for k in sides:
            d_n1 = d_n1 + rs_3[k - 1].astype(F32)
        resid = tok_ref[mine, :].astype(F32)
        r1 = inverse_rms(resid)
        weighted = d_n1 * ga_ref[...]
        inner = jnp.mean(weighted * resid, axis=-1, keepdims=True)
        gain_buf[0:1, :] = jnp.sum(d_n1 * resid * r1, axis=0, keepdims=True)
        d_x = dh1_buf[...] + (r1 * weighted - resid * (r1 * r1 * r1) * inner)
        in_buf[mine, :] = d_x.astype(BF16)
        start(side_gain + share_in)
        arrived(da_z)
        start(da_c)

    @pl.when(step == 8)
    def _():
        arrived(side_gain)
        gain = gain_buf[...]
        for k in sides:
            gain = gain + gain_t[k - 1]
        gain_zs[...] = gain
        start(plane_gain)

    @pl.when(step == 9)
    def _():
        arrived(plane_gain)
        gain = gain_zs[:, columns(z)]
        for k in others:
            gain = gain + gain_z[k - 1]
        gain_c[0] = gain
        start(pair_gain)

    first = c * (2 * pl.num_programs(0)) + 2 * step
    wd_pair = wd_ref[...].reshape(2 * width, model)
    gate_pair = pair_of_gates(split[...], first, width)
    dh_pair = dot_nt(g_rest[...], wd_pair)
    for k in range(2):
        lanes = slice(k * width, (k + 1) * width)
        both = dot(x_rest[:, :model], jnp.concatenate([wg_ref[k], wu_ref[k]], axis=1))
        _, ghid, dgp, dup = swiglu(both, dh_pair[:, lanes], gate_pair[:, lanes])
        ghid_ref[:, lanes] = ghid
        dgp_ref[:, lanes] = dgp
        dup_ref[:, lanes] = dup

    @pl.when(step == last)
    def _():
        arrived(d_z)
        start(d_c)
        arrived(pair_gain)
        gains_ref[...] = gain_c[0] + gain_c[1]
        arrived(share_out + share_in + att_own + da_own + d_own + att_c + da_c + d_c)
        out_ref[...] = out_buf[...]
        in_ref[...] = in_buf[...]
        for copy in (keep_att, keep_da, keep_d):
            copy.wait()
        sent = pair_bd + pair_mo + att_z + att_c + att_own + side_bd + side_mo + share_da
        sent = sent + da_z + da_c + da_own + share_out + d_z + d_c + d_own + side_3 + share_in
        for copy in sent + side_gain + plane_gain + pair_gain:
            copy.wait_send()


def whole_spec(a):
    shape = a.shape
    return pl.BlockSpec(shape, lambda *_: (0,) * len(shape), pipeline_mode=pl.Buffered(1))


def backward(dp, tp, arrays, streamed, weights):
    tokens = arrays[5]
    wq, wk, wv = arrays[10:13]
    all_rows, model = streamed[1].shape
    rest_rows = all_rows - all_rows // dp
    count, _, width = weights[0].shape
    length = tokens.shape[0]
    own, part = length // tp, model // dp
    q_width = wq.shape[1]
    wide = q_width + wk.shape[1] + wv.shape[1] + EXTRA
    others, sides = dp - 1, tp - 1
    copies = 3 + 3 * (2 * others + 1) + 9 * sides + sides + others + 1
    by_pair = lambda shape: pl.BlockSpec((2,) + shape, lambda i: (i, 0, 0))
    saved = pl.BlockSpec((rest_rows, 2 * width), lambda i: (0, i))
    shapes = [
        ((length, model), BF16),
        ((length, model), BF16),
        ((all_rows, q_width), BF16),
        ((all_rows, part), BF16),
        ((all_rows, wide), BF16),
        ((8, part), F32),
        ((rest_rows, count * width), BF16),
        ((rest_rows, count * width), BF16),
        ((rest_rows, count * width), BF16),
    ]
    shapes = [jax.ShapeDtypeStruct(*s) for s in shapes]
    full, block, slots = (length, model), (own, model), (sides, own, model)
    scratch = [
        ((rest_rows, streamed[0].shape[1]), BF16),
        ((rest_rows, model), BF16),
        ((rest_rows, 2 * EXTRA), BF16),
        (full, BF16),
        (full, BF16),
        ((length, EXTRA), F32),
        (full, BF16),
        (full, BF16),
        ((length, EXTRA), F32),
        (slots, BF16),
        (slots, BF16),
        ((sides, own, EXTRA), F32),
        (block, F32),
        (full, BF16),
        ((length, EXTRA), BF16),
        ((length, wide), BF16),
        ((length, q_width), BF16),
        (full, BF16),
        (slots, BF16),
        ((8, model), F32),
        ((sides, 8, model), F32),
        ((others, 8, part), F32),
        ((8, model), F32),
        ((2, 8, part), F32),
        (full, BF16),
        (full, BF16),
    ]
    return pl.pallas_call(
        functools.partial(backward_kernel, dp, tp),
        grid=(count // 2,),
        out_shape=shapes,
        in_specs=[whole_spec(a) for a in arrays]
        + [ANY, ANY]
        + [by_pair((model, width)), by_pair((model, width)), by_pair((width, model))],
        out_specs=[whole_spec(shapes[0]), whole_spec(shapes[1]), ANY, ANY, ANY]
        + [whole_spec(shapes[5])]
        + [saved] * 3,
        scratch_shapes=[pltpu.VMEM(*s) for s in scratch]
        + [
            pltpu.SemaphoreType.DMA((copies,)),
            pltpu.SemaphoreType.DMA((copies,)),
            pltpu.SemaphoreType.DMA((5,)),
        ],
        compiler_params=pltpu.CompilerParams(
            collective_id=2, has_side_effects=True, vmem_limit_bytes=VMEM_LIMIT
        ),
        name="backward",
    )(*arrays, *streamed, *weights)


def weights_kernel(
    place_ref,
    x_ref,
    g_ref,
    att_ref,
    da_ref,
    n1_ref,
    d_ref,
    ghid_ref,
    dgp_ref,
    dup_ref,
    ghid_rest,
    dgp_rest,
    dup_rest,
    gate_grad_ref,
    up_grad_ref,
    down_grad_ref,
    query_ref,
    key_ref,
    value_ref,
    out_grad_ref,
    router_ref,
    xt_buf,
    gt_buf,
    side_buf,
):
    step = pl.program_id(0)
    c = place_ref[1]
    width = gate_grad_ref.shape[2]
    plane_rows = ghid_ref.shape[0]

    @pl.when(step == 0)
    def _():
        xt_buf[...] = x_ref[...].T
        gt_buf[...] = g_ref[...].T
        q_width, kv_width = query_ref.shape[1], key_ref.shape[1]
        half = query_ref.shape[0]
        at = pl.ds(pl.multiple_of(c * half, 8), half)
        tail = d_ref.shape[1] - EXTRA
        side_buf[:, :tail] = dot_tn(n1_ref[...], d_ref[:, :tail])
        side_buf[:, tail:] = dot(xt_buf[...], d_ref[:, tail:])
        query_ref[...] = side_buf[at, :q_width]
        key_ref[...] = side_buf[at, q_width : q_width + kv_width]
        value_ref[...] = side_buf[at, q_width + kv_width : q_width + 2 * kv_width]
        router_ref[...] = side_buf[at, tail:][:, : router_ref.shape[1]]
        out_all = dot_tn(att_ref[...], da_ref[...])
        out_grad_ref[...] = jnp.where(c == 0, out_all[:, :half], out_all[:, half:])

    def contract(left, own, rest):
        return dot(left[:, :plane_rows], own[...]) + dot(left[:, plane_rows:], rest[...])

    gate_both = contract(xt_buf, dgp_ref, dgp_rest)
    up_both = contract(xt_buf, dup_ref, dup_rest)
    down_both = contract(gt_buf, ghid_ref, ghid_rest).T
    for k in range(2):
        lanes = slice(k * width, (k + 1) * width)
        gate_grad_ref[k] = gate_both[:, lanes]
        up_grad_ref[k] = up_both[:, lanes]
        down_grad_ref[k] = down_both[lanes, :]


def weight_grads(place, x, g, sides, own, rest, count, kv_width, experts):
    rows = x.shape[0]
    att, _, n1, d = sides
    width = own[0].shape[1] // count
    part = n1.shape[1]
    q_width, half = att.shape[1], part // 2
    by_pair = lambda shape: pl.BlockSpec((2,) + shape, lambda i, p: (i, 0, 0))
    saved = lambda a: pl.BlockSpec((a.shape[0], 2 * width), lambda i, p: (0, i))
    columns = pl.BlockSpec((rows, part), lambda i, p: (0, p[0]), pipeline_mode=pl.Buffered(1))
    shapes = [
        (count, part, width),
        (count, part, width),
        (count, width, part),
        (half, q_width),
        (half, kv_width),
        (half, kv_width),
        (q_width, half),
        (half, experts),
    ]
    shapes = [jax.ShapeDtypeStruct(s, F32) for s in shapes]
    return pl.pallas_call(
        weights_kernel,
        grid_spec=pltpu.PrefetchScalarGridSpec(
            num_scalar_prefetch=1,
            grid=(count // 2,),
            in_specs=[columns, columns]
            + [whole_spec(a) for a in sides]
            + [saved(a) for a in own]
            + [saved(a) for a in rest],
            out_specs=[by_pair((part, width)), by_pair((part, width)), by_pair((width, part))]
            + [whole_spec(s) for s in shapes[3:]],
            scratch_shapes=[
                pltpu.VMEM((part, rows), BF16),
                pltpu.VMEM((part, rows), BF16),
                pltpu.VMEM((part, d.shape[1]), F32),
            ],
        ),
        out_shape=shapes,
        compiler_params=pltpu.CompilerParams(vmem_limit_bytes=VMEM_LIMIT),
        name="weight_grads",
    )(place, x, g, *sides, *own, *rest)


def rope_rows(length):
    positions = jnp.arange(length, dtype=F32)
    cos, sin = rope_tables(positions, HEAD_SIZE)
    none = jnp.zeros_like(sin)
    double = lambda first, second: jnp.concatenate([first, second, first, second], axis=1)
    return jnp.stack([double(cos, cos), double(-sin, none), double(none, sin)])


def gather_plan(
    tokens,
    gain_attn,
    w_query,
    key_projection,
    value_projection,
    w_out,
    gain_moe,
    w_router,
    w_gate,
    w_up,
    w_down,
    routes,
    cotangent,
):
    dp, tp = lax.axis_size("dp"), lax.axis_size("tensor")
    experts = w_router.shape[1]
    half = tokens.shape[1] // dp // 2
    rope = rope_rows(tokens.shape[0])
    ga, gm = gain_attn[None, :], gain_moe[None, :]
    wr = jnp.pad(w_router, ((0, 0), (0, EXTRA - experts)))
    heads = (w_query, key_projection, value_projection, w_out)
    x, g, gz, h1, n1, qkv, att, lse = forward(
        dp, tp, tokens, cotangent, routes, ga, gm, *heads, rope
    )
    x_all, g_all, n1_cols, moe, back, dgate, gates, ghid, dgp, dup = plane_experts(
        dp, tp, x, g, gz, n1, wr, w_gate, w_up, w_down
    )
    output, input_grad, att_all, da_cols, d_all, gains, *rest = backward(
        dp,
        tp,
        (back, moe, dgate, gates, h1, tokens, cotangent, ga, gm, wr, *heads, qkv, att, lse, rope),
        (x_all, g_all),
        (w_gate, w_up, w_down),
    )
    z, core = lax.axis_index("dp"), lax.axis_index("expert")
    place = jnp.stack([z, core]).astype(jnp.int32)
    gate_grad, up_grad, down_grad, query_grad, key_grad, value_grad, out_grad, router_grad = weight_grads(
        place,
        x_all,
        g_all,
        (att_all, da_cols, n1_cols, d_all),
        (ghid, dgp, dup),
        rest,
        w_gate.shape[0],
        key_projection.shape[1],
        experts,
    )
    gains = lax.dynamic_slice_in_dim(gains, core * half, half, axis=1)
    return (
        output,
        input_grad,
        gains[0],
        query_grad,
        key_grad,
        value_grad,
        out_grad,
        gains[1],
        router_grad,
        gate_grad,
        up_grad,
        down_grad,
    )


def solution(mesh):
    placed = (
        P(("dp", "expert"), None),
        P(),
        P(None, "tensor"),
        P(None, "tensor"),
        P(None, "tensor"),
        P("tensor", None),
        P(),
        P(),
        P("expert", None, "tensor"),
        P("expert", None, "tensor"),
        P("expert", "tensor", None),
        P(("dp", "expert"), None),
        P(("dp", "expert"), None),
    )
    sequences = mesh.shape["dp"] * mesh.shape["expert"]
    few = sequences * SEQUENCE_LENGTH <= GATHER_ROWS
    few = few and mesh.shape["tensor"] > 1 and mesh.shape["expert"] == 2
    return jax.shard_map(
        gather_plan if few else reduce_plan,
        mesh=mesh,
        in_specs=placed,
        out_specs=(
            P(("dp", "expert"), None),
            P(("dp", "expert"), None),
            P(("dp", "expert")),
            P(("dp", "expert"), "tensor"),
            P(("dp", "expert"), "tensor"),
            P(("dp", "expert"), "tensor"),
            P("tensor", ("dp", "expert")),
            P(("dp", "expert")),
            P(("dp", "expert"), None),
            P("expert", "dp", "tensor"),
            P("expert", "dp", "tensor"),
            P("expert", "tensor", "dp"),
        ),
        check_vma=False,
    )
```

```python
import functools
import math

import jax
import jax.numpy as jnp
import numpy as np
from jax import lax
from jax.experimental import pallas as pl
from jax.experimental.pallas import tpu as pltpu
from jax.sharding import PartitionSpec as P

HEAD_SIZE = 64
SEQUENCE_LENGTH = 256
CAP = 64


EPSILON = 1e-06
ROPE_BASE = 10000.0
BLOCK_ROWS = 512


def split_up(x, dim, count):
    dims = x.shape
    tiles = x.reshape(*dims[:dim], count, dims[dim] // count, *dims[dim + 1 :])
    return jnp.moveaxis(tiles, dim, 0)


def sum_at_owner(x, axis, dim):
    tiles = split_up(x, dim, lax.axis_size(axis))
    arrived = lax.all_to_all(tiles, axis, split_axis=0, concat_axis=0, tiled=True)
    return arrived.astype(jnp.float32).sum(axis=0)


def side_by_side(arrays, axis, dim, along):
    both = jnp.concatenate(arrays, axis=along)
    filled, at, outs = (sum_at_owner(both, axis, dim), 0, [])
    for a in arrays:
        outs.append(lax.slice_in_dim(filled, at, at + a.shape[along], axis=along))
        at += a.shape[along]
    return tuple(outs)


def sent_together(arrays, axis, dim, along):
    widths = [math.prod(a.shape[along:]) for a in arrays]
    both = jnp.concatenate(
        [a.reshape(*a.shape[:along], w) for a, w in zip(arrays, widths)], axis=along
    )
    filled = sum_at_owner(both, axis, dim)
    tiles = jnp.split(filled, [sum(widths[:k]) for k in range(1, len(widths))], axis=along)
    return tuple(
        (b.reshape(*filled.shape[:along], *a.shape[along:]) for a, b in zip(arrays, tiles))
    )


def rms_scale(hidden):
    return lax.rsqrt(jnp.mean(hidden * hidden, axis=-1, keepdims=True) + EPSILON)


def norm_back(hidden, scaling, gain_vec, grad_out):
    weighted = grad_out * gain_vec
    gain_grad = jnp.sum(grad_out * hidden * scaling, axis=0)
    inner_mean = jnp.mean(weighted * hidden, axis=-1, keepdims=True)
    return (scaling * weighted - hidden * (scaling * scaling * scaling) * inner_mean, gain_grad)


def rope_tables(positions, head_dim):
    half_dim = head_dim // 2
    frequency = jnp.exp(
        jnp.arange(half_dim, dtype=jnp.float32) * (-2.0 * math.log(ROPE_BASE) / head_dim)
    )
    angles = positions[:, None] * frequency[None, :]
    return (jnp.cos(angles), jnp.sin(angles))


def apply_rotary(vectors, cosine_table, sine_component):
    half_dim = vectors.shape[-1] // 2
    first_half = vectors[..., :half_dim]
    second_half = vectors[..., half_dim:]
    cos_rows = cosine_table[:, None, :]
    sin_rows = sine_component[:, None, :]
    return jnp.concatenate(
        [
            first_half * cos_rows - second_half * sin_rows,
            first_half * sin_rows + second_half * cos_rows,
        ],
        axis=-1,
    )


def slot_table(route_ids, expert_count, capacity):
    number_of_rows, top_count = route_ids.shape
    flat_ids = route_ids.reshape(-1)
    one_hot = (flat_ids[:, None] == jnp.arange(expert_count, dtype=jnp.int32)[None, :]).astype(
        jnp.int32
    )
    earlier = jnp.cumsum(one_hot, axis=0) - one_hot
    slot_ids = jnp.sum(earlier * one_hot, axis=1)
    slot_where = flat_ids * capacity + slot_ids
    pick_ids = jnp.arange(number_of_rows * top_count, dtype=jnp.int32)
    token_of = (
        jnp.full((expert_count * capacity,), number_of_rows, jnp.int32)
        .at[slot_where]
        .set(pick_ids // top_count)
    )
    pick_of = (
        jnp.full((expert_count * capacity,), number_of_rows * top_count, jnp.int32)
        .at[slot_where]
        .set(pick_ids)
    )
    return (slot_where, token_of, pick_of)


def block_scores(query_rows, key_rows, query_group_width):
    block_len = query_rows.shape[0]
    key_count, kv_heads, head_dim = key_rows.shape
    grouped = query_rows.reshape(block_len, kv_heads, query_group_width, head_dim)
    scores = jnp.einsum(
        "qhgd,khd->hgqk", grouped, key_rows, preferred_element_type=jnp.float32
    ) * head_dim ** (-0.5)
    row_pos = jnp.arange(block_len, dtype=jnp.int32)[:, None]
    col_pos = jnp.arange(key_count, dtype=jnp.int32)[None, :]
    return (jnp.where(col_pos <= row_pos, scores, -1e30), grouped)


def sequence_forward(query_rows, key_rows, value_rows, query_group_width):
    length, kv_heads, head_dim = key_rows.shape
    block_len = min(BLOCK_ROWS, length)
    scores, grouped = block_scores(query_rows, key_rows, query_group_width)
    largest = jnp.max(scores, axis=-1, keepdims=True)
    log_total = largest + jnp.log(jnp.sum(jnp.exp(scores - largest), axis=-1, keepdims=True))
    weights = jnp.exp(scores - log_total).astype(jnp.bfloat16)
    attended = jnp.einsum("hgqk,khd->qhgd", weights, value_rows, preferred_element_type=jnp.float32)
    outputs = attended.reshape(block_len, -1, head_dim).astype(jnp.bfloat16)
    return (outputs, log_total)


def sequence_backward(
    query_rows, key_rows, value_rows, attended, log_total, d_attended, query_group_width
):
    length, kv_heads, head_dim = key_rows.shape
    block_len = min(BLOCK_ROWS, length)
    scale_factor = head_dim ** (-0.5)
    key_gradient = jnp.zeros((length, kv_heads, head_dim), jnp.float32)
    value_gradient = jnp.zeros((length, kv_heads, head_dim), jnp.float32)
    scores, grouped = block_scores(query_rows, key_rows, query_group_width)
    weights = jnp.exp(scores - log_total)
    d_grouped = d_attended.reshape(block_len, kv_heads, query_group_width, head_dim)
    o_grouped = attended.reshape(block_len, kv_heads, query_group_width, head_dim)
    delta = jnp.sum(d_grouped.astype(jnp.float32) * o_grouped.astype(jnp.float32), axis=-1)
    delta = jnp.transpose(delta, (1, 2, 0))[..., None]
    d_weights = jnp.einsum(
        "qhgd,khd->hgqk", d_grouped, value_rows, preferred_element_type=jnp.float32
    )
    d_scores = (weights * (d_weights - delta)).astype(jnp.bfloat16)
    block_query = (
        jnp.einsum("hgqk,khd->qhgd", d_scores, key_rows, preferred_element_type=jnp.float32)
        * scale_factor
    )
    query_parts = block_query.reshape(block_len, -1, head_dim)
    key_gradient = key_gradient.at[:block_len].add(
        jnp.einsum("hgqk,qhgd->khd", d_scores, grouped, preferred_element_type=jnp.float32)
        * scale_factor
    )
    value_gradient = value_gradient.at[:block_len].add(
        jnp.einsum(
            "hgqk,qhgd->khd",
            weights.astype(jnp.bfloat16),
            d_grouped,
            preferred_element_type=jnp.float32,
        )
    )
    return (query_parts, key_gradient, value_gradient)


def reduce_plan(
    tokens,
    gain_attn,
    w_query,
    key_projection,
    value_projection,
    w_out,
    gain_moe,
    w_router,
    w_gate,
    w_up,
    w_down,
    routes,
    cotangent,
):
    number_of_rows, model_width = tokens.shape
    head_dim = HEAD_SIZE
    query_heads = w_query.shape[1] // head_dim
    kv_heads = key_projection.shape[1] // head_dim
    query_group_width = query_heads // kv_heads
    expert_count = w_router.shape[1]
    local_experts = w_gate.shape[0]
    source_count = expert_count // local_experts
    capacity = CAP
    top_count = routes.shape[1]
    resid = tokens.astype(jnp.float32)
    scale_one = rms_scale(resid)
    first_normalized = (resid * scale_one * gain_attn).astype(jnp.bfloat16)
    positions = (jnp.arange(number_of_rows, dtype=jnp.int32) % SEQUENCE_LENGTH).astype(jnp.float32)
    cosine_table, sine_component = rope_tables(positions, head_dim)
    q_lin = jnp.dot(first_normalized, w_query, preferred_element_type=jnp.float32).reshape(
        number_of_rows, query_heads, head_dim
    )
    linear_key = jnp.dot(
        first_normalized, key_projection, preferred_element_type=jnp.float32
    ).reshape(number_of_rows, kv_heads, head_dim)
    value_reduced = (
        jnp.dot(first_normalized, value_projection, preferred_element_type=jnp.float32)
        .astype(jnp.bfloat16)
        .reshape(number_of_rows, kv_heads, head_dim)
    )
    q_rot = apply_rotary(q_lin, cosine_table, sine_component).astype(jnp.bfloat16)
    rotated_key = apply_rotary(linear_key, cosine_table, sine_component).astype(jnp.bfloat16)
    attended, log_total = sequence_forward(q_rot, rotated_key, value_reduced, query_group_width)
    flat_att = attended.reshape(number_of_rows, query_heads * head_dim)
    attn_part = jnp.dot(flat_att, w_out, preferred_element_type=jnp.float32)
    hidden1 = resid + lax.psum(attn_part.astype(jnp.bfloat16), "tensor").astype(jnp.float32)
    scale_two = rms_scale(hidden1)
    normed2 = (hidden1 * scale_two * gain_moe).astype(jnp.bfloat16)
    logits = jnp.dot(normed2, w_router, preferred_element_type=jnp.float32)
    chosen = jnp.take_along_axis(logits, routes, axis=1)
    gate_probs = jax.nn.softmax(chosen, axis=-1)
    slot_where, token_of, pick_of = slot_table(routes, expert_count, capacity)
    normed_pad = jnp.concatenate([normed2, jnp.zeros((1, model_width), jnp.bfloat16)], axis=0)
    outgoing = normed_pad[token_of].reshape(expert_count, capacity, model_width)
    received = lax.all_to_all(outgoing, "expert", split_axis=0, concat_axis=0, tiled=True)
    arrived = received.reshape(source_count, local_experts, capacity, model_width)
    gate_pre = jnp.einsum("secd,edh->sech", arrived, w_gate, preferred_element_type=jnp.float32)
    up_pre = jnp.einsum("secd,edh->sech", arrived, w_up, preferred_element_type=jnp.float32)
    sig_gate = jax.nn.sigmoid(gate_pre)
    activated = gate_pre * sig_gate
    hid_low = (activated * up_pre).astype(jnp.bfloat16)
    expert_out = jnp.einsum(
        "sech,ehd->secd", hid_low, w_down, preferred_element_type=jnp.float32
    ).astype(jnp.bfloat16)
    returned = lax.all_to_all(
        expert_out.reshape(expert_count, capacity, model_width),
        "expert",
        split_axis=0,
        concat_axis=0,
        tiled=True,
    )
    picked = returned.reshape(expert_count * capacity, model_width)[slot_where].reshape(
        number_of_rows, top_count, model_width
    )
    moe_part = jnp.zeros((number_of_rows, model_width), jnp.float32)
    for choice_index in range(top_count):
        moe_part = (
            moe_part
            + picked[:, choice_index].astype(jnp.float32)
            * gate_probs[:, choice_index : choice_index + 1]
        )
    moe_out = lax.psum(moe_part.astype(jnp.bfloat16), "tensor").astype(jnp.float32)
    output = (hidden1 + moe_out).astype(jnp.bfloat16)
    grad = cotangent.astype(jnp.float32)
    gate_dot = jnp.einsum("rjd,rd->rj", picked, cotangent, preferred_element_type=jnp.float32)
    grad_pad = jnp.concatenate([cotangent, jnp.zeros((1, model_width), jnp.bfloat16)], axis=0)
    gate_pad = jnp.concatenate([gate_probs.reshape(-1), jnp.zeros((1,), jnp.float32)], axis=0)
    sent_grad = (grad_pad[token_of].astype(jnp.float32) * gate_pad[pick_of][:, None]).astype(
        jnp.bfloat16
    )
    sent_grad = sent_grad.reshape(expert_count, capacity, model_width)
    grad_received = lax.all_to_all(sent_grad, "expert", split_axis=0, concat_axis=0, tiled=True)
    arrived_grad = grad_received.reshape(source_count, local_experts, capacity, model_width)
    d_hid = jnp.einsum("secd,ehd->sech", arrived_grad, w_down, preferred_element_type=jnp.float32)
    down_local = jnp.einsum(
        "sech,secd->ehd", hid_low, arrived_grad, preferred_element_type=jnp.float32
    )
    d_gate = (d_hid * up_pre * sig_gate * (1.0 + gate_pre * (1.0 - sig_gate))).astype(jnp.bfloat16)
    d_up = (d_hid * activated).astype(jnp.bfloat16)
    gate_local = jnp.einsum("secd,sech->edh", arrived, d_gate, preferred_element_type=jnp.float32)
    up_local = jnp.einsum("secd,sech->edh", arrived, d_up, preferred_element_type=jnp.float32)
    back_rows = jnp.einsum("sech,edh->secd", d_gate, w_gate, preferred_element_type=jnp.float32)
    back_rows = (
        back_rows + jnp.einsum("sech,edh->secd", d_up, w_up, preferred_element_type=jnp.float32)
    ).astype(jnp.bfloat16)
    came_back = lax.all_to_all(
        back_rows.reshape(expert_count, capacity, model_width),
        "expert",
        split_axis=0,
        concat_axis=0,
        tiled=True,
    )
    back_picked = came_back.reshape(expert_count * capacity, model_width)[slot_where].reshape(
        number_of_rows, top_count, model_width
    )
    back_part = jnp.zeros((number_of_rows, model_width), jnp.float32)
    for choice_index in range(top_count):
        back_part = back_part + back_picked[:, choice_index].astype(jnp.float32)
    back_total, dgate = (
        lax.psum(back_part.astype(jnp.bfloat16), "tensor").astype(jnp.float32),
        lax.psum(gate_dot.astype(jnp.bfloat16), "tensor").astype(jnp.float32),
    )
    inner_sum = jnp.sum(gate_probs * dgate, axis=1, keepdims=True)
    d_chosen = gate_probs * (dgate - inner_sum)
    matches = routes[:, :, None] == jnp.arange(expert_count, dtype=jnp.int32)[None, None, :]
    d_logits = jnp.sum(jnp.where(matches, d_chosen[:, :, None], 0.0), axis=1).astype(jnp.bfloat16)
    router_local = jnp.dot(normed2.T, d_logits, preferred_element_type=jnp.float32)
    d_normed2 = back_total + jnp.dot(d_logits, w_router.T, preferred_element_type=jnp.float32)
    d_hidden_part, gain_moe_local = norm_back(hidden1, scale_two, gain_moe, d_normed2)
    d_hidden1 = grad + d_hidden_part
    d_mixed = d_hidden1.astype(jnp.bfloat16)
    out_local = jnp.dot(flat_att.T, d_mixed, preferred_element_type=jnp.float32)
    d_att = (
        jnp.dot(d_mixed, w_out.T, preferred_element_type=jnp.float32)
        .astype(jnp.bfloat16)
        .reshape(number_of_rows, query_heads, head_dim)
    )
    dq_rot, rotated_key_gradient, dv_rows = sequence_backward(
        q_rot, rotated_key, value_reduced, attended, log_total, d_att, query_group_width
    )
    d_query = (
        apply_rotary(dq_rot, cosine_table, -sine_component)
        .astype(jnp.bfloat16)
        .reshape(number_of_rows, query_heads * head_dim)
    )
    key_gradient = (
        apply_rotary(rotated_key_gradient, cosine_table, -sine_component)
        .astype(jnp.bfloat16)
        .reshape(number_of_rows, kv_heads * head_dim)
    )
    value_gradient = dv_rows.astype(jnp.bfloat16).reshape(number_of_rows, kv_heads * head_dim)
    query_local = jnp.dot(first_normalized.T, d_query, preferred_element_type=jnp.float32)
    key_local = jnp.dot(first_normalized.T, key_gradient, preferred_element_type=jnp.float32)
    value_local = jnp.dot(first_normalized.T, value_gradient, preferred_element_type=jnp.float32)
    d_normed_part = jnp.dot(d_query, w_query.T, preferred_element_type=jnp.float32)
    d_normed_part = d_normed_part + jnp.dot(
        key_gradient, key_projection.T, preferred_element_type=jnp.float32
    )
    d_normed_part = d_normed_part + jnp.dot(
        value_gradient, value_projection.T, preferred_element_type=jnp.float32
    )
    d_normed1 = lax.psum(d_normed_part.astype(jnp.bfloat16), "tensor").astype(jnp.float32)
    d_resid_part, gain_attn_local = norm_back(resid, scale_one, gain_attn, d_normed1)
    input_grad = (d_hidden1 + d_resid_part).astype(jnp.bfloat16)
    gate_grad, up_grad, down_grad = (
        lax.psum_scatter(
            gate_local.astype(jnp.bfloat16), "dp", scatter_dimension=1, tiled=True
        ).astype(jnp.float32),
        lax.psum_scatter(
            up_local.astype(jnp.bfloat16), "dp", scatter_dimension=1, tiled=True
        ).astype(jnp.float32),
        lax.psum_scatter(
            down_local.astype(jnp.bfloat16), "dp", scatter_dimension=2, tiled=True
        ).astype(jnp.float32),
    )
    query_grad, key_grad, value_grad, out_grad, router_grad, gain_attn_grad, gain_moe_grad = (
        *side_by_side(
            (
                query_local.astype(jnp.bfloat16),
                key_local.astype(jnp.bfloat16),
                value_local.astype(jnp.bfloat16),
            ),
            ("dp", "expert"),
            0,
            1,
        ),
        sum_at_owner(out_local.astype(jnp.bfloat16), ("dp", "expert"), 1),
        *sent_together(
            (
                router_local.astype(jnp.bfloat16),
                gain_attn_local.astype(jnp.bfloat16),
                gain_moe_local.astype(jnp.bfloat16),
            ),
            ("dp", "expert"),
            0,
            1,
        ),
    )
    return (
        output,
        input_grad,
        gain_attn_grad,
        query_grad,
        key_grad,
        value_grad,
        out_grad,
        gain_moe_grad,
        router_grad,
        gate_grad,
        up_grad,
        down_grad,
    )


GATHER_ROWS = 4096
MESH = pl.DeviceIdType.MESH
VMEM = pl.BlockSpec(memory_space=pltpu.VMEM)
ANY = pl.BlockSpec(memory_space=pl.ANY)
EXTRA = 128
VMEM_LIMIT = 60 * 2**20
F32, BF16 = jnp.float32, jnp.bfloat16


def dot(a, b):
    return jnp.dot(a, b, preferred_element_type=F32)


def dot_nt(a, b):
    return lax.dot_general(a, b, (((1,), (1,)), ((), ())), preferred_element_type=F32)


def dot_tn(a, b):
    return lax.dot_general(a, b, (((0,), (0,)), ((), ())), preferred_element_type=F32)


def ds(index, size):
    return pl.ds(pl.multiple_of(index * size, size), size)


class Peers:
    def __init__(self, dp, tp, send_sem, recv_sem):
        self.z, self.c, self.t = (lax.axis_index(a) for a in ("dp", "expert", "tensor"))
        self.dp, self.tp = dp, tp
        self.send_sem, self.recv_sem = send_sem, recv_sem
        self.used = 0
        self.open = []

    def tensor(self, k):
        return (self.z, self.c, lax.rem(self.t + k, self.tp))

    def near(self, axis):
        row, col = self.t // 2, self.t % 2
        index = row * 2 + (1 - col) if axis == 0 else (1 - row) * 2 + col
        return (self.z, self.c, index)

    def plane(self, k):
        return (lax.rem(self.z + k, self.dp), self.c, self.t)

    def partner(self):
        return (self.z, 1 - self.c, self.t)

    def greet(self):
        barrier = pltpu.get_barrier_semaphore()
        everyone = [self.tensor(k) for k in range(1, self.tp)]
        everyone += [self.plane(k) for k in range(1, self.dp)] + [self.partner()]
        for peer in everyone:
            pl.semaphore_signal(barrier, inc=1, device_id=peer, device_id_type=MESH)
        pl.semaphore_wait(barrier, len(everyone))

    def number(self, count):
        first = self.used
        self.used += count
        return first

    def make(self, src, dst, number, device):
        return pltpu.make_async_remote_copy(
            src_ref=src,
            dst_ref=dst,
            send_sem=self.send_sem.at[number],
            recv_sem=self.recv_sem.at[number],
            device_id=device,
            device_id_type=MESH,
        )

    def to(self, src, dst, device):
        copy = self.make(src, dst, self.number(1), device)
        copy.start()
        self.open.append(copy)
        return copy

    def keep(self, src, dst, sem):
        copy = pltpu.make_async_copy(src, dst, sem)
        copy.start()
        return copy

    def drain(self):
        for copy in self.open:
            copy.wait_send()


def arrived(copies):
    for copy in copies:
        copy.wait_recv()


def rotate(u, rope_ref, sign):
    width = u.shape[1]
    tiles = []
    for at in range(0, width, 128):
        v = u[:, at : at + 128]
        side = pltpu.roll(v, 96, 1) * rope_ref[1] + pltpu.roll(v, 32, 1) * rope_ref[2]
        tiles.append(v * rope_ref[0] + sign * side)
    return tiles[0] if len(tiles) == 1 else jnp.concatenate(tiles, axis=1)


def inverse_rms(u):
    return lax.rsqrt(jnp.mean(u * u, axis=-1, keepdims=True) + EPSILON)


def causal(length):
    row = lax.broadcasted_iota(jnp.int32, (length, length), 0)
    col = lax.broadcasted_iota(jnp.int32, (length, length), 1)
    return col <= row


def forward_kernel(
    dp,
    tp,
    tok_ref,
    cot_ref,
    routes_ref,
    ga_ref,
    gm_ref,
    wq_ref,
    wk_ref,
    wv_ref,
    wo_ref,
    rope_ref,
    x_ref,
    g_ref,
    gz_ref,
    h1_ref,
    n1_ref,
    qkv_ref,
    att_ref,
    lse_ref,
    part_buf,
    rs_buf,
    send_sem,
    recv_sem,
):
    net = Peers(dp, tp, send_sem, recv_sem)
    z, c, t = net.z, net.c, net.t
    length, model = tok_ref.shape
    own = length // tp
    q_width, kv_width = wq_ref.shape[1], wk_ref.shape[1]
    group = q_width // kv_width
    net.greet()
    seq_rows = ds(c, length)
    got_g = [net.to(cot_ref, g_ref.at[seq_rows], net.partner())]
    for k in range(1, dp):
        got_g.append(net.to(cot_ref.at[ds(t, own)], gz_ref.at[dp - 1 - k], net.plane(k)))
    g_ref[seq_rows, :] = cot_ref[...]

    resid = tok_ref[...].astype(F32)
    n1 = (resid * inverse_rms(resid) * ga_ref[...].reshape(1, -1)).astype(BF16)
    n1_ref[...] = n1
    qkv_ref[:, :q_width] = rotate(dot(n1, wq_ref[...]), rope_ref, 1.0).astype(BF16)
    qkv_ref[:, q_width : q_width + kv_width] = rotate(dot(n1, wk_ref[...]), rope_ref, 1.0).astype(BF16)
    qkv_ref[:, q_width + kv_width :] = dot(n1, wv_ref[...]).astype(BF16)

    seen = causal(length)
    lane = lax.broadcasted_iota(jnp.int32, lse_ref.shape, 1)
    lse_all = jnp.zeros(lse_ref.shape, F32)
    scale = HEAD_SIZE ** (-0.5)
    for h in range(q_width // HEAD_SIZE):
        kv = h // group
        at_k = q_width + kv * HEAD_SIZE
        at_v = q_width + kv_width + kv * HEAD_SIZE
        q = qkv_ref[:, h * HEAD_SIZE : (h + 1) * HEAD_SIZE]
        key = qkv_ref[:, at_k : at_k + HEAD_SIZE]
        val = qkv_ref[:, at_v : at_v + HEAD_SIZE]
        s = jnp.where(seen, dot_nt(q, key) * scale, -1e30)
        top = jnp.max(s, axis=-1, keepdims=True)
        lse = top + jnp.log(jnp.sum(jnp.exp(s - top), axis=-1, keepdims=True))
        prob = jnp.exp(s - lse).astype(BF16)
        att_ref[:, h * HEAD_SIZE : (h + 1) * HEAD_SIZE] = dot(prob, val).astype(BF16)
        lse_all = jnp.where(lane == h, lse, lse_all)
    lse_ref[...] = lse_all
    part_buf[...] = dot(att_ref[...], wo_ref[...]).astype(BF16)

    got = []
    for k in range(1, tp):
        block = part_buf.at[ds(lax.rem(t + k, tp), own)]
        got.append(net.to(block, rs_buf.at[k - 1], net.tensor(k)))
    total = tok_ref[ds(t, own), :].astype(F32) + part_buf[ds(t, own), :].astype(F32)
    picked = routes_ref[ds(t, own), :]
    ids = lax.broadcasted_iota(jnp.int32, (own, EXTRA), 1)
    chosen = picked[:, 0:1] == ids
    for j in range(1, picked.shape[1]):
        chosen = chosen | (picked[:, j : j + 1] == ids)
    arrived(got)
    for k in range(1, tp):
        total = total + rs_buf[k - 1].astype(F32)
    h1_ref[...] = total
    n2 = (total * inverse_rms(total) * gm_ref[...].reshape(1, -1)).astype(BF16)
    mine = ds(c * tp + t, own)
    x_ref[mine, :model] = n2
    x_ref[mine, model:] = jnp.where(chosen, 1.0, 0.0).astype(BF16)
    got = [net.to(x_ref.at[mine], x_ref.at[mine], net.tensor(k)) for k in range(1, tp)]
    arrived(got)
    got = [net.to(x_ref.at[seq_rows], x_ref.at[seq_rows], net.partner())]
    arrived(got_g + got)
    net.drain()


def forward(dp, tp, tokens, cotangent, routes, ga, gm, wq, wk, wv, wo, rope):
    length, model = tokens.shape
    own, wide = length // tp, model + EXTRA
    widths = wq.shape[1] + wk.shape[1] + wv.shape[1]
    copies = 2 + (dp - 1) + 2 * (tp - 1)
    shapes = [
        ((2 * length, wide), BF16),
        ((2 * length, model), BF16),
        ((dp - 1, own, model), BF16),
        ((own, model), F32),
        ((length, model), BF16),
        ((length, widths), BF16),
        ((length, wq.shape[1]), BF16),
        ((length, 128), F32),
    ]
    return pl.pallas_call(
        functools.partial(forward_kernel, dp, tp),
        out_shape=[jax.ShapeDtypeStruct(*s) for s in shapes],
        in_specs=[VMEM] * 10,
        out_specs=[VMEM] * len(shapes),
        scratch_shapes=[
            pltpu.VMEM((length, model), BF16),
            pltpu.VMEM((tp - 1, own, model), BF16),
            pltpu.SemaphoreType.DMA((copies,)),
            pltpu.SemaphoreType.DMA((copies,)),
        ],
        compiler_params=pltpu.CompilerParams(
            collective_id=0, has_side_effects=True, vmem_limit_bytes=VMEM_LIMIT
        ),
        name="forward",
    )(tokens, cotangent, routes, ga, gm, wq, wk, wv, wo, rope)


def gates_of(x_ref, wr_ref, model):
    logits = dot(x_ref[:, :model], wr_ref[...])
    chosen = x_ref[:, model:].astype(F32) > 0.5
    top = jnp.max(jnp.where(chosen, logits, -jnp.inf), axis=1, keepdims=True)
    weight = jnp.where(chosen, jnp.exp(jnp.where(chosen, logits - top, 0.0)), 0.0)
    return weight / jnp.sum(weight, axis=1, keepdims=True)


def store_split(gates, split_ref):
    high = gates.astype(BF16)
    split_ref[:, :EXTRA] = high
    split_ref[:, EXTRA:] = (gates - high.astype(F32)).astype(BF16)


def pair_of_gates(split, first, width):
    k_pos = lax.broadcasted_iota(jnp.int32, (2 * EXTRA, 2 * width), 0)
    l_pos = lax.broadcasted_iota(jnp.int32, (2 * EXTRA, 2 * width), 1)
    pick = jnp.where(k_pos % EXTRA == first + l_pos // width, 1.0, 0.0).astype(BF16)
    return dot(split, pick)


def swiglu(both, dh, gate):
    width = dh.shape[1]
    gate_pre, up_pre = both[:, :width], both[:, width:]
    sig = jax.nn.sigmoid(gate_pre)
    act = gate_pre * sig
    hid = act * up_pre
    d_hid = dh * gate
    d_gate = d_hid * up_pre * sig * (1.0 + gate_pre * (1.0 - sig))
    return hid, (hid * gate).astype(BF16), d_gate.astype(BF16), (d_hid * act).astype(BF16)


def plane_kernel(
    dp,
    tp,
    x_ref,
    g_ref,
    gz_ref,
    wr_ref,
    wg_ref,
    wu_ref,
    wd_ref,
    xr_ref,
    gr_ref,
    moe_ref,
    back_ref,
    dgate_ref,
    gates_ref,
    ghid_ref,
    dgp_ref,
    dup_ref,
    split,
    moe_acc,
    back_acc,
    send_sem,
    recv_sem,
    keep_sem,
):
    step, last = pl.program_id(0), pl.num_programs(0) - 1
    net = Peers(dp, tp, send_sem, recv_sem)
    z, c, t = net.z, net.c, net.t
    rows, model = g_ref.shape
    length = rows // 2
    own = length // tp
    width = wg_ref.shape[2]
    others = range(1, dp)

    def block(plane, core, tensor):
        return ds((plane * 2 + core) * tp + tensor, own)

    def link(src, dst, device):
        return net.make(src, dst, net.number(1), device)

    def start(copies):
        for copy in copies:
            copy.start()

    mine = ds(c * tp + t, own)
    near = [net.near(axis) for axis in range(2)]
    far = tp - 1 - t
    half = own // 2

    def piece(plane, tensor, part_of):
        at = (((plane * 2 + c) * tp + tensor) * 2 + part_of) * half
        return pl.ds(pl.multiple_of(at, half), half)

    def spread(ref, sources):
        direct = [
            link(sources[p - 1], ref.at[block(p, c, t)], near[axis])
            for p in others
            for axis in range(2)
        ]
        relay = []
        for p in others:
            for axis in range(2):
                rows = piece(p, near[axis][2], axis)
                relay.append(link(ref.at[rows], ref.at[rows], near[1 - axis]))
        to_core = [link(sources[p - 1], ref.at[block(p, c, t)], net.partner()) for p in others]
        near_core, far_core = [], []
        for p in others:
            for axis in range(2):
                rows = block(p, c, near[axis][2])
                near_core.append(link(ref.at[rows], ref.at[rows], net.partner()))
            rows = block(p, c, far)
            far_core.append(link(ref.at[rows], ref.at[rows], net.partner()))
        return direct, relay, to_core, near_core, far_core

    x_z = [link(x_ref.at[mine], xr_ref.at[block(dp - k, c, t)], net.plane(k)) for k in others]
    g_direct, g_relay, g_core, g_near, g_far = spread(gr_ref, [gz_ref.at[p - 1] for p in others])
    x_direct, x_relay, x_core, x_near, x_far = spread(
        xr_ref, [xr_ref.at[block(p, c, t)] for p in others]
    )
    kept = [
        pltpu.make_async_copy(x_ref, xr_ref.at[pl.ds(0, rows)], keep_sem.at[0]),
        pltpu.make_async_copy(g_ref, gr_ref.at[pl.ds(0, rows)], keep_sem.at[1]),
    ] + [
        pltpu.make_async_copy(gz_ref.at[p - 1], gr_ref.at[block(p, c, t)], keep_sem.at[1 + p])
        for p in others
    ]

    @pl.when(step == 0)
    def _():
        net.greet()
        start(x_z + g_direct + g_core)
        start(kept)
        moe_acc[...] = jnp.zeros_like(moe_acc)
        back_acc[...] = jnp.zeros_like(back_acc)
        dgate_ref[...] = jnp.zeros_like(dgate_ref)
        gates = gates_of(x_ref, wr_ref, model)
        gates_ref[...] = gates
        store_split(gates, split)

    @pl.when(step == 3)
    def _():
        arrived(g_direct)
        start(g_relay + g_near)

    @pl.when(step == 5)
    def _():
        arrived(x_z)
        start(x_direct + x_core)

    @pl.when(step == 6)
    def _():
        arrived(g_relay)
        start(g_far)

    @pl.when(step == 8)
    def _():
        arrived(x_direct)
        start(x_relay + x_near)

    first = c * (2 * pl.num_programs(0)) + 2 * step
    gate_pair = pair_of_gates(split[...], first, width)
    wd_pair = wd_ref[...].reshape(2 * width, model)
    dh_pair = dot_nt(g_ref[...], wd_pair)
    lane = lax.broadcasted_iota(jnp.int32, dgate_ref.shape, 1)
    for k in range(2):
        lanes = slice(k * width, (k + 1) * width)
        w_both = jnp.concatenate([wg_ref[k], wu_ref[k]], axis=1)
        both = dot(x_ref[:, :model], w_both)
        dh = dh_pair[:, lanes]
        hid, ghid, dgp, dup = swiglu(both, dh, gate_pair[:, lanes])
        ghid_ref[:, lanes] = ghid
        dgp_ref[:, lanes] = dgp
        dup_ref[:, lanes] = dup
        row_sum = jnp.sum(hid * dh, axis=1, keepdims=True)
        dgate_ref[...] += jnp.where(lane == first + k, row_sum, 0.0)
        back_acc[...] += dot_nt(jnp.concatenate([dgp, dup], axis=1), w_both)
    moe_acc[...] += dot(ghid_ref[...], wd_pair)

    @pl.when(step == last)
    def _():
        moe_ref[...] = moe_acc[...].astype(BF16)
        back_ref[...] = back_acc[...].astype(BF16)
        for copy in kept:
            copy.wait()
        arrived(g_core + g_near + g_far + x_core + x_relay)
        start(x_far)
        arrived(x_near + x_far)
        for copy in x_z + g_direct + g_relay + g_core + g_near + g_far:
            copy.wait_send()
        for copy in x_direct + x_relay + x_core + x_near + x_far:
            copy.wait_send()


def plane_experts(dp, tp, x, g, gz, wr, w_gate, w_up, w_down):
    rows, model = g.shape
    length = rows // 2
    count, _, width = w_gate.shape
    all_rows = rows * dp
    others = dp - 1
    copies = others + 2 * 8 * others

    def whole(a):
        shape = a.shape
        return pl.BlockSpec(shape, lambda i: (0,) * len(shape), pipeline_mode=pl.Buffered(1))

    by_pair = lambda shape: pl.BlockSpec((2,) + shape, lambda i: (i, 0, 0))
    saved = pl.BlockSpec((rows, 2 * width), lambda i: (0, i))
    shapes = [
        ((all_rows, x.shape[1]), BF16),
        ((all_rows, model), BF16),
        ((rows, model), BF16),
        ((rows, model), BF16),
        ((rows, EXTRA), F32),
        ((rows, EXTRA), F32),
        ((rows, count * width), BF16),
        ((rows, count * width), BF16),
        ((rows, count * width), BF16),
    ]
    shapes = [jax.ShapeDtypeStruct(*s) for s in shapes]
    return pl.pallas_call(
        functools.partial(plane_kernel, dp, tp),
        grid=(count // 2,),
        out_shape=shapes,
        in_specs=[whole(x), whole(g), whole(gz), whole(wr)]
        + [by_pair((model, width)), by_pair((model, width)), by_pair((width, model))],
        out_specs=[ANY, ANY] + [whole(s) for s in shapes[2:6]] + [saved] * 3,
        scratch_shapes=[
            pltpu.VMEM((rows, 2 * EXTRA), BF16),
            pltpu.VMEM((rows, model), F32),
            pltpu.VMEM((rows, model), F32),
            pltpu.SemaphoreType.DMA((copies,)),
            pltpu.SemaphoreType.DMA((copies,)),
            pltpu.SemaphoreType.DMA((2 + others,)),
        ],
        compiler_params=pltpu.CompilerParams(
            collective_id=1, has_side_effects=True, vmem_limit_bytes=VMEM_LIMIT
        ),
        name="plane_experts",
    )(x, g, gz, wr, w_gate, w_up, w_down)


def backward_kernel(
    dp,
    tp,
    back_ref,
    moe_ref,
    dgate_ref,
    gates_ref,
    h1_ref,
    tok_ref,
    cot_ref,
    ga_ref,
    gm_ref,
    wr_ref,
    wq_ref,
    wk_ref,
    wv_ref,
    wo_ref,
    qkv_ref,
    att_ref,
    lse_ref,
    n1_ref,
    rope_ref,
    xr_ref,
    gr_ref,
    wg_ref,
    wu_ref,
    wd_ref,
    out_ref,
    in_ref,
    dl_all,
    qkv_grad_ref,
    o_grad_ref,
    gains_ref,
    ghid_ref,
    dgp_ref,
    dup_ref,
    x_rest,
    g_rest,
    split,
    pair_b,
    pair_m,
    pair_d,
    sum_b,
    sum_m,
    sum_d,
    rs_b,
    rs_m,
    rs_d,
    dh1_buf,
    da_buf,
    dl_buf,
    d_buf,
    do_buf,
    part_buf,
    rs_3,
    gain_buf,
    gain_t,
    gain_z,
    gain_zs,
    gain_c,
    out_buf,
    in_buf,
    q_part,
    q_pair,
    q_sum,
    q_in,
    o_part,
    o_pair,
    o_sum,
    o_in,
    send_sem,
    recv_sem,
    keep_sem,
):
    step, last = pl.program_id(0), pl.num_programs(0) - 1
    net = Peers(dp, tp, send_sem, recv_sem)
    z, c, t = net.z, net.c, net.t
    length, model = tok_ref.shape
    own = length // tp
    part = model // dp
    width = wg_ref.shape[2]
    q_width, kv_width = wq_ref.shape[1], wk_ref.shape[1]
    group = q_width // kv_width
    others, sides = range(1, dp), range(1, tp)
    mine = ds(t, own)
    here, there = ds(c, length), ds(1 - c, length)

    def columns(index):
        return pl.ds(pl.multiple_of(index * part, 128), part)

    def link(src, dst, device):
        return net.make(src, dst, net.number(1), device)

    def to_sides(ref, into):
        return [
            link(ref.at[ds(lax.rem(t + k, tp), own)], into.at[k - 1], net.tensor(k)) for k in sides
        ]

    def share(ref):
        return [link(ref.at[mine], ref.at[mine], net.tensor(k)) for k in sides]

    def on_to_partner(ref):
        rows = [ds(p * 2 + c, length) for p in others]
        return [link(ref.at[r], ref.at[r], net.partner()) for r in rows]

    def over_planes(ref, into):
        return [link(ref, into.at[ds((dp - k) * 2 + c, length)], net.plane(k)) for k in others]

    def start(copies):
        for copy in copies:
            copy.start()

    pair_bd = [
        link(back_ref.at[there], pair_b, net.partner()),
        link(dgate_ref.at[there], pair_d, net.partner()),
    ]
    pair_mo = [link(moe_ref.at[there], pair_m, net.partner())]
    side_bd = to_sides(sum_b, rs_b) + to_sides(sum_d, rs_d)
    side_mo = to_sides(sum_m, rs_m)
    share_da = share(da_buf) + share(dl_buf)
    dl_z = over_planes(dl_buf, dl_all)
    dl_own = [link(dl_buf, dl_all.at[here], net.partner())]
    dl_c = on_to_partner(dl_all)
    q_core = [link(q_part.at[:, 1 - c], q_pair, net.partner())]
    q_z = [link(q_sum.at[lax.rem(z + k, dp)], q_in.at[k - 1], net.plane(k)) for k in others]
    o_core = [link(o_part.at[:, 1 - c], o_pair, net.partner())]
    o_z = [link(o_sum.at[lax.rem(z + k, dp)], o_in.at[k - 1], net.plane(k)) for k in others]
    share_out = share(out_buf)
    side_3 = to_sides(part_buf, rs_3)
    share_in = share(in_buf)
    side_gain = [link(gain_buf, gain_t.at[k - 1], net.tensor(k)) for k in sides]
    plane_gain = [
        link(gain_zs.at[:, columns(lax.rem(z + k, dp))], gain_z.at[k - 1], net.plane(k))
        for k in others
    ]
    pair_gain = [link(gain_c.at[0], gain_c.at[1], net.partner())]
    keep_dl = pltpu.make_async_copy(dl_buf, dl_all.at[here], keep_sem.at[0])
    plane_rows = xr_ref.shape[0] // dp
    rest = pl.ds(plane_rows, xr_ref.shape[0] - plane_rows)
    load_x = pltpu.make_async_copy(xr_ref.at[rest], x_rest, keep_sem.at[1])
    load_g = pltpu.make_async_copy(gr_ref.at[rest], g_rest, keep_sem.at[2])

    @pl.when(step == 0)
    def _():
        load_x.start()
        load_g.start()
        net.greet()
        start(pair_bd)
        load_x.wait()
        store_split(gates_of(x_rest, wr_ref, model), split)
        load_g.wait()

    @pl.when(step == 1)
    def _():
        arrived(pair_bd)
        sum_b[...] = (back_ref[here, :].astype(F32) + pair_b[...].astype(F32)).astype(BF16)
        sum_d[...] = dgate_ref[here, :] + pair_d[...]
        start(side_bd + pair_mo)

    def over_pair(part, pair, total):
        total[...] = (part[:, c].astype(F32) + pair[...].astype(F32)).astype(BF16)

    def over_z(total, came, out):
        value = total[z].astype(F32)
        for k in others:
            value = value + came[k - 1].astype(F32)
        out[...] = value

    @pl.when(step == 3)
    def _():
        arrived(side_bd)
        d_n2 = sum_b[mine, :].astype(F32)
        dgate = sum_d[mine, :]
        for k in sides:
            d_n2 = d_n2 + rs_b[k - 1].astype(F32)
            dgate = dgate + rs_d[k - 1]
        gates = gates_ref[ds(c * tp + t, own), :]
        d_logits = gates * (dgate - jnp.sum(gates * dgate, axis=1, keepdims=True))
        dl_buf[mine, :] = d_logits.astype(BF16)
        d_n2 = d_n2 + dot_nt(d_logits.astype(BF16), wr_ref[...])
        h1 = h1_ref[...]
        r2 = inverse_rms(h1)
        weighted = d_n2 * gm_ref[...].reshape(1, -1)
        inner = jnp.mean(weighted * h1, axis=-1, keepdims=True)
        gain_buf[...] = jnp.zeros_like(gain_buf)
        gain_buf[1:2, :] = jnp.sum(d_n2 * h1 * r2, axis=0, keepdims=True)
        d_h1 = cot_ref[mine, :].astype(F32) + (r2 * weighted - h1 * (r2 * r2 * r2) * inner)
        dh1_buf[...] = d_h1
        da_buf[mine, :] = d_h1.astype(BF16)
        start(share_da)
        arrived(pair_mo)
        sum_m[...] = (moe_ref[here, :].astype(F32) + pair_m[...].astype(F32)).astype(BF16)

    @pl.when(step == 5)
    def _():
        arrived(share_da)
        start(side_mo + dl_z + dl_own)
        keep_dl.start()
        do_buf[...] = dot_nt(da_buf[...], wo_ref[...]).astype(BF16)
        o_part[...] = dot_tn(da_buf[...], att_ref[...]).astype(BF16).reshape(o_part.shape)
        start(o_core)
        seen = causal(length)
        scale = HEAD_SIZE ** (-0.5)
        d_key, d_val, d_query = [], [], []
        for kv in range(kv_width // HEAD_SIZE):
            if kv == 1:
                arrived(o_core)
                over_pair(o_part, o_pair, o_sum)
                start(o_z)
            at_k = q_width + kv * HEAD_SIZE
            at_v = q_width + kv_width + kv * HEAD_SIZE
            key = qkv_ref[:, at_k : at_k + HEAD_SIZE]
            val = qkv_ref[:, at_v : at_v + HEAD_SIZE]
            dk = jnp.zeros((length, HEAD_SIZE), F32)
            dv = jnp.zeros((length, HEAD_SIZE), F32)
            for h in range(kv * group, (kv + 1) * group):
                at = slice(h * HEAD_SIZE, (h + 1) * HEAD_SIZE)
                q = qkv_ref[:, at]
                d_out = do_buf[:, at]
                s = jnp.where(seen, dot_nt(q, key) * scale, -1e30)
                prob = jnp.exp(s - lse_ref[:, h : h + 1])
                delta = jnp.sum(
                    d_out.astype(F32) * att_ref[:, at].astype(F32), axis=-1, keepdims=True
                )
                d_s = (prob * (dot_nt(d_out, val) - delta)).astype(BF16)
                d_query.append(dot(d_s, key) * scale)
                dk = dk + dot_tn(d_s, q)
                dv = dv + dot_tn(prob.astype(BF16), d_out)
            d_key.append(dk * scale)
            d_val.append(dv)
        d_buf[:, :q_width] = rotate(jnp.concatenate(d_query, axis=1), rope_ref, -1.0).astype(BF16)
        d_buf[:, q_width : q_width + kv_width] = rotate(
            jnp.concatenate(d_key, axis=1), rope_ref, -1.0
        ).astype(BF16)
        d_buf[:, q_width + kv_width :] = jnp.concatenate(d_val, axis=1).astype(BF16)
        part_n1 = dot_nt(d_buf[:, :q_width], wq_ref[...])
        part_n1 = part_n1 + dot_nt(d_buf[:, q_width : q_width + kv_width], wk_ref[...])
        part_n1 = part_n1 + dot_nt(d_buf[:, q_width + kv_width :], wv_ref[...])
        part_buf[...] = part_n1.astype(BF16)
        start(side_3)
        q_part[...] = dot_tn(n1_ref[...], d_buf[...]).astype(BF16).reshape(q_part.shape)
        start(q_core)

    @pl.when(step == 6)
    def _():
        arrived(q_core)
        over_pair(q_part, q_pair, q_sum)
        start(q_z)
        arrived(side_mo)
        total = h1_ref[...] + sum_m[mine, :].astype(F32)
        for k in sides:
            total = total + rs_m[k - 1].astype(F32)
        out_buf[mine, :] = total.astype(BF16)
        arrived(dl_z)
        start(dl_c)

    @pl.when(step == 7)
    def _():
        arrived(side_3)
        d_n1 = part_buf[mine, :].astype(F32)
        for k in sides:
            d_n1 = d_n1 + rs_3[k - 1].astype(F32)
        resid = tok_ref[mine, :].astype(F32)
        r1 = inverse_rms(resid)
        weighted = d_n1 * ga_ref[...].reshape(1, -1)
        inner = jnp.mean(weighted * resid, axis=-1, keepdims=True)
        gain_buf[0:1, :] = jnp.sum(d_n1 * resid * r1, axis=0, keepdims=True)
        d_x = dh1_buf[...] + (r1 * weighted - resid * (r1 * r1 * r1) * inner)
        in_buf[mine, :] = d_x.astype(BF16)
        start(side_gain + share_in)

    @pl.when(step == 8)
    def _():
        arrived(side_gain)
        gain = gain_buf[...]
        for k in sides:
            gain = gain + gain_t[k - 1]
        gain_zs[...] = gain
        start(plane_gain + share_out)

    @pl.when(step == 9)
    def _():
        arrived(plane_gain)
        gain = gain_zs[:, columns(z)]
        for k in others:
            gain = gain + gain_z[k - 1]
        gain_c[0] = gain
        start(pair_gain)

    first = c * (2 * pl.num_programs(0)) + 2 * step
    wd_pair = wd_ref[...].reshape(2 * width, model)
    gate_pair = pair_of_gates(split[...], first, width)
    dh_pair = dot_nt(g_rest[...], wd_pair)
    for k in range(2):
        lanes = slice(k * width, (k + 1) * width)
        both = dot(x_rest[:, :model], jnp.concatenate([wg_ref[k], wu_ref[k]], axis=1))
        _, ghid, dgp, dup = swiglu(both, dh_pair[:, lanes], gate_pair[:, lanes])
        ghid_ref[:, lanes] = ghid
        dgp_ref[:, lanes] = dgp
        dup_ref[:, lanes] = dup

    @pl.when(step == last)
    def _():
        arrived(pair_gain)
        gains_ref[...] = gain_c[0] + gain_c[1]
        arrived(o_z)
        over_z(o_sum, o_in, o_grad_ref)
        arrived(share_out + share_in)
        out_ref[...] = out_buf[...]
        in_ref[...] = in_buf[...]
        arrived(q_z)
        over_z(q_sum, q_in, qkv_grad_ref)
        arrived(dl_own + dl_c)
        keep_dl.wait()
        sent = pair_bd + pair_mo + side_bd + side_mo + share_da + share_out + share_in + side_3
        sent = sent + dl_z + dl_own + dl_c + q_core + q_z + o_core + o_z
        for copy in sent + side_gain + plane_gain + pair_gain:
            copy.wait_send()


def whole_spec(a):
    shape = a.shape
    return pl.BlockSpec(shape, lambda *_: (0,) * len(shape), pipeline_mode=pl.Buffered(1))


def backward(dp, tp, arrays, streamed, weights):
    tokens = arrays[5]
    wq, wk, wv = arrays[10:13]
    all_rows, model = streamed[1].shape
    rest_rows = all_rows - all_rows // dp
    count, _, width = weights[0].shape
    length = tokens.shape[0]
    own, part = length // tp, model // dp
    q_width = wq.shape[1]
    wide = q_width + wk.shape[1] + wv.shape[1]
    others, sides = dp - 1, tp - 1
    copies = 3 + 9 * sides + (2 * others + 1) + 2 * (1 + others) + sides + others + 1
    by_pair = lambda shape: pl.BlockSpec((2,) + shape, lambda i: (i, 0, 0))
    saved = pl.BlockSpec((rest_rows, 2 * width), lambda i: (0, i))
    shapes = [
        ((length, model), BF16),
        ((length, model), BF16),
        ((all_rows, EXTRA), BF16),
        ((part // 2, wide), F32),
        ((part // 2, q_width), F32),
        ((8, part), F32),
        ((rest_rows, count * width), BF16),
        ((rest_rows, count * width), BF16),
        ((rest_rows, count * width), BF16),
    ]
    shapes = [jax.ShapeDtypeStruct(*s) for s in shapes]
    full, block, slots = (length, model), (own, model), (sides, own, model)
    scratch = [
        ((rest_rows, streamed[0].shape[1]), BF16),
        ((rest_rows, model), BF16),
        ((rest_rows, 2 * EXTRA), BF16),
        (full, BF16),
        (full, BF16),
        ((length, EXTRA), F32),
        (full, BF16),
        (full, BF16),
        ((length, EXTRA), F32),
        (slots, BF16),
        (slots, BF16),
        ((sides, own, EXTRA), F32),
        (block, F32),
        (full, BF16),
        ((length, EXTRA), BF16),
        ((length, wide), BF16),
        ((length, q_width), BF16),
        (full, BF16),
        (slots, BF16),
        ((8, model), F32),
        ((sides, 8, model), F32),
        ((others, 8, part), F32),
        ((8, model), F32),
        ((2, 8, part), F32),
        (full, BF16),
        (full, BF16),
        ((dp, 2, part // 2, wide), BF16),
        ((dp, part // 2, wide), BF16),
        ((dp, part // 2, wide), BF16),
        ((others, part // 2, wide), BF16),
        ((dp, 2, part // 2, q_width), BF16),
        ((dp, part // 2, q_width), BF16),
        ((dp, part // 2, q_width), BF16),
        ((others, part // 2, q_width), BF16),
    ]
    return pl.pallas_call(
        functools.partial(backward_kernel, dp, tp),
        grid=(count // 2,),
        out_shape=shapes,
        in_specs=[whole_spec(a) for a in arrays]
        + [ANY, ANY]
        + [by_pair((model, width)), by_pair((model, width)), by_pair((width, model))],
        out_specs=[whole_spec(shapes[0]), whole_spec(shapes[1]), ANY]
        + [whole_spec(s) for s in shapes[3:6]]
        + [saved] * 3,
        scratch_shapes=[pltpu.VMEM(*s) for s in scratch]
        + [
            pltpu.SemaphoreType.DMA((copies,)),
            pltpu.SemaphoreType.DMA((copies,)),
            pltpu.SemaphoreType.DMA((3,)),
        ],
        compiler_params=pltpu.CompilerParams(
            collective_id=2, has_side_effects=True, vmem_limit_bytes=VMEM_LIMIT
        ),
        name="backward",
    )(*arrays, *streamed, *weights)


def weights_kernel(
    place_ref,
    x_ref,
    g_ref,
    dl_ref,
    qkv_grad_ref,
    o_grad_ref,
    gains_ref,
    out_in_ref,
    in_in_ref,
    ghid_ref,
    dgp_ref,
    dup_ref,
    ghid_rest,
    dgp_rest,
    dup_rest,
    gate_grad_ref,
    up_grad_ref,
    down_grad_ref,
    query_ref,
    key_ref,
    value_ref,
    out_grad_ref,
    router_ref,
    ga_grad_ref,
    gm_grad_ref,
    out_ref,
    in_ref,
    xt_buf,
    gt_buf,
):
    step = pl.program_id(0)
    c = place_ref[1]
    width = gate_grad_ref.shape[2]
    plane_rows = ghid_ref.shape[0]

    @pl.when(step == 0)
    def _():
        xt_buf[...] = x_ref[...].T
        gt_buf[...] = g_ref[...].T
        q_width, kv_width = query_ref.shape[1], key_ref.shape[1]
        half = query_ref.shape[0]
        query_ref[...] = qkv_grad_ref[:, :q_width]
        key_ref[...] = qkv_grad_ref[:, q_width : q_width + kv_width]
        value_ref[...] = qkv_grad_ref[:, q_width + kv_width :]
        out_grad_ref[...] = o_grad_ref[...]
        out_ref[...] = out_in_ref[...]
        in_ref[...] = in_in_ref[...]
        router = dot(xt_buf[...], dl_ref[...]).T[: router_ref.shape[0]]
        router_ref[...] = jnp.where(c == 0, router[:, :half], router[:, half:])
        gains = jnp.where(c == 0, gains_ref[:, :half], gains_ref[:, half:])
        ga_grad_ref[...] = gains[0:1, :]
        gm_grad_ref[...] = gains[1:2, :]

    def contract(left, own, rest):
        return dot(left[:, :plane_rows], own[...]) + dot(left[:, plane_rows:], rest[...])

    gate_both = contract(xt_buf, dgp_ref, dgp_rest)
    up_both = contract(xt_buf, dup_ref, dup_rest)
    down_both = contract(gt_buf, ghid_ref, ghid_rest).T
    for k in range(2):
        lanes = slice(k * width, (k + 1) * width)
        gate_grad_ref[k] = gate_both[:, lanes]
        up_grad_ref[k] = up_both[:, lanes]
        down_grad_ref[k] = down_both[lanes, :]


def weight_grads(place, x, g, sides, own, rest, count, kv_width, experts):
    rows = x.shape[0]
    _, qkv_grad, o_grad, gains, output, _ = sides
    width = own[0].shape[1] // count
    part = gains.shape[1]
    q_width, half = o_grad.shape[1], part // 2
    by_pair = lambda shape: pl.BlockSpec((2,) + shape, lambda i, p: (i, 0, 0))
    saved = lambda a: pl.BlockSpec((a.shape[0], 2 * width), lambda i, p: (0, i))
    columns = pl.BlockSpec((rows, part), lambda i, p: (0, p[0]), pipeline_mode=pl.Buffered(1))
    shapes = [
        (count, part, width),
        (count, part, width),
        (count, width, part),
        (half, q_width),
        (half, kv_width),
        (half, kv_width),
        (half, q_width),
        (experts, half),
        (1, half),
        (1, half),
    ]
    shapes = [jax.ShapeDtypeStruct(s, F32) for s in shapes]
    shapes += [jax.ShapeDtypeStruct(output.shape, BF16)] * 2
    return pl.pallas_call(
        weights_kernel,
        grid_spec=pltpu.PrefetchScalarGridSpec(
            num_scalar_prefetch=1,
            grid=(count // 2,),
            in_specs=[columns, columns]
            + [whole_spec(a) for a in sides]
            + [saved(a) for a in own]
            + [saved(a) for a in rest],
            out_specs=[by_pair((part, width)), by_pair((part, width)), by_pair((width, part))]
            + [whole_spec(s) for s in shapes[3:]],
            scratch_shapes=[pltpu.VMEM((part, rows), BF16), pltpu.VMEM((part, rows), BF16)],
        ),
        out_shape=shapes,
        compiler_params=pltpu.CompilerParams(vmem_limit_bytes=VMEM_LIMIT),
        name="weight_grads",
    )(place, x, g, *sides, *own, *rest)


def rope_rows(length):
    half = HEAD_SIZE // 2
    frequency = ROPE_BASE ** (np.arange(half) * (-2.0 / HEAD_SIZE))
    angles = np.arange(length)[:, None] * frequency[None, :]
    cos, sin, none = np.cos(angles), np.sin(angles), np.zeros((length, half))
    double = lambda first, second: np.concatenate([first, second, first, second], axis=1)
    return np.stack([double(cos, cos), double(-sin, none), double(none, sin)]).astype(np.float32)


def gather_plan(
    tokens,
    gain_attn,
    w_query,
    key_projection,
    value_projection,
    w_out,
    gain_moe,
    w_router,
    w_gate,
    w_up,
    w_down,
    routes,
    cotangent,
):
    dp, tp = lax.axis_size("dp"), lax.axis_size("tensor")
    experts = w_router.shape[1]
    rope = jnp.asarray(rope_rows(tokens.shape[0]))
    ga, gm = gain_attn, gain_moe
    wr = jnp.pad(w_router, ((0, 0), (0, EXTRA - experts)))
    heads = (w_query, key_projection, value_projection, w_out)
    x, g, gz, h1, n1, qkv, att, lse = forward(
        dp, tp, tokens, cotangent, routes, ga, gm, *heads, rope
    )
    x_all, g_all, moe, back, dgate, gates, ghid, dgp, dup = plane_experts(
        dp, tp, x, g, gz, wr, w_gate, w_up, w_down
    )
    local = (back, moe, dgate, gates, h1, tokens, cotangent, ga, gm, wr, *heads)
    output, input_grad, d_logits, qkv_grad, o_grad, gains, *rest = backward(
        dp, tp, (*local, qkv, att, lse, n1, rope), (x_all, g_all), (w_gate, w_up, w_down)
    )
    place = jnp.stack([lax.axis_index("dp"), lax.axis_index("expert")]).astype(jnp.int32)
    (
        gate_grad,
        up_grad,
        down_grad,
        query_grad,
        key_grad,
        value_grad,
        out_grad,
        router_grad,
        gain_attn_grad,
        gain_moe_grad,
        output,
        input_grad,
    ) = weight_grads(
        place,
        x_all,
        g_all,
        (d_logits, qkv_grad, o_grad, gains, output, input_grad),
        (ghid, dgp, dup),
        rest,
        w_gate.shape[0],
        key_projection.shape[1],
        experts,
    )
    return (
        output,
        input_grad,
        gain_attn_grad[0],
        query_grad,
        key_grad,
        value_grad,
        out_grad.T,
        gain_moe_grad[0],
        router_grad.T,
        gate_grad,
        up_grad,
        down_grad,
    )


def solution(mesh):
    placed = (
        P(("dp", "expert"), None),
        P(),
        P(None, "tensor"),
        P(None, "tensor"),
        P(None, "tensor"),
        P("tensor", None),
        P(),
        P(),
        P("expert", None, "tensor"),
        P("expert", None, "tensor"),
        P("expert", "tensor", None),
        P(("dp", "expert"), None),
        P(("dp", "expert"), None),
    )
    sequences = mesh.shape["dp"] * mesh.shape["expert"]
    few = sequences * SEQUENCE_LENGTH <= GATHER_ROWS
    few = few and mesh.shape["tensor"] == 4 and mesh.shape["expert"] == 2
    return jax.shard_map(
        gather_plan if few else reduce_plan,
        mesh=mesh,
        in_specs=placed,
        out_specs=(
            P(("dp", "expert"), None),
            P(("dp", "expert"), None),
            P(("dp", "expert")),
            P(("dp", "expert"), "tensor"),
            P(("dp", "expert"), "tensor"),
            P(("dp", "expert"), "tensor"),
            P("tensor", ("dp", "expert")),
            P(("dp", "expert")),
            P(("dp", "expert"), None),
            P("expert", "dp", "tensor"),
            P("expert", "dp", "tensor"),
            P("expert", "tensor", "dp"),
        ),
        check_vma=False,
    )
```

```python
import functools
import math

import jax
import jax.numpy as jnp
import numpy as np
from jax import lax
from jax.experimental import pallas as pl
from jax.experimental.pallas import tpu as pltpu
from jax.sharding import PartitionSpec as P

HEAD_SIZE = 64
SEQUENCE_LENGTH = 256
CAP = 64


EPSILON = 1e-06
ROPE_BASE = 10000.0
BLOCK_ROWS = 512


def split_up(x, dim, count):
    dims = x.shape
    tiles = x.reshape(*dims[:dim], count, dims[dim] // count, *dims[dim + 1 :])
    return jnp.moveaxis(tiles, dim, 0)


def sum_at_owner(x, axis, dim):
    tiles = split_up(x, dim, lax.axis_size(axis))
    arrived = lax.all_to_all(tiles, axis, split_axis=0, concat_axis=0, tiled=True)
    return arrived.astype(jnp.float32).sum(axis=0)


def side_by_side(arrays, axis, dim, along):
    both = jnp.concatenate(arrays, axis=along)
    filled, at, outs = (sum_at_owner(both, axis, dim), 0, [])
    for a in arrays:
        outs.append(lax.slice_in_dim(filled, at, at + a.shape[along], axis=along))
        at += a.shape[along]
    return tuple(outs)


def sent_together(arrays, axis, dim, along):
    widths = [math.prod(a.shape[along:]) for a in arrays]
    both = jnp.concatenate(
        [a.reshape(*a.shape[:along], w) for a, w in zip(arrays, widths)], axis=along
    )
    filled = sum_at_owner(both, axis, dim)
    tiles = jnp.split(filled, [sum(widths[:k]) for k in range(1, len(widths))], axis=along)
    return tuple(
        (b.reshape(*filled.shape[:along], *a.shape[along:]) for a, b in zip(arrays, tiles))
    )


def rms_scale(hidden):
    return lax.rsqrt(jnp.mean(hidden * hidden, axis=-1, keepdims=True) + EPSILON)


def norm_back(hidden, scaling, gain_vec, grad_out):
    weighted = grad_out * gain_vec
    gain_grad = jnp.sum(grad_out * hidden * scaling, axis=0)
    inner_mean = jnp.mean(weighted * hidden, axis=-1, keepdims=True)
    return (scaling * weighted - hidden * (scaling * scaling * scaling) * inner_mean, gain_grad)


def rope_tables(positions, head_dim):
    half_dim = head_dim // 2
    frequency = jnp.exp(
        jnp.arange(half_dim, dtype=jnp.float32) * (-2.0 * math.log(ROPE_BASE) / head_dim)
    )
    angles = positions[:, None] * frequency[None, :]
    return (jnp.cos(angles), jnp.sin(angles))


def apply_rotary(vectors, cosine_table, sine_component):
    half_dim = vectors.shape[-1] // 2
    first_half = vectors[..., :half_dim]
    second_half = vectors[..., half_dim:]
    cos_rows = cosine_table[:, None, :]
    sin_rows = sine_component[:, None, :]
    return jnp.concatenate(
        [
            first_half * cos_rows - second_half * sin_rows,
            first_half * sin_rows + second_half * cos_rows,
        ],
        axis=-1,
    )


def slot_table(route_ids, expert_count, capacity):
    number_of_rows, top_count = route_ids.shape
    flat_ids = route_ids.reshape(-1)
    one_hot = (flat_ids[:, None] == jnp.arange(expert_count, dtype=jnp.int32)[None, :]).astype(
        jnp.int32
    )
    earlier = jnp.cumsum(one_hot, axis=0) - one_hot
    slot_ids = jnp.sum(earlier * one_hot, axis=1)
    slot_where = flat_ids * capacity + slot_ids
    pick_ids = jnp.arange(number_of_rows * top_count, dtype=jnp.int32)
    token_of = (
        jnp.full((expert_count * capacity,), number_of_rows, jnp.int32)
        .at[slot_where]
        .set(pick_ids // top_count)
    )
    pick_of = (
        jnp.full((expert_count * capacity,), number_of_rows * top_count, jnp.int32)
        .at[slot_where]
        .set(pick_ids)
    )
    return (slot_where, token_of, pick_of)


def block_scores(query_rows, key_rows, query_group_width):
    block_len = query_rows.shape[0]
    key_count, kv_heads, head_dim = key_rows.shape
    grouped = query_rows.reshape(block_len, kv_heads, query_group_width, head_dim)
    scores = jnp.einsum(
        "qhgd,khd->hgqk", grouped, key_rows, preferred_element_type=jnp.float32
    ) * head_dim ** (-0.5)
    row_pos = jnp.arange(block_len, dtype=jnp.int32)[:, None]
    col_pos = jnp.arange(key_count, dtype=jnp.int32)[None, :]
    return (jnp.where(col_pos <= row_pos, scores, -1e30), grouped)


def sequence_forward(query_rows, key_rows, value_rows, query_group_width):
    length, kv_heads, head_dim = key_rows.shape
    block_len = min(BLOCK_ROWS, length)
    scores, grouped = block_scores(query_rows, key_rows, query_group_width)
    largest = jnp.max(scores, axis=-1, keepdims=True)
    log_total = largest + jnp.log(jnp.sum(jnp.exp(scores - largest), axis=-1, keepdims=True))
    weights = jnp.exp(scores - log_total).astype(jnp.bfloat16)
    attended = jnp.einsum("hgqk,khd->qhgd", weights, value_rows, preferred_element_type=jnp.float32)
    outputs = attended.reshape(block_len, -1, head_dim).astype(jnp.bfloat16)
    return (outputs, log_total)


def sequence_backward(
    query_rows, key_rows, value_rows, attended, log_total, d_attended, query_group_width
):
    length, kv_heads, head_dim = key_rows.shape
    block_len = min(BLOCK_ROWS, length)
    scale_factor = head_dim ** (-0.5)
    key_gradient = jnp.zeros((length, kv_heads, head_dim), jnp.float32)
    value_gradient = jnp.zeros((length, kv_heads, head_dim), jnp.float32)
    scores, grouped = block_scores(query_rows, key_rows, query_group_width)
    weights = jnp.exp(scores - log_total)
    d_grouped = d_attended.reshape(block_len, kv_heads, query_group_width, head_dim)
    o_grouped = attended.reshape(block_len, kv_heads, query_group_width, head_dim)
    delta = jnp.sum(d_grouped.astype(jnp.float32) * o_grouped.astype(jnp.float32), axis=-1)
    delta = jnp.transpose(delta, (1, 2, 0))[..., None]
    d_weights = jnp.einsum(
        "qhgd,khd->hgqk", d_grouped, value_rows, preferred_element_type=jnp.float32
    )
    d_scores = (weights * (d_weights - delta)).astype(jnp.bfloat16)
    block_query = (
        jnp.einsum("hgqk,khd->qhgd", d_scores, key_rows, preferred_element_type=jnp.float32)
        * scale_factor
    )
    query_parts = block_query.reshape(block_len, -1, head_dim)
    key_gradient = key_gradient.at[:block_len].add(
        jnp.einsum("hgqk,qhgd->khd", d_scores, grouped, preferred_element_type=jnp.float32)
        * scale_factor
    )
    value_gradient = value_gradient.at[:block_len].add(
        jnp.einsum(
            "hgqk,qhgd->khd",
            weights.astype(jnp.bfloat16),
            d_grouped,
            preferred_element_type=jnp.float32,
        )
    )
    return (query_parts, key_gradient, value_gradient)


def reduce_plan(
    tokens,
    gain_attn,
    w_query,
    key_projection,
    value_projection,
    w_out,
    gain_moe,
    w_router,
    w_gate,
    w_up,
    w_down,
    routes,
    cotangent,
):
    number_of_rows, model_width = tokens.shape
    head_dim = HEAD_SIZE
    query_heads = w_query.shape[1] // head_dim
    kv_heads = key_projection.shape[1] // head_dim
    query_group_width = query_heads // kv_heads
    expert_count = w_router.shape[1]
    local_experts = w_gate.shape[0]
    source_count = expert_count // local_experts
    capacity = CAP
    top_count = routes.shape[1]
    resid = tokens.astype(jnp.float32)
    scale_one = rms_scale(resid)
    first_normalized = (resid * scale_one * gain_attn).astype(jnp.bfloat16)
    positions = (jnp.arange(number_of_rows, dtype=jnp.int32) % SEQUENCE_LENGTH).astype(jnp.float32)
    cosine_table, sine_component = rope_tables(positions, head_dim)
    q_lin = jnp.dot(first_normalized, w_query, preferred_element_type=jnp.float32).reshape(
        number_of_rows, query_heads, head_dim
    )
    linear_key = jnp.dot(
        first_normalized, key_projection, preferred_element_type=jnp.float32
    ).reshape(number_of_rows, kv_heads, head_dim)
    value_reduced = (
        jnp.dot(first_normalized, value_projection, preferred_element_type=jnp.float32)
        .astype(jnp.bfloat16)
        .reshape(number_of_rows, kv_heads, head_dim)
    )
    q_rot = apply_rotary(q_lin, cosine_table, sine_component).astype(jnp.bfloat16)
    rotated_key = apply_rotary(linear_key, cosine_table, sine_component).astype(jnp.bfloat16)
    attended, log_total = sequence_forward(q_rot, rotated_key, value_reduced, query_group_width)
    flat_att = attended.reshape(number_of_rows, query_heads * head_dim)
    attn_part = jnp.dot(flat_att, w_out, preferred_element_type=jnp.float32)
    hidden1 = resid + lax.psum(attn_part.astype(jnp.bfloat16), "tensor").astype(jnp.float32)
    scale_two = rms_scale(hidden1)
    normed2 = (hidden1 * scale_two * gain_moe).astype(jnp.bfloat16)
    logits = jnp.dot(normed2, w_router, preferred_element_type=jnp.float32)
    chosen = jnp.take_along_axis(logits, routes, axis=1)
    gate_probs = jax.nn.softmax(chosen, axis=-1)
    slot_where, token_of, pick_of = slot_table(routes, expert_count, capacity)
    normed_pad = jnp.concatenate([normed2, jnp.zeros((1, model_width), jnp.bfloat16)], axis=0)
    outgoing = normed_pad[token_of].reshape(expert_count, capacity, model_width)
    received = lax.all_to_all(outgoing, "expert", split_axis=0, concat_axis=0, tiled=True)
    arrived = received.reshape(source_count, local_experts, capacity, model_width)
    gate_pre = jnp.einsum("secd,edh->sech", arrived, w_gate, preferred_element_type=jnp.float32)
    up_pre = jnp.einsum("secd,edh->sech", arrived, w_up, preferred_element_type=jnp.float32)
    sig_gate = jax.nn.sigmoid(gate_pre)
    activated = gate_pre * sig_gate
    hid_low = (activated * up_pre).astype(jnp.bfloat16)
    expert_out = jnp.einsum(
        "sech,ehd->secd", hid_low, w_down, preferred_element_type=jnp.float32
    ).astype(jnp.bfloat16)
    returned = lax.all_to_all(
        expert_out.reshape(expert_count, capacity, model_width),
        "expert",
        split_axis=0,
        concat_axis=0,
        tiled=True,
    )
    picked = returned.reshape(expert_count * capacity, model_width)[slot_where].reshape(
        number_of_rows, top_count, model_width
    )
    moe_part = jnp.zeros((number_of_rows, model_width), jnp.float32)
    for choice_index in range(top_count):
        moe_part = (
            moe_part
            + picked[:, choice_index].astype(jnp.float32)
            * gate_probs[:, choice_index : choice_index + 1]
        )
    moe_out = lax.psum(moe_part.astype(jnp.bfloat16), "tensor").astype(jnp.float32)
    output = (hidden1 + moe_out).astype(jnp.bfloat16)
    grad = cotangent.astype(jnp.float32)
    gate_dot = jnp.einsum("rjd,rd->rj", picked, cotangent, preferred_element_type=jnp.float32)
    grad_pad = jnp.concatenate([cotangent, jnp.zeros((1, model_width), jnp.bfloat16)], axis=0)
    gate_pad = jnp.concatenate([gate_probs.reshape(-1), jnp.zeros((1,), jnp.float32)], axis=0)
    sent_grad = (grad_pad[token_of].astype(jnp.float32) * gate_pad[pick_of][:, None]).astype(
        jnp.bfloat16
    )
    sent_grad = sent_grad.reshape(expert_count, capacity, model_width)
    grad_received = lax.all_to_all(sent_grad, "expert", split_axis=0, concat_axis=0, tiled=True)
    arrived_grad = grad_received.reshape(source_count, local_experts, capacity, model_width)
    d_hid = jnp.einsum("secd,ehd->sech", arrived_grad, w_down, preferred_element_type=jnp.float32)
    down_local = jnp.einsum(
        "sech,secd->ehd", hid_low, arrived_grad, preferred_element_type=jnp.float32
    )
    d_gate = (d_hid * up_pre * sig_gate * (1.0 + gate_pre * (1.0 - sig_gate))).astype(jnp.bfloat16)
    d_up = (d_hid * activated).astype(jnp.bfloat16)
    gate_local = jnp.einsum("secd,sech->edh", arrived, d_gate, preferred_element_type=jnp.float32)
    up_local = jnp.einsum("secd,sech->edh", arrived, d_up, preferred_element_type=jnp.float32)
    back_rows = jnp.einsum("sech,edh->secd", d_gate, w_gate, preferred_element_type=jnp.float32)
    back_rows = (
        back_rows + jnp.einsum("sech,edh->secd", d_up, w_up, preferred_element_type=jnp.float32)
    ).astype(jnp.bfloat16)
    came_back = lax.all_to_all(
        back_rows.reshape(expert_count, capacity, model_width),
        "expert",
        split_axis=0,
        concat_axis=0,
        tiled=True,
    )
    back_picked = came_back.reshape(expert_count * capacity, model_width)[slot_where].reshape(
        number_of_rows, top_count, model_width
    )
    back_part = jnp.zeros((number_of_rows, model_width), jnp.float32)
    for choice_index in range(top_count):
        back_part = back_part + back_picked[:, choice_index].astype(jnp.float32)
    back_total, dgate = (
        lax.psum(back_part.astype(jnp.bfloat16), "tensor").astype(jnp.float32),
        lax.psum(gate_dot.astype(jnp.bfloat16), "tensor").astype(jnp.float32),
    )
    inner_sum = jnp.sum(gate_probs * dgate, axis=1, keepdims=True)
    d_chosen = gate_probs * (dgate - inner_sum)
    matches = routes[:, :, None] == jnp.arange(expert_count, dtype=jnp.int32)[None, None, :]
    d_logits = jnp.sum(jnp.where(matches, d_chosen[:, :, None], 0.0), axis=1).astype(jnp.bfloat16)
    router_local = jnp.dot(normed2.T, d_logits, preferred_element_type=jnp.float32)
    d_normed2 = back_total + jnp.dot(d_logits, w_router.T, preferred_element_type=jnp.float32)
    d_hidden_part, gain_moe_local = norm_back(hidden1, scale_two, gain_moe, d_normed2)
    d_hidden1 = grad + d_hidden_part
    d_mixed = d_hidden1.astype(jnp.bfloat16)
    out_local = jnp.dot(flat_att.T, d_mixed, preferred_element_type=jnp.float32)
    d_att = (
        jnp.dot(d_mixed, w_out.T, preferred_element_type=jnp.float32)
        .astype(jnp.bfloat16)
        .reshape(number_of_rows, query_heads, head_dim)
    )
    dq_rot, rotated_key_gradient, dv_rows = sequence_backward(
        q_rot, rotated_key, value_reduced, attended, log_total, d_att, query_group_width
    )
    d_query = (
        apply_rotary(dq_rot, cosine_table, -sine_component)
        .astype(jnp.bfloat16)
        .reshape(number_of_rows, query_heads * head_dim)
    )
    key_gradient = (
        apply_rotary(rotated_key_gradient, cosine_table, -sine_component)
        .astype(jnp.bfloat16)
        .reshape(number_of_rows, kv_heads * head_dim)
    )
    value_gradient = dv_rows.astype(jnp.bfloat16).reshape(number_of_rows, kv_heads * head_dim)
    query_local = jnp.dot(first_normalized.T, d_query, preferred_element_type=jnp.float32)
    key_local = jnp.dot(first_normalized.T, key_gradient, preferred_element_type=jnp.float32)
    value_local = jnp.dot(first_normalized.T, value_gradient, preferred_element_type=jnp.float32)
    d_normed_part = jnp.dot(d_query, w_query.T, preferred_element_type=jnp.float32)
    d_normed_part = d_normed_part + jnp.dot(
        key_gradient, key_projection.T, preferred_element_type=jnp.float32
    )
    d_normed_part = d_normed_part + jnp.dot(
        value_gradient, value_projection.T, preferred_element_type=jnp.float32
    )
    d_normed1 = lax.psum(d_normed_part.astype(jnp.bfloat16), "tensor").astype(jnp.float32)
    d_resid_part, gain_attn_local = norm_back(resid, scale_one, gain_attn, d_normed1)
    input_grad = (d_hidden1 + d_resid_part).astype(jnp.bfloat16)
    gate_grad, up_grad, down_grad = (
        lax.psum_scatter(
            gate_local.astype(jnp.bfloat16), "dp", scatter_dimension=1, tiled=True
        ).astype(jnp.float32),
        lax.psum_scatter(
            up_local.astype(jnp.bfloat16), "dp", scatter_dimension=1, tiled=True
        ).astype(jnp.float32),
        lax.psum_scatter(
            down_local.astype(jnp.bfloat16), "dp", scatter_dimension=2, tiled=True
        ).astype(jnp.float32),
    )
    query_grad, key_grad, value_grad, out_grad, router_grad, gain_attn_grad, gain_moe_grad = (
        *side_by_side(
            (
                query_local.astype(jnp.bfloat16),
                key_local.astype(jnp.bfloat16),
                value_local.astype(jnp.bfloat16),
            ),
            ("dp", "expert"),
            0,
            1,
        ),
        sum_at_owner(out_local.astype(jnp.bfloat16), ("dp", "expert"), 1),
        *sent_together(
            (
                router_local.astype(jnp.bfloat16),
                gain_attn_local.astype(jnp.bfloat16),
                gain_moe_local.astype(jnp.bfloat16),
            ),
            ("dp", "expert"),
            0,
            1,
        ),
    )
    return (
        output,
        input_grad,
        gain_attn_grad,
        query_grad,
        key_grad,
        value_grad,
        out_grad,
        gain_moe_grad,
        router_grad,
        gate_grad,
        up_grad,
        down_grad,
    )


GATHER_ROWS = 4096
MESH = pl.DeviceIdType.MESH
VMEM = pl.BlockSpec(memory_space=pltpu.VMEM)
ANY = pl.BlockSpec(memory_space=pl.ANY)
EXTRA = 128
VMEM_LIMIT = 60 * 2**20
F32, BF16 = jnp.float32, jnp.bfloat16


def dot(a, b):
    return jnp.dot(a, b, preferred_element_type=F32)


def dot_nt(a, b):
    return lax.dot_general(a, b, (((1,), (1,)), ((), ())), preferred_element_type=F32)


def dot_tn(a, b):
    return lax.dot_general(a, b, (((0,), (0,)), ((), ())), preferred_element_type=F32)


def ds(index, size):
    return pl.ds(pl.multiple_of(index * size, size), size)


class Peers:
    def __init__(self, dp, tp, send_sem, recv_sem):
        self.z, self.c, self.t = (lax.axis_index(a) for a in ("dp", "expert", "tensor"))
        self.dp, self.tp = dp, tp
        self.send_sem, self.recv_sem = send_sem, recv_sem
        self.used = 0
        self.open = []

    def tensor(self, k):
        return (self.z, self.c, lax.rem(self.t + k, self.tp))

    def near(self, axis):
        row, col = self.t // 2, self.t % 2
        index = row * 2 + (1 - col) if axis == 0 else (1 - row) * 2 + col
        return (self.z, self.c, index)

    def plane(self, k):
        return (lax.rem(self.z + k, self.dp), self.c, self.t)

    def partner(self):
        return (self.z, 1 - self.c, self.t)

    def greet(self):
        barrier = pltpu.get_barrier_semaphore()
        everyone = [self.tensor(k) for k in range(1, self.tp)]
        everyone += [self.plane(k) for k in range(1, self.dp)] + [self.partner()]
        for peer in everyone:
            pl.semaphore_signal(barrier, inc=1, device_id=peer, device_id_type=MESH)
        pl.semaphore_wait(barrier, len(everyone))

    def number(self, count):
        first = self.used
        self.used += count
        return first

    def make(self, src, dst, number, device):
        return pltpu.make_async_remote_copy(
            src_ref=src,
            dst_ref=dst,
            send_sem=self.send_sem.at[number],
            recv_sem=self.recv_sem.at[number],
            device_id=device,
            device_id_type=MESH,
        )

    def to(self, src, dst, device):
        copy = self.make(src, dst, self.number(1), device)
        copy.start()
        self.open.append(copy)
        return copy

    def keep(self, src, dst, sem):
        copy = pltpu.make_async_copy(src, dst, sem)
        copy.start()
        return copy

    def drain(self):
        for copy in self.open:
            copy.wait_send()


def arrived(copies):
    for copy in copies:
        copy.wait_recv()


def rotate(u, rope_ref, sign):
    width = u.shape[1]
    tiles = []
    for at in range(0, width, 128):
        v = u[:, at : at + 128]
        side = pltpu.roll(v, 96, 1) * rope_ref[1] + pltpu.roll(v, 32, 1) * rope_ref[2]
        tiles.append(v * rope_ref[0] + sign * side)
    return tiles[0] if len(tiles) == 1 else jnp.concatenate(tiles, axis=1)


def inverse_rms(u):
    return lax.rsqrt(jnp.mean(u * u, axis=-1, keepdims=True) + EPSILON)


def causal(length):
    row = lax.broadcasted_iota(jnp.int32, (length, length), 0)
    col = lax.broadcasted_iota(jnp.int32, (length, length), 1)
    return col <= row


def gates_of(x_ref, wr_ref, model):
    logits = dot(x_ref[:, :model], wr_ref[...])
    chosen = x_ref[:, model:].astype(F32) > 0.5
    top = jnp.max(jnp.where(chosen, logits, -jnp.inf), axis=1, keepdims=True)
    weight = jnp.where(chosen, jnp.exp(jnp.where(chosen, logits - top, 0.0)), 0.0)
    return weight / jnp.sum(weight, axis=1, keepdims=True)


def store_split(gates, split_ref):
    high = gates.astype(BF16)
    split_ref[:, :EXTRA] = high
    split_ref[:, EXTRA:] = (gates - high.astype(F32)).astype(BF16)


def pair_of_gates(split, first, width):
    k_pos = lax.broadcasted_iota(jnp.int32, (2 * EXTRA, 2 * width), 0)
    l_pos = lax.broadcasted_iota(jnp.int32, (2 * EXTRA, 2 * width), 1)
    pick = jnp.where(k_pos % EXTRA == first + l_pos // width, 1.0, 0.0).astype(BF16)
    return dot(split, pick)


def swiglu(both, dh, gate):
    width = dh.shape[1]
    gate_pre, up_pre = both[:, :width], both[:, width:]
    sig = jax.nn.sigmoid(gate_pre)
    act = gate_pre * sig
    hid = act * up_pre
    d_hid = dh * gate
    d_gate = d_hid * up_pre * sig * (1.0 + gate_pre * (1.0 - sig))
    return hid, (hid * gate).astype(BF16), d_gate.astype(BF16), (d_hid * act).astype(BF16)


def front_kernel(
    dp,
    tp,
    tok_ref,
    cot_ref,
    routes_ref,
    ga_ref,
    gm_ref,
    wr_ref,
    wq_ref,
    wk_ref,
    wv_ref,
    wo_ref,
    rope_ref,
    wg_ref,
    wu_ref,
    wd_ref,
    xr_ref,
    gr_ref,
    moe_ref,
    back_ref,
    dgate_ref,
    gates_ref,
    h1_ref,
    qkv_ref,
    att_ref,
    prob_ref,
    prob_t_ref,
    n1t_ref,
    ghid_ref,
    dgp_ref,
    dup_ref,
    x_buf,
    g_buf,
    gz_buf,
    n1_buf,
    part_buf,
    rs_buf,
    dh_buf,
    split,
    moe_acc,
    back_acc,
    send_sem,
    recv_sem,
    keep_sem,
):
    step, last = pl.program_id(0), pl.num_programs(0) - 1
    pairs = pl.num_programs(0) // 2
    net = Peers(dp, tp, send_sem, recv_sem)
    z, c, t = net.z, net.c, net.t
    length, model = tok_ref.shape
    rows = 2 * length
    own = length // tp
    width = wg_ref.shape[2]
    q_width, kv_width = wq_ref.shape[1], wk_ref.shape[1]
    group = q_width // kv_width
    others, sides = range(1, dp), range(1, tp)

    def block(plane, core, tensor):
        return ds((plane * 2 + core) * tp + tensor, own)

    def link(src, dst, device):
        return net.make(src, dst, net.number(1), device)

    def start(copies):
        for copy in copies:
            copy.start()

    mine = ds(c * tp + t, own)
    seq_rows = ds(c, length)
    near = [net.near(axis) for axis in range(2)]
    far = tp - 1 - t
    half = own // 2

    def piece(plane, tensor, part_of):
        at = (((plane * 2 + c) * tp + tensor) * 2 + part_of) * half
        return pl.ds(pl.multiple_of(at, half), half)

    def spread(ref, sources, relayed):
        direct = [
            link(sources[p - 1], ref.at[block(p, c, t)], near[axis])
            for p in others
            for axis in range(2)
        ]
        relay = []
        for p in others if relayed else ():
            for axis in range(2):
                at = piece(p, near[axis][2], axis)
                relay.append(link(ref.at[at], ref.at[at], near[1 - axis]))
        to_core = [link(sources[p - 1], ref.at[block(p, c, t)], net.partner()) for p in others]
        near_core, far_core = [], []
        for p in others:
            for axis in range(2):
                at = block(p, c, near[axis][2])
                near_core.append(link(ref.at[at], ref.at[at], net.partner()))
            at = block(p, c, far)
            far_core.append(link(ref.at[at], ref.at[at], net.partner()))
        return direct, relay, to_core, near_core, far_core

    g_own = [link(cot_ref, g_buf.at[seq_rows], net.partner())]
    g_z = [link(cot_ref.at[ds(t, own)], gz_buf.at[dp - 1 - k], net.plane(k)) for k in others]
    side_h = [
        link(part_buf.at[ds(lax.rem(t + k, tp), own)], rs_buf.at[k - 1], net.tensor(k))
        for k in sides
    ]
    x_t = [link(x_buf.at[mine], x_buf.at[mine], net.tensor(k)) for k in sides]
    x_own = [link(x_buf.at[mine], x_buf.at[mine], net.partner())]
    x_seen = []
    for k in sides:
        at = ds(c * tp + lax.rem(t + tp - k, tp), own)
        x_seen.append(link(x_buf.at[at], x_buf.at[at], net.partner()))
    x_z = [link(x_buf.at[mine], xr_ref.at[block(dp - k, c, t)], net.plane(k)) for k in others]
    g_direct, g_relay, g_core, g_near, g_far = spread(
        gr_ref, [gz_buf.at[p - 1] for p in others], True
    )
    x_direct, _, x_core, x_near, x_far = spread(
        xr_ref, [xr_ref.at[block(p, c, t)] for p in others], False
    )
    x_z2 = [
        link(x_buf.at[ds(c * tp + far, own)], xr_ref.at[block(dp - k, c, far)], net.plane(k))
        for k in others
    ]
    keep_x = pltpu.make_async_copy(x_buf, xr_ref.at[pl.ds(0, rows)], keep_sem.at[0])
    keep_g = [pltpu.make_async_copy(g_buf, gr_ref.at[pl.ds(0, rows)], keep_sem.at[1])] + [
        pltpu.make_async_copy(gz_buf.at[p - 1], gr_ref.at[block(p, c, t)], keep_sem.at[1 + p])
        for p in others
    ]

    @pl.when(step == 0)
    def _():
        net.greet()
        start(g_own + g_z)
        g_buf[seq_rows, :] = cot_ref[...]
        resid = tok_ref[...].astype(F32)
        n1 = (resid * inverse_rms(resid) * ga_ref[...].reshape(1, -1)).astype(BF16)
        n1_buf[...] = n1
        qkv_ref[:, :q_width] = rotate(dot(n1, wq_ref[...]), rope_ref, 1.0).astype(BF16)
        qkv_ref[:, q_width : q_width + kv_width] = rotate(
            dot(n1, wk_ref[...]), rope_ref, 1.0
        ).astype(BF16)
        qkv_ref[:, q_width + kv_width :] = dot(n1, wv_ref[...]).astype(BF16)
        seen = causal(length)
        scale = HEAD_SIZE ** (-0.5)
        for h in range(q_width // HEAD_SIZE):
            kv = h // group
            at_k = q_width + kv * HEAD_SIZE
            at_v = q_width + kv_width + kv * HEAD_SIZE
            q = qkv_ref[:, h * HEAD_SIZE : (h + 1) * HEAD_SIZE]
            key = qkv_ref[:, at_k : at_k + HEAD_SIZE]
            val = qkv_ref[:, at_v : at_v + HEAD_SIZE]
            s = jnp.where(seen, dot_nt(q, key) * scale, -1e30)
            top = jnp.max(s, axis=-1, keepdims=True)
            lse = top + jnp.log(jnp.sum(jnp.exp(s - top), axis=-1, keepdims=True))
            prob = jnp.exp(s - lse).astype(BF16)
            prob_ref[h] = prob
            att_ref[:, h * HEAD_SIZE : (h + 1) * HEAD_SIZE] = dot(prob, val).astype(BF16)
        part_buf[...] = dot(att_ref[...], wo_ref[...]).astype(BF16)
        start(side_h)
        moe_acc[...] = jnp.zeros_like(moe_acc)
        back_acc[...] = jnp.zeros_like(back_acc)
        dgate_ref[...] = jnp.zeros_like(dgate_ref)
        arrived(g_own)

    @pl.when(step < pairs)
    def _():
        dh_buf[step] = dot_nt(g_buf[...], wd_ref[...].reshape(2 * width, model))

    @pl.when(step == pairs)
    def _():
        total = tok_ref[ds(t, own), :].astype(F32) + part_buf[ds(t, own), :].astype(F32)
        picked = routes_ref[ds(t, own), :]
        ids = lax.broadcasted_iota(jnp.int32, (own, EXTRA), 1)
        chosen = picked[:, 0:1] == ids
        for j in range(1, picked.shape[1]):
            chosen = chosen | (picked[:, j : j + 1] == ids)
        arrived(side_h)
        for k in sides:
            total = total + rs_buf[k - 1].astype(F32)
        n2 = (total * inverse_rms(total) * gm_ref[...].reshape(1, -1)).astype(BF16)
        x_buf[mine, :model] = n2
        x_buf[mine, model:] = jnp.where(chosen, 1.0, 0.0).astype(BF16)
        start(x_t + x_own + x_z)
        h1_ref[...] = total
        for h in range(q_width // HEAD_SIZE):
            prob_t_ref[h] = prob_ref[h].T
        n1t_ref[...] = n1_buf[...].T
        for k in sides:
            arrived(x_t[k - 1 : k])
            start(x_seen[k - 1 : k])
        arrived(g_z)
        start(g_direct + g_core + keep_g)
        arrived(x_own + x_seen)
        keep_x.start()
        gates = gates_of(x_buf, wr_ref, model)
        gates_ref[...] = gates
        store_split(gates, split)

    @pl.when(step == pairs + 3)
    def _():
        arrived(x_z)
        start(x_direct + x_core + x_z2)

    @pl.when(step == pairs + 6)
    def _():
        arrived(g_direct)
        start(g_relay + g_near)

    @pl.when(step == pairs + 9)
    def _():
        arrived(g_relay)
        start(g_far)
        arrived(x_direct)
        start(x_near)
        arrived(x_z2)
        start(x_far)

    @pl.when(step >= pairs)
    def _():
        pair = step - pairs
        first = c * (2 * pairs) + 2 * pair
        gate_pair = pair_of_gates(split[...], first, width)
        lane = lax.broadcasted_iota(jnp.int32, dgate_ref.shape, 1)
        for k in range(2):
            lanes = slice(k * width, (k + 1) * width)
            w_both = jnp.concatenate([wg_ref[k], wu_ref[k]], axis=1)
            both = dot(x_buf[:, :model], w_both)
            dh = dh_buf[pair, :, lanes]
            hid, ghid, dgp, dup = swiglu(both, dh, gate_pair[:, lanes])
            ghid_ref[:, lanes] = ghid
            dgp_ref[:, lanes] = dgp
            dup_ref[:, lanes] = dup
            row_sum = jnp.sum(hid * dh, axis=1, keepdims=True)
            dgate_ref[...] += jnp.where(lane == first + k, row_sum, 0.0)
            back_acc[...] += dot_nt(jnp.concatenate([dgp, dup], axis=1), w_both)
        moe_acc[...] += dot(ghid_ref[...], wd_ref[...].reshape(2 * width, model))

    @pl.when(step == last)
    def _():
        moe_ref[...] = moe_acc[...].astype(BF16)
        back_ref[...] = back_acc[...].astype(BF16)
        keep_x.wait()
        for copy in keep_g:
            copy.wait()
        arrived(g_core + g_near + g_far + x_core + x_near + x_far)
        sent = g_own + g_z + side_h + x_t + x_own + x_seen + x_z
        sent = sent + g_direct + g_relay + g_core + g_near + g_far
        for copy in sent + x_direct + x_z2 + x_core + x_near + x_far:
            copy.wait_send()


def whole_spec(a):
    shape = a.shape
    return pl.BlockSpec(shape, lambda *_: (0,) * len(shape), pipeline_mode=pl.Buffered(1))


def front(dp, tp, arrays, weights):
    tokens, wq, wk, wv = arrays[0], *arrays[6:9]
    length, model = tokens.shape
    count, _, width = weights[0].shape
    pairs = count // 2
    rows, own = 2 * length, length // tp
    heads, wide = wq.shape[1] // HEAD_SIZE, model + EXTRA
    q_width = wq.shape[1]
    widths = q_width + wk.shape[1] + wv.shape[1]
    others, sides = dp - 1, tp - 1
    copies = 1 + others + sides + sides + 1 + sides + 2 * others + (8 + 6) * others
    later = lambda i: jnp.maximum(i - pairs, 0)
    up = lambda shape: pl.BlockSpec((2,) + shape, lambda i: (later(i), 0, 0))
    down = pl.BlockSpec((2, width, model), lambda i: (lax.rem(i, pairs), 0, 0))
    saved = pl.BlockSpec((rows, 2 * width), lambda i: (0, later(i)))
    shapes = [
        ((rows * dp, wide), BF16),
        ((rows * dp, model), BF16),
        ((rows, model), BF16),
        ((rows, model), BF16),
        ((rows, EXTRA), F32),
        ((rows, EXTRA), F32),
        ((own, model), F32),
        ((length, widths), BF16),
        ((length, q_width), BF16),
        ((heads, length, length), BF16),
        ((heads, length, length), BF16),
        ((model, length), BF16),
        ((rows, count * width), BF16),
        ((rows, count * width), BF16),
        ((rows, count * width), BF16),
    ]
    shapes = [jax.ShapeDtypeStruct(*s) for s in shapes]
    scratch = [
        ((rows, wide), BF16),
        ((rows, model), BF16),
        ((others, own, model), BF16),
        ((length, model), BF16),
        ((length, model), BF16),
        ((sides, own, model), BF16),
        ((pairs, rows, 2 * width), F32),
        ((rows, 2 * EXTRA), BF16),
        ((rows, model), F32),
        ((rows, model), F32),
    ]
    return pl.pallas_call(
        functools.partial(front_kernel, dp, tp),
        grid=(2 * pairs,),
        out_shape=shapes,
        in_specs=[whole_spec(a) for a in arrays] + [up((model, width)), up((model, width)), down],
        out_specs=[ANY, ANY] + [whole_spec(s) for s in shapes[2:12]] + [saved] * 3,
        scratch_shapes=[pltpu.VMEM(*s) for s in scratch]
        + [
            pltpu.SemaphoreType.DMA((copies,)),
            pltpu.SemaphoreType.DMA((copies,)),
            pltpu.SemaphoreType.DMA((2 + others,)),
        ],
        compiler_params=pltpu.CompilerParams(
            collective_id=0, has_side_effects=True, vmem_limit_bytes=VMEM_LIMIT
        ),
        name="front",
    )(*arrays, *weights)


def backward_kernel(
    dp,
    tp,
    back_hbm,
    moe_hbm,
    dgate_hbm,
    gates_ref,
    h1_ref,
    tok_hbm,
    cot_hbm,
    ga_ref,
    gm_ref,
    wr_ref,
    wq_hbm,
    wk_hbm,
    wv_hbm,
    wo_hbm,
    qkv_hbm,
    att_hbm,
    prob_hbm,
    prob_t_hbm,
    n1t_hbm,
    rope_hbm,
    xr_ref,
    gr_ref,
    wg_ref,
    wu_ref,
    wd_ref,
    out_ref,
    in_ref,
    dl_all,
    qkv_grad_ref,
    o_grad_ref,
    gains_ref,
    ghid_ref,
    dgp_ref,
    dup_ref,
    back_ref,
    moe_ref,
    dgate_ref,
    tok_ref,
    cot_ref,
    wq_ref,
    wk_ref,
    wv_ref,
    wo_ref,
    qkv_ref,
    att_ref,
    prob_ref,
    prob_t_ref,
    n1t_ref,
    rope_ref,
    x_rest,
    g_rest,
    split,
    pair_b,
    pair_m,
    pair_d,
    sum_b,
    sum_m,
    sum_d,
    rs_b,
    rs_m,
    rs_d,
    dh1_buf,
    da_buf,
    dl_buf,
    d_buf,
    do_buf,
    part_buf,
    rs_3,
    gain_buf,
    gain_t,
    gain_z,
    gain_zs,
    gain_c,
    out_buf,
    in_buf,
    q_part,
    q_pair,
    q_sum,
    q_in,
    o_part,
    o_pair,
    o_sum,
    o_in,
    send_sem,
    recv_sem,
    keep_sem,
    load_sem,
):
    step, last = pl.program_id(0), pl.num_programs(0) - 1
    net = Peers(dp, tp, send_sem, recv_sem)
    z, c, t = net.z, net.c, net.t
    length, model = tok_ref.shape
    own = length // tp
    part = model // dp
    width = wg_ref.shape[2]
    q_width, kv_width = wq_ref.shape[1], wk_ref.shape[1]
    group = q_width // kv_width
    others, sides = range(1, dp), range(1, tp)
    mine = ds(t, own)
    here, there = ds(c, length), ds(1 - c, length)

    def columns(index):
        return pl.ds(pl.multiple_of(index * part, 128), part)

    def link(src, dst, device):
        return net.make(src, dst, net.number(1), device)

    def to_sides(ref, into):
        return [
            link(ref.at[ds(lax.rem(t + k, tp), own)], into.at[k - 1], net.tensor(k)) for k in sides
        ]

    def share(ref):
        return [link(ref.at[mine], ref.at[mine], net.tensor(k)) for k in sides]

    def on_to_partner(ref):
        rows = [ds(p * 2 + c, length) for p in others]
        return [link(ref.at[r], ref.at[r], net.partner()) for r in rows]

    def over_planes(ref, into):
        return [link(ref, into.at[ds((dp - k) * 2 + c, length)], net.plane(k)) for k in others]

    def start(copies):
        for copy in copies:
            copy.start()

    pair_bd = [
        link(back_hbm.at[there], pair_b, net.partner()),
        link(dgate_hbm.at[there], pair_d, net.partner()),
    ]
    pair_mo = [link(moe_hbm.at[there], pair_m, net.partner())]
    side_bd = to_sides(sum_b, rs_b) + to_sides(sum_d, rs_d)
    side_mo = to_sides(sum_m, rs_m)
    share_da = share(da_buf) + share(dl_buf)
    dl_z = over_planes(dl_buf, dl_all)
    dl_own = [link(dl_buf, dl_all.at[here], net.partner())]
    dl_c = on_to_partner(dl_all)
    q_core = [link(q_part.at[:, 1 - c], q_pair, net.partner())]
    q_z = [link(q_sum.at[lax.rem(z + k, dp)], q_in.at[k - 1], net.plane(k)) for k in others]
    o_core = [link(o_part.at[:, 1 - c], o_pair, net.partner())]
    o_z = [link(o_sum.at[lax.rem(z + k, dp)], o_in.at[k - 1], net.plane(k)) for k in others]
    share_out = share(out_buf)
    side_3 = to_sides(part_buf, rs_3)
    share_in = share(in_buf)
    side_gain = [link(gain_buf, gain_t.at[k - 1], net.tensor(k)) for k in sides]
    plane_gain = [
        link(gain_zs.at[:, columns(lax.rem(z + k, dp))], gain_z.at[k - 1], net.plane(k))
        for k in others
    ]
    pair_gain = [link(gain_c.at[0], gain_c.at[1], net.partner())]
    keep_dl = pltpu.make_async_copy(dl_buf, dl_all.at[here], keep_sem.at[0])
    plane_rows = xr_ref.shape[0] // dp
    rest = pl.ds(plane_rows, xr_ref.shape[0] - plane_rows)
    late = [
        (back_hbm.at[here], back_ref),
        (dgate_hbm.at[here], dgate_ref),
        (moe_hbm.at[here], moe_ref),
        (cot_hbm, cot_ref),
        (wo_hbm, wo_ref),
        (att_hbm, att_ref),
        (qkv_hbm, qkv_ref),
        (prob_hbm, prob_ref),
        (prob_t_hbm, prob_t_ref),
        (rope_hbm, rope_ref),
        (wq_hbm, wq_ref),
        (wk_hbm, wk_ref),
        (wv_hbm, wv_ref),
        (n1t_hbm, n1t_ref),
        (tok_hbm, tok_ref),
    ]
    late = [pltpu.make_async_copy(src, dst, load_sem.at[i]) for i, (src, dst) in enumerate(late)]

    def loaded(first, end):
        for copy in late[first:end]:
            copy.wait()

    load_x = pltpu.make_async_copy(xr_ref.at[rest], x_rest, keep_sem.at[1])
    load_g = pltpu.make_async_copy(gr_ref.at[rest], g_rest, keep_sem.at[2])

    @pl.when(step == 0)
    def _():
        load_x.start()
        load_g.start()
        start(late[:2])
        net.greet()
        start(pair_bd)
        start(late[2:])
        load_x.wait()
        store_split(gates_of(x_rest, wr_ref, model), split)
        load_g.wait()

    @pl.when(step == 1)
    def _():
        arrived(pair_bd)
        loaded(0, 2)
        sum_b[...] = (back_ref[...].astype(F32) + pair_b[...].astype(F32)).astype(BF16)
        sum_d[...] = dgate_ref[...] + pair_d[...]
        start(side_bd + pair_mo)

    def over_pair(part, pair, total):
        total[...] = (part[:, c].astype(F32) + pair[...].astype(F32)).astype(BF16)

    def over_z(total, came, out):
        value = total[z].astype(F32)
        for k in others:
            value = value + came[k - 1].astype(F32)
        out[...] = value

    @pl.when(step == 3)
    def _():
        arrived(side_bd)
        loaded(2, 4)
        d_n2 = sum_b[mine, :].astype(F32)
        dgate = sum_d[mine, :]
        for k in sides:
            d_n2 = d_n2 + rs_b[k - 1].astype(F32)
            dgate = dgate + rs_d[k - 1]
        gates = gates_ref[ds(c * tp + t, own), :]
        d_logits = gates * (dgate - jnp.sum(gates * dgate, axis=1, keepdims=True))
        dl_buf[mine, :] = d_logits.astype(BF16)
        d_n2 = d_n2 + dot_nt(d_logits.astype(BF16), wr_ref[...])
        h1 = h1_ref[...]
        r2 = inverse_rms(h1)
        weighted = d_n2 * gm_ref[...].reshape(1, -1)
        inner = jnp.mean(weighted * h1, axis=-1, keepdims=True)
        gain_buf[...] = jnp.zeros_like(gain_buf)
        gain_buf[1:2, :] = jnp.sum(d_n2 * h1 * r2, axis=0, keepdims=True)
        d_h1 = cot_ref[mine, :].astype(F32) + (r2 * weighted - h1 * (r2 * r2 * r2) * inner)
        dh1_buf[...] = d_h1
        da_buf[mine, :] = d_h1.astype(BF16)
        start(share_da)
        arrived(pair_mo)
        sum_m[...] = (moe_ref[...].astype(F32) + pair_m[...].astype(F32)).astype(BF16)

    @pl.when(step == 5)
    def _():
        loaded(4, len(late))
        arrived(share_da)
        start(side_mo + dl_z + dl_own)
        keep_dl.start()
        do_buf[...] = dot_nt(da_buf[...], wo_ref[...]).astype(BF16)
        o_part[...] = dot_tn(da_buf[...], att_ref[...]).astype(BF16).reshape(o_part.shape)
        start(o_core)
        scale = HEAD_SIZE ** (-0.5)
        d_key, d_val, d_query = [], [], []
        for kv in range(kv_width // HEAD_SIZE):
            if kv == 1:
                arrived(o_core)
                over_pair(o_part, o_pair, o_sum)
                start(o_z)
            at_k = q_width + kv * HEAD_SIZE
            at_v = q_width + kv_width + kv * HEAD_SIZE
            key = qkv_ref[:, at_k : at_k + HEAD_SIZE]
            val = qkv_ref[:, at_v : at_v + HEAD_SIZE]
            dk = jnp.zeros((length, HEAD_SIZE), F32)
            dv = jnp.zeros((length, HEAD_SIZE), F32)
            for h in range(kv * group, (kv + 1) * group):
                at = slice(h * HEAD_SIZE, (h + 1) * HEAD_SIZE)
                q = qkv_ref[:, at]
                d_out = do_buf[:, at]
                delta = jnp.sum(
                    d_out.astype(F32) * att_ref[:, at].astype(F32), axis=-1, keepdims=True
                )
                d_s = (prob_ref[h].astype(F32) * (dot_nt(d_out, val) - delta)).astype(BF16)
                d_query.append(dot(d_s, key) * scale)
                dk = dk + dot_tn(d_s, q)
                dv = dv + dot(prob_t_ref[h], d_out)
            d_key.append(dk * scale)
            d_val.append(dv)
        arrived(side_mo)
        total = h1_ref[...] + sum_m[mine, :].astype(F32)
        for k in sides:
            total = total + rs_m[k - 1].astype(F32)
        out_buf[mine, :] = total.astype(BF16)
        start(share_out)
        d_buf[:, :q_width] = rotate(jnp.concatenate(d_query, axis=1), rope_ref, -1.0).astype(BF16)
        d_buf[:, q_width : q_width + kv_width] = rotate(
            jnp.concatenate(d_key, axis=1), rope_ref, -1.0
        ).astype(BF16)
        d_buf[:, q_width + kv_width :] = jnp.concatenate(d_val, axis=1).astype(BF16)
        part_n1 = dot_nt(d_buf[:, :q_width], wq_ref[...])
        part_n1 = part_n1 + dot_nt(d_buf[:, q_width : q_width + kv_width], wk_ref[...])
        part_n1 = part_n1 + dot_nt(d_buf[:, q_width + kv_width :], wv_ref[...])
        part_buf[...] = part_n1.astype(BF16)
        start(side_3)
        q_part[...] = dot(n1t_ref[...], d_buf[...]).astype(BF16).reshape(q_part.shape)
        start(q_core)

    @pl.when(step == 6)
    def _():
        arrived(q_core)
        over_pair(q_part, q_pair, q_sum)
        start(q_z)
        arrived(dl_z)
        start(dl_c)

    @pl.when(step == 7)
    def _():
        arrived(side_3)
        d_n1 = part_buf[mine, :].astype(F32)
        for k in sides:
            d_n1 = d_n1 + rs_3[k - 1].astype(F32)
        resid = tok_ref[mine, :].astype(F32)
        r1 = inverse_rms(resid)
        weighted = d_n1 * ga_ref[...].reshape(1, -1)
        inner = jnp.mean(weighted * resid, axis=-1, keepdims=True)
        gain_buf[0:1, :] = jnp.sum(d_n1 * resid * r1, axis=0, keepdims=True)
        d_x = dh1_buf[...] + (r1 * weighted - resid * (r1 * r1 * r1) * inner)
        in_buf[mine, :] = d_x.astype(BF16)
        start(side_gain + share_in)

    @pl.when(step == 8)
    def _():
        arrived(side_gain)
        gain = gain_buf[...]
        for k in sides:
            gain = gain + gain_t[k - 1]
        gain_zs[...] = gain
        start(plane_gain)

    @pl.when(step == 9)
    def _():
        arrived(plane_gain)
        gain = gain_zs[:, columns(z)]
        for k in others:
            gain = gain + gain_z[k - 1]
        gain_c[0] = gain
        start(pair_gain)

    first = c * (2 * pl.num_programs(0)) + 2 * step
    wd_pair = wd_ref[...].reshape(2 * width, model)
    gate_pair = pair_of_gates(split[...], first, width)
    dh_pair = dot_nt(g_rest[...], wd_pair)
    for k in range(2):
        lanes = slice(k * width, (k + 1) * width)
        both = dot(x_rest[:, :model], jnp.concatenate([wg_ref[k], wu_ref[k]], axis=1))
        _, ghid, dgp, dup = swiglu(both, dh_pair[:, lanes], gate_pair[:, lanes])
        ghid_ref[:, lanes] = ghid
        dgp_ref[:, lanes] = dgp
        dup_ref[:, lanes] = dup

    @pl.when(step == last)
    def _():
        arrived(pair_gain)
        gains_ref[...] = gain_c[0] + gain_c[1]
        arrived(o_z)
        over_z(o_sum, o_in, o_grad_ref)
        arrived(share_out + share_in)
        out_ref[...] = out_buf[...]
        in_ref[...] = in_buf[...]
        arrived(q_z)
        over_z(q_sum, q_in, qkv_grad_ref)
        arrived(dl_own + dl_c)
        keep_dl.wait()
        sent = pair_bd + pair_mo + side_bd + side_mo + share_da + share_out + share_in + side_3
        sent = sent + dl_z + dl_own + dl_c + q_core + q_z + o_core + o_z
        for copy in sent + side_gain + plane_gain + pair_gain:
            copy.wait_send()


def backward(dp, tp, arrays, streamed, weights):
    tokens = arrays[5]
    wq, wk, wv = arrays[10:13]
    all_rows, model = streamed[1].shape
    rest_rows = all_rows - all_rows // dp
    count, _, width = weights[0].shape
    length = tokens.shape[0]
    own, part = length // tp, model // dp
    q_width = wq.shape[1]
    wide = q_width + wk.shape[1] + wv.shape[1]
    others, sides = dp - 1, tp - 1
    copies = 3 + 9 * sides + (2 * others + 1) + 2 * (1 + others) + sides + others + 1
    by_pair = lambda shape: pl.BlockSpec((2,) + shape, lambda i: (i, 0, 0))
    saved = pl.BlockSpec((rest_rows, 2 * width), lambda i: (0, i))
    shapes = [
        ((length, model), BF16),
        ((length, model), BF16),
        ((all_rows, EXTRA), BF16),
        ((part // 2, wide), F32),
        ((part // 2, q_width), F32),
        ((8, part), F32),
        ((rest_rows, count * width), BF16),
        ((rest_rows, count * width), BF16),
        ((rest_rows, count * width), BF16),
    ]
    shapes = [jax.ShapeDtypeStruct(*s) for s in shapes]
    full, block, slots = (length, model), (own, model), (sides, own, model)
    copied = [arrays[i] for i in (5, 6, *range(10, len(arrays)))]
    scratch = [
        (full, BF16),
        (full, BF16),
        ((length, EXTRA), F32),
        *((a.shape, a.dtype) for a in copied),
        ((rest_rows, streamed[0].shape[1]), BF16),
        ((rest_rows, model), BF16),
        ((rest_rows, 2 * EXTRA), BF16),
        (full, BF16),
        (full, BF16),
        ((length, EXTRA), F32),
        (full, BF16),
        (full, BF16),
        ((length, EXTRA), F32),
        (slots, BF16),
        (slots, BF16),
        ((sides, own, EXTRA), F32),
        (block, F32),
        (full, BF16),
        ((length, EXTRA), BF16),
        ((length, wide), BF16),
        ((length, q_width), BF16),
        (full, BF16),
        (slots, BF16),
        ((8, model), F32),
        ((sides, 8, model), F32),
        ((others, 8, part), F32),
        ((8, model), F32),
        ((2, 8, part), F32),
        (full, BF16),
        (full, BF16),
        ((dp, 2, part // 2, wide), BF16),
        ((dp, part // 2, wide), BF16),
        ((dp, part // 2, wide), BF16),
        ((others, part // 2, wide), BF16),
        ((dp, 2, part // 2, q_width), BF16),
        ((dp, part // 2, q_width), BF16),
        ((dp, part // 2, q_width), BF16),
        ((others, part // 2, q_width), BF16),
    ]
    return pl.pallas_call(
        functools.partial(backward_kernel, dp, tp),
        grid=(count // 2,),
        out_shape=shapes,
        in_specs=[whole_spec(a) if i in (3, 4, 7, 8, 9) else ANY for i, a in enumerate(arrays)]
        + [ANY, ANY]
        + [by_pair((model, width)), by_pair((model, width)), by_pair((width, model))],
        out_specs=[whole_spec(shapes[0]), whole_spec(shapes[1]), ANY]
        + [whole_spec(s) for s in shapes[3:6]]
        + [saved] * 3,
        scratch_shapes=[pltpu.VMEM(*s) for s in scratch]
        + [
            pltpu.SemaphoreType.DMA((copies,)),
            pltpu.SemaphoreType.DMA((copies,)),
            pltpu.SemaphoreType.DMA((3,)),
            pltpu.SemaphoreType.DMA((3 + len(copied),)),
        ],
        compiler_params=pltpu.CompilerParams(
            collective_id=2, has_side_effects=True, vmem_limit_bytes=VMEM_LIMIT
        ),
        name="backward",
    )(*arrays, *streamed, *weights)


def weights_kernel(
    place_ref,
    x_ref,
    g_ref,
    dl_ref,
    qkv_grad_ref,
    o_grad_ref,
    gains_ref,
    out_in_ref,
    in_in_ref,
    ghid_ref,
    dgp_ref,
    dup_ref,
    ghid_rest,
    dgp_rest,
    dup_rest,
    gate_grad_ref,
    up_grad_ref,
    down_grad_ref,
    query_ref,
    key_ref,
    value_ref,
    out_grad_ref,
    router_ref,
    ga_grad_ref,
    gm_grad_ref,
    out_ref,
    in_ref,
    xt_buf,
    gt_buf,
):
    step = pl.program_id(0)
    c = place_ref[1]
    width = gate_grad_ref.shape[2]
    plane_rows = ghid_ref.shape[0]

    @pl.when(step == 0)
    def _():
        xt_buf[...] = x_ref[...].T
        gt_buf[...] = g_ref[...].T
        q_width, kv_width = query_ref.shape[1], key_ref.shape[1]
        half = query_ref.shape[0]
        query_ref[...] = qkv_grad_ref[:, :q_width]
        key_ref[...] = qkv_grad_ref[:, q_width : q_width + kv_width]
        value_ref[...] = qkv_grad_ref[:, q_width + kv_width :]
        out_grad_ref[...] = o_grad_ref[...]
        out_ref[...] = out_in_ref[...]
        in_ref[...] = in_in_ref[...]
        router = dot(xt_buf[...], dl_ref[...]).T[: router_ref.shape[0]]
        router_ref[...] = jnp.where(c == 0, router[:, :half], router[:, half:])
        gains = jnp.where(c == 0, gains_ref[:, :half], gains_ref[:, half:])
        ga_grad_ref[...] = gains[0:1, :]
        gm_grad_ref[...] = gains[1:2, :]

    def contract(left, own, rest):
        return dot(left[:, :plane_rows], own[...]) + dot(left[:, plane_rows:], rest[...])

    gate_both = contract(xt_buf, dgp_ref, dgp_rest)
    up_both = contract(xt_buf, dup_ref, dup_rest)
    down_both = contract(gt_buf, ghid_ref, ghid_rest).T
    for k in range(2):
        lanes = slice(k * width, (k + 1) * width)
        gate_grad_ref[k] = gate_both[:, lanes]
        up_grad_ref[k] = up_both[:, lanes]
        down_grad_ref[k] = down_both[lanes, :]


def weight_grads(place, x, g, sides, own, rest, count, kv_width, experts):
    rows = x.shape[0]
    _, qkv_grad, o_grad, gains, output, _ = sides
    width = own[0].shape[1] // count
    part = gains.shape[1]
    q_width, half = o_grad.shape[1], part // 2
    by_pair = lambda shape: pl.BlockSpec((2,) + shape, lambda i, p: (i, 0, 0))
    saved = lambda a: pl.BlockSpec((a.shape[0], 2 * width), lambda i, p: (0, i))
    columns = pl.BlockSpec((rows, part), lambda i, p: (0, p[0]), pipeline_mode=pl.Buffered(1))
    shapes = [
        (count, part, width),
        (count, part, width),
        (count, width, part),
        (half, q_width),
        (half, kv_width),
        (half, kv_width),
        (half, q_width),
        (experts, half),
        (1, half),
        (1, half),
    ]
    shapes = [jax.ShapeDtypeStruct(s, F32) for s in shapes]
    shapes += [jax.ShapeDtypeStruct(output.shape, BF16)] * 2
    return pl.pallas_call(
        weights_kernel,
        grid_spec=pltpu.PrefetchScalarGridSpec(
            num_scalar_prefetch=1,
            grid=(count // 2,),
            in_specs=[columns, columns]
            + [whole_spec(a) for a in sides]
            + [saved(a) for a in own]
            + [saved(a) for a in rest],
            out_specs=[by_pair((part, width)), by_pair((part, width)), by_pair((width, part))]
            + [whole_spec(s) for s in shapes[3:]],
            scratch_shapes=[pltpu.VMEM((part, rows), BF16), pltpu.VMEM((part, rows), BF16)],
        ),
        out_shape=shapes,
        compiler_params=pltpu.CompilerParams(vmem_limit_bytes=VMEM_LIMIT),
        name="weight_grads",
    )(place, x, g, *sides, *own, *rest)


def rope_rows(length):
    half = HEAD_SIZE // 2
    frequency = ROPE_BASE ** (np.arange(half) * (-2.0 / HEAD_SIZE))
    angles = np.arange(length)[:, None] * frequency[None, :]
    cos, sin, none = np.cos(angles), np.sin(angles), np.zeros((length, half))
    double = lambda first, second: np.concatenate([first, second, first, second], axis=1)
    return np.stack([double(cos, cos), double(-sin, none), double(none, sin)]).astype(np.float32)


def gather_plan(
    tokens,
    gain_attn,
    w_query,
    key_projection,
    value_projection,
    w_out,
    gain_moe,
    w_router,
    w_gate,
    w_up,
    w_down,
    routes,
    cotangent,
):
    dp, tp = lax.axis_size("dp"), lax.axis_size("tensor")
    experts = w_router.shape[1]
    rope = jnp.asarray(rope_rows(tokens.shape[0]))
    ga, gm = gain_attn, gain_moe
    wr = jnp.pad(w_router, ((0, 0), (0, EXTRA - experts)))
    heads = (w_query, key_projection, value_projection, w_out)
    x_all, g_all, moe, back, dgate, gates, h1, *saved, ghid, dgp, dup = front(
        dp, tp, (tokens, cotangent, routes, ga, gm, wr, *heads, rope), (w_gate, w_up, w_down)
    )
    local = (back, moe, dgate, gates, h1, tokens, cotangent, ga, gm, wr, *heads)
    output, input_grad, d_logits, qkv_grad, o_grad, gains, *rest = backward(
        dp, tp, (*local, *saved, rope), (x_all, g_all), (w_gate, w_up, w_down)
    )
    place = jnp.stack([lax.axis_index("dp"), lax.axis_index("expert")]).astype(jnp.int32)
    (
        gate_grad,
        up_grad,
        down_grad,
        query_grad,
        key_grad,
        value_grad,
        out_grad,
        router_grad,
        gain_attn_grad,
        gain_moe_grad,
        output,
        input_grad,
    ) = weight_grads(
        place,
        x_all,
        g_all,
        (d_logits, qkv_grad, o_grad, gains, output, input_grad),
        (ghid, dgp, dup),
        rest,
        w_gate.shape[0],
        key_projection.shape[1],
        experts,
    )
    return (
        output,
        input_grad,
        gain_attn_grad[0],
        query_grad,
        key_grad,
        value_grad,
        out_grad.T,
        gain_moe_grad[0],
        router_grad.T,
        gate_grad,
        up_grad,
        down_grad,
    )


def solution(mesh):
    placed = (
        P(("dp", "expert"), None),
        P(),
        P(None, "tensor"),
        P(None, "tensor"),
        P(None, "tensor"),
        P("tensor", None),
        P(),
        P(),
        P("expert", None, "tensor"),
        P("expert", None, "tensor"),
        P("expert", "tensor", None),
        P(("dp", "expert"), None),
        P(("dp", "expert"), None),
    )
    sequences = mesh.shape["dp"] * mesh.shape["expert"]
    few = sequences * SEQUENCE_LENGTH <= GATHER_ROWS
    few = few and mesh.shape["tensor"] == 4 and mesh.shape["expert"] == 2
    return jax.shard_map(
        gather_plan if few else reduce_plan,
        mesh=mesh,
        in_specs=placed,
        out_specs=(
            P(("dp", "expert"), None),
            P(("dp", "expert"), None),
            P(("dp", "expert")),
            P(("dp", "expert"), "tensor"),
            P(("dp", "expert"), "tensor"),
            P(("dp", "expert"), "tensor"),
            P("tensor", ("dp", "expert")),
            P(("dp", "expert")),
            P(("dp", "expert"), None),
            P("expert", "dp", "tensor"),
            P("expert", "dp", "tensor"),
            P("expert", "tensor", "dp"),
        ),
        check_vma=False,
    )
```

```python
import functools
import math

import jax
import jax.numpy as jnp
import numpy as np
from jax import lax
from jax.experimental import pallas as pl
from jax.experimental.pallas import tpu as pltpu
from jax.sharding import PartitionSpec as P

HEAD_SIZE = 64
SEQUENCE_LENGTH = 256
CAP = 64


EPSILON = 1e-06
ROPE_BASE = 10000.0
BLOCK_ROWS = 512


def split_up(x, dim, count):
    dims = x.shape
    tiles = x.reshape(*dims[:dim], count, dims[dim] // count, *dims[dim + 1 :])
    return jnp.moveaxis(tiles, dim, 0)


def sum_at_owner(x, axis, dim):
    tiles = split_up(x, dim, lax.axis_size(axis))
    arrived = lax.all_to_all(tiles, axis, split_axis=0, concat_axis=0, tiled=True)
    return arrived.astype(jnp.float32).sum(axis=0)


def side_by_side(arrays, axis, dim, along):
    both = jnp.concatenate(arrays, axis=along)
    filled, at, outs = (sum_at_owner(both, axis, dim), 0, [])
    for a in arrays:
        outs.append(lax.slice_in_dim(filled, at, at + a.shape[along], axis=along))
        at += a.shape[along]
    return tuple(outs)


def sent_together(arrays, axis, dim, along):
    widths = [math.prod(a.shape[along:]) for a in arrays]
    both = jnp.concatenate(
        [a.reshape(*a.shape[:along], w) for a, w in zip(arrays, widths)], axis=along
    )
    filled = sum_at_owner(both, axis, dim)
    tiles = jnp.split(filled, [sum(widths[:k]) for k in range(1, len(widths))], axis=along)
    return tuple(
        (b.reshape(*filled.shape[:along], *a.shape[along:]) for a, b in zip(arrays, tiles))
    )


def rms_scale(hidden):
    return lax.rsqrt(jnp.mean(hidden * hidden, axis=-1, keepdims=True) + EPSILON)


def norm_back(hidden, scaling, gain_vec, grad_out):
    weighted = grad_out * gain_vec
    gain_grad = jnp.sum(grad_out * hidden * scaling, axis=0)
    inner_mean = jnp.mean(weighted * hidden, axis=-1, keepdims=True)
    return (scaling * weighted - hidden * (scaling * scaling * scaling) * inner_mean, gain_grad)


def rope_tables(positions, head_dim):
    half_dim = head_dim // 2
    frequency = jnp.exp(
        jnp.arange(half_dim, dtype=jnp.float32) * (-2.0 * math.log(ROPE_BASE) / head_dim)
    )
    angles = positions[:, None] * frequency[None, :]
    return (jnp.cos(angles), jnp.sin(angles))


def apply_rotary(vectors, cosine_table, sine_component):
    half_dim = vectors.shape[-1] // 2
    first_half = vectors[..., :half_dim]
    second_half = vectors[..., half_dim:]
    cos_rows = cosine_table[:, None, :]
    sin_rows = sine_component[:, None, :]
    return jnp.concatenate(
        [
            first_half * cos_rows - second_half * sin_rows,
            first_half * sin_rows + second_half * cos_rows,
        ],
        axis=-1,
    )


def slot_table(route_ids, expert_count, capacity):
    number_of_rows, top_count = route_ids.shape
    flat_ids = route_ids.reshape(-1)
    one_hot = (flat_ids[:, None] == jnp.arange(expert_count, dtype=jnp.int32)[None, :]).astype(
        jnp.int32
    )
    earlier = jnp.cumsum(one_hot, axis=0) - one_hot
    slot_ids = jnp.sum(earlier * one_hot, axis=1)
    slot_where = flat_ids * capacity + slot_ids
    pick_ids = jnp.arange(number_of_rows * top_count, dtype=jnp.int32)
    token_of = (
        jnp.full((expert_count * capacity,), number_of_rows, jnp.int32)
        .at[slot_where]
        .set(pick_ids // top_count)
    )
    pick_of = (
        jnp.full((expert_count * capacity,), number_of_rows * top_count, jnp.int32)
        .at[slot_where]
        .set(pick_ids)
    )
    return (slot_where, token_of, pick_of)


def block_scores(query_rows, key_rows, query_group_width):
    block_len = query_rows.shape[0]
    key_count, kv_heads, head_dim = key_rows.shape
    grouped = query_rows.reshape(block_len, kv_heads, query_group_width, head_dim)
    scores = jnp.einsum(
        "qhgd,khd->hgqk", grouped, key_rows, preferred_element_type=jnp.float32
    ) * head_dim ** (-0.5)
    row_pos = jnp.arange(block_len, dtype=jnp.int32)[:, None]
    col_pos = jnp.arange(key_count, dtype=jnp.int32)[None, :]
    return (jnp.where(col_pos <= row_pos, scores, -1e30), grouped)


def sequence_forward(query_rows, key_rows, value_rows, query_group_width):
    length, kv_heads, head_dim = key_rows.shape
    block_len = min(BLOCK_ROWS, length)
    scores, grouped = block_scores(query_rows, key_rows, query_group_width)
    largest = jnp.max(scores, axis=-1, keepdims=True)
    log_total = largest + jnp.log(jnp.sum(jnp.exp(scores - largest), axis=-1, keepdims=True))
    weights = jnp.exp(scores - log_total).astype(jnp.bfloat16)
    attended = jnp.einsum("hgqk,khd->qhgd", weights, value_rows, preferred_element_type=jnp.float32)
    outputs = attended.reshape(block_len, -1, head_dim).astype(jnp.bfloat16)
    return (outputs, log_total)


def sequence_backward(
    query_rows, key_rows, value_rows, attended, log_total, d_attended, query_group_width
):
    length, kv_heads, head_dim = key_rows.shape
    block_len = min(BLOCK_ROWS, length)
    scale_factor = head_dim ** (-0.5)
    key_gradient = jnp.zeros((length, kv_heads, head_dim), jnp.float32)
    value_gradient = jnp.zeros((length, kv_heads, head_dim), jnp.float32)
    scores, grouped = block_scores(query_rows, key_rows, query_group_width)
    weights = jnp.exp(scores - log_total)
    d_grouped = d_attended.reshape(block_len, kv_heads, query_group_width, head_dim)
    o_grouped = attended.reshape(block_len, kv_heads, query_group_width, head_dim)
    delta = jnp.sum(d_grouped.astype(jnp.float32) * o_grouped.astype(jnp.float32), axis=-1)
    delta = jnp.transpose(delta, (1, 2, 0))[..., None]
    d_weights = jnp.einsum(
        "qhgd,khd->hgqk", d_grouped, value_rows, preferred_element_type=jnp.float32
    )
    d_scores = (weights * (d_weights - delta)).astype(jnp.bfloat16)
    block_query = (
        jnp.einsum("hgqk,khd->qhgd", d_scores, key_rows, preferred_element_type=jnp.float32)
        * scale_factor
    )
    query_parts = block_query.reshape(block_len, -1, head_dim)
    key_gradient = key_gradient.at[:block_len].add(
        jnp.einsum("hgqk,qhgd->khd", d_scores, grouped, preferred_element_type=jnp.float32)
        * scale_factor
    )
    value_gradient = value_gradient.at[:block_len].add(
        jnp.einsum(
            "hgqk,qhgd->khd",
            weights.astype(jnp.bfloat16),
            d_grouped,
            preferred_element_type=jnp.float32,
        )
    )
    return (query_parts, key_gradient, value_gradient)


def reduce_plan(
    tokens,
    gain_attn,
    w_query,
    key_projection,
    value_projection,
    w_out,
    gain_moe,
    w_router,
    w_gate,
    w_up,
    w_down,
    routes,
    cotangent,
):
    number_of_rows, model_width = tokens.shape
    head_dim = HEAD_SIZE
    query_heads = w_query.shape[1] // head_dim
    kv_heads = key_projection.shape[1] // head_dim
    query_group_width = query_heads // kv_heads
    expert_count = w_router.shape[1]
    local_experts = w_gate.shape[0]
    source_count = expert_count // local_experts
    capacity = CAP
    top_count = routes.shape[1]
    resid = tokens.astype(jnp.float32)
    scale_one = rms_scale(resid)
    first_normalized = (resid * scale_one * gain_attn).astype(jnp.bfloat16)
    positions = (jnp.arange(number_of_rows, dtype=jnp.int32) % SEQUENCE_LENGTH).astype(jnp.float32)
    cosine_table, sine_component = rope_tables(positions, head_dim)
    q_lin = jnp.dot(first_normalized, w_query, preferred_element_type=jnp.float32).reshape(
        number_of_rows, query_heads, head_dim
    )
    linear_key = jnp.dot(
        first_normalized, key_projection, preferred_element_type=jnp.float32
    ).reshape(number_of_rows, kv_heads, head_dim)
    value_reduced = (
        jnp.dot(first_normalized, value_projection, preferred_element_type=jnp.float32)
        .astype(jnp.bfloat16)
        .reshape(number_of_rows, kv_heads, head_dim)
    )
    q_rot = apply_rotary(q_lin, cosine_table, sine_component).astype(jnp.bfloat16)
    rotated_key = apply_rotary(linear_key, cosine_table, sine_component).astype(jnp.bfloat16)
    attended, log_total = sequence_forward(q_rot, rotated_key, value_reduced, query_group_width)
    flat_att = attended.reshape(number_of_rows, query_heads * head_dim)
    attn_part = jnp.dot(flat_att, w_out, preferred_element_type=jnp.float32)
    hidden1 = resid + lax.psum(attn_part.astype(jnp.bfloat16), "tensor").astype(jnp.float32)
    scale_two = rms_scale(hidden1)
    normed2 = (hidden1 * scale_two * gain_moe).astype(jnp.bfloat16)
    logits = jnp.dot(normed2, w_router, preferred_element_type=jnp.float32)
    chosen = jnp.take_along_axis(logits, routes, axis=1)
    gate_probs = jax.nn.softmax(chosen, axis=-1)
    slot_where, token_of, pick_of = slot_table(routes, expert_count, capacity)
    normed_pad = jnp.concatenate([normed2, jnp.zeros((1, model_width), jnp.bfloat16)], axis=0)
    outgoing = normed_pad[token_of].reshape(expert_count, capacity, model_width)
    received = lax.all_to_all(outgoing, "expert", split_axis=0, concat_axis=0, tiled=True)
    arrived = received.reshape(source_count, local_experts, capacity, model_width)
    gate_pre = jnp.einsum("secd,edh->sech", arrived, w_gate, preferred_element_type=jnp.float32)
    up_pre = jnp.einsum("secd,edh->sech", arrived, w_up, preferred_element_type=jnp.float32)
    sig_gate = jax.nn.sigmoid(gate_pre)
    activated = gate_pre * sig_gate
    hid_low = (activated * up_pre).astype(jnp.bfloat16)
    expert_out = jnp.einsum(
        "sech,ehd->secd", hid_low, w_down, preferred_element_type=jnp.float32
    ).astype(jnp.bfloat16)
    returned = lax.all_to_all(
        expert_out.reshape(expert_count, capacity, model_width),
        "expert",
        split_axis=0,
        concat_axis=0,
        tiled=True,
    )
    picked = returned.reshape(expert_count * capacity, model_width)[slot_where].reshape(
        number_of_rows, top_count, model_width
    )
    moe_part = jnp.zeros((number_of_rows, model_width), jnp.float32)
    for choice_index in range(top_count):
        moe_part = (
            moe_part
            + picked[:, choice_index].astype(jnp.float32)
            * gate_probs[:, choice_index : choice_index + 1]
        )
    moe_out = lax.psum(moe_part.astype(jnp.bfloat16), "tensor").astype(jnp.float32)
    output = (hidden1 + moe_out).astype(jnp.bfloat16)
    grad = cotangent.astype(jnp.float32)
    gate_dot = jnp.einsum("rjd,rd->rj", picked, cotangent, preferred_element_type=jnp.float32)
    grad_pad = jnp.concatenate([cotangent, jnp.zeros((1, model_width), jnp.bfloat16)], axis=0)
    gate_pad = jnp.concatenate([gate_probs.reshape(-1), jnp.zeros((1,), jnp.float32)], axis=0)
    sent_grad = (grad_pad[token_of].astype(jnp.float32) * gate_pad[pick_of][:, None]).astype(
        jnp.bfloat16
    )
    sent_grad = sent_grad.reshape(expert_count, capacity, model_width)
    grad_received = lax.all_to_all(sent_grad, "expert", split_axis=0, concat_axis=0, tiled=True)
    arrived_grad = grad_received.reshape(source_count, local_experts, capacity, model_width)
    d_hid = jnp.einsum("secd,ehd->sech", arrived_grad, w_down, preferred_element_type=jnp.float32)
    down_local = jnp.einsum(
        "sech,secd->ehd", hid_low, arrived_grad, preferred_element_type=jnp.float32
    )
    d_gate = (d_hid * up_pre * sig_gate * (1.0 + gate_pre * (1.0 - sig_gate))).astype(jnp.bfloat16)
    d_up = (d_hid * activated).astype(jnp.bfloat16)
    gate_local = jnp.einsum("secd,sech->edh", arrived, d_gate, preferred_element_type=jnp.float32)
    up_local = jnp.einsum("secd,sech->edh", arrived, d_up, preferred_element_type=jnp.float32)
    back_rows = jnp.einsum("sech,edh->secd", d_gate, w_gate, preferred_element_type=jnp.float32)
    back_rows = (
        back_rows + jnp.einsum("sech,edh->secd", d_up, w_up, preferred_element_type=jnp.float32)
    ).astype(jnp.bfloat16)
    came_back = lax.all_to_all(
        back_rows.reshape(expert_count, capacity, model_width),
        "expert",
        split_axis=0,
        concat_axis=0,
        tiled=True,
    )
    back_picked = came_back.reshape(expert_count * capacity, model_width)[slot_where].reshape(
        number_of_rows, top_count, model_width
    )
    back_part = jnp.zeros((number_of_rows, model_width), jnp.float32)
    for choice_index in range(top_count):
        back_part = back_part + back_picked[:, choice_index].astype(jnp.float32)
    back_total, dgate = (
        lax.psum(back_part.astype(jnp.bfloat16), "tensor").astype(jnp.float32),
        lax.psum(gate_dot.astype(jnp.bfloat16), "tensor").astype(jnp.float32),
    )
    inner_sum = jnp.sum(gate_probs * dgate, axis=1, keepdims=True)
    d_chosen = gate_probs * (dgate - inner_sum)
    matches = routes[:, :, None] == jnp.arange(expert_count, dtype=jnp.int32)[None, None, :]
    d_logits = jnp.sum(jnp.where(matches, d_chosen[:, :, None], 0.0), axis=1).astype(jnp.bfloat16)
    router_local = jnp.dot(normed2.T, d_logits, preferred_element_type=jnp.float32)
    d_normed2 = back_total + jnp.dot(d_logits, w_router.T, preferred_element_type=jnp.float32)
    d_hidden_part, gain_moe_local = norm_back(hidden1, scale_two, gain_moe, d_normed2)
    d_hidden1 = grad + d_hidden_part
    d_mixed = d_hidden1.astype(jnp.bfloat16)
    out_local = jnp.dot(flat_att.T, d_mixed, preferred_element_type=jnp.float32)
    d_att = (
        jnp.dot(d_mixed, w_out.T, preferred_element_type=jnp.float32)
        .astype(jnp.bfloat16)
        .reshape(number_of_rows, query_heads, head_dim)
    )
    dq_rot, rotated_key_gradient, dv_rows = sequence_backward(
        q_rot, rotated_key, value_reduced, attended, log_total, d_att, query_group_width
    )
    d_query = (
        apply_rotary(dq_rot, cosine_table, -sine_component)
        .astype(jnp.bfloat16)
        .reshape(number_of_rows, query_heads * head_dim)
    )
    key_gradient = (
        apply_rotary(rotated_key_gradient, cosine_table, -sine_component)
        .astype(jnp.bfloat16)
        .reshape(number_of_rows, kv_heads * head_dim)
    )
    value_gradient = dv_rows.astype(jnp.bfloat16).reshape(number_of_rows, kv_heads * head_dim)
    query_local = jnp.dot(first_normalized.T, d_query, preferred_element_type=jnp.float32)
    key_local = jnp.dot(first_normalized.T, key_gradient, preferred_element_type=jnp.float32)
    value_local = jnp.dot(first_normalized.T, value_gradient, preferred_element_type=jnp.float32)
    d_normed_part = jnp.dot(d_query, w_query.T, preferred_element_type=jnp.float32)
    d_normed_part = d_normed_part + jnp.dot(
        key_gradient, key_projection.T, preferred_element_type=jnp.float32
    )
    d_normed_part = d_normed_part + jnp.dot(
        value_gradient, value_projection.T, preferred_element_type=jnp.float32
    )
    d_normed1 = lax.psum(d_normed_part.astype(jnp.bfloat16), "tensor").astype(jnp.float32)
    d_resid_part, gain_attn_local = norm_back(resid, scale_one, gain_attn, d_normed1)
    input_grad = (d_hidden1 + d_resid_part).astype(jnp.bfloat16)
    gate_grad, up_grad, down_grad = (
        lax.psum_scatter(
            gate_local.astype(jnp.bfloat16), "dp", scatter_dimension=1, tiled=True
        ).astype(jnp.float32),
        lax.psum_scatter(
            up_local.astype(jnp.bfloat16), "dp", scatter_dimension=1, tiled=True
        ).astype(jnp.float32),
        lax.psum_scatter(
            down_local.astype(jnp.bfloat16), "dp", scatter_dimension=2, tiled=True
        ).astype(jnp.float32),
    )
    query_grad, key_grad, value_grad, out_grad, router_grad, gain_attn_grad, gain_moe_grad = (
        *side_by_side(
            (
                query_local.astype(jnp.bfloat16),
                key_local.astype(jnp.bfloat16),
                value_local.astype(jnp.bfloat16),
            ),
            ("dp", "expert"),
            0,
            1,
        ),
        sum_at_owner(out_local.astype(jnp.bfloat16), ("dp", "expert"), 1),
        *sent_together(
            (
                router_local.astype(jnp.bfloat16),
                gain_attn_local.astype(jnp.bfloat16),
                gain_moe_local.astype(jnp.bfloat16),
            ),
            ("dp", "expert"),
            0,
            1,
        ),
    )
    return (
        output,
        input_grad,
        gain_attn_grad,
        query_grad,
        key_grad,
        value_grad,
        out_grad,
        gain_moe_grad,
        router_grad,
        gate_grad,
        up_grad,
        down_grad,
    )


GATHER_ROWS = 4096
MESH = pl.DeviceIdType.MESH
VMEM = pl.BlockSpec(memory_space=pltpu.VMEM)
ANY = pl.BlockSpec(memory_space=pl.ANY)
EXTRA = 128
VMEM_LIMIT = 60 * 2**20
STAGE_PLACES = (1, 5, 9, 11, 14, 16, 18)
F32, BF16 = jnp.float32, jnp.bfloat16


def dot(a, b):
    return jnp.dot(a, b, preferred_element_type=F32)


def dot_nt(a, b):
    return lax.dot_general(a, b, (((1,), (1,)), ((), ())), preferred_element_type=F32)


def dot_tn(a, b):
    return lax.dot_general(a, b, (((0,), (0,)), ((), ())), preferred_element_type=F32)


def ds(index, size):
    return pl.ds(pl.multiple_of(index * size, size), size)


class Peers:
    def __init__(self, dp, tp, send_sem, recv_sem):
        self.z, self.c, self.t = (lax.axis_index(a) for a in ("dp", "expert", "tensor"))
        self.dp, self.tp = dp, tp
        self.send_sem, self.recv_sem = send_sem, recv_sem
        self.used = 0
        self.open = []

    def tensor(self, k):
        return (self.z, self.c, lax.rem(self.t + k, self.tp))

    def near(self, axis):
        row, col = self.t // 2, self.t % 2
        index = row * 2 + (1 - col) if axis == 0 else (1 - row) * 2 + col
        return (self.z, self.c, index)

    def plane(self, k):
        return (lax.rem(self.z + k, self.dp), self.c, self.t)

    def partner(self):
        return (self.z, 1 - self.c, self.t)

    def greet(self):
        barrier = pltpu.get_barrier_semaphore()
        everyone = [self.tensor(k) for k in range(1, self.tp)]
        everyone += [self.plane(k) for k in range(1, self.dp)] + [self.partner()]
        for peer in everyone:
            pl.semaphore_signal(barrier, inc=1, device_id=peer, device_id_type=MESH)
        pl.semaphore_wait(barrier, len(everyone))

    def number(self, count):
        first = self.used
        self.used += count
        return first

    def make(self, src, dst, number, device):
        return pltpu.make_async_remote_copy(
            src_ref=src,
            dst_ref=dst,
            send_sem=self.send_sem.at[number],
            recv_sem=self.recv_sem.at[number],
            device_id=device,
            device_id_type=MESH,
        )

    def to(self, src, dst, device):
        copy = self.make(src, dst, self.number(1), device)
        copy.start()
        self.open.append(copy)
        return copy

    def keep(self, src, dst, sem):
        copy = pltpu.make_async_copy(src, dst, sem)
        copy.start()
        return copy

    def drain(self):
        for copy in self.open:
            copy.wait_send()


def arrived(copies):
    for copy in copies:
        copy.wait_recv()


def rotate(u, rope_ref, scale=1.0, sign=1.0):
    width = u.shape[1]
    tiles = []
    for at in range(0, width, 128):
        v = u[:, at : at + 128]
        side = pltpu.roll(v, 96, 1) * rope_ref[1] + pltpu.roll(v, 32, 1) * rope_ref[2]
        turned = v * rope_ref[0] + side if sign > 0 else v * rope_ref[0] - side
        tiles.append(turned if scale == 1.0 else turned * scale)
    return tiles[0] if len(tiles) == 1 else jnp.concatenate(tiles, axis=1)


def stack_heads(u, kv, group):
    heads = [kv * group + j for j in range(group)]
    return jnp.concatenate([u[:, h * HEAD_SIZE : (h + 1) * HEAD_SIZE] for h in heads], axis=0)


def inverse_rms(u):
    return lax.rsqrt(jnp.mean(u * u, axis=-1, keepdims=True) + EPSILON)


def causal(length):
    row = lax.broadcasted_iota(jnp.int32, (length, length), 0)
    col = lax.broadcasted_iota(jnp.int32, (length, length), 1)
    return col <= row


def pad_router(wr_ref, wr_buf):
    wr_buf[...] = jnp.zeros_like(wr_buf)
    wr_buf[: wr_ref.shape[0], :] = wr_ref[...]


def gates_of(x_ref, wr_buf, model):
    logits = dot_nt(x_ref[:, :model], wr_buf[...])
    chosen = x_ref[:, model:].astype(F32) > 0.5
    top = jnp.max(jnp.where(chosen, logits, -jnp.inf), axis=1, keepdims=True)
    weight = jnp.where(chosen, jnp.exp(jnp.where(chosen, logits - top, 0.0)), 0.0)
    return weight / jnp.sum(weight, axis=1, keepdims=True)


def store_split(gates, split_ref):
    high = gates.astype(BF16)
    split_ref[:, :EXTRA] = high
    split_ref[:, EXTRA:] = (gates - high.astype(F32)).astype(BF16)


def pair_of_gates(split, first, width):
    k_pos = lax.broadcasted_iota(jnp.int32, (2 * EXTRA, 2 * width), 0)
    l_pos = lax.broadcasted_iota(jnp.int32, (2 * EXTRA, 2 * width), 1)
    pick = jnp.where(k_pos % EXTRA == first + l_pos // width, 1.0, 0.0).astype(BF16)
    return dot(split, pick)


def swiglu(both, dh, gate):
    width = dh.shape[1]
    gate_pre, up_pre = both[:, :width], both[:, width:]
    sig = jax.nn.sigmoid(gate_pre)
    act = gate_pre * sig
    hid = act * up_pre
    d_hid = dh * gate
    d_gate = d_hid * up_pre * sig * (1.0 + gate_pre * (1.0 - sig))
    return hid, (hid * gate).astype(BF16), d_gate.astype(BF16), (d_hid * act).astype(BF16)


def front_kernel(
    dp,
    tp,
    tok_ref,
    cot_ref,
    routes_ref,
    ga_ref,
    gm_ref,
    wr_ref,
    wq_ref,
    wk_ref,
    wv_ref,
    wo_ref,
    rope_ref,
    wg_ref,
    wu_ref,
    wd_ref,
    xr_ref,
    gr_ref,
    moe_ref,
    back_ref,
    dgate_ref,
    gates_ref,
    h1_ref,
    kv_ref,
    att_ref,
    qs_ref,
    as_ref,
    prob_ref,
    prob_t_ref,
    n1t_ref,
    ghid_ref,
    dgp_ref,
    dup_ref,
    place_ref,
    x_buf,
    g_buf,
    gz_buf,
    wr_buf,
    routes_buf,
    n1_buf,
    part_buf,
    rs_buf,
    dh_buf,
    split,
    moe_acc,
    back_acc,
    send_sem,
    recv_sem,
    keep_sem,
):
    step, last = pl.program_id(0), pl.num_programs(0) - 1
    pairs = pl.num_programs(0) // 2
    net = Peers(dp, tp, send_sem, recv_sem)
    z, c, t = net.z, net.c, net.t
    length, model = tok_ref.shape
    rows = 2 * length
    own = length // tp
    width = wg_ref.shape[2]
    q_width, kv_width = wq_ref.shape[1], wk_ref.shape[1]
    group = q_width // kv_width
    others, sides = range(1, dp), range(1, tp)

    def block(plane, core, tensor):
        return ds((plane * 2 + core) * tp + tensor, own)

    def link(src, dst, device):
        return net.make(src, dst, net.number(1), device)

    def start(copies):
        for copy in copies:
            copy.start()

    mine = ds(c * tp + t, own)
    seq_rows = ds(c, length)
    near = [net.near(axis) for axis in range(2)]
    far = tp - 1 - t
    half = own // 2

    def piece(plane, tensor, part_of):
        at = (((plane * 2 + c) * tp + tensor) * 2 + part_of) * half
        return pl.ds(pl.multiple_of(at, half), half)

    def spread(ref, sources, relayed):
        direct = [
            link(sources[p - 1], ref.at[block(p, c, t)], near[axis])
            for p in others
            for axis in range(2)
        ]
        relay = []
        for p in others if relayed else ():
            for axis in range(2):
                at = piece(p, near[axis][2], axis)
                relay.append(link(ref.at[at], ref.at[at], near[1 - axis]))
        to_core = [link(sources[p - 1], ref.at[block(p, c, t)], net.partner()) for p in others]
        near_core, far_core = [], []
        for p in others:
            for axis in range(2):
                at = block(p, c, near[axis][2])
                near_core.append(link(ref.at[at], ref.at[at], net.partner()))
            at = block(p, c, far)
            far_core.append(link(ref.at[at], ref.at[at], net.partner()))
        return direct, relay, to_core, near_core, far_core

    g_own = [link(cot_ref, g_buf.at[seq_rows], net.partner())]
    g_z = [link(cot_ref.at[ds(t, own)], gz_buf.at[dp - 1 - k], net.plane(k)) for k in others]
    side_h = [
        link(part_buf.at[ds(lax.rem(t + k, tp), own)], rs_buf.at[k - 1], net.tensor(k))
        for k in sides
    ]
    x_t = [link(x_buf.at[mine], x_buf.at[mine], net.tensor(k)) for k in sides]
    x_own = [link(x_buf.at[mine], x_buf.at[mine], net.partner())]
    x_seen = []
    for k in sides:
        at = ds(c * tp + lax.rem(t + tp - k, tp), own)
        x_seen.append(link(x_buf.at[at], x_buf.at[at], net.partner()))
    x_z = [link(x_buf.at[mine], xr_ref.at[block(dp - k, c, t)], net.plane(k)) for k in others]
    g_direct, g_relay, g_core, g_near, g_far = spread(
        gr_ref, [gz_buf.at[p - 1] for p in others], True
    )
    x_direct, _, x_core, x_near, x_far = spread(
        xr_ref, [xr_ref.at[block(p, c, t)] for p in others], False
    )
    x_z2 = [
        link(x_buf.at[ds(c * tp + far, own)], xr_ref.at[block(dp - k, c, far)], net.plane(k))
        for k in others
    ]
    keep_x = pltpu.make_async_copy(x_buf, xr_ref.at[pl.ds(0, rows)], keep_sem.at[0])
    keep_g = [pltpu.make_async_copy(g_buf, gr_ref.at[pl.ds(0, rows)], keep_sem.at[1])] + [
        pltpu.make_async_copy(gz_buf.at[p - 1], gr_ref.at[block(p, c, t)], keep_sem.at[1 + p])
        for p in others
    ]

    @pl.when(step == 0)
    def _():
        net.greet()
        start(g_own + g_z)
        g_buf[seq_rows, :] = cot_ref[...]
        resid = tok_ref[...].astype(F32)
        n1 = (resid * inverse_rms(resid) * ga_ref[...].reshape(1, -1)).astype(BF16)
        n1_buf[...] = n1
        q_all = rotate(dot(n1, wq_ref[...]), rope_ref, HEAD_SIZE ** (-0.5)).astype(BF16)
        kv_ref[:, :kv_width] = rotate(dot(n1, wk_ref[...]), rope_ref).astype(BF16)
        kv_ref[:, kv_width:] = dot(n1, wv_ref[...]).astype(BF16)
        seen = causal(length)
        for kv in range(kv_width // HEAD_SIZE):
            key = kv_ref[:, kv * HEAD_SIZE : (kv + 1) * HEAD_SIZE]
            val = kv_ref[:, kv_width + kv * HEAD_SIZE : kv_width + (kv + 1) * HEAD_SIZE]
            q = stack_heads(q_all, kv, group)
            qs_ref[kv] = q
            s = dot_nt(q, key).reshape(group, length, length)
            s = jnp.where(seen[None], s, -1e30)
            up_to = jnp.exp(s - jnp.max(s, axis=-1, keepdims=True))
            prob = up_to * (1.0 / jnp.sum(up_to, axis=-1, keepdims=True))
            prob = prob.reshape(group * length, length).astype(BF16)
            prob_ref[kv] = prob
            att = dot(prob, val).astype(BF16)
            as_ref[kv] = att
            for j in range(group):
                h = kv * group + j
                att_ref[:, h * HEAD_SIZE : (h + 1) * HEAD_SIZE] = att[j * length : (j + 1) * length]
        part_buf[...] = dot(att_ref[...], wo_ref[...]).astype(BF16)
        start(side_h)
        moe_acc[...] = jnp.zeros_like(moe_acc)
        back_acc[...] = jnp.zeros_like(back_acc)
        dgate_ref[...] = jnp.zeros_like(dgate_ref)
        pad_router(wr_ref, wr_buf)
        place_ref[0] = z
        place_ref[1] = c
        arrived(g_own)

    @pl.when(step < pairs)
    def _():
        dh_buf[step] = dot_nt(g_buf[...], wd_ref[...].reshape(2 * width, model))

    @pl.when(step == pairs)
    def _():
        total = tok_ref[ds(t, own), :].astype(F32) + part_buf[ds(t, own), :].astype(F32)
        routes_buf[...] = routes_ref[...].T
        picked = routes_buf[ds(t, own), :]
        ids = lax.broadcasted_iota(jnp.int32, (own, EXTRA), 1)
        chosen = picked[:, 0:1] == ids
        for j in range(1, picked.shape[1]):
            chosen = chosen | (picked[:, j : j + 1] == ids)
        arrived(side_h)
        for k in sides:
            total = total + rs_buf[k - 1].astype(F32)
        n2 = (total * inverse_rms(total) * gm_ref[...].reshape(1, -1)).astype(BF16)
        x_buf[mine, :model] = n2
        x_buf[mine, model:] = jnp.where(chosen, 1.0, 0.0).astype(BF16)
        start(x_t + x_own + x_z)
        h1_ref[...] = total
        for kv in range(kv_width // HEAD_SIZE):
            prob_t_ref[kv] = prob_ref[kv].T
        n1t_ref[...] = n1_buf[...].T
        for k in sides:
            arrived(x_t[k - 1 : k])
            start(x_seen[k - 1 : k])
        arrived(g_z)
        start(g_direct + g_core + keep_g)
        arrived(x_own + x_seen)
        keep_x.start()
        gates = gates_of(x_buf, wr_buf, model)
        gates_ref[...] = gates
        store_split(gates, split)

    @pl.when(step == pairs + 3)
    def _():
        arrived(x_z)
        start(x_direct + x_core + x_z2)

    @pl.when(step == pairs + 6)
    def _():
        arrived(g_direct)
        start(g_relay + g_near)

    @pl.when(step == pairs + 9)
    def _():
        arrived(g_relay)
        start(g_far)
        arrived(x_direct)
        start(x_near)
        arrived(x_z2)
        start(x_far)

    @pl.when(step >= pairs)
    def _():
        pair = step - pairs
        first = c * (2 * pairs) + 2 * pair
        gate_pair = pair_of_gates(split[...], first, width)
        lane = lax.broadcasted_iota(jnp.int32, dgate_ref.shape, 1)
        for k in range(2):
            lanes = slice(k * width, (k + 1) * width)
            w_both = jnp.concatenate([wg_ref[k], wu_ref[k]], axis=1)
            both = dot(x_buf[:, :model], w_both)
            dh = dh_buf[pair, :, lanes]
            hid, ghid, dgp, dup = swiglu(both, dh, gate_pair[:, lanes])
            ghid_ref[:, lanes] = ghid
            dgp_ref[:, lanes] = dgp
            dup_ref[:, lanes] = dup
            row_sum = jnp.sum(hid * dh, axis=1, keepdims=True)
            dgate_ref[...] += jnp.where(lane == first + k, row_sum, 0.0)
            back_acc[...] += dot_nt(jnp.concatenate([dgp, dup], axis=1), w_both)
        moe_acc[...] += dot(ghid_ref[...], wd_ref[...].reshape(2 * width, model))

    @pl.when(step == last)
    def _():
        moe_ref[...] = moe_acc[...].astype(BF16)
        back_ref[...] = back_acc[...].astype(BF16)
        keep_x.wait()
        for copy in keep_g:
            copy.wait()
        arrived(g_core + g_near + g_far + x_core + x_near + x_far)
        sent = g_own + g_z + side_h + x_t + x_own + x_seen + x_z
        sent = sent + g_direct + g_relay + g_core + g_near + g_far
        for copy in sent + x_direct + x_z2 + x_core + x_near + x_far:
            copy.wait_send()


def whole_spec(a):
    shape = a.shape
    return pl.BlockSpec(shape, lambda *_: (0,) * len(shape), pipeline_mode=pl.Buffered(1))


def front(dp, tp, arrays, weights):
    tokens, wq, wk = arrays[0], arrays[6], arrays[7]
    length, model = tokens.shape
    count, _, width = weights[0].shape
    pairs = count // 2
    rows, own = 2 * length, length // tp
    wide, q_width = model + EXTRA, wq.shape[1]
    kv_heads, group = wk.shape[1] // HEAD_SIZE, q_width // wk.shape[1]
    others, sides = dp - 1, tp - 1
    copies = 1 + others + sides + sides + 1 + sides + 2 * others + (8 + 6) * others
    later = lambda i: jnp.maximum(i - pairs, 0)
    up = lambda shape: pl.BlockSpec((2,) + shape, lambda i: (later(i), 0, 0))
    down = pl.BlockSpec((2, width, model), lambda i: (lax.rem(i, pairs), 0, 0))
    saved = pl.BlockSpec((rows, 2 * width), lambda i: (0, later(i)))
    shapes = [
        ((rows * dp, wide), BF16),
        ((rows * dp, model), BF16),
        ((rows, model), BF16),
        ((rows, model), BF16),
        ((rows, EXTRA), F32),
        ((rows, EXTRA), F32),
        ((own, model), F32),
        ((length, 2 * wk.shape[1]), BF16),
        ((length, q_width), BF16),
        ((kv_heads, group * length, HEAD_SIZE), BF16),
        ((kv_heads, group * length, HEAD_SIZE), BF16),
        ((kv_heads, group * length, length), BF16),
        ((kv_heads, length, group * length), BF16),
        ((model, length), BF16),
        ((rows, count * width), BF16),
        ((rows, count * width), BF16),
        ((rows, count * width), BF16),
    ]
    shapes.append(((2,), jnp.int32))
    shapes = [jax.ShapeDtypeStruct(*s) for s in shapes]
    scratch = [
        ((rows, wide), BF16),
        ((rows, model), BF16),
        ((others, own, model), BF16),
        ((EXTRA, model), BF16),
        ((length, arrays[2].shape[0]), jnp.int32),
        ((length, model), BF16),
        ((length, model), BF16),
        ((sides, own, model), BF16),
        ((pairs, rows, 2 * width), F32),
        ((rows, 2 * EXTRA), BF16),
        ((rows, model), F32),
        ((rows, model), F32),
    ]
    return pl.pallas_call(
        functools.partial(front_kernel, dp, tp),
        grid=(2 * pairs,),
        out_shape=shapes,
        in_specs=[whole_spec(a) for a in arrays] + [up((model, width)), up((model, width)), down],
        out_specs=[ANY, ANY]
        + [whole_spec(s) for s in shapes[2:14]]
        + [saved] * 3
        + [pl.BlockSpec(memory_space=pltpu.SMEM)],
        scratch_shapes=[pltpu.VMEM(*s) for s in scratch]
        + [
            pltpu.SemaphoreType.DMA((copies,)),
            pltpu.SemaphoreType.DMA((copies,)),
            pltpu.SemaphoreType.DMA((2 + others,)),
        ],
        compiler_params=pltpu.CompilerParams(
            collective_id=0, has_side_effects=True, vmem_limit_bytes=VMEM_LIMIT
        ),
        name="front",
    )(*arrays, *weights)


def backward_kernel(
    dp,
    tp,
    back_hbm,
    moe_hbm,
    dgate_hbm,
    gates_ref,
    h1_ref,
    tok_hbm,
    cot_hbm,
    ga_ref,
    gm_ref,
    wr_ref,
    wq_hbm,
    wk_hbm,
    wv_hbm,
    wo_hbm,
    kv_hbm,
    att_hbm,
    qs_hbm,
    as_hbm,
    prob_hbm,
    prob_t_hbm,
    n1t_hbm,
    rope_hbm,
    xr_ref,
    gr_ref,
    own_ref,
    wg_ref,
    wu_ref,
    wd_ref,
    out_ref,
    in_ref,
    dl_all,
    qkv_grad_ref,
    o_grad_ref,
    gains_ref,
    down_ref,
    dgp_ref,
    dup_ref,
    back_ref,
    moe_ref,
    dgate_ref,
    tok_ref,
    cot_ref,
    wq_ref,
    wk_ref,
    wv_ref,
    wo_ref,
    kv_ref,
    att_ref,
    qs_ref,
    as_ref,
    prob_ref,
    prob_t_ref,
    n1t_ref,
    rope_ref,
    x_rest,
    g_rest,
    wr_buf,
    g_plane,
    gt_buf,
    split,
    pair_b,
    pair_m,
    pair_d,
    sum_b,
    sum_m,
    sum_d,
    rs_b,
    rs_m,
    rs_d,
    dh1_buf,
    da_buf,
    dl_buf,
    d_buf,
    do_buf,
    part_buf,
    rs_3,
    gain_buf,
    gain_t,
    gain_z,
    gain_zs,
    gain_c,
    out_buf,
    in_buf,
    q_part,
    q_pair,
    q_sum,
    q_in,
    o_part,
    o_pair,
    o_sum,
    o_in,
    send_sem,
    recv_sem,
    keep_sem,
    load_sem,
):
    step, last = pl.program_id(0), pl.num_programs(0) - 1
    net = Peers(dp, tp, send_sem, recv_sem)
    z, c, t = net.z, net.c, net.t
    length, model = tok_ref.shape
    own = length // tp
    part = model // dp
    width = wg_ref.shape[2]
    q_width, kv_width = wq_ref.shape[1], wk_ref.shape[1]
    group = q_width // kv_width
    others, sides = range(1, dp), range(1, tp)
    mine = ds(t, own)
    here, there = ds(c, length), ds(1 - c, length)

    def columns(index):
        return pl.ds(pl.multiple_of(index * part, 128), part)

    def link(src, dst, device):
        return net.make(src, dst, net.number(1), device)

    def to_sides(ref, into):
        return [
            link(ref.at[ds(lax.rem(t + k, tp), own)], into.at[k - 1], net.tensor(k)) for k in sides
        ]

    def share(ref):
        return [link(ref.at[mine], ref.at[mine], net.tensor(k)) for k in sides]

    def on_to_partner(ref):
        rows = [ds(p * 2 + c, length) for p in others]
        return [link(ref.at[r], ref.at[r], net.partner()) for r in rows]

    def over_planes(ref, into):
        return [link(ref, into.at[ds((dp - k) * 2 + c, length)], net.plane(k)) for k in others]

    def start(copies):
        for copy in copies:
            copy.start()

    pair_bd = [
        link(back_hbm.at[there], pair_b, net.partner()),
        link(dgate_hbm.at[there], pair_d, net.partner()),
    ]
    pair_mo = [link(moe_hbm.at[there], pair_m, net.partner())]
    side_bd = to_sides(sum_b, rs_b) + to_sides(sum_d, rs_d)
    side_mo = to_sides(sum_m, rs_m)
    share_da = share(da_buf) + share(dl_buf)
    dl_z = over_planes(dl_buf, dl_all)
    dl_own = [link(dl_buf, dl_all.at[here], net.partner())]
    dl_c = on_to_partner(dl_all)
    q_core = [link(q_part.at[:, 1 - c], q_pair, net.partner())]
    q_z = [link(q_sum.at[lax.rem(z + k, dp)], q_in.at[k - 1], net.plane(k)) for k in others]
    o_core = [link(o_part.at[:, 1 - c], o_pair, net.partner())]
    o_z = [link(o_sum.at[lax.rem(z + k, dp)], o_in.at[k - 1], net.plane(k)) for k in others]
    share_out = share(out_buf)
    side_3 = to_sides(part_buf, rs_3)
    share_in = share(in_buf)
    side_gain = [link(gain_buf, gain_t.at[k - 1], net.tensor(k)) for k in sides]
    plane_gain = [
        link(gain_zs.at[:, columns(lax.rem(z + k, dp))], gain_z.at[k - 1], net.plane(k))
        for k in others
    ]
    pair_gain = [link(gain_c.at[0], gain_c.at[1], net.partner())]
    keep_dl = pltpu.make_async_copy(dl_buf, dl_all.at[here], keep_sem.at[0])
    plane_rows = xr_ref.shape[0] // dp
    rest = pl.ds(plane_rows, xr_ref.shape[0] - plane_rows)
    late = [
        (back_hbm.at[here], back_ref),
        (dgate_hbm.at[here], dgate_ref),
        (moe_hbm.at[here], moe_ref),
        (cot_hbm, cot_ref),
        (wo_hbm, wo_ref),
        (att_hbm, att_ref),
        (kv_hbm, kv_ref),
        (qs_hbm, qs_ref),
        (as_hbm, as_ref),
        (prob_hbm, prob_ref),
        (prob_t_hbm, prob_t_ref),
        (rope_hbm, rope_ref),
        (wq_hbm, wq_ref),
        (wk_hbm, wk_ref),
        (wv_hbm, wv_ref),
        (n1t_hbm, n1t_ref),
        (tok_hbm, tok_ref),
    ]
    late = [pltpu.make_async_copy(src, dst, load_sem.at[i]) for i, (src, dst) in enumerate(late)]

    def loaded(first, end):
        for copy in late[first:end]:
            copy.wait()

    load_x = pltpu.make_async_copy(xr_ref.at[rest], x_rest, keep_sem.at[1])
    load_g = pltpu.make_async_copy(gr_ref.at[rest], g_rest, keep_sem.at[2])
    load_own = pltpu.make_async_copy(
        gr_ref.at[pl.ds(0, plane_rows), columns(z)], g_plane, keep_sem.at[3]
    )

    @pl.when(step == 0)
    def _():
        load_x.start()
        load_g.start()
        load_own.start()
        start(late[:2])
        net.greet()
        start(pair_bd)
        load_x.wait()
        pad_router(wr_ref, wr_buf)
        store_split(gates_of(x_rest, wr_buf, model), split)
        load_g.wait()
        load_own.wait()
        start(late[2:])
        gt_buf[:, :plane_rows] = g_plane[...].T
        gt_buf[:, plane_rows:] = g_rest[:, columns(z)].T

    def pair_sum():
        arrived(pair_bd)
        loaded(0, 2)
        sum_b[...] = (back_ref[...].astype(F32) + pair_b[...].astype(F32)).astype(BF16)
        sum_d[...] = dgate_ref[...] + pair_d[...]
        start(side_bd + pair_mo)

    def over_pair(part, pair, total):
        total[...] = (part[:, c].astype(F32) + pair[...].astype(F32)).astype(BF16)

    def over_z(total, came, out):
        value = total[z].astype(F32)
        for k in others:
            value = value + came[k - 1].astype(F32)
        out[...] = value

    def moe_backward():
        arrived(side_bd)
        loaded(2, 4)
        d_n2 = sum_b[mine, :].astype(F32)
        dgate = sum_d[mine, :]
        for k in sides:
            d_n2 = d_n2 + rs_b[k - 1].astype(F32)
            dgate = dgate + rs_d[k - 1]
        gates = gates_ref[ds(c * tp + t, own), :]
        d_logits = gates * (dgate - jnp.sum(gates * dgate, axis=1, keepdims=True))
        dl_buf[mine, :] = d_logits.astype(BF16)
        d_n2 = d_n2 + dot(d_logits.astype(BF16), wr_buf[...])
        h1 = h1_ref[...]
        r2 = inverse_rms(h1)
        weighted = d_n2 * gm_ref[...].reshape(1, -1)
        inner = jnp.mean(weighted * h1, axis=-1, keepdims=True)
        gain_buf[...] = jnp.zeros_like(gain_buf)
        gain_buf[1:2, :] = jnp.sum(d_n2 * h1 * r2, axis=0, keepdims=True)
        d_h1 = cot_ref[mine, :].astype(F32) + (r2 * weighted - h1 * (r2 * r2 * r2) * inner)
        dh1_buf[...] = d_h1
        da_buf[mine, :] = d_h1.astype(BF16)
        start(share_da)
        arrived(pair_mo)
        sum_m[...] = (moe_ref[...].astype(F32) + pair_m[...].astype(F32)).astype(BF16)

    def attention_backward():
        loaded(4, len(late))
        arrived(share_da)
        start(side_mo + dl_z + dl_own)
        keep_dl.start()
        do_buf[...] = dot_nt(da_buf[...], wo_ref[...]).astype(BF16)
        o_part[...] = dot_tn(da_buf[...], att_ref[...]).astype(BF16).reshape(o_part.shape)
        start(o_core)
        scale = HEAD_SIZE ** (-0.5)
        d_key, d_val, d_query = [], [], []
        for kv in range(kv_width // HEAD_SIZE):
            if kv == 1:
                arrived(o_core)
                over_pair(o_part, o_pair, o_sum)
                start(o_z)
            key = kv_ref[:, kv * HEAD_SIZE : (kv + 1) * HEAD_SIZE]
            val = kv_ref[:, kv_width + kv * HEAD_SIZE : kv_width + (kv + 1) * HEAD_SIZE]
            d_out = stack_heads(do_buf, kv, group)
            delta = jnp.sum(d_out.astype(F32) * as_ref[kv].astype(F32), axis=-1, keepdims=True)
            d_s = (prob_ref[kv].astype(F32) * (dot_nt(d_out, val) - delta)).astype(BF16)
            d_q = dot(d_s, key) * scale
            d_query += [d_q[j * length : (j + 1) * length] for j in range(group)]
            d_key.append(dot_tn(d_s, qs_ref[kv]))
            d_val.append(dot(prob_t_ref[kv], d_out))
        arrived(side_mo)
        total = h1_ref[...] + sum_m[mine, :].astype(F32)
        for k in sides:
            total = total + rs_m[k - 1].astype(F32)
        out_buf[mine, :] = total.astype(BF16)
        start(share_out)
        d_buf[:, :q_width] = rotate(jnp.concatenate(d_query, axis=1), rope_ref, sign=-1.0).astype(BF16)
        d_buf[:, q_width : q_width + kv_width] = rotate(
            jnp.concatenate(d_key, axis=1), rope_ref, sign=-1.0
        ).astype(BF16)
        d_buf[:, q_width + kv_width :] = jnp.concatenate(d_val, axis=1).astype(BF16)
        part_n1 = dot_nt(d_buf[:, :q_width], wq_ref[...])
        part_n1 = part_n1 + dot_nt(d_buf[:, q_width : q_width + kv_width], wk_ref[...])
        part_n1 = part_n1 + dot_nt(d_buf[:, q_width + kv_width :], wv_ref[...])
        part_buf[...] = part_n1.astype(BF16)
        start(side_3)
        q_part[...] = dot(n1t_ref[...], d_buf[...]).astype(BF16).reshape(q_part.shape)
        start(q_core)

    def send_parts():
        arrived(q_core)
        over_pair(q_part, q_pair, q_sum)
        start(q_z)
        arrived(dl_z)
        start(dl_c)

    def input_gradient():
        arrived(side_3)
        d_n1 = part_buf[mine, :].astype(F32)
        for k in sides:
            d_n1 = d_n1 + rs_3[k - 1].astype(F32)
        resid = tok_ref[mine, :].astype(F32)
        r1 = inverse_rms(resid)
        weighted = d_n1 * ga_ref[...].reshape(1, -1)
        inner = jnp.mean(weighted * resid, axis=-1, keepdims=True)
        gain_buf[0:1, :] = jnp.sum(d_n1 * resid * r1, axis=0, keepdims=True)
        d_x = dh1_buf[...] + (r1 * weighted - resid * (r1 * r1 * r1) * inner)
        in_buf[mine, :] = d_x.astype(BF16)
        start(side_gain + share_in)

    def gain_over_planes():
        arrived(side_gain)
        gain = gain_buf[...]
        for k in sides:
            gain = gain + gain_t[k - 1]
        gain_zs[...] = gain
        start(plane_gain)

    def gain_over_pair():
        arrived(plane_gain)
        gain = gain_zs[:, columns(z)]
        for k in others:
            gain = gain + gain_z[k - 1]
        gain_c[0] = gain
        start(pair_gain)

    stages = (pair_sum, moe_backward, attention_backward, send_parts, input_gradient, gain_over_planes, gain_over_pair)

    def stages_at(half):
        for stage, place in zip(stages, STAGE_PLACES):
            if place % 2 == half:
                pl.when(step == place // 2)(stage)

    stages_at(0)
    first = c * (2 * pl.num_programs(0)) + 2 * step
    wd_pair = wd_ref[...].reshape(2 * width, model)
    gate_pair = pair_of_gates(split[...], first, width)
    dh_pair = dot_nt(g_rest[...], wd_pair)
    hidden = []
    for k in range(2):
        if k == 1:
            stages_at(1)
        lanes = slice(k * width, (k + 1) * width)
        both = dot(x_rest[:, :model], jnp.concatenate([wg_ref[k], wu_ref[k]], axis=1))
        _, ghid, dgp, dup = swiglu(both, dh_pair[:, lanes], gate_pair[:, lanes])
        hidden.append(ghid)
        dgp_ref[:, lanes] = dgp
        dup_ref[:, lanes] = dup
    down = dot(gt_buf[:, :plane_rows], own_ref[...])
    down = (down + dot(gt_buf[:, plane_rows:], jnp.concatenate(hidden, axis=1))).T
    for k in range(2):
        down_ref[k] = down[k * width : (k + 1) * width]

    @pl.when(step == last)
    def _():
        arrived(pair_gain)
        gains_ref[...] = gain_c[0] + gain_c[1]
        arrived(o_z)
        over_z(o_sum, o_in, o_grad_ref)
        arrived(share_out + share_in)
        out_ref[...] = out_buf[...]
        in_ref[...] = in_buf[...]
        arrived(q_z)
        over_z(q_sum, q_in, qkv_grad_ref)
        arrived(dl_own + dl_c)
        keep_dl.wait()
        sent = pair_bd + pair_mo + side_bd + side_mo + share_da + share_out + share_in + side_3
        sent = sent + dl_z + dl_own + dl_c + q_core + q_z + o_core + o_z
        for copy in sent + side_gain + plane_gain + pair_gain:
            copy.wait_send()


def backward(dp, tp, arrays, streamed, own_hid, weights):
    tokens = arrays[5]
    wq, wk, wv = arrays[10:13]
    all_rows, model = streamed[1].shape
    rest_rows = all_rows - all_rows // dp
    count, _, width = weights[0].shape
    length = tokens.shape[0]
    own, part = length // tp, model // dp
    q_width = wq.shape[1]
    wide = q_width + wk.shape[1] + wv.shape[1]
    others, sides = dp - 1, tp - 1
    copies = 3 + 9 * sides + (2 * others + 1) + 2 * (1 + others) + sides + others + 1
    by_pair = lambda shape: pl.BlockSpec((2,) + shape, lambda i: (i, 0, 0))
    saved = pl.BlockSpec((rest_rows, 2 * width), lambda i: (0, i))
    shapes = [
        ((length, model), BF16),
        ((length, model), BF16),
        ((all_rows, EXTRA), BF16),
        ((part // 2, wide), F32),
        ((part // 2, q_width), F32),
        ((8, part), F32),
        ((count, width, part), F32),
        ((rest_rows, count * width), BF16),
        ((rest_rows, count * width), BF16),
    ]
    shapes = [jax.ShapeDtypeStruct(*s) for s in shapes]
    full, block, slots = (length, model), (own, model), (sides, own, model)
    copied = [arrays[i] for i in (5, 6, *range(10, len(arrays)))]
    scratch = [
        (full, BF16),
        (full, BF16),
        ((length, EXTRA), F32),
        *((a.shape, a.dtype) for a in copied),
        ((rest_rows, streamed[0].shape[1]), BF16),
        ((rest_rows, model), BF16),
        ((EXTRA, model), BF16),
        ((all_rows - rest_rows, part), BF16),
        ((part, all_rows), BF16),
        ((rest_rows, 2 * EXTRA), BF16),
        (full, BF16),
        (full, BF16),
        ((length, EXTRA), F32),
        (full, BF16),
        (full, BF16),
        ((length, EXTRA), F32),
        (slots, BF16),
        (slots, BF16),
        ((sides, own, EXTRA), F32),
        (block, F32),
        (full, BF16),
        ((length, EXTRA), BF16),
        ((length, wide), BF16),
        ((length, q_width), BF16),
        (full, BF16),
        (slots, BF16),
        ((8, model), F32),
        ((sides, 8, model), F32),
        ((others, 8, part), F32),
        ((8, model), F32),
        ((2, 8, part), F32),
        (full, BF16),
        (full, BF16),
        ((dp, 2, part // 2, wide), BF16),
        ((dp, part // 2, wide), BF16),
        ((dp, part // 2, wide), BF16),
        ((others, part // 2, wide), BF16),
        ((dp, 2, part // 2, q_width), BF16),
        ((dp, part // 2, q_width), BF16),
        ((dp, part // 2, q_width), BF16),
        ((others, part // 2, q_width), BF16),
    ]
    return pl.pallas_call(
        functools.partial(backward_kernel, dp, tp),
        grid=(count // 2,),
        out_shape=shapes,
        in_specs=[whole_spec(a) if i in (3, 4, 7, 8, 9) else ANY for i, a in enumerate(arrays)]
        + [ANY, ANY, pl.BlockSpec((own_hid.shape[0], 2 * width), lambda i: (0, i))]
        + [by_pair((model, width)), by_pair((model, width)), by_pair((width, model))],
        out_specs=[whole_spec(shapes[0]), whole_spec(shapes[1]), ANY]
        + [whole_spec(s) for s in shapes[3:6]]
        + [by_pair((width, part)), saved, saved],
        scratch_shapes=[pltpu.VMEM(*s) for s in scratch]
        + [
            pltpu.SemaphoreType.DMA((copies,)),
            pltpu.SemaphoreType.DMA((copies,)),
            pltpu.SemaphoreType.DMA((4,)),
            pltpu.SemaphoreType.DMA((3 + len(copied),)),
        ],
        compiler_params=pltpu.CompilerParams(
            collective_id=2, has_side_effects=True, vmem_limit_bytes=VMEM_LIMIT
        ),
        name="backward",
    )(*arrays, *streamed, own_hid, *weights)


def weights_kernel(
    place_ref,
    x_ref,
    dl_ref,
    qkv_grad_ref,
    o_grad_ref,
    gains_ref,
    out_in_ref,
    in_in_ref,
    dgp_ref,
    dup_ref,
    down_ref,
    dgp_rest,
    dup_rest,
    gate_grad_ref,
    up_grad_ref,
    down_grad_ref,
    query_ref,
    key_ref,
    value_ref,
    out_grad_ref,
    router_ref,
    ga_grad_ref,
    gm_grad_ref,
    out_ref,
    in_ref,
    xt_buf,
):
    step = pl.program_id(0)
    c = place_ref[1]
    width = gate_grad_ref.shape[2]
    plane_rows = dgp_ref.shape[0]

    @pl.when(step == 0)
    def _():
        xt_buf[...] = x_ref[...].T
        q_width, kv_width = query_ref.shape[1], key_ref.shape[1]
        half = query_ref.shape[0]
        query_ref[...] = qkv_grad_ref[:, :q_width]
        key_ref[...] = qkv_grad_ref[:, q_width : q_width + kv_width]
        value_ref[...] = qkv_grad_ref[:, q_width + kv_width :]
        out_grad_ref[...] = o_grad_ref[...]
        out_ref[...] = out_in_ref[...]
        in_ref[...] = in_in_ref[...]
        router = dot(xt_buf[...], dl_ref[...]).T[: router_ref.shape[0]]
        router_ref[...] = jnp.where(c == 0, router[:, :half], router[:, half:])
        gains = jnp.where(c == 0, gains_ref[:, :half], gains_ref[:, half:])
        ga_grad_ref[...] = gains[0:1, :]
        gm_grad_ref[...] = gains[1:2, :]

    def contract(own, rest):
        return dot(xt_buf[:, :plane_rows], own[...]) + dot(xt_buf[:, plane_rows:], rest[...])

    gate_both = contract(dgp_ref, dgp_rest)
    up_both = contract(dup_ref, dup_rest)
    down_grad_ref[...] = down_ref[...]
    for k in range(2):
        lanes = slice(k * width, (k + 1) * width)
        gate_grad_ref[k] = gate_both[:, lanes]
        up_grad_ref[k] = up_both[:, lanes]


def weight_grads(place, x, sides, own, rest, count, kv_width, experts):
    rows = x.shape[0]
    _, qkv_grad, o_grad, gains, output, _ = sides
    width = own[0].shape[1] // count
    part = gains.shape[1]
    q_width, half = o_grad.shape[1], part // 2
    by_pair = lambda shape: pl.BlockSpec((2,) + shape, lambda i, p: (i, 0, 0))
    saved = lambda a: pl.BlockSpec((a.shape[0], 2 * width), lambda i, p: (0, i))
    columns = pl.BlockSpec((rows, part), lambda i, p: (0, p[0]), pipeline_mode=pl.Buffered(1))
    shapes = [
        (count, part, width),
        (count, part, width),
        (count, width, part),
        (half, q_width),
        (half, kv_width),
        (half, kv_width),
        (half, q_width),
        (experts, half),
        (1, half),
        (1, half),
    ]
    shapes = [jax.ShapeDtypeStruct(s, F32) for s in shapes]
    shapes += [jax.ShapeDtypeStruct(output.shape, BF16)] * 2
    return pl.pallas_call(
        weights_kernel,
        grid_spec=pltpu.PrefetchScalarGridSpec(
            num_scalar_prefetch=1,
            grid=(count // 2,),
            in_specs=[columns]
            + [whole_spec(a) for a in sides]
            + [saved(a) for a in own]
            + [by_pair((width, part))]
            + [saved(a) for a in rest[1:]],
            out_specs=[by_pair((part, width)), by_pair((part, width)), by_pair((width, part))]
            + [whole_spec(s) for s in shapes[3:]],
            scratch_shapes=[pltpu.VMEM((part, rows), BF16)],
        ),
        out_shape=shapes,
        compiler_params=pltpu.CompilerParams(vmem_limit_bytes=VMEM_LIMIT),
        name="weight_grads",
    )(place, x, *sides, *own, *rest)


def rope_rows(length):
    half = HEAD_SIZE // 2
    frequency = ROPE_BASE ** (np.arange(half) * (-2.0 / HEAD_SIZE))
    angles = np.arange(length)[:, None] * frequency[None, :]
    cos, sin, none = np.cos(angles), np.sin(angles), np.zeros((length, half))
    double = lambda first, second: np.concatenate([first, second, first, second], axis=1)
    return np.stack([double(cos, cos), double(-sin, none), double(none, sin)]).astype(np.float32)


def gather_plan(
    tokens,
    gain_attn,
    w_query,
    key_projection,
    value_projection,
    w_out,
    gain_moe,
    w_router,
    w_gate,
    w_up,
    w_down,
    routes,
    cotangent,
):
    dp, tp = lax.axis_size("dp"), lax.axis_size("tensor")
    experts = w_router.shape[1]
    rope = jnp.asarray(rope_rows(tokens.shape[0]))
    ga, gm = gain_attn, gain_moe
    wr = w_router.T
    heads = (w_query, key_projection, value_projection, w_out)
    x_all, g_all, moe, back, dgate, gates, h1, *saved, ghid, dgp, dup, place = front(
        dp, tp, (tokens, cotangent, routes.T, ga, gm, wr, *heads, rope), (w_gate, w_up, w_down)
    )
    local = (back, moe, dgate, gates, h1, tokens, cotangent, ga, gm, wr, *heads)
    output, input_grad, d_logits, qkv_grad, o_grad, gains, *rest = backward(
        dp, tp, (*local, *saved, rope), (x_all, g_all), ghid, (w_gate, w_up, w_down)
    )
    (
        gate_grad,
        up_grad,
        down_grad,
        query_grad,
        key_grad,
        value_grad,
        out_grad,
        router_grad,
        gain_attn_grad,
        gain_moe_grad,
        output,
        input_grad,
    ) = weight_grads(
        place,
        x_all,
        (d_logits, qkv_grad, o_grad, gains, output, input_grad),
        (dgp, dup),
        rest,
        w_gate.shape[0],
        key_projection.shape[1],
        experts,
    )
    return (
        output,
        input_grad,
        gain_attn_grad[0],
        query_grad,
        key_grad,
        value_grad,
        out_grad.T,
        gain_moe_grad[0],
        router_grad.T,
        gate_grad,
        up_grad,
        down_grad,
    )


def solution(mesh):
    placed = (
        P(("dp", "expert"), None),
        P(),
        P(None, "tensor"),
        P(None, "tensor"),
        P(None, "tensor"),
        P("tensor", None),
        P(),
        P(),
        P("expert", None, "tensor"),
        P("expert", None, "tensor"),
        P("expert", "tensor", None),
        P(("dp", "expert"), None),
        P(("dp", "expert"), None),
    )
    sequences = mesh.shape["dp"] * mesh.shape["expert"]
    few = sequences * SEQUENCE_LENGTH <= GATHER_ROWS
    few = few and mesh.shape["tensor"] == 4 and mesh.shape["expert"] == 2
    return jax.shard_map(
        gather_plan if few else reduce_plan,
        mesh=mesh,
        in_specs=placed,
        out_specs=(
            P(("dp", "expert"), None),
            P(("dp", "expert"), None),
            P(("dp", "expert")),
            P(("dp", "expert"), "tensor"),
            P(("dp", "expert"), "tensor"),
            P(("dp", "expert"), "tensor"),
            P("tensor", ("dp", "expert")),
            P(("dp", "expert")),
            P(("dp", "expert"), None),
            P("expert", "dp", "tensor"),
            P("expert", "dp", "tensor"),
            P("expert", "tensor", "dp"),
        ),
        check_vma=False,
    )
```

```python
import functools
import math

import jax
import jax.numpy as jnp
import numpy as np
from jax import lax
from jax.experimental import pallas as pl
from jax.experimental.pallas import tpu as pltpu
from jax.sharding import PartitionSpec as P

HEAD_SIZE = 64
SEQUENCE_LENGTH = 256
CAP = 64


EPSILON = 1e-06
ROPE_BASE = 10000.0
BLOCK_ROWS = 512


def split_up(x, dim, count):
    dims = x.shape
    tiles = x.reshape(*dims[:dim], count, dims[dim] // count, *dims[dim + 1 :])
    return jnp.moveaxis(tiles, dim, 0)


def sum_at_owner(x, axis, dim):
    tiles = split_up(x, dim, lax.axis_size(axis))
    arrived = lax.all_to_all(tiles, axis, split_axis=0, concat_axis=0, tiled=True)
    return arrived.astype(jnp.float32).sum(axis=0)


def side_by_side(arrays, axis, dim, along):
    both = jnp.concatenate(arrays, axis=along)
    filled, at, outs = (sum_at_owner(both, axis, dim), 0, [])
    for a in arrays:
        outs.append(lax.slice_in_dim(filled, at, at + a.shape[along], axis=along))
        at += a.shape[along]
    return tuple(outs)


def sent_together(arrays, axis, dim, along):
    widths = [math.prod(a.shape[along:]) for a in arrays]
    both = jnp.concatenate(
        [a.reshape(*a.shape[:along], w) for a, w in zip(arrays, widths)], axis=along
    )
    filled = sum_at_owner(both, axis, dim)
    tiles = jnp.split(filled, [sum(widths[:k]) for k in range(1, len(widths))], axis=along)
    return tuple(
        (b.reshape(*filled.shape[:along], *a.shape[along:]) for a, b in zip(arrays, tiles))
    )


def rms_scale(hidden):
    return lax.rsqrt(jnp.mean(hidden * hidden, axis=-1, keepdims=True) + EPSILON)


def norm_back(hidden, scaling, gain_vec, grad_out):
    weighted = grad_out * gain_vec
    gain_grad = jnp.sum(grad_out * hidden * scaling, axis=0)
    inner_mean = jnp.mean(weighted * hidden, axis=-1, keepdims=True)
    return (scaling * weighted - hidden * (scaling * scaling * scaling) * inner_mean, gain_grad)


def rope_tables(positions, head_dim):
    half_dim = head_dim // 2
    frequency = jnp.exp(
        jnp.arange(half_dim, dtype=jnp.float32) * (-2.0 * math.log(ROPE_BASE) / head_dim)
    )
    angles = positions[:, None] * frequency[None, :]
    return (jnp.cos(angles), jnp.sin(angles))


def apply_rotary(vectors, cosine_table, sine_component):
    half_dim = vectors.shape[-1] // 2
    first_half = vectors[..., :half_dim]
    second_half = vectors[..., half_dim:]
    cos_rows = cosine_table[:, None, :]
    sin_rows = sine_component[:, None, :]
    return jnp.concatenate(
        [
            first_half * cos_rows - second_half * sin_rows,
            first_half * sin_rows + second_half * cos_rows,
        ],
        axis=-1,
    )


def slot_table(route_ids, expert_count, capacity):
    number_of_rows, top_count = route_ids.shape
    flat_ids = route_ids.reshape(-1)
    one_hot = (flat_ids[:, None] == jnp.arange(expert_count, dtype=jnp.int32)[None, :]).astype(
        jnp.int32
    )
    earlier = jnp.cumsum(one_hot, axis=0) - one_hot
    slot_ids = jnp.sum(earlier * one_hot, axis=1)
    slot_where = flat_ids * capacity + slot_ids
    pick_ids = jnp.arange(number_of_rows * top_count, dtype=jnp.int32)
    token_of = (
        jnp.full((expert_count * capacity,), number_of_rows, jnp.int32)
        .at[slot_where]
        .set(pick_ids // top_count)
    )
    pick_of = (
        jnp.full((expert_count * capacity,), number_of_rows * top_count, jnp.int32)
        .at[slot_where]
        .set(pick_ids)
    )
    return (slot_where, token_of, pick_of)


def block_scores(query_rows, key_rows, query_group_width):
    block_len = query_rows.shape[0]
    key_count, kv_heads, head_dim = key_rows.shape
    grouped = query_rows.reshape(block_len, kv_heads, query_group_width, head_dim)
    scores = jnp.einsum(
        "qhgd,khd->hgqk", grouped, key_rows, preferred_element_type=jnp.float32
    ) * head_dim ** (-0.5)
    row_pos = jnp.arange(block_len, dtype=jnp.int32)[:, None]
    col_pos = jnp.arange(key_count, dtype=jnp.int32)[None, :]
    return (jnp.where(col_pos <= row_pos, scores, -1e30), grouped)


def sequence_forward(query_rows, key_rows, value_rows, query_group_width):
    length, kv_heads, head_dim = key_rows.shape
    block_len = min(BLOCK_ROWS, length)
    scores, grouped = block_scores(query_rows, key_rows, query_group_width)
    largest = jnp.max(scores, axis=-1, keepdims=True)
    log_total = largest + jnp.log(jnp.sum(jnp.exp(scores - largest), axis=-1, keepdims=True))
    weights = jnp.exp(scores - log_total).astype(jnp.bfloat16)
    attended = jnp.einsum("hgqk,khd->qhgd", weights, value_rows, preferred_element_type=jnp.float32)
    outputs = attended.reshape(block_len, -1, head_dim).astype(jnp.bfloat16)
    return (outputs, log_total)


def sequence_backward(
    query_rows, key_rows, value_rows, attended, log_total, d_attended, query_group_width
):
    length, kv_heads, head_dim = key_rows.shape
    block_len = min(BLOCK_ROWS, length)
    scale_factor = head_dim ** (-0.5)
    key_gradient = jnp.zeros((length, kv_heads, head_dim), jnp.float32)
    value_gradient = jnp.zeros((length, kv_heads, head_dim), jnp.float32)
    scores, grouped = block_scores(query_rows, key_rows, query_group_width)
    weights = jnp.exp(scores - log_total)
    d_grouped = d_attended.reshape(block_len, kv_heads, query_group_width, head_dim)
    o_grouped = attended.reshape(block_len, kv_heads, query_group_width, head_dim)
    delta = jnp.sum(d_grouped.astype(jnp.float32) * o_grouped.astype(jnp.float32), axis=-1)
    delta = jnp.transpose(delta, (1, 2, 0))[..., None]
    d_weights = jnp.einsum(
        "qhgd,khd->hgqk", d_grouped, value_rows, preferred_element_type=jnp.float32
    )
    d_scores = (weights * (d_weights - delta)).astype(jnp.bfloat16)
    block_query = (
        jnp.einsum("hgqk,khd->qhgd", d_scores, key_rows, preferred_element_type=jnp.float32)
        * scale_factor
    )
    query_parts = block_query.reshape(block_len, -1, head_dim)
    key_gradient = key_gradient.at[:block_len].add(
        jnp.einsum("hgqk,qhgd->khd", d_scores, grouped, preferred_element_type=jnp.float32)
        * scale_factor
    )
    value_gradient = value_gradient.at[:block_len].add(
        jnp.einsum(
            "hgqk,qhgd->khd",
            weights.astype(jnp.bfloat16),
            d_grouped,
            preferred_element_type=jnp.float32,
        )
    )
    return (query_parts, key_gradient, value_gradient)


def reduce_plan(
    tokens,
    gain_attn,
    w_query,
    key_projection,
    value_projection,
    w_out,
    gain_moe,
    w_router,
    w_gate,
    w_up,
    w_down,
    routes,
    cotangent,
):
    number_of_rows, model_width = tokens.shape
    head_dim = HEAD_SIZE
    query_heads = w_query.shape[1] // head_dim
    kv_heads = key_projection.shape[1] // head_dim
    query_group_width = query_heads // kv_heads
    expert_count = w_router.shape[1]
    local_experts = w_gate.shape[0]
    source_count = expert_count // local_experts
    capacity = CAP
    top_count = routes.shape[1]
    resid = tokens.astype(jnp.float32)
    scale_one = rms_scale(resid)
    first_normalized = (resid * scale_one * gain_attn).astype(jnp.bfloat16)
    positions = (jnp.arange(number_of_rows, dtype=jnp.int32) % SEQUENCE_LENGTH).astype(jnp.float32)
    cosine_table, sine_component = rope_tables(positions, head_dim)
    q_lin = jnp.dot(first_normalized, w_query, preferred_element_type=jnp.float32).reshape(
        number_of_rows, query_heads, head_dim
    )
    linear_key = jnp.dot(
        first_normalized, key_projection, preferred_element_type=jnp.float32
    ).reshape(number_of_rows, kv_heads, head_dim)
    value_reduced = (
        jnp.dot(first_normalized, value_projection, preferred_element_type=jnp.float32)
        .astype(jnp.bfloat16)
        .reshape(number_of_rows, kv_heads, head_dim)
    )
    q_rot = apply_rotary(q_lin, cosine_table, sine_component).astype(jnp.bfloat16)
    rotated_key = apply_rotary(linear_key, cosine_table, sine_component).astype(jnp.bfloat16)
    attended, log_total = sequence_forward(q_rot, rotated_key, value_reduced, query_group_width)
    flat_att = attended.reshape(number_of_rows, query_heads * head_dim)
    attn_part = jnp.dot(flat_att, w_out, preferred_element_type=jnp.float32)
    hidden1 = resid + lax.psum(attn_part.astype(jnp.bfloat16), "tensor").astype(jnp.float32)
    scale_two = rms_scale(hidden1)
    normed2 = (hidden1 * scale_two * gain_moe).astype(jnp.bfloat16)
    logits = jnp.dot(normed2, w_router, preferred_element_type=jnp.float32)
    chosen = jnp.take_along_axis(logits, routes, axis=1)
    gate_probs = jax.nn.softmax(chosen, axis=-1)
    slot_where, token_of, pick_of = slot_table(routes, expert_count, capacity)
    normed_pad = jnp.concatenate([normed2, jnp.zeros((1, model_width), jnp.bfloat16)], axis=0)
    outgoing = normed_pad[token_of].reshape(expert_count, capacity, model_width)
    received = lax.all_to_all(outgoing, "expert", split_axis=0, concat_axis=0, tiled=True)
    arrived = received.reshape(source_count, local_experts, capacity, model_width)
    gate_pre = jnp.einsum("secd,edh->sech", arrived, w_gate, preferred_element_type=jnp.float32)
    up_pre = jnp.einsum("secd,edh->sech", arrived, w_up, preferred_element_type=jnp.float32)
    sig_gate = jax.nn.sigmoid(gate_pre)
    activated = gate_pre * sig_gate
    hid_low = (activated * up_pre).astype(jnp.bfloat16)
    expert_out = jnp.einsum(
        "sech,ehd->secd", hid_low, w_down, preferred_element_type=jnp.float32
    ).astype(jnp.bfloat16)
    returned = lax.all_to_all(
        expert_out.reshape(expert_count, capacity, model_width),
        "expert",
        split_axis=0,
        concat_axis=0,
        tiled=True,
    )
    picked = returned.reshape(expert_count * capacity, model_width)[slot_where].reshape(
        number_of_rows, top_count, model_width
    )
    moe_part = jnp.zeros((number_of_rows, model_width), jnp.float32)
    for choice_index in range(top_count):
        moe_part = (
            moe_part
            + picked[:, choice_index].astype(jnp.float32)
            * gate_probs[:, choice_index : choice_index + 1]
        )
    moe_out = lax.psum(moe_part.astype(jnp.bfloat16), "tensor").astype(jnp.float32)
    output = (hidden1 + moe_out).astype(jnp.bfloat16)
    grad = cotangent.astype(jnp.float32)
    gate_dot = jnp.einsum("rjd,rd->rj", picked, cotangent, preferred_element_type=jnp.float32)
    grad_pad = jnp.concatenate([cotangent, jnp.zeros((1, model_width), jnp.bfloat16)], axis=0)
    gate_pad = jnp.concatenate([gate_probs.reshape(-1), jnp.zeros((1,), jnp.float32)], axis=0)
    sent_grad = (grad_pad[token_of].astype(jnp.float32) * gate_pad[pick_of][:, None]).astype(
        jnp.bfloat16
    )
    sent_grad = sent_grad.reshape(expert_count, capacity, model_width)
    grad_received = lax.all_to_all(sent_grad, "expert", split_axis=0, concat_axis=0, tiled=True)
    arrived_grad = grad_received.reshape(source_count, local_experts, capacity, model_width)
    d_hid = jnp.einsum("secd,ehd->sech", arrived_grad, w_down, preferred_element_type=jnp.float32)
    down_local = jnp.einsum(
        "sech,secd->ehd", hid_low, arrived_grad, preferred_element_type=jnp.float32
    )
    d_gate = (d_hid * up_pre * sig_gate * (1.0 + gate_pre * (1.0 - sig_gate))).astype(jnp.bfloat16)
    d_up = (d_hid * activated).astype(jnp.bfloat16)
    gate_local = jnp.einsum("secd,sech->edh", arrived, d_gate, preferred_element_type=jnp.float32)
    up_local = jnp.einsum("secd,sech->edh", arrived, d_up, preferred_element_type=jnp.float32)
    back_rows = jnp.einsum("sech,edh->secd", d_gate, w_gate, preferred_element_type=jnp.float32)
    back_rows = (
        back_rows + jnp.einsum("sech,edh->secd", d_up, w_up, preferred_element_type=jnp.float32)
    ).astype(jnp.bfloat16)
    came_back = lax.all_to_all(
        back_rows.reshape(expert_count, capacity, model_width),
        "expert",
        split_axis=0,
        concat_axis=0,
        tiled=True,
    )
    back_picked = came_back.reshape(expert_count * capacity, model_width)[slot_where].reshape(
        number_of_rows, top_count, model_width
    )
    back_part = jnp.zeros((number_of_rows, model_width), jnp.float32)
    for choice_index in range(top_count):
        back_part = back_part + back_picked[:, choice_index].astype(jnp.float32)
    back_total, dgate = (
        lax.psum(back_part.astype(jnp.bfloat16), "tensor").astype(jnp.float32),
        lax.psum(gate_dot.astype(jnp.bfloat16), "tensor").astype(jnp.float32),
    )
    inner_sum = jnp.sum(gate_probs * dgate, axis=1, keepdims=True)
    d_chosen = gate_probs * (dgate - inner_sum)
    matches = routes[:, :, None] == jnp.arange(expert_count, dtype=jnp.int32)[None, None, :]
    d_logits = jnp.sum(jnp.where(matches, d_chosen[:, :, None], 0.0), axis=1).astype(jnp.bfloat16)
    router_local = jnp.dot(normed2.T, d_logits, preferred_element_type=jnp.float32)
    d_normed2 = back_total + jnp.dot(d_logits, w_router.T, preferred_element_type=jnp.float32)
    d_hidden_part, gain_moe_local = norm_back(hidden1, scale_two, gain_moe, d_normed2)
    d_hidden1 = grad + d_hidden_part
    d_mixed = d_hidden1.astype(jnp.bfloat16)
    out_local = jnp.dot(flat_att.T, d_mixed, preferred_element_type=jnp.float32)
    d_att = (
        jnp.dot(d_mixed, w_out.T, preferred_element_type=jnp.float32)
        .astype(jnp.bfloat16)
        .reshape(number_of_rows, query_heads, head_dim)
    )
    dq_rot, rotated_key_gradient, dv_rows = sequence_backward(
        q_rot, rotated_key, value_reduced, attended, log_total, d_att, query_group_width
    )
    d_query = (
        apply_rotary(dq_rot, cosine_table, -sine_component)
        .astype(jnp.bfloat16)
        .reshape(number_of_rows, query_heads * head_dim)
    )
    key_gradient = (
        apply_rotary(rotated_key_gradient, cosine_table, -sine_component)
        .astype(jnp.bfloat16)
        .reshape(number_of_rows, kv_heads * head_dim)
    )
    value_gradient = dv_rows.astype(jnp.bfloat16).reshape(number_of_rows, kv_heads * head_dim)
    query_local = jnp.dot(first_normalized.T, d_query, preferred_element_type=jnp.float32)
    key_local = jnp.dot(first_normalized.T, key_gradient, preferred_element_type=jnp.float32)
    value_local = jnp.dot(first_normalized.T, value_gradient, preferred_element_type=jnp.float32)
    d_normed_part = jnp.dot(d_query, w_query.T, preferred_element_type=jnp.float32)
    d_normed_part = d_normed_part + jnp.dot(
        key_gradient, key_projection.T, preferred_element_type=jnp.float32
    )
    d_normed_part = d_normed_part + jnp.dot(
        value_gradient, value_projection.T, preferred_element_type=jnp.float32
    )
    d_normed1 = lax.psum(d_normed_part.astype(jnp.bfloat16), "tensor").astype(jnp.float32)
    d_resid_part, gain_attn_local = norm_back(resid, scale_one, gain_attn, d_normed1)
    input_grad = (d_hidden1 + d_resid_part).astype(jnp.bfloat16)
    gate_grad, up_grad, down_grad = (
        lax.psum_scatter(
            gate_local.astype(jnp.bfloat16), "dp", scatter_dimension=1, tiled=True
        ).astype(jnp.float32),
        lax.psum_scatter(
            up_local.astype(jnp.bfloat16), "dp", scatter_dimension=1, tiled=True
        ).astype(jnp.float32),
        lax.psum_scatter(
            down_local.astype(jnp.bfloat16), "dp", scatter_dimension=2, tiled=True
        ).astype(jnp.float32),
    )
    query_grad, key_grad, value_grad, out_grad, router_grad, gain_attn_grad, gain_moe_grad = (
        *side_by_side(
            (
                query_local.astype(jnp.bfloat16),
                key_local.astype(jnp.bfloat16),
                value_local.astype(jnp.bfloat16),
            ),
            ("dp", "expert"),
            0,
            1,
        ),
        sum_at_owner(out_local.astype(jnp.bfloat16), ("dp", "expert"), 1),
        *sent_together(
            (
                router_local.astype(jnp.bfloat16),
                gain_attn_local.astype(jnp.bfloat16),
                gain_moe_local.astype(jnp.bfloat16),
            ),
            ("dp", "expert"),
            0,
            1,
        ),
    )
    return (
        output,
        input_grad,
        gain_attn_grad,
        query_grad,
        key_grad,
        value_grad,
        out_grad,
        gain_moe_grad,
        router_grad,
        gate_grad,
        up_grad,
        down_grad,
    )


GATHER_ROWS = 4096
MESH = pl.DeviceIdType.MESH
VMEM = pl.BlockSpec(memory_space=pltpu.VMEM)
ANY = pl.BlockSpec(memory_space=pl.ANY)
EXTRA = 128
VMEM_LIMIT = 63 * 2**20
STAGE_PLACES = (1, 5, 9, 10, 14, 16, 18)
F32, BF16 = jnp.float32, jnp.bfloat16


def dot(a, b):
    return jnp.dot(a, b, preferred_element_type=F32)


def dot_nt(a, b):
    return lax.dot_general(a, b, (((1,), (1,)), ((), ())), preferred_element_type=F32)


def dot_tn(a, b):
    return lax.dot_general(a, b, (((0,), (0,)), ((), ())), preferred_element_type=F32)


def ds(index, size):
    return pl.ds(pl.multiple_of(index * size, size), size)


class Peers:
    def __init__(self, dp, tp, send_sem, recv_sem):
        self.z, self.c, self.t = (lax.axis_index(a) for a in ("dp", "expert", "tensor"))
        self.dp, self.tp = dp, tp
        self.send_sem, self.recv_sem = send_sem, recv_sem
        self.used = 0
        self.open = []

    def tensor(self, k):
        return (self.z, self.c, lax.rem(self.t + k, self.tp))

    def near(self, axis):
        row, col = self.t // 2, self.t % 2
        index = row * 2 + (1 - col) if axis == 0 else (1 - row) * 2 + col
        return (self.z, self.c, index)

    def plane(self, k):
        return (lax.rem(self.z + k, self.dp), self.c, self.t)

    def partner(self):
        return (self.z, 1 - self.c, self.t)

    def greet(self):
        barrier = pltpu.get_barrier_semaphore()
        everyone = [self.tensor(k) for k in range(1, self.tp)]
        everyone += [self.plane(k) for k in range(1, self.dp)] + [self.partner()]
        for peer in everyone:
            pl.semaphore_signal(barrier, inc=1, device_id=peer, device_id_type=MESH)
        pl.semaphore_wait(barrier, len(everyone))

    def number(self, count):
        first = self.used
        self.used += count
        return first

    def make(self, src, dst, number, device):
        return pltpu.make_async_remote_copy(
            src_ref=src,
            dst_ref=dst,
            send_sem=self.send_sem.at[number],
            recv_sem=self.recv_sem.at[number],
            device_id=device,
            device_id_type=MESH,
        )

    def to(self, src, dst, device):
        copy = self.make(src, dst, self.number(1), device)
        copy.start()
        self.open.append(copy)
        return copy

    def keep(self, src, dst, sem):
        copy = pltpu.make_async_copy(src, dst, sem)
        copy.start()
        return copy

    def drain(self):
        for copy in self.open:
            copy.wait_send()


def arrived(copies):
    for copy in copies:
        copy.wait_recv()


def rotate(u, rope_ref, scale=1.0, sign=1.0):
    width = u.shape[1]
    tiles = []
    for at in range(0, width, 128):
        v = u[:, at : at + 128]
        side = pltpu.roll(v, 96, 1) * rope_ref[1] + pltpu.roll(v, 32, 1) * rope_ref[2]
        turned = v * rope_ref[0] + side if sign > 0 else v * rope_ref[0] - side
        tiles.append(turned if scale == 1.0 else turned * scale)
    return tiles[0] if len(tiles) == 1 else jnp.concatenate(tiles, axis=1)


def stack_heads(u, kv, group):
    heads = [kv * group + j for j in range(group)]
    return jnp.concatenate([u[:, h * HEAD_SIZE : (h + 1) * HEAD_SIZE] for h in heads], axis=0)


def inverse_rms(u):
    return lax.rsqrt(jnp.mean(u * u, axis=-1, keepdims=True) + EPSILON)


def causal(length):
    row = lax.broadcasted_iota(jnp.int32, (length, length), 0)
    col = lax.broadcasted_iota(jnp.int32, (length, length), 1)
    return col <= row


def pad_router(wr_ref, wr_buf):
    wr_buf[...] = jnp.zeros_like(wr_buf)
    wr_buf[: wr_ref.shape[0], :] = wr_ref[...]


def chosen_of(routes_ref, sequences):
    masks = []
    for i in sequences:
        picked = routes_ref[i]
        ids = lax.broadcasted_iota(jnp.int32, (EXTRA, picked.shape[1]), 0)
        chosen = ids == picked[0:1, :]
        for j in range(1, picked.shape[0]):
            chosen = chosen | (ids == picked[j : j + 1, :])
        masks.append(jnp.where(chosen, 1.0, 0.0).T)
    return jnp.concatenate(masks, axis=0) > 0.5


def gates_of(x_ref, chosen, wr_buf):
    logits = dot_nt(x_ref[...], wr_buf[...])
    top = jnp.max(jnp.where(chosen, logits, -jnp.inf), axis=1, keepdims=True)
    weight = jnp.where(chosen, jnp.exp(jnp.where(chosen, logits - top, 0.0)), 0.0)
    return weight / jnp.sum(weight, axis=1, keepdims=True)


def store_split(gates, split_ref):
    high = gates.astype(BF16)
    split_ref[:, :EXTRA] = high
    split_ref[:, EXTRA:] = (gates - high.astype(F32)).astype(BF16)


def pair_of_gates(split, first, width):
    k_pos = lax.broadcasted_iota(jnp.int32, (2 * EXTRA, 2 * width), 0)
    l_pos = lax.broadcasted_iota(jnp.int32, (2 * EXTRA, 2 * width), 1)
    pick = jnp.where(k_pos % EXTRA == first + l_pos // width, 1.0, 0.0).astype(BF16)
    return dot(split, pick)


def swiglu(both, dh, gate):
    width = dh.shape[1]
    gate_pre, up_pre = both[:, :width], both[:, width:]
    sig = jax.nn.sigmoid(gate_pre)
    act = gate_pre * sig
    hid = act * up_pre
    d_hid = dh * gate
    d_gate = d_hid * up_pre * sig * (1.0 + gate_pre * (1.0 - sig))
    return hid, (hid * gate).astype(BF16), d_gate.astype(BF16), (d_hid * act).astype(BF16)


def front_kernel(
    dp,
    tp,
    tok_ref,
    cot_ref,
    routes_ref,
    ga_ref,
    gm_ref,
    wr_ref,
    wq_ref,
    wk_ref,
    wv_ref,
    wo_ref,
    rope_ref,
    wg_ref,
    wu_ref,
    wd_ref,
    xr_ref,
    gr_ref,
    moe_ref,
    back_ref,
    dgate_ref,
    gates_ref,
    h1_ref,
    kv_ref,
    att_ref,
    qs_ref,
    as_ref,
    prob_ref,
    prob_t_ref,
    n1t_ref,
    ghid_ref,
    dgu_ref,
    mask_ref,
    place_ref,
    x_buf,
    g_buf,
    gz_buf,
    wr_buf,
    routes_buf,
    n1_buf,
    part_buf,
    rs_buf,
    dh_buf,
    split,
    moe_acc,
    back_acc,
    send_sem,
    recv_sem,
    keep_sem,
):
    step, last = pl.program_id(0), pl.num_programs(0) - 1
    pairs = pl.num_programs(0) // 2
    net = Peers(dp, tp, send_sem, recv_sem)
    z, c, t = net.z, net.c, net.t
    length, model = tok_ref.shape
    rows = 2 * length
    own = length // tp
    width = wg_ref.shape[2]
    q_width, kv_width = wq_ref.shape[1], wk_ref.shape[1]
    group = q_width // kv_width
    others, sides = range(1, dp), range(1, tp)

    def block(plane, core, tensor):
        return ds((plane * 2 + core) * tp + tensor, own)

    def link(src, dst, device):
        return net.make(src, dst, net.number(1), device)

    def start(copies):
        for copy in copies:
            copy.start()

    mine = ds(c * tp + t, own)
    seq_rows = ds(c, length)
    near = [net.near(axis) for axis in range(2)]
    far = tp - 1 - t
    half = own // 2

    def piece(plane, tensor, part_of):
        at = (((plane * 2 + c) * tp + tensor) * 2 + part_of) * half
        return pl.ds(pl.multiple_of(at, half), half)

    def spread(ref, sources, relayed):
        direct = [
            link(sources[p - 1], ref.at[block(p, c, t)], near[axis])
            for p in others
            for axis in range(2)
        ]
        relay = []
        for p in others if relayed else ():
            for axis in range(2):
                at = piece(p, near[axis][2], axis)
                relay.append(link(ref.at[at], ref.at[at], near[1 - axis]))
        to_core = [link(sources[p - 1], ref.at[block(p, c, t)], net.partner()) for p in others]
        near_core, far_core = [], []
        for p in others:
            for axis in range(2):
                at = block(p, c, near[axis][2])
                near_core.append(link(ref.at[at], ref.at[at], net.partner()))
            at = block(p, c, far)
            far_core.append(link(ref.at[at], ref.at[at], net.partner()))
        return direct, relay, to_core, near_core, far_core

    g_own = [link(cot_ref, g_buf.at[seq_rows], net.partner())]
    g_z = [link(cot_ref.at[ds(t, own)], gz_buf.at[dp - 1 - k], net.plane(k)) for k in others]
    side_h = [
        link(part_buf.at[ds(lax.rem(t + k, tp), own)], rs_buf.at[k - 1], net.tensor(k))
        for k in sides
    ]
    x_t = [link(x_buf.at[mine], x_buf.at[mine], net.tensor(k)) for k in sides]
    x_own = [link(x_buf.at[mine], x_buf.at[mine], net.partner())]
    x_seen = []
    for k in sides:
        at = ds(c * tp + lax.rem(t + tp - k, tp), own)
        x_seen.append(link(x_buf.at[at], x_buf.at[at], net.partner()))
    x_z = [link(x_buf.at[mine], xr_ref.at[block(dp - k, c, t)], net.plane(k)) for k in others]
    g_direct, g_relay, g_core, g_near, g_far = spread(
        gr_ref, [gz_buf.at[p - 1] for p in others], True
    )
    x_direct, _, x_core, x_near, x_far = spread(
        xr_ref, [xr_ref.at[block(p, c, t)] for p in others], False
    )
    x_z2 = [
        link(x_buf.at[ds(c * tp + far, own)], xr_ref.at[block(dp - k, c, far)], net.plane(k))
        for k in others
    ]
    r_own = [link(routes_ref, routes_buf.at[c], net.partner())]
    r_z = [link(routes_ref, routes_buf.at[(dp - k) * 2 + c], net.plane(k)) for k in others]
    r_core = [
        link(routes_buf.at[p * 2 + c], routes_buf.at[p * 2 + c], net.partner()) for p in others
    ]
    keep_x = pltpu.make_async_copy(x_buf, xr_ref.at[pl.ds(0, rows)], keep_sem.at[0])
    keep_g = [pltpu.make_async_copy(g_buf, gr_ref.at[pl.ds(0, rows)], keep_sem.at[1])] + [
        pltpu.make_async_copy(gz_buf.at[p - 1], gr_ref.at[block(p, c, t)], keep_sem.at[1 + p])
        for p in others
    ]

    @pl.when(step == 0)
    def _():
        net.greet()
        start(r_own + r_z + g_own + g_z)
        g_buf[seq_rows, :] = cot_ref[...]
        routes_buf[c] = routes_ref[...]
        resid = tok_ref[...].astype(F32)
        n1 = (resid * inverse_rms(resid) * ga_ref[...].reshape(1, -1)).astype(BF16)
        n1_buf[...] = n1
        q_all = rotate(dot(n1, wq_ref[...]), rope_ref, HEAD_SIZE ** (-0.5)).astype(BF16)
        kv_ref[:, :kv_width] = rotate(dot(n1, wk_ref[...]), rope_ref).astype(BF16)
        kv_ref[:, kv_width:] = dot(n1, wv_ref[...]).astype(BF16)
        seen = causal(length)
        for kv in range(kv_width // HEAD_SIZE):
            key = kv_ref[:, kv * HEAD_SIZE : (kv + 1) * HEAD_SIZE]
            val = kv_ref[:, kv_width + kv * HEAD_SIZE : kv_width + (kv + 1) * HEAD_SIZE]
            q = stack_heads(q_all, kv, group)
            qs_ref[kv] = q
            s = dot_nt(q, key).reshape(group, length, length)
            s = jnp.where(seen[None], s, -1e30)
            up_to = jnp.exp(s - jnp.max(s, axis=-1, keepdims=True))
            prob = up_to * (1.0 / jnp.sum(up_to, axis=-1, keepdims=True))
            prob = prob.reshape(group * length, length).astype(BF16)
            prob_ref[kv] = prob
            att = dot(prob, val).astype(BF16)
            as_ref[kv] = att
            for j in range(group):
                h = kv * group + j
                att_ref[:, h * HEAD_SIZE : (h + 1) * HEAD_SIZE] = att[j * length : (j + 1) * length]
        part_buf[...] = dot(att_ref[...], wo_ref[...]).astype(BF16)
        start(side_h)
        moe_acc[...] = jnp.zeros_like(moe_acc)
        back_acc[...] = jnp.zeros_like(back_acc)
        dgate_ref[...] = jnp.zeros_like(dgate_ref)
        pad_router(wr_ref, wr_buf)
        place_ref[0] = z
        place_ref[1] = c
        arrived(g_own)

    @pl.when(step < pairs)
    def _():
        dh_buf[step] = dot_nt(g_buf[...], wd_ref[...].reshape(2 * width, model))

    @pl.when(step == pairs // 2)
    def _():
        arrived(r_z)
        start(r_core)

    @pl.when(step == pairs - 1)
    def _():
        arrived(r_core)
        for i in range(2, 2 * dp):
            masked = chosen_of(routes_buf, range(i, i + 1))
            mask_ref[(i - 2) * length : (i - 1) * length, :] = jnp.where(masked, 1.0, 0.0).astype(BF16)

    @pl.when(step == pairs)
    def _():
        total = tok_ref[ds(t, own), :].astype(F32) + part_buf[ds(t, own), :].astype(F32)
        arrived(side_h)
        for k in sides:
            total = total + rs_buf[k - 1].astype(F32)
        n2 = (total * inverse_rms(total) * gm_ref[...].reshape(1, -1)).astype(BF16)
        x_buf[mine, :] = n2
        start(x_t + x_own + x_z)
        arrived(r_own)
        chosen = chosen_of(routes_buf, range(2))
        h1_ref[...] = total
        for kv in range(kv_width // HEAD_SIZE):
            prob_t_ref[kv] = prob_ref[kv].T
        n1t_ref[...] = n1_buf[...].T
        for k in sides:
            arrived(x_t[k - 1 : k])
            start(x_seen[k - 1 : k])
        arrived(g_z)
        start(g_direct + g_core + keep_g)
        arrived(x_own + x_seen)
        keep_x.start()
        gates = gates_of(x_buf, chosen, wr_buf)
        gates_ref[...] = gates
        store_split(gates, split)

    @pl.when(step == pairs + 3)
    def _():
        arrived(x_z)
        start(x_direct + x_core + x_z2)

    @pl.when(step == pairs + 6)
    def _():
        arrived(g_direct)
        start(g_relay + g_near)

    @pl.when(step == pairs + 9)
    def _():
        arrived(g_relay)
        start(g_far)
        arrived(x_direct)
        start(x_near)
        arrived(x_z2)
        start(x_far)

    @pl.when(step >= pairs)
    def _():
        pair = step - pairs
        first = c * (2 * pairs) + 2 * pair
        gate_pair = pair_of_gates(split[...], first, width)
        lane = lax.broadcasted_iota(jnp.int32, dgate_ref.shape, 1)
        w_pair = jnp.concatenate([wg_ref[0], wu_ref[0], wg_ref[1], wu_ref[1]], axis=1)
        both_pair = dot(x_buf[...], w_pair)
        for k in range(2):
            lanes = slice(k * width, (k + 1) * width)
            dh = dh_buf[pair, :, lanes]
            both = both_pair[:, 2 * k * width : 2 * (k + 1) * width]
            hid, ghid, dgp, dup = swiglu(both, dh, gate_pair[:, lanes])
            ghid_ref[:, lanes] = ghid
            dgu_ref[:, 2 * k * width : (2 * k + 1) * width] = dgp
            dgu_ref[:, (2 * k + 1) * width : 2 * (k + 1) * width] = dup
            row_sum = jnp.sum(hid * dh, axis=1, keepdims=True)
            dgate_ref[...] += jnp.where(lane == first + k, row_sum, 0.0)
        back_acc[...] += dot_nt(dgu_ref[...], w_pair)
        moe_acc[...] += dot(ghid_ref[...], wd_ref[...].reshape(2 * width, model))

    @pl.when(step == last)
    def _():
        moe_ref[...] = moe_acc[...].astype(BF16)
        back_ref[...] = back_acc[...].astype(BF16)
        keep_x.wait()
        for copy in keep_g:
            copy.wait()
        arrived(g_core + g_near + g_far + x_core + x_near + x_far)
        sent = g_own + g_z + side_h + x_t + x_own + x_seen + x_z + r_own + r_z + r_core
        sent = sent + g_direct + g_relay + g_core + g_near + g_far
        for copy in sent + x_direct + x_z2 + x_core + x_near + x_far:
            copy.wait_send()


def whole_spec(a):
    shape = a.shape
    return pl.BlockSpec(shape, lambda *_: (0,) * len(shape), pipeline_mode=pl.Buffered(1))


def front(dp, tp, arrays, weights):
    tokens, wq, wk = arrays[0], arrays[6], arrays[7]
    length, model = tokens.shape
    count, _, width = weights[0].shape
    pairs = count // 2
    rows, own = 2 * length, length // tp
    q_width = wq.shape[1]
    kv_heads, group = wk.shape[1] // HEAD_SIZE, q_width // wk.shape[1]
    others, sides = dp - 1, tp - 1
    copies = 1 + others + sides + sides + 1 + sides + 2 * others + (8 + 6) * others + 1 + 2 * others
    later = lambda i: jnp.maximum(i - pairs, 0)
    up = lambda shape: pl.BlockSpec((2,) + shape, lambda i: (later(i), 0, 0))
    down = pl.BlockSpec((2, width, model), lambda i: (lax.rem(i, pairs), 0, 0))
    saved = pl.BlockSpec((rows, 2 * width), lambda i: (0, later(i)))
    saved_both = pl.BlockSpec((rows, 4 * width), lambda i: (0, later(i)))
    shapes = [
        ((rows * dp, model), BF16),
        ((rows * dp, model), BF16),
        ((rows, model), BF16),
        ((rows, model), BF16),
        ((rows, EXTRA), F32),
        ((rows, EXTRA), F32),
        ((own, model), F32),
        ((length, 2 * wk.shape[1]), BF16),
        ((length, q_width), BF16),
        ((kv_heads, group * length, HEAD_SIZE), BF16),
        ((kv_heads, group * length, HEAD_SIZE), BF16),
        ((kv_heads, group * length, length), BF16),
        ((kv_heads, length, group * length), BF16),
        ((model, length), BF16),
        ((rows, count * width), BF16),
        ((rows, 2 * count * width), BF16),
        ((rows * others, EXTRA), BF16),
        ((2,), jnp.int32),
    ]
    shapes = [jax.ShapeDtypeStruct(*s) for s in shapes]
    scratch = [
        ((rows, model), BF16),
        ((rows, model), BF16),
        ((others, own, model), BF16),
        ((EXTRA, model), BF16),
        ((2 * dp, *arrays[2].shape), jnp.int32),
        ((length, model), BF16),
        ((length, model), BF16),
        ((sides, own, model), BF16),
        ((pairs, rows, 2 * width), F32),
        ((rows, 2 * EXTRA), BF16),
        ((rows, model), F32),
        ((rows, model), F32),
    ]
    return pl.pallas_call(
        functools.partial(front_kernel, dp, tp),
        grid=(2 * pairs,),
        out_shape=shapes,
        in_specs=[whole_spec(a) for a in arrays] + [up((model, width)), up((model, width)), down],
        out_specs=[ANY, ANY]
        + [whole_spec(s) for s in shapes[2:14]]
        + [saved, saved_both, whole_spec(shapes[16]), pl.BlockSpec(memory_space=pltpu.SMEM)],
        scratch_shapes=[pltpu.VMEM(*s) for s in scratch]
        + [
            pltpu.SemaphoreType.DMA((copies,)),
            pltpu.SemaphoreType.DMA((copies,)),
            pltpu.SemaphoreType.DMA((2 + others,)),
        ],
        compiler_params=pltpu.CompilerParams(
            collective_id=0, has_side_effects=True, vmem_limit_bytes=VMEM_LIMIT
        ),
        name="front",
    )(*arrays, *weights)


def backward_kernel(
    dp,
    tp,
    back_hbm,
    moe_hbm,
    dgate_hbm,
    gates_ref,
    h1_ref,
    tok_hbm,
    cot_hbm,
    ga_ref,
    gm_ref,
    wr_ref,
    wq_hbm,
    wk_hbm,
    wv_hbm,
    wo_hbm,
    kv_hbm,
    att_hbm,
    qs_hbm,
    as_hbm,
    prob_hbm,
    prob_t_hbm,
    n1t_hbm,
    rope_hbm,
    xr_ref,
    gr_ref,
    own_ref,
    mask_ref,
    wg_ref,
    wu_ref,
    wd_ref,
    out_ref,
    in_ref,
    dl_all,
    qkv_grad_ref,
    o_grad_ref,
    gains_ref,
    down_ref,
    dgu_ref,
    back_ref,
    moe_ref,
    dgate_ref,
    tok_ref,
    cot_ref,
    wq_ref,
    wk_ref,
    wv_ref,
    wo_ref,
    kv_ref,
    att_ref,
    qs_ref,
    as_ref,
    prob_ref,
    prob_t_ref,
    n1t_ref,
    rope_ref,
    x_rest,
    g_rest,
    wr_buf,
    g_plane,
    gt_buf,
    split,
    pair_b,
    pair_m,
    pair_d,
    sum_b,
    sum_m,
    sum_d,
    rs_b,
    rs_m,
    rs_d,
    dh1_buf,
    da_buf,
    dl_buf,
    d_buf,
    do_buf,
    part_buf,
    rs_3,
    gain_buf,
    gain_t,
    gain_z,
    gain_zs,
    gain_c,
    out_buf,
    in_buf,
    q_part,
    q_pair,
    q_sum,
    q_in,
    o_part,
    o_pair,
    o_sum,
    o_in,
    send_sem,
    recv_sem,
    keep_sem,
    load_sem,
):
    step, last = pl.program_id(0), pl.num_programs(0) - 1
    net = Peers(dp, tp, send_sem, recv_sem)
    z, c, t = net.z, net.c, net.t
    length, model = tok_ref.shape
    own = length // tp
    part = model // dp
    width = wg_ref.shape[2]
    q_width, kv_width = wq_ref.shape[1], wk_ref.shape[1]
    group = q_width // kv_width
    others, sides = range(1, dp), range(1, tp)
    mine = ds(t, own)
    here, there = ds(c, length), ds(1 - c, length)

    def columns(index):
        return pl.ds(pl.multiple_of(index * part, 128), part)

    def link(src, dst, device):
        return net.make(src, dst, net.number(1), device)

    def to_sides(ref, into):
        return [
            link(ref.at[ds(lax.rem(t + k, tp), own)], into.at[k - 1], net.tensor(k)) for k in sides
        ]

    def share(ref):
        return [link(ref.at[mine], ref.at[mine], net.tensor(k)) for k in sides]

    def on_to_partner(ref):
        rows = [ds(p * 2 + c, length) for p in others]
        return [link(ref.at[r], ref.at[r], net.partner()) for r in rows]

    def over_planes(ref, into):
        return [link(ref, into.at[ds((dp - k) * 2 + c, length)], net.plane(k)) for k in others]

    def start(copies):
        for copy in copies:
            copy.start()

    pair_bd = [
        link(back_hbm.at[there], pair_b, net.partner()),
        link(dgate_hbm.at[there], pair_d, net.partner()),
    ]
    pair_mo = [link(moe_hbm.at[there], pair_m, net.partner())]
    side_bd = to_sides(sum_b, rs_b) + to_sides(sum_d, rs_d)
    side_mo = to_sides(sum_m, rs_m)
    share_da = share(da_buf) + share(dl_buf)
    dl_z = over_planes(dl_buf, dl_all)
    dl_own = [link(dl_buf, dl_all.at[here], net.partner())]
    dl_c = on_to_partner(dl_all)
    q_core = [link(q_part.at[:, 1 - c], q_pair, net.partner())]
    q_z = [link(q_sum.at[lax.rem(z + k, dp)], q_in.at[k - 1], net.plane(k)) for k in others]
    o_core = [link(o_part.at[:, 1 - c], o_pair, net.partner())]
    o_z = [link(o_sum.at[lax.rem(z + k, dp)], o_in.at[k - 1], net.plane(k)) for k in others]
    share_out = share(out_buf)
    side_3 = to_sides(part_buf, rs_3)
    share_in = share(in_buf)
    side_gain = [link(gain_buf, gain_t.at[k - 1], net.tensor(k)) for k in sides]
    plane_gain = [
        link(gain_zs.at[:, columns(lax.rem(z + k, dp))], gain_z.at[k - 1], net.plane(k))
        for k in others
    ]
    pair_gain = [link(gain_c.at[0], gain_c.at[1], net.partner())]
    keep_dl = pltpu.make_async_copy(dl_buf, dl_all.at[here], keep_sem.at[0])
    plane_rows = xr_ref.shape[0] // dp
    rest = pl.ds(plane_rows, xr_ref.shape[0] - plane_rows)
    late = [
        (back_hbm.at[here], back_ref),
        (dgate_hbm.at[here], dgate_ref),
        (moe_hbm.at[here], moe_ref),
        (cot_hbm, cot_ref),
        (wo_hbm, wo_ref),
        (att_hbm, att_ref),
        (kv_hbm, kv_ref),
        (qs_hbm, qs_ref),
        (as_hbm, as_ref),
        (prob_hbm, prob_ref),
        (prob_t_hbm, prob_t_ref),
        (rope_hbm, rope_ref),
        (wq_hbm, wq_ref),
        (wk_hbm, wk_ref),
        (wv_hbm, wv_ref),
        (n1t_hbm, n1t_ref),
        (tok_hbm, tok_ref),
    ]
    late = [pltpu.make_async_copy(src, dst, load_sem.at[i]) for i, (src, dst) in enumerate(late)]

    def loaded(first, end):
        for copy in late[first:end]:
            copy.wait()

    load_x = pltpu.make_async_copy(xr_ref.at[rest], x_rest, keep_sem.at[1])
    load_g = pltpu.make_async_copy(gr_ref.at[rest], g_rest, keep_sem.at[2])
    load_own = pltpu.make_async_copy(
        gr_ref.at[pl.ds(0, plane_rows), columns(z)], g_plane, keep_sem.at[3]
    )

    @pl.when(step == 0)
    def _():
        load_x.start()
        load_g.start()
        load_own.start()
        start(late[:2])
        net.greet()
        start(pair_bd)
        load_x.wait()
        pad_router(wr_ref, wr_buf)
        chosen = mask_ref[...].astype(F32) > 0.5
        store_split(gates_of(x_rest, chosen, wr_buf), split)
        load_g.wait()
        load_own.wait()
        start(late[2:])
        gt_buf[:, :plane_rows] = g_plane[...].T
        gt_buf[:, plane_rows:] = g_rest[:, columns(z)].T

    def pair_sum():
        arrived(pair_bd)
        loaded(0, 2)
        sum_b[...] = (back_ref[...].astype(F32) + pair_b[...].astype(F32)).astype(BF16)
        sum_d[...] = dgate_ref[...] + pair_d[...]
        start(side_bd + pair_mo)

    def over_pair(part, pair, total):
        total[...] = (part[:, c].astype(F32) + pair[...].astype(F32)).astype(BF16)

    def over_z(total, came, out):
        value = total[z].astype(F32)
        for k in others:
            value = value + came[k - 1].astype(F32)
        out[...] = value

    def moe_backward():
        arrived(side_bd)
        loaded(2, 4)
        d_n2 = sum_b[mine, :].astype(F32)
        dgate = sum_d[mine, :]
        for k in sides:
            d_n2 = d_n2 + rs_b[k - 1].astype(F32)
            dgate = dgate + rs_d[k - 1]
        gates = gates_ref[ds(c * tp + t, own), :]
        d_logits = gates * (dgate - jnp.sum(gates * dgate, axis=1, keepdims=True))
        dl_buf[mine, :] = d_logits.astype(BF16)
        d_n2 = d_n2 + dot(d_logits.astype(BF16), wr_buf[...])
        h1 = h1_ref[...]
        r2 = inverse_rms(h1)
        weighted = d_n2 * gm_ref[...].reshape(1, -1)
        inner = jnp.mean(weighted * h1, axis=-1, keepdims=True)
        gain_buf[...] = jnp.zeros_like(gain_buf)
        gain_buf[1:2, :] = jnp.sum(d_n2 * h1 * r2, axis=0, keepdims=True)
        d_h1 = cot_ref[mine, :].astype(F32) + (r2 * weighted - h1 * (r2 * r2 * r2) * inner)
        dh1_buf[...] = d_h1
        da_buf[mine, :] = d_h1.astype(BF16)
        start(share_da)
        arrived(pair_mo)
        sum_m[...] = (moe_ref[...].astype(F32) + pair_m[...].astype(F32)).astype(BF16)

    def attention_backward():
        loaded(4, len(late))
        arrived(share_da)
        start(side_mo + dl_z + dl_own)
        keep_dl.start()
        do_buf[...] = dot_nt(da_buf[...], wo_ref[...]).astype(BF16)
        o_part[...] = dot_tn(da_buf[...], att_ref[...]).astype(BF16).reshape(o_part.shape)
        start(o_core)
        scale = HEAD_SIZE ** (-0.5)
        d_key, d_val, d_query = [], [], []
        for kv in range(kv_width // HEAD_SIZE):
            if kv == 1:
                arrived(o_core)
                over_pair(o_part, o_pair, o_sum)
                start(o_z)
            key = kv_ref[:, kv * HEAD_SIZE : (kv + 1) * HEAD_SIZE]
            val = kv_ref[:, kv_width + kv * HEAD_SIZE : kv_width + (kv + 1) * HEAD_SIZE]
            d_out = stack_heads(do_buf, kv, group)
            delta = jnp.sum(d_out.astype(F32) * as_ref[kv].astype(F32), axis=-1, keepdims=True)
            d_s = (prob_ref[kv].astype(F32) * (dot_nt(d_out, val) - delta)).astype(BF16)
            d_q = dot(d_s, key) * scale
            d_query += [d_q[j * length : (j + 1) * length] for j in range(group)]
            d_key.append(dot_tn(d_s, qs_ref[kv]))
            d_val.append(dot(prob_t_ref[kv], d_out))
        arrived(side_mo)
        total = h1_ref[...] + sum_m[mine, :].astype(F32)
        for k in sides:
            total = total + rs_m[k - 1].astype(F32)
        out_buf[mine, :] = total.astype(BF16)
        d_buf[:, :q_width] = rotate(jnp.concatenate(d_query, axis=1), rope_ref, sign=-1.0).astype(BF16)
        d_buf[:, q_width : q_width + kv_width] = rotate(
            jnp.concatenate(d_key, axis=1), rope_ref, sign=-1.0
        ).astype(BF16)
        d_buf[:, q_width + kv_width :] = jnp.concatenate(d_val, axis=1).astype(BF16)
        part_n1 = dot_nt(d_buf[:, :q_width], wq_ref[...])
        part_n1 = part_n1 + dot_nt(d_buf[:, q_width : q_width + kv_width], wk_ref[...])
        part_n1 = part_n1 + dot_nt(d_buf[:, q_width + kv_width :], wv_ref[...])
        part_buf[...] = part_n1.astype(BF16)
        start(side_3)
        q_part[...] = dot(n1t_ref[...], d_buf[...]).astype(BF16).reshape(q_part.shape)
        start(q_core)

    def send_parts():
        arrived(q_core)
        over_pair(q_part, q_pair, q_sum)
        start(q_z)
        arrived(dl_z)
        start(dl_c)
        start(share_out)

    def input_gradient():
        arrived(side_3)
        d_n1 = part_buf[mine, :].astype(F32)
        for k in sides:
            d_n1 = d_n1 + rs_3[k - 1].astype(F32)
        resid = tok_ref[mine, :].astype(F32)
        r1 = inverse_rms(resid)
        weighted = d_n1 * ga_ref[...].reshape(1, -1)
        inner = jnp.mean(weighted * resid, axis=-1, keepdims=True)
        gain_buf[0:1, :] = jnp.sum(d_n1 * resid * r1, axis=0, keepdims=True)
        d_x = dh1_buf[...] + (r1 * weighted - resid * (r1 * r1 * r1) * inner)
        in_buf[mine, :] = d_x.astype(BF16)
        start(side_gain + share_in)

    def gain_over_planes():
        arrived(side_gain)
        gain = gain_buf[...]
        for k in sides:
            gain = gain + gain_t[k - 1]
        gain_zs[...] = gain
        start(plane_gain)

    def gain_over_pair():
        arrived(plane_gain)
        gain = gain_zs[:, columns(z)]
        for k in others:
            gain = gain + gain_z[k - 1]
        gain_c[0] = gain
        start(pair_gain)

    stages = (pair_sum, moe_backward, attention_backward, send_parts, input_gradient, gain_over_planes, gain_over_pair)

    def stages_at(half):
        for stage, place in zip(stages, STAGE_PLACES):
            if place % 2 == half:
                pl.when(step == place // 2)(stage)

    stages_at(0)
    first = c * (2 * pl.num_programs(0)) + 2 * step
    wd_pair = wd_ref[...].reshape(2 * width, model)
    gate_pair = pair_of_gates(split[...], first, width)
    dh_pair = dot_nt(g_rest[...], wd_pair)
    hidden = []
    for k in range(2):
        if k == 1:
            stages_at(1)
        lanes = slice(k * width, (k + 1) * width)
        both = dot(x_rest[:, :model], jnp.concatenate([wg_ref[k], wu_ref[k]], axis=1))
        _, ghid, dgp, dup = swiglu(both, dh_pair[:, lanes], gate_pair[:, lanes])
        hidden.append(ghid)
        dgu_ref[:, 2 * k * width : (2 * k + 1) * width] = dgp
        dgu_ref[:, (2 * k + 1) * width : 2 * (k + 1) * width] = dup
    down = dot(gt_buf[:, :plane_rows], own_ref[...])
    down = (down + dot(gt_buf[:, plane_rows:], jnp.concatenate(hidden, axis=1))).T
    for k in range(2):
        down_ref[k] = down[k * width : (k + 1) * width]

    @pl.when(step == last)
    def _():
        arrived(pair_gain)
        gains_ref[...] = gain_c[0] + gain_c[1]
        arrived(o_z)
        over_z(o_sum, o_in, o_grad_ref)
        arrived(share_out + share_in)
        out_ref[...] = out_buf[...]
        in_ref[...] = in_buf[...]
        arrived(q_z)
        over_z(q_sum, q_in, qkv_grad_ref)
        arrived(dl_own + dl_c)
        keep_dl.wait()
        sent = pair_bd + pair_mo + side_bd + side_mo + share_da + share_out + share_in + side_3
        sent = sent + dl_z + dl_own + dl_c + q_core + q_z + o_core + o_z
        for copy in sent + side_gain + plane_gain + pair_gain:
            copy.wait_send()


def backward(dp, tp, arrays, streamed, own_hid, mask, weights):
    tokens = arrays[5]
    wq, wk, wv = arrays[10:13]
    all_rows, model = streamed[1].shape
    rest_rows = all_rows - all_rows // dp
    count, _, width = weights[0].shape
    length = tokens.shape[0]
    own, part = length // tp, model // dp
    q_width = wq.shape[1]
    wide = q_width + wk.shape[1] + wv.shape[1]
    others, sides = dp - 1, tp - 1
    copies = 3 + 9 * sides + (2 * others + 1) + 2 * (1 + others) + sides + others + 1
    by_pair = lambda shape: pl.BlockSpec((2,) + shape, lambda i: (i, 0, 0))
    saved = pl.BlockSpec((rest_rows, 4 * width), lambda i: (0, i))
    shapes = [
        ((length, model), BF16),
        ((length, model), BF16),
        ((all_rows, EXTRA), BF16),
        ((part // 2, wide), F32),
        ((part // 2, q_width), F32),
        ((8, part), F32),
        ((count, width, part), F32),
        ((rest_rows, 2 * count * width), BF16),
    ]
    shapes = [jax.ShapeDtypeStruct(*s) for s in shapes]
    full, block, slots = (length, model), (own, model), (sides, own, model)
    copied = [arrays[i] for i in (5, 6, *range(10, len(arrays)))]
    scratch = [
        (full, BF16),
        (full, BF16),
        ((length, EXTRA), F32),
        *((a.shape, a.dtype) for a in copied),
        ((rest_rows, streamed[0].shape[1]), BF16),
        ((rest_rows, model), BF16),
        ((EXTRA, model), BF16),
        ((all_rows - rest_rows, part), BF16),
        ((part, all_rows), BF16),
        ((rest_rows, 2 * EXTRA), BF16),
        (full, BF16),
        (full, BF16),
        ((length, EXTRA), F32),
        (full, BF16),
        (full, BF16),
        ((length, EXTRA), F32),
        (slots, BF16),
        (slots, BF16),
        ((sides, own, EXTRA), F32),
        (block, F32),
        (full, BF16),
        ((length, EXTRA), BF16),
        ((length, wide), BF16),
        ((length, q_width), BF16),
        (full, BF16),
        (slots, BF16),
        ((8, model), F32),
        ((sides, 8, model), F32),
        ((others, 8, part), F32),
        ((8, model), F32),
        ((2, 8, part), F32),
        (full, BF16),
        (full, BF16),
        ((dp, 2, part // 2, wide), BF16),
        ((dp, part // 2, wide), BF16),
        ((dp, part // 2, wide), BF16),
        ((others, part // 2, wide), BF16),
        ((dp, 2, part // 2, q_width), BF16),
        ((dp, part // 2, q_width), BF16),
        ((dp, part // 2, q_width), BF16),
        ((others, part // 2, q_width), BF16),
    ]
    return pl.pallas_call(
        functools.partial(backward_kernel, dp, tp),
        grid=(count // 2,),
        out_shape=shapes,
        in_specs=[whole_spec(a) if i in (3, 4, 7, 8, 9) else ANY for i, a in enumerate(arrays)]
        + [ANY, ANY, pl.BlockSpec((own_hid.shape[0], 2 * width), lambda i: (0, i)), whole_spec(mask)]
        + [by_pair((model, width)), by_pair((model, width)), by_pair((width, model))],
        out_specs=[whole_spec(shapes[0]), whole_spec(shapes[1]), ANY]
        + [whole_spec(s) for s in shapes[3:6]]
        + [by_pair((width, part)), saved],
        scratch_shapes=[pltpu.VMEM(*s) for s in scratch]
        + [
            pltpu.SemaphoreType.DMA((copies,)),
            pltpu.SemaphoreType.DMA((copies,)),
            pltpu.SemaphoreType.DMA((4,)),
            pltpu.SemaphoreType.DMA((3 + len(copied),)),
        ],
        compiler_params=pltpu.CompilerParams(
            collective_id=2, has_side_effects=True, vmem_limit_bytes=VMEM_LIMIT
        ),
        name="backward",
    )(*arrays, *streamed, own_hid, mask, *weights)


def weights_kernel(
    place_ref,
    x_ref,
    dl_ref,
    qkv_grad_ref,
    o_grad_ref,
    gains_ref,
    out_in_ref,
    in_in_ref,
    dgu_ref,
    down_ref,
    dgu_rest,
    gate_grad_ref,
    up_grad_ref,
    down_grad_ref,
    query_ref,
    key_ref,
    value_ref,
    out_grad_ref,
    router_ref,
    ga_grad_ref,
    gm_grad_ref,
    out_ref,
    in_ref,
    xt_buf,
):
    step = pl.program_id(0)
    c = place_ref[1]
    width = gate_grad_ref.shape[2]
    plane_rows = dgu_ref.shape[0]

    @pl.when(step == 0)
    def _():
        xt_buf[...] = x_ref[...].T
        q_width, kv_width = query_ref.shape[1], key_ref.shape[1]
        half = query_ref.shape[0]
        query_ref[...] = qkv_grad_ref[:, :q_width]
        key_ref[...] = qkv_grad_ref[:, q_width : q_width + kv_width]
        value_ref[...] = qkv_grad_ref[:, q_width + kv_width :]
        out_grad_ref[...] = o_grad_ref[...]
        out_ref[...] = out_in_ref[...]
        in_ref[...] = in_in_ref[...]
        router = dot(xt_buf[...], dl_ref[...]).T[: router_ref.shape[0]]
        router_ref[...] = jnp.where(c == 0, router[:, :half], router[:, half:])
        gains = jnp.where(c == 0, gains_ref[:, :half], gains_ref[:, half:])
        ga_grad_ref[...] = gains[0:1, :]
        gm_grad_ref[...] = gains[1:2, :]

    down_grad_ref[...] = down_ref[...]
    for k in range(2):
        lanes = slice(2 * k * width, 2 * (k + 1) * width)
        both = dot(xt_buf[:, :plane_rows], dgu_ref[:, lanes])
        both = both + dot(xt_buf[:, plane_rows:], dgu_rest[:, lanes])
        gate_grad_ref[k] = both[:, :width]
        up_grad_ref[k] = both[:, width:]


def weight_grads(place, x, sides, own, down, rest, kv_width, experts):
    rows = x.shape[0]
    _, qkv_grad, o_grad, gains, output, _ = sides
    count, width, _ = down.shape
    part = gains.shape[1]
    q_width, half = o_grad.shape[1], part // 2
    by_pair = lambda shape: pl.BlockSpec((2,) + shape, lambda i, p: (i, 0, 0))
    saved = lambda a: pl.BlockSpec((a.shape[0], 4 * width), lambda i, p: (0, i))
    columns = pl.BlockSpec((rows, part), lambda i, p: (0, p[0]), pipeline_mode=pl.Buffered(1))
    shapes = [
        (count, part, width),
        (count, part, width),
        (count, width, part),
        (half, q_width),
        (half, kv_width),
        (half, kv_width),
        (half, q_width),
        (experts, half),
        (1, half),
        (1, half),
    ]
    shapes = [jax.ShapeDtypeStruct(s, F32) for s in shapes]
    shapes += [jax.ShapeDtypeStruct(output.shape, BF16)] * 2
    return pl.pallas_call(
        weights_kernel,
        grid_spec=pltpu.PrefetchScalarGridSpec(
            num_scalar_prefetch=1,
            grid=(count // 2,),
            in_specs=[columns]
            + [whole_spec(a) for a in sides]
            + [saved(own), by_pair((width, part)), saved(rest)],
            out_specs=[by_pair((part, width)), by_pair((part, width)), by_pair((width, part))]
            + [whole_spec(s) for s in shapes[3:]],
            scratch_shapes=[pltpu.VMEM((part, rows), BF16)],
        ),
        out_shape=shapes,
        compiler_params=pltpu.CompilerParams(vmem_limit_bytes=VMEM_LIMIT),
        name="weight_grads",
    )(place, x, *sides, own, down, rest)


def rope_rows(length):
    half = HEAD_SIZE // 2
    frequency = ROPE_BASE ** (np.arange(half) * (-2.0 / HEAD_SIZE))
    angles = np.arange(length)[:, None] * frequency[None, :]
    cos, sin, none = np.cos(angles), np.sin(angles), np.zeros((length, half))
    double = lambda first, second: np.concatenate([first, second, first, second], axis=1)
    return np.stack([double(cos, cos), double(-sin, none), double(none, sin)]).astype(np.float32)


def gather_plan(
    tokens,
    gain_attn,
    w_query,
    key_projection,
    value_projection,
    w_out,
    gain_moe,
    w_router,
    w_gate,
    w_up,
    w_down,
    routes,
    cotangent,
):
    dp, tp = lax.axis_size("dp"), lax.axis_size("tensor")
    experts = w_router.shape[1]
    rope = jnp.asarray(rope_rows(tokens.shape[0]))
    ga, gm = gain_attn, gain_moe
    wr = w_router.T
    heads = (w_query, key_projection, value_projection, w_out)
    x_all, g_all, moe, back, dgate, gates, h1, *saved, ghid, dgu, mask, place = front(
        dp, tp, (tokens, cotangent, routes.T, ga, gm, wr, *heads, rope), (w_gate, w_up, w_down)
    )
    local = (back, moe, dgate, gates, h1, tokens, cotangent, ga, gm, wr, *heads)
    output, input_grad, d_logits, qkv_grad, o_grad, gains, down, dgu_rest = backward(
        dp, tp, (*local, *saved, rope), (x_all, g_all), ghid, mask, (w_gate, w_up, w_down)
    )
    (
        gate_grad,
        up_grad,
        down_grad,
        query_grad,
        key_grad,
        value_grad,
        out_grad,
        router_grad,
        gain_attn_grad,
        gain_moe_grad,
        output,
        input_grad,
    ) = weight_grads(
        place,
        x_all,
        (d_logits, qkv_grad, o_grad, gains, output, input_grad),
        dgu,
        down,
        dgu_rest,
        key_projection.shape[1],
        experts,
    )
    return (
        output,
        input_grad,
        gain_attn_grad[0],
        query_grad,
        key_grad,
        value_grad,
        out_grad.T,
        gain_moe_grad[0],
        router_grad.T,
        gate_grad,
        up_grad,
        down_grad,
    )


def solution(mesh):
    placed = (
        P(("dp", "expert"), None),
        P(),
        P(None, "tensor"),
        P(None, "tensor"),
        P(None, "tensor"),
        P("tensor", None),
        P(),
        P(),
        P("expert", None, "tensor"),
        P("expert", None, "tensor"),
        P("expert", "tensor", None),
        P(("dp", "expert"), None),
        P(("dp", "expert"), None),
    )
    sequences = mesh.shape["dp"] * mesh.shape["expert"]
    few = sequences * SEQUENCE_LENGTH <= GATHER_ROWS
    few = few and mesh.shape["tensor"] == 4 and mesh.shape["expert"] == 2
    return jax.shard_map(
        gather_plan if few else reduce_plan,
        mesh=mesh,
        in_specs=placed,
        out_specs=(
            P(("dp", "expert"), None),
            P(("dp", "expert"), None),
            P(("dp", "expert")),
            P(("dp", "expert"), "tensor"),
            P(("dp", "expert"), "tensor"),
            P(("dp", "expert"), "tensor"),
            P("tensor", ("dp", "expert")),
            P(("dp", "expert")),
            P(("dp", "expert"), None),
            P("expert", "dp", "tensor"),
            P("expert", "dp", "tensor"),
            P("expert", "tensor", "dp"),
        ),
        check_vma=False,
    )
```
